128 devices in a mesh: fsdp: 16 (over z, y), model: 8 (over x, core).
Axes of the slice: x: 4, y: 4, z: 4, core: 2. Of those that a mesh axis runs over, the one named last changes fastest.
Arguments:
- x_in: bfloat16 [16, 512, 4096], P('fsdp', 'model')
- dy_in: bfloat16 [16, 512, 4096], P('fsdp', 'model')
- norm_gain: float32 [4096], replicated
- w_qkv: bfloat16 [4096, 6144], P('fsdp', 'model')
- w_out: bfloat16 [4096, 4096], P('model', 'fsdp')
- w_gate: bfloat16 [4096, 14336], P('fsdp', 'model')
- w_up: bfloat16 [4096, 14336], P('fsdp', 'model')
- w_down: bfloat16 [14336, 4096], P('model', 'fsdp')
- rope_cos: float32 [512, 64], replicated
- rope_sin: float32 [512, 64], replicated
Outputs:
- output 1: bfloat16 [16, 512, 4096], P('fsdp', 'model')
- output 2: bfloat16 [16, 512, 4096], P('fsdp', 'model')
- output 3: float32 [4096, 6144], P('fsdp', 'model')
- output 4: float32 [4096, 4096], P('model', 'fsdp')
- output 5: float32 [4096, 14336], P('fsdp', 'model')
- output 6: float32 [4096, 14336], P('fsdp', 'model')
- output 7: float32 [14336, 4096], P('model', 'fsdp')
All inputs are finite; a program needn't handle non-finite values.
Results may differ from the reference program's by a relative error of at most 0.00910965.
Values are sent between devices in bfloat16 or wider.
A program may use at most 1 GiB of HBM per device.

```python
import math
import jax
import jax.numpy as jnp
from jax import lax

D = 4096
FF = 14336
HEADS = 32
KV_HEADS = 8
HEAD = 128
BATCH = 16
SEQ = 512
ROPE_THETA = 500000

NORM_EPS = 1e-5
GROUP_SIZE = HEADS // KV_HEADS
QKV_COLS = (HEADS + 2 * KV_HEADS) * HEAD


def rope_tables(key):
    pos_gaps = jax.random.randint(key, (SEQ,), 1, 4)
    positions = (jnp.cumsum(pos_gaps) - pos_gaps[0]).astype(jnp.float32)
    inv_freq = jnp.exp(jnp.arange(HEAD // 2, dtype=jnp.float32) * (-2.0 * math.log(ROPE_THETA) / HEAD))
    angles = positions[:, None] * inv_freq[None, :]
    return jnp.cos(angles), jnp.sin(angles)


def setup_inputs(seed: int = 0) -> dict:
    key_list = jax.random.split(jax.random.key(seed), 9)
    x_in = jax.random.normal(key_list[0], (BATCH, SEQ, D), jnp.float32)
    dy_in = jax.random.normal(key_list[1], (BATCH, SEQ, D), jnp.float32)
    norm_gain = jax.random.uniform(key_list[2], (D,), jnp.float32, 0.5, 1.5)
    w_qkv = jax.random.normal(key_list[3], (D, QKV_COLS), jnp.float32) * D ** -0.5
    w_out = jax.random.normal(key_list[4], (HEADS * HEAD, D), jnp.float32) * (HEADS * HEAD) ** -0.5
    w_gate = jax.random.normal(key_list[5], (D, FF), jnp.float32) * D ** -0.5
    w_up = jax.random.normal(key_list[6], (D, FF), jnp.float32) * D ** -0.5
    w_down = jax.random.normal(key_list[7], (FF, D), jnp.float32) * FF ** -0.5
    rope_cos, rope_sin = rope_tables(key_list[8])
    return {
        "x_in": x_in.astype(jnp.bfloat16),
        "dy_in": dy_in.astype(jnp.bfloat16),
        "norm_gain": norm_gain,
        "w_qkv": w_qkv.astype(jnp.bfloat16),
        "w_out": w_out.astype(jnp.bfloat16),
        "w_gate": w_gate.astype(jnp.bfloat16),
        "w_up": w_up.astype(jnp.bfloat16),
        "w_down": w_down.astype(jnp.bfloat16),
        "rope_cos": rope_cos,
        "rope_sin": rope_sin,
    }


def rotate(tensor, cos_tab, sin_tab):
    half_dim = HEAD // 2
    wide = tensor.astype(jnp.float32)
    lower_half = wide[..., :half_dim]
    upper_half = wide[..., half_dim:]
    return jnp.concatenate([lower_half * cos_tab - upper_half * sin_tab, upper_half * cos_tab + lower_half * sin_tab], axis=-1).astype(jnp.bfloat16)


def swiglu(gate_val, up_val):
    return (jax.nn.silu(gate_val.astype(jnp.float32)) * up_val.astype(jnp.float32)).astype(jnp.bfloat16)


def attention(qkv_seq, rope_cos, rope_sin):
    queries = rotate(qkv_seq[:, :, :GROUP_SIZE, :], rope_cos[:, None, None, :], rope_sin[:, None, None, :])
    key_rot = rotate(qkv_seq[:, :, GROUP_SIZE, :], rope_cos[:, None, :], rope_sin[:, None, :])
    values = qkv_seq[:, :, GROUP_SIZE + 1, :]
    scores = jnp.einsum("qkgh,pkh->kgqp", queries.astype(jnp.float32), key_rot.astype(jnp.float32)) * HEAD ** -0.5
    causal = jnp.arange(SEQ)[:, None] >= jnp.arange(SEQ)[None, :]
    attn_probs = jax.nn.softmax(jnp.where(causal, scores, -1e30), axis=-1).astype(jnp.bfloat16)
    attn_out = jnp.einsum("kgqp,pkh->qkgh", attn_probs.astype(jnp.float32), values.astype(jnp.float32))
    return attn_out.astype(jnp.bfloat16).reshape(SEQ, HEADS * HEAD)


def reference(x_in, dy_in, norm_gain, w_qkv, w_out, w_gate, w_up, w_down, rope_cos, rope_sin):
    tokens = BATCH * SEQ
    x_rows = x_in.reshape(tokens, D).astype(jnp.float32)
    dy_rows = dy_in.reshape(tokens, D)
    normed, norm_pull = jax.vjp(lambda row_vals: row_vals * lax.rsqrt(jnp.mean(row_vals * row_vals, axis=-1, keepdims=True) + NORM_EPS) * norm_gain, x_rows)
    h_val = normed.astype(jnp.bfloat16)
    qkv_seqs = jnp.dot(h_val, w_qkv, preferred_element_type=jnp.float32).astype(jnp.bfloat16).reshape(BATCH, SEQ, KV_HEADS, GROUP_SIZE + 2, HEAD)
    attn_fn = lambda packed: attention(packed, rope_cos, rope_sin)
    attn_val = lax.map(attn_fn, qkv_seqs).reshape(tokens, HEADS * HEAD)
    gate_val = jnp.dot(h_val, w_gate, preferred_element_type=jnp.float32).astype(jnp.bfloat16)
    up_val = jnp.dot(h_val, w_up, preferred_element_type=jnp.float32).astype(jnp.bfloat16)
    act_val, act_pull = jax.vjp(swiglu, gate_val, up_val)
    mix_sum = jnp.dot(attn_val, w_out, preferred_element_type=jnp.float32) + jnp.dot(act_val, w_down, preferred_element_type=jnp.float32)
    y_out = (x_rows + mix_sum).astype(jnp.bfloat16)
    d_attn = jnp.dot(dy_rows, w_out.T, preferred_element_type=jnp.float32).astype(jnp.bfloat16)
    d_act = jnp.dot(dy_rows, w_down.T, preferred_element_type=jnp.float32).astype(jnp.bfloat16)
    d_gate, d_up = act_pull(d_act)

    def seq_grad(seq_pair):
        seq_pull = jax.vjp(attn_fn, seq_pair[0])[1]
        return seq_pull(seq_pair[1])[0]

    d_qkv = lax.map(seq_grad, (qkv_seqs, d_attn.reshape(BATCH, SEQ, HEADS * HEAD))).reshape(tokens, QKV_COLS)
    d_h = (jnp.dot(d_qkv, w_qkv.T, preferred_element_type=jnp.float32) + jnp.dot(d_gate, w_gate.T, preferred_element_type=jnp.float32) + jnp.dot(d_up, w_up.T, preferred_element_type=jnp.float32)).astype(jnp.bfloat16)
    dx_rows = (dy_rows.astype(jnp.float32) + norm_pull(d_h.astype(jnp.float32))[0]).astype(jnp.bfloat16)
    return (
        y_out.reshape(BATCH, SEQ, D),
        dx_rows.reshape(BATCH, SEQ, D),
        jnp.dot(h_val.T, d_qkv, preferred_element_type=jnp.float32),
        jnp.dot(attn_val.T, dy_rows, preferred_element_type=jnp.float32),
        jnp.dot(h_val.T, d_gate, preferred_element_type=jnp.float32),
        jnp.dot(h_val.T, d_up, preferred_element_type=jnp.float32),
        jnp.dot(act_val.T, dy_rows, preferred_element_type=jnp.float32),
    )
```

```python
import jax
import jax.numpy as jnp
from jax import lax
from jax.sharding import Mesh, PartitionSpec as P

NORM_EPS = 1e-5
NZ = 4
NY = 4
NX = 4
NC = 2
HEAD_GROUP = 4
F32 = jnp.float32
BF16 = jnp.bfloat16


def norm_fwd(row_vals, norm_gain):
    return row_vals * lax.rsqrt(jnp.mean(row_vals * row_vals, axis=-1, keepdims=True) + NORM_EPS) * norm_gain


def swiglu(gate_val, up_val):
    return (jax.nn.silu(gate_val.astype(F32)) * up_val.astype(F32)).astype(BF16)


def rotate(tensor, cos_tab, sin_tab):
    half_dim = tensor.shape[-1] // 2
    wide = tensor.astype(F32)
    lower_half = wide[..., :half_dim]
    upper_half = wide[..., half_dim:]
    return jnp.concatenate([lower_half * cos_tab - upper_half * sin_tab, upper_half * cos_tab + lower_half * sin_tab], axis=-1).astype(BF16)


def rotate_back(tensor, cos_tab, sin_tab):
    half_dim = tensor.shape[-1] // 2
    wide = tensor.astype(F32)
    lower_half = wide[..., :half_dim]
    upper_half = wide[..., half_dim:]
    return jnp.concatenate([lower_half * cos_tab + upper_half * sin_tab, upper_half * cos_tab - lower_half * sin_tab], axis=-1).astype(BF16)


def ring(step, size):
    return [(src, (src + step) % size) for src in range(size)]


def hop_z(val, step):
    return lax.ppermute(val, "z", ring(step, NZ))


def swap_c(val):
    return lax.ppermute(val, "c", [(0, 1), (1, 0)])


def swap_y(val):
    return lax.ppermute(val, "y", [(src, src ^ 1) for src in range(NY)])


def yc_index(y_pos, c_pos):
    return y_pos * NC + c_pos


def yc_pairs(row_bit, col_bit):
    return [(yc_index(y_src, c_src), yc_index(2 * c_src + col_bit, y_src // 2)) for y_src in range(NY) if y_src % 2 == row_bit for c_src in range(NC)]


def dot_nn(left, right):
    return lax.dot_general(left, right, (((1,), (0,)), ((), ())), preferred_element_type=F32)


def dot_nt(left, right):
    return lax.dot_general(left, right, (((1,), (1,)), ((), ())), preferred_element_type=F32)


def dot_tn(left, right):
    return lax.dot_general(left, right, (((0,), (0,)), ((), ())), preferred_element_type=F32)


def solution(mesh):
    wide_mesh = Mesh(mesh.devices.reshape(NZ, NY, NX, NC), ("z", "y", "x", "c"))
    rows = ("z", "y")
    cols = ("x", "c")
    act_spec = P(rows, cols, None)
    col_spec = P(rows, cols)
    row_spec = P(cols, rows)

    def layer_body(x_in, dy_in, norm_gain, w_qkv, w_out, w_gate, w_up, w_down, rope_cos, rope_sin):
        z_pos = lax.axis_index("z")
        y_pos = lax.axis_index("y")
        c_pos = lax.axis_index("c")
        even_y = y_pos % 2 == 0
        first_c = c_pos == 0
        depth = x_in.shape[-1]
        chunk = x_in.shape[1]
        d_rows = w_gate.shape[0]
        head = 2 * rope_cos.shape[1]
        seq = rope_cos.shape[0]
        tokens = NY * NX * chunk
        ff_blk = w_gate.shape[1] // 2
        o_blk = w_out.shape[0] // 2
        heads_dev = o_blk // head

        def gather_weight(blocks):
            width = blocks[0].shape[1]
            got = []
            for row_bit in range(2):
                halves = [lax.ppermute(blocks[col_bit], ("y", "c"), yc_pairs(row_bit, col_bit)) for col_bit in range(2)]
                got.append(jnp.where(even_y, halves[0], halves[1]))
            piece = jnp.concatenate(got, axis=0)
            left = hop_z(piece, 1)
            right = hop_z(piece, -1)
            far = jnp.concatenate([hop_z(left[:d_rows], 1), hop_z(right[d_rows:], -1)], axis=0)
            full = jnp.zeros((NZ, NC, 2 * d_rows, width), BF16)
            for step, part in ((0, piece), (3, left), (1, right), (2, far)):
                z_src = (z_pos + step) % NZ
                full = lax.dynamic_update_slice(full, part[None, None], (z_src, c_pos, 0, 0))
                full = lax.dynamic_update_slice(full, swap_c(part)[None, None], (z_src, 1 - c_pos, 0, 0))
            return full.reshape(NZ * NC * 2 * d_rows, width)

        def scatter_grad(grad):
            def part(step, half):
                return lax.dynamic_slice(grad, ((z_pos + step) % NZ, half * d_rows, 0), (1, d_rows, grad.shape[2]))[0]

            from_left = hop_z(part(2, 0), 1)
            from_right = hop_z(part(2, 1), -1)
            left = [hop_z(part(1, 0) + from_left, 1), hop_z(part(1, 1), 1)]
            right = [hop_z(part(3, 0), -1), hop_z(part(3, 1) + from_right, -1)]
            total = [part(0, half) + left[half] + right[half] for half in range(2)]
            blocks = []
            for col_bit in range(2):
                back = [lax.ppermute(total[row_bit], ("y", "c"), [(dst, src) for src, dst in yc_pairs(row_bit, col_bit)]) for row_bit in range(2)]
                blocks.append(jnp.where(even_y, back[0], back[1]))
            return blocks

        def to_sequences(val):
            val = val.reshape(2, 2, NX, chunk, -1)
            mine = lax.dynamic_index_in_dim(val, c_pos, 0, keepdims=False)
            other = swap_c(lax.dynamic_index_in_dim(val, 1 - c_pos, 0, keepdims=False))
            both = jnp.stack([jnp.where(first_c, mine, other), jnp.where(first_c, other, mine)], axis=2)
            return both.reshape(2, seq, -1)

        def to_tokens(val):
            val = val.reshape(2, NX, 2, chunk, -1)
            mine = lax.dynamic_index_in_dim(val, c_pos, 2, keepdims=False)
            other = swap_c(lax.dynamic_index_in_dim(val, 1 - c_pos, 2, keepdims=False))
            both = jnp.stack([jnp.where(first_c, mine, other), jnp.where(first_c, other, mine)], axis=0)
            return both.reshape(tokens, -1)

        def col_halves(val):
            val = val.reshape(tokens, NZ, 2, 2 * d_rows)
            mine = lax.dynamic_index_in_dim(val, c_pos, 2, keepdims=False).reshape(tokens, NZ * 2 * d_rows)
            other = lax.dynamic_index_in_dim(val, 1 - c_pos, 2, keepdims=False).reshape(tokens, NZ * 2 * d_rows)
            return jnp.concatenate([mine, swap_c(other)], axis=0)

        x_rows = x_in[0].astype(F32)
        normed, norm_pull = jax.vjp(lambda row_vals: norm_fwd(row_vals, norm_gain), x_rows)
        h_all = lax.all_gather(normed.astype(BF16), ("y", "x"), axis=0, tiled=True)
        dy_all = lax.all_gather(dy_in[0], ("y", "x"), axis=0, tiled=True)

        def qkv_cols(bit):
            first = 2 * head * bit
            third = HEAD_GROUP * head + head * bit
            return jnp.concatenate([w_qkv[:, first : first + 2 * head], w_qkv[:, third : third + head]], axis=1)

        down_t = w_down.T
        out_t = w_out.T
        w_first = gather_weight([jnp.concatenate([w_gate[:, j * ff_blk : (j + 1) * ff_blk], w_up[:, j * ff_blk : (j + 1) * ff_blk], qkv_cols(j)], axis=1) for j in range(2)])
        w_second = gather_weight([jnp.concatenate([down_t[:, j * ff_blk : (j + 1) * ff_blk], out_t[:, j * o_blk : (j + 1) * o_blk]], axis=1) for j in range(2)])

        proj = dot_nn(h_all, w_first).astype(BF16)
        gate_val = proj[:, :ff_blk]
        up_val = proj[:, ff_blk : 2 * ff_blk]
        act_val, act_pull = jax.vjp(swiglu, gate_val, up_val)
        qkv_seq = to_sequences(proj[:, 2 * ff_blk :])
        queries = qkv_seq[:, :, : 2 * head].reshape(2, seq, heads_dev, head)
        third_mine = qkv_seq[:, :, 2 * head :]
        third_other = swap_y(third_mine)
        keys = jnp.where(even_y, third_mine, third_other)
        values = jnp.where(even_y, third_other, third_mine)
        q_rot = rotate(queries, rope_cos[None, :, None, :], rope_sin[None, :, None, :])
        k_rot = rotate(keys, rope_cos[None], rope_sin[None])
        scores = jnp.einsum("bqgh,bph->bgqp", q_rot, k_rot, preferred_element_type=F32) * head**-0.5
        causal = jnp.arange(seq)[:, None] >= jnp.arange(seq)[None, :]
        probs = jax.nn.softmax(jnp.where(causal, scores, -1e30), axis=-1)
        probs_b = probs.astype(BF16)
        attn_seq = jnp.einsum("bgqp,bph->bqgh", probs_b, values, preferred_element_type=F32).astype(BF16)
        attn_tok = to_tokens(attn_seq.reshape(2, seq, o_blk))
        mixed = jnp.concatenate([act_val, attn_tok], axis=1)
        y_part = dot_nt(mixed, w_second)
        mix_sum = lax.psum_scatter(y_part, ("y", "x"), scatter_dimension=0, tiled=True)
        y_out = (x_rows + mix_sum).astype(BF16)[None]

        d_mixed = dot_nn(dy_all, w_second).astype(BF16)
        d_gate, d_up = act_pull(d_mixed[:, :ff_blk])
        d_attn = to_sequences(d_mixed[:, ff_blk:]).reshape(2, seq, heads_dev, head)
        d_values = jnp.einsum("bgqp,bqgh->bph", probs_b, d_attn, preferred_element_type=F32)
        d_probs = jnp.einsum("bqgh,bph->bgqp", d_attn, values, preferred_element_type=F32).astype(BF16).astype(F32)
        d_scores = probs * (d_probs - jnp.sum(d_probs * probs, axis=-1, keepdims=True))
        d_scores = (jnp.where(causal, d_scores, 0.0) * head**-0.5).astype(BF16)
        d_q_rot = jnp.einsum("bgqp,bph->bqgh", d_scores, k_rot, preferred_element_type=F32).astype(BF16)
        d_k_rot = jnp.einsum("bgqp,bqgh->bph", d_scores, q_rot, preferred_element_type=F32)
        d_third = jnp.where(even_y, d_k_rot, d_values) + swap_y(jnp.where(even_y, d_values, d_k_rot))
        d_third = d_third.astype(BF16)
        d_third = jnp.where(even_y, rotate_back(d_third, rope_cos[None], rope_sin[None]), d_third)
        d_queries = rotate_back(d_q_rot, rope_cos[None, :, None, :], rope_sin[None, :, None, :])
        d_qkv = to_tokens(jnp.concatenate([d_queries.reshape(2, seq, 2 * head), d_third], axis=2))
        d_proj = jnp.concatenate([d_gate, d_up, d_qkv], axis=1)
        dh_part = dot_nt(d_proj, w_first)
        d_h = lax.psum_scatter(dh_part, ("y", "x"), scatter_dimension=0, tiled=True).astype(BF16)
        dx_out = (dy_in[0].astype(F32) + norm_pull(d_h.astype(F32))[0]).astype(BF16)[None]

        h_half = col_halves(h_all)
        dy_half = col_halves(dy_all)
        mixed_both = jnp.concatenate([mixed, swap_c(mixed)], axis=0)
        d_proj_both = jnp.concatenate([d_proj, swap_c(d_proj)], axis=0)

        def grad_blocks(acts, cots):
            return scatter_grad(dot_tn(acts, cots).reshape(NZ, 2 * d_rows, -1))

        g_second = grad_blocks(dy_half, mixed_both)
        g_gate = grad_blocks(h_half, d_proj_both[:, :ff_blk])
        g_up = grad_blocks(h_half, d_proj_both[:, ff_blk : 2 * ff_blk])
        g_qkv = grad_blocks(h_half, d_proj_both[:, 2 * ff_blk :])
        dw_down = jnp.concatenate([blk[:, :ff_blk] for blk in g_second], axis=1).T
        dw_out = jnp.concatenate([blk[:, ff_blk:] for blk in g_second], axis=1).T
        dw_gate = jnp.concatenate(g_gate, axis=1)
        dw_up = jnp.concatenate(g_up, axis=1)
        dw_qkv = jnp.concatenate([blk[:, : 2 * head] for blk in g_qkv] + [blk[:, 2 * head :] for blk in g_qkv], axis=1)
        return y_out, dx_out, dw_qkv, dw_out, dw_gate, dw_up, dw_down

    return jax.shard_map(
        layer_body,
        mesh=wide_mesh,
        in_specs=(act_spec, act_spec, P(), col_spec, row_spec, col_spec, col_spec, row_spec, P(), P()),
        out_specs=(act_spec, act_spec, col_spec, row_spec, col_spec, col_spec, row_spec),
        check_vma=False,
    )
```

```python
import functools

import jax
import jax.numpy as jnp
from jax import lax
from jax.experimental import pallas as pl
from jax.experimental.pallas import tpu as pltpu
from jax.sharding import Mesh, PartitionSpec as P


NORM_EPS = 1e-5
NZ = 4
NY = 4
NX = 4
NC = 2
HEAD_GROUP = 4
F32 = jnp.float32
BF16 = jnp.bfloat16
VMEM_LIMIT = 60 * 1024 * 1024


def norm_fwd(row_vals, norm_gain):
    return row_vals * lax.rsqrt(jnp.mean(row_vals * row_vals, axis=-1, keepdims=True) + NORM_EPS) * norm_gain


def rotate(wide, cos_tab, sin_tab):
    return wide * cos_tab + pltpu.roll(wide, wide.shape[-1] // 2, wide.ndim - 1) * sin_tab


def rotate_back(wide, cos_tab, sin_tab):
    return wide * cos_tab - pltpu.roll(wide, wide.shape[-1] // 2, wide.ndim - 1) * sin_tab


def cost(flops, bytes_accessed):
    return pl.CostEstimate(flops=int(flops) // 20, bytes_accessed=int(bytes_accessed), transcendentals=0)


def params(**extra):
    return pltpu.CompilerParams(vmem_limit_bytes=VMEM_LIMIT, **extra)


def head_probs(q_rot, k_rot, scale):
    scores = dot_nt(q_rot, k_rot) * scale
    row_ids = lax.broadcasted_iota(jnp.int32, scores.shape, 0)
    col_ids = lax.broadcasted_iota(jnp.int32, scores.shape, 1)
    scores = jnp.where(row_ids >= col_ids, scores, -1e30)
    weights = jnp.exp(scores - jnp.max(scores, axis=-1, keepdims=True))
    return weights / jnp.sum(weights, axis=-1, keepdims=True)


def attn_fwd_kernel(heads, head, q_ref, k_ref, v_ref, cos_ref, sin_ref, o_ref):
    cos_tab, sin_tab = cos_ref[...], sin_ref[...]
    k_rot = rotate(k_ref[0].astype(F32), cos_tab, sin_tab).astype(BF16)
    values = v_ref[0]
    for idx in range(heads):
        lanes = slice(idx * head, (idx + 1) * head)
        q_rot = rotate(q_ref[0, :, lanes].astype(F32), cos_tab, sin_tab).astype(BF16)
        probs = head_probs(q_rot, k_rot, head**-0.5)
        o_ref[0, :, lanes] = dot_nn(probs.astype(BF16), values).astype(BF16)


def attn_bwd_kernel(heads, head, even_ref, q_ref, k_ref, v_ref, do_ref, cos_ref, sin_ref, dq_ref, keep_ref, send_ref):
    cos_tab, sin_tab = cos_ref[...], sin_ref[...]
    k_rot = rotate(k_ref[0].astype(F32), cos_tab, sin_tab).astype(BF16)
    values = v_ref[0]
    d_keys = jnp.zeros(k_rot.shape, F32)
    d_values = jnp.zeros(k_rot.shape, F32)
    for idx in range(heads):
        lanes = slice(idx * head, (idx + 1) * head)
        q_rot = rotate(q_ref[0, :, lanes].astype(F32), cos_tab, sin_tab).astype(BF16)
        d_out = do_ref[0, :, lanes]
        probs = head_probs(q_rot, k_rot, head**-0.5)
        d_values += dot_tn(probs.astype(BF16), d_out)
        d_probs = dot_nt(d_out, values).astype(BF16).astype(F32)
        d_scores = probs * (d_probs - jnp.sum(d_probs * probs, axis=-1, keepdims=True))
        d_scores = (d_scores * head**-0.5).astype(BF16)
        d_q_rot = dot_nn(d_scores, k_rot).astype(BF16)
        dq_ref[0, :, lanes] = rotate_back(d_q_rot.astype(F32), cos_tab, sin_tab).astype(BF16)
        d_keys += dot_tn(d_scores, q_rot)

    @pl.when(even_ref[0] == 1)
    def _():
        keep_ref[0] = d_keys
        send_ref[0] = d_values

    @pl.when(even_ref[0] == 0)
    def _():
        keep_ref[0] = d_values
        send_ref[0] = d_keys


def attn_fwd(queries, keys, values, cos_tab, sin_tab):
    count, seq, width = queries.shape
    head = keys.shape[2]
    wide = pl.BlockSpec((1, seq, width), lambda i: (i, 0, 0))
    slim = pl.BlockSpec((1, seq, head), lambda i: (i, 0, 0))
    table = pl.BlockSpec((seq, head), lambda i: (0, 0))
    return pl.pallas_call(
        functools.partial(attn_fwd_kernel, width // head, head),
        grid=(count,),
        in_specs=[wide, slim, slim, table, table],
        out_specs=wide,
        out_shape=jax.ShapeDtypeStruct(queries.shape, BF16),
        compiler_params=params(),
        cost_estimate=cost(16e9, 4e6),
        name="attn_fwd",
    )(queries, keys, values, cos_tab, sin_tab)


def attn_bwd(even_y, queries, keys, values, d_out, cos_tab, sin_tab):
    count, seq, width = queries.shape
    head = keys.shape[2]
    wide = pl.BlockSpec((1, seq, width), lambda i, e: (i, 0, 0))
    slim = pl.BlockSpec((1, seq, head), lambda i, e: (i, 0, 0))
    table = pl.BlockSpec((seq, head), lambda i, e: (0, 0))
    part = jax.ShapeDtypeStruct(keys.shape, F32)
    return pl.pallas_call(
        functools.partial(attn_bwd_kernel, width // head, head),
        grid_spec=pltpu.PrefetchScalarGridSpec(
            num_scalar_prefetch=1,
            grid=(count,),
            in_specs=[wide, slim, slim, wide, table, table],
            out_specs=[wide, slim, slim],
        ),
        out_shape=[jax.ShapeDtypeStruct(queries.shape, BF16), part, part],
        compiler_params=params(),
        cost_estimate=cost(16e9, 4e6),
        name="attn_bwd",
    )(even_y, queries, keys, values, d_out, cos_tab, sin_tab)


def act_fwd_kernel(half, ab_ref, u_ref, ut_ref):
    gate_val = ab_ref[:, :half].astype(F32)
    up_val = ab_ref[:, half:].astype(F32)
    act_val = gate_val * jax.nn.sigmoid(gate_val) * up_val
    u_ref[...] = act_val.astype(BF16)
    ut_ref[...] = act_val.T.astype(BF16)


def act_fwd(gate_up):
    tokens, width = gate_up.shape
    half = width // 2
    rows = tokens // 4
    return pl.pallas_call(
        functools.partial(act_fwd_kernel, half),
        grid=(4,),
        in_specs=[pl.BlockSpec((rows, width), lambda i: (i, 0))],
        out_specs=[pl.BlockSpec((rows, half), lambda i: (i, 0)), pl.BlockSpec((half, rows), lambda i: (0, i))],
        out_shape=[jax.ShapeDtypeStruct((tokens, half), BF16), jax.ShapeDtypeStruct((half, tokens), BF16)],
        compiler_params=params(),
        cost_estimate=cost(4e9, 8e6),
        name="act_fwd",
    )(gate_up)


def act_bwd_kernel(half, ab_ref, du_ref, dab_ref, dabt_ref):
    gate_val = ab_ref[:, :half].astype(F32)
    up_val = ab_ref[:, half:].astype(F32)
    d_act = du_ref[...].astype(F32)
    sig = jax.nn.sigmoid(gate_val)
    d_silu = d_act * up_val
    d_gate = d_silu * sig + d_silu * gate_val * (sig * (1.0 - sig))
    d_up = d_act * (gate_val * sig)
    dab_ref[:, :half] = d_gate.astype(BF16)
    dab_ref[:, half:] = d_up.astype(BF16)
    dabt_ref[:half, :] = d_gate.T.astype(BF16)
    dabt_ref[half:, :] = d_up.T.astype(BF16)


def act_bwd(gate_up, d_mixed):
    tokens, width = gate_up.shape
    half = width // 2
    rows = tokens // 4
    return pl.pallas_call(
        functools.partial(act_bwd_kernel, half),
        grid=(4,),
        in_specs=[pl.BlockSpec((rows, width), lambda i: (i, 0)), pl.BlockSpec((rows, half), lambda i: (i, 0))],
        out_specs=[pl.BlockSpec((rows, width), lambda i: (i, 0)), pl.BlockSpec((width, rows), lambda i: (0, i))],
        out_shape=[jax.ShapeDtypeStruct((tokens, width), BF16), jax.ShapeDtypeStruct((width, tokens), BF16)],
        compiler_params=params(),
        cost_estimate=cost(8e9, 14e6),
        name="act_bwd",
    )(gate_up, d_mixed)


def sum_nt_kernel(count, *refs):
    total = dot_nt(refs[0][...], refs[count][...])
    for idx in range(1, count):
        total += dot_nt(refs[idx][...], refs[count + idx][...])
    refs[2 * count][...] = total


def sum_nt(lefts, rights):
    tokens = lefts[0].shape[0]
    depth = rights[0].shape[0]
    cols = depth // 8
    inner = sum(left.shape[1] for left in lefts)
    return pl.pallas_call(
        functools.partial(sum_nt_kernel, len(lefts)),
        grid=(8,),
        in_specs=[pl.BlockSpec(left.shape, lambda i: (0, 0)) for left in lefts] + [pl.BlockSpec((cols, right.shape[1]), lambda i: (i, 0)) for right in rights],
        out_specs=pl.BlockSpec((tokens, cols), lambda i: (0, i)),
        out_shape=jax.ShapeDtypeStruct((tokens, depth), F32),
        compiler_params=params(),
        cost_estimate=cost(2 * tokens * depth * inner, 2 * depth * inner + 4 * tokens * depth),
    )(*lefts, *rights)


def pick_cols(pos, acts):
    tokens, depth = acts.shape
    block = depth // (2 * NZ)
    spec = pl.BlockSpec((tokens, block), lambda i, pos: (0, 2 * i + 1 - pos[1]))

    def kernel(pos_ref, in_ref, out_ref):
        out_ref[...] = in_ref[...]

    return pl.pallas_call(
        kernel,
        grid_spec=pltpu.PrefetchScalarGridSpec(
            num_scalar_prefetch=1, grid=(NZ,), in_specs=[spec], out_specs=pl.BlockSpec((tokens, block), lambda i, pos: (0, i))
        ),
        out_shape=jax.ShapeDtypeStruct((tokens, depth // 2), BF16),
        compiler_params=params(),
        cost_estimate=cost(3e9, 2 * tokens * depth),
        name="pick_cols",
    )(pos, acts)


def grad_kernel(row_starts, add_ids, *refs):
    pairs = len(row_starts) - 1
    ins = refs[1 : 1 + 4 * pairs]
    adds = refs[1 + 4 * pairs : 1 + 4 * pairs + len(add_ids)]
    outs = refs[1 + 4 * pairs + len(add_ids) :]
    step = pl.program_id(1)
    for idx in range(pairs):
        own, recv, acts, acts_recv = ins[4 * idx : 4 * idx + 4]
        rows = slice(row_starts[idx], row_starts[idx + 1])
        total = dot_nn(own[...], acts[...]) + dot_nn(recv[...], acts_recv[...])
        for out_id, out_ref in enumerate(outs):

            @pl.when(step == out_id)
            def _(out_id=out_id, out_ref=out_ref):
                value = total
                for add_id, add_ref in zip(add_ids, adds):
                    if add_id == out_id:
                        value = value + add_ref[rows, :]
                out_ref[rows, :] = value


def grad_pieces(kind, pos, pairs, adds, blocks):
    base, steps = {"far": (2, 2), "near": (1, 4), "own": (0, 2)}[kind]
    tokens, depth = pairs[0][2].shape
    cols = depth // (NZ * NY)
    heights = [pair[0].shape[0] // blocks for pair in pairs]
    starts = [sum(heights[:idx]) for idx in range(len(pairs) + 1)]

    def z_of(n, pos):
        return lax.rem(pos[0] + base + 2 * (n // 2), NZ)

    in_specs = []
    args = []
    for (own, recv, acts, acts_recv), height in zip(pairs, heights):
        in_specs += [
            pl.BlockSpec((height, tokens), lambda m, n, pos: (m, 0)),
            pl.BlockSpec((height, tokens), lambda m, n, pos: (m, 0)),
            pl.BlockSpec((tokens, cols), lambda m, n, pos: (0, z_of(n, pos) * NY + 2 * pos[1] + n % 2)),
            pl.BlockSpec((tokens, cols), lambda m, n, pos: (0, z_of(n, pos) * 2 + n % 2)),
        ]
        args += [own, recv, acts, acts_recv]
    piece = pl.BlockSpec((starts[-1], cols), lambda m, n, pos: (m, 0))
    total_rows = starts[-1] * blocks
    return pl.pallas_call(
        functools.partial(grad_kernel, starts, [add[0] for add in adds]),
        grid_spec=pltpu.PrefetchScalarGridSpec(
            num_scalar_prefetch=1,
            grid=(blocks, steps),
            in_specs=in_specs + [piece] * len(adds),
            out_specs=[piece] * steps,
        ),
        out_shape=[jax.ShapeDtypeStruct((total_rows, cols), F32)] * steps,
        compiler_params=params(),
        cost_estimate=cost(4 * total_rows * tokens * cols * steps, 4 * tokens * cols * steps),
    )(pos, *args, *[add[1] for add in adds])


def after(val, *earlier):
    return lax.optimization_barrier((val, *earlier))[0]


def ring(step, size):
    return [(src, (src + step) % size) for src in range(size)]


def hop_z(val, step):
    return lax.ppermute(val, "z", ring(step, NZ))


def swap_c(val):
    return lax.ppermute(val, "c", [(0, 1), (1, 0)])


def swap_y(val):
    return lax.ppermute(val, "y", [(src, src ^ 1) for src in range(NY)])


def yc_index(y_pos, c_pos):
    return y_pos * NC + c_pos


def yc_pairs(row_bit, col_bit):
    return [(yc_index(y_src, c_src), yc_index(2 * c_src + col_bit, y_src // 2)) for y_src in range(NY) if y_src % 2 == row_bit for c_src in range(NC)]


def dot_nn(left, right):
    return lax.dot_general(left, right, (((1,), (0,)), ((), ())), preferred_element_type=F32)


def dot_nt(left, right):
    return lax.dot_general(left, right, (((1,), (1,)), ((), ())), preferred_element_type=F32)


def dot_tn(left, right):
    return lax.dot_general(left, right, (((0,), (0,)), ((), ())), preferred_element_type=F32)


def solution(mesh):
    wide_mesh = Mesh(mesh.devices.reshape(NZ, NY, NX, NC), ("z", "y", "x", "c"))
    rows = ("z", "y")
    cols = ("x", "c")
    act_spec = P(rows, cols, None)
    col_spec = P(rows, cols)
    row_spec = P(cols, rows)

    def layer(x_in, dy_in, norm_gain, w_qkv, w_out, w_gate, w_up, w_down, rope_cos, rope_sin):
        z_pos = lax.axis_index("z")
        y_pos = lax.axis_index("y")
        c_pos = lax.axis_index("c")
        even_y = y_pos % 2 == 0
        first_c = c_pos == 0
        chunk = x_in.shape[1]
        d_rows = w_gate.shape[0]
        head = 2 * rope_cos.shape[1]
        seq = rope_cos.shape[0]
        tokens = NY * NX * chunk
        ff_blk = w_gate.shape[1] // 2
        o_blk = w_out.shape[0] // 2
        pos = jnp.stack([z_pos, c_pos]).astype(jnp.int32)

        def gather_rows(blocks):
            got = []
            for row_bit in range(2):
                halves = [lax.ppermute(blocks[col_bit], ("y", "c"), yc_pairs(row_bit, col_bit)) for col_bit in range(2)]
                got.append(jnp.where(even_y, halves[0], halves[1]))
            return jnp.concatenate(got, axis=0)

        def gather_weight(piece):
            left = hop_z(piece, 1)
            right = hop_z(piece, -1)
            far = jnp.concatenate([hop_z(left[:d_rows], 1), hop_z(right[d_rows:], -1)], axis=0)
            return [(step, part, swap_c(part)) for step, part in ((0, piece), (3, left), (1, right), (2, far))]

        def whole_weight(parts, *earlier):
            full = jnp.zeros((NZ, NC, *parts[0][1].shape), BF16)
            for step, part, swapped in parts:
                part, swapped = part[None, None], swapped[None, None]
                if step == 2 and earlier:
                    full = after(full, *earlier)
                z_src = (z_pos + step) % NZ
                full = lax.dynamic_update_slice(full, part, (z_src, c_pos, 0, 0))
                full = lax.dynamic_update_slice(full, swapped, (z_src, 1 - c_pos, 0, 0))
            return full.reshape(-1, full.shape[3])

        def grad_far(pairs, blocks, *earlier):
            far = grad_pieces("far", after(pos, *earlier), pairs, [], blocks)
            return far, (hop_z(far[0], 1), hop_z(far[1], -1))

        def grad_near(pairs, blocks, got, *earlier):
            near = grad_pieces("near", after(pos, *earlier), pairs, [(0, got[0]), (3, got[1])], blocks)
            return near, ([hop_z(near[0], 1), hop_z(near[1], 1)], [hop_z(near[2], -1), hop_z(near[3], -1)])

        def grad_own(pairs, blocks, got, *earlier):
            total = grad_pieces("own", after(pos, *earlier), pairs, [(half, side[half]) for half in range(2) for side in got], blocks)
            blocks_out = []
            for col_bit in range(2):
                back = [lax.ppermute(total[row_bit], ("y", "c"), [(dst, src) for src, dst in yc_pairs(row_bit, col_bit)]) for row_bit in range(2)]
                blocks_out.append(jnp.where(even_y, back[0], back[1]))
            return total, blocks_out

        def to_sequences(val):
            val = val.reshape(2, 2, NX, chunk, -1)
            mine = lax.dynamic_index_in_dim(val, c_pos, 0, keepdims=False)
            other = swap_c(lax.dynamic_index_in_dim(val, 1 - c_pos, 0, keepdims=False))
            both = jnp.stack([jnp.where(first_c, mine, other), jnp.where(first_c, other, mine)], axis=2)
            return both.reshape(2, seq, -1)

        def to_tokens(val):
            val = val.reshape(2, NX, 2, chunk, -1)
            mine = lax.dynamic_index_in_dim(val, c_pos, 2, keepdims=False)
            other = swap_c(lax.dynamic_index_in_dim(val, 1 - c_pos, 2, keepdims=False))
            both = jnp.stack([jnp.where(first_c, mine, other), jnp.where(first_c, other, mine)], axis=0)
            return both.reshape(tokens, -1)

        cos_tab = jnp.concatenate([rope_cos, rope_cos], axis=1)
        sin_tab = jnp.concatenate([-rope_sin, rope_sin], axis=1)

        x_rows = x_in[0].astype(F32)
        normed, norm_pull = jax.vjp(lambda row_vals: norm_fwd(row_vals, norm_gain), x_rows)
        h_own, dy_own = lax.optimization_barrier((normed.astype(BF16), dy_in[0]))
        h_all = lax.all_gather(h_own, ("y", "x"), axis=0, tiled=True)
        dy_all = lax.all_gather(dy_own, ("y", "x"), axis=0, tiled=True)

        def qkv_cols(bit):
            first = 2 * head * bit
            third = HEAD_GROUP * head + head * bit
            return jnp.concatenate([w_qkv[:, first : first + 2 * head], w_qkv[:, third : third + head]], axis=1)

        down_t = w_down.T
        out_t = w_out.T
        wq_piece = gather_rows([qkv_cols(j) for j in range(2)])
        wf_piece = gather_rows([jnp.concatenate([w_gate[:, j * ff_blk : (j + 1) * ff_blk], w_up[:, j * ff_blk : (j + 1) * ff_blk]], axis=1) for j in range(2)])
        ws_blocks = [jnp.concatenate([down_t[:, j * ff_blk : (j + 1) * ff_blk], out_t[:, j * o_blk : (j + 1) * o_blk]], axis=1) for j in range(2)]
        ws_piece = gather_rows([after(blk, wq_piece) for blk in ws_blocks])
        wq_full = whole_weight(gather_weight(wq_piece))
        wf_full = whole_weight(gather_weight(wf_piece))
        ws_parts = gather_weight(after(ws_piece, wf_piece))

        qkv_seq = to_sequences(dot_nn(h_all, wq_full).astype(BF16))
        queries = qkv_seq[:, :, : 2 * head]
        third_mine = qkv_seq[:, :, 2 * head :]
        third_other = swap_y(third_mine)
        keys = jnp.where(even_y, third_mine, third_other)
        values = jnp.where(even_y, third_other, third_mine)
        attn_seq = attn_fwd(queries, keys, values, cos_tab, sin_tab)
        attn_tok = to_tokens(attn_seq)
        h_recv = swap_c(pick_cols(pos, h_all))
        gate_up = dot_nn(h_all, wf_full).astype(BF16)
        act_val, act_t = act_fwd(gate_up)
        dy_recv = swap_c(pick_cols(pos, dy_all))
        pairs_act = [(act_t, swap_c(act_t), dy_all, dy_recv)]
        far_act, got_act = grad_far(pairs_act, 2)
        ws_full = whole_weight(ws_parts, far_act[0])
        mixed = jnp.concatenate([act_val, attn_tok], axis=1)
        y_part = sum_nt([mixed], [ws_full])
        mix_sum = lax.psum_scatter(y_part, ("y", "x"), scatter_dimension=0, tiled=True)
        y_out = (x_rows + mix_sum).astype(BF16)[None]

        d_mixed = dot_nn(after(dy_all, y_part), ws_full).astype(BF16)
        d_gate_up, d_gate_up_t = act_bwd(gate_up, d_mixed)
        near_act, got_act = grad_near(pairs_act, 2, got_act, d_gate_up)
        pairs_gate_up = [(d_gate_up_t, swap_c(d_gate_up_t), h_all, h_recv)]
        far_gate_up, got_gate_up = grad_far(pairs_gate_up, 4, near_act[0])
        d_attn = to_sequences(d_mixed[:, ff_blk:])
        even_flag = after(even_y.astype(jnp.int32).reshape(1), far_gate_up[0])
        d_queries, keep, send = attn_bwd(even_flag, queries, keys, values, d_attn, cos_tab, sin_tab)
        d_third = (keep + swap_y(send)).astype(BF16)
        wide_third = d_third.astype(F32)
        swapped = jnp.concatenate([wide_third[..., head // 2 :], wide_third[..., : head // 2]], axis=-1)
        d_third = jnp.where(even_y, (wide_third * cos_tab - swapped * sin_tab).astype(BF16), d_third)
        d_qkv = to_tokens(jnp.concatenate([d_queries, d_third], axis=2))
        attn_t = attn_tok.T
        d_qkv_t = d_qkv.T
        pairs_attn = [(attn_t, swap_c(attn_t), dy_all, dy_recv), (d_qkv_t, swap_c(d_qkv_t), h_all, h_recv)]
        dh_part = sum_nt([d_gate_up, d_qkv], [wf_full, wq_full])
        d_h = lax.psum_scatter(dh_part, ("y", "x"), scatter_dimension=0, tiled=True)
        d_h = d_h.astype(BF16)
        dx_out = (dy_in[0].astype(F32) + norm_pull(d_h.astype(F32))[0]).astype(BF16)[None]

        far_attn, got_attn = grad_far(pairs_attn, 1, dh_part)
        near_gate_up, got_gate_up = grad_near(pairs_gate_up, 4, got_gate_up, far_attn[0])
        _, g_act = grad_own(pairs_act, 2, got_act, near_gate_up[0])
        near_attn, got_attn = grad_near(pairs_attn, 1, got_attn, near_gate_up[0])
        own_gate_up, g_gate_up = grad_own(pairs_gate_up, 4, got_gate_up, near_attn[0])
        _, g_attn = grad_own(pairs_attn, 1, got_attn, own_gate_up[0])

        dw_down = jnp.concatenate(g_act, axis=0)
        dw_gate = jnp.concatenate([blk[:ff_blk] for blk in g_gate_up], axis=0).T
        dw_up = jnp.concatenate([blk[ff_blk:] for blk in g_gate_up], axis=0).T
        dw_out = jnp.concatenate([blk[:o_blk] for blk in g_attn], axis=0)
        dw_qkv = jnp.concatenate([blk[o_blk : o_blk + 2 * head] for blk in g_attn] + [blk[o_blk + 2 * head :] for blk in g_attn], axis=0).T
        return y_out, dx_out, dw_qkv, dw_out, dw_gate, dw_up, dw_down


    return jax.shard_map(
        layer,
        mesh=wide_mesh,
        in_specs=(act_spec, act_spec, P(), col_spec, row_spec, col_spec, col_spec, row_spec, P(), P()),
        out_specs=(act_spec, act_spec, col_spec, row_spec, col_spec, col_spec, row_spec),
        check_vma=False,
    )
```

```python
import functools

import jax
import jax.numpy as jnp
from jax import lax
from jax.experimental import pallas as pl
from jax.experimental.pallas import tpu as pltpu
from jax.sharding import Mesh, PartitionSpec as P


NORM_EPS = 1e-5
NZ = 4
NY = 4
NX = 4
NC = 2
HEAD_GROUP = 4
F32 = jnp.float32
BF16 = jnp.bfloat16
VMEM_LIMIT = 60 * 1024 * 1024
TILE = 256


def norm_fwd(row_vals, norm_gain):
    return row_vals * lax.rsqrt(jnp.mean(row_vals * row_vals, axis=-1, keepdims=True) + NORM_EPS) * norm_gain


def rotate(wide, cos_tab, sin_tab):
    return wide * cos_tab + pltpu.roll(wide, wide.shape[-1] // 2, wide.ndim - 1) * sin_tab


def rotate_back(wide, cos_tab, sin_tab):
    return wide * cos_tab - pltpu.roll(wide, wide.shape[-1] // 2, wide.ndim - 1) * sin_tab


def cost(flops, bytes_accessed):
    return pl.CostEstimate(flops=int(flops) // 20, bytes_accessed=int(bytes_accessed), transcendentals=0)


def params(**extra):
    return pltpu.CompilerParams(vmem_limit_bytes=VMEM_LIMIT, **extra)


def head_probs(q_rot, k_rot, scale):
    scores = dot_nt(q_rot, k_rot) * scale
    row_ids = lax.broadcasted_iota(jnp.int32, scores.shape, 0)
    col_ids = lax.broadcasted_iota(jnp.int32, scores.shape, 1)
    scores = jnp.where(row_ids >= col_ids, scores, -1e30)
    weights = jnp.exp(scores - jnp.max(scores, axis=-1, keepdims=True))
    return weights / jnp.sum(weights, axis=-1, keepdims=True)


def half_rows(core, idx, chunk):
    return pl.ds(pl.multiple_of((NC * idx + core) * chunk, chunk), chunk)


def chunk_rows(idx, chunk):
    return slice(idx * chunk, (idx + 1) * chunk)


def attn_fwd_kernel(heads, head, pos_ref, own_ref, other_ref, own_third_ref, other_third_ref, cos_ref, sin_ref, seq_ref, o_ref, o_other_ref, o_buf):
    core, odd = pos_ref[1], pos_ref[2]
    chunk = own_ref.shape[0] // NX
    width = heads * head
    mine = pl.ds(pl.multiple_of(width + odd * head, head), head)
    theirs = pl.ds(pl.multiple_of(width + (1 - odd) * head, head), head)
    for side, part_ref, third_ref in ((core, own_ref, own_third_ref), (1 - core, other_ref, other_third_ref)):
        for idx in range(NX):
            rows = half_rows(side, idx, chunk)
            seq_ref[0, rows, pl.ds(0, width)] = part_ref[chunk_rows(idx, chunk), :width]
            seq_ref[0, rows, mine] = part_ref[chunk_rows(idx, chunk), width:]
            seq_ref[0, rows, theirs] = third_ref[chunk_rows(idx, chunk), :]
    cos_tab, sin_tab = cos_ref[...], sin_ref[...]
    k_rot = rotate(seq_ref[0, :, width : width + head].astype(F32), cos_tab, sin_tab).astype(BF16)
    values = seq_ref[0, :, width + head :]
    for idx in range(heads):
        lanes = slice(idx * head, (idx + 1) * head)
        q_rot = rotate(seq_ref[0, :, lanes].astype(F32), cos_tab, sin_tab).astype(BF16)
        probs = head_probs(q_rot, k_rot, head**-0.5)
        o_buf[:, lanes] = dot_nn(probs.astype(BF16), values).astype(BF16)
    for side, out_ref in ((core, o_ref), (1 - core, o_other_ref)):
        for idx in range(NX):
            out_ref[chunk_rows(idx, chunk), :] = o_buf[half_rows(side, idx, chunk), :]


def attn_bwd_kernel(heads, head, pos_ref, seq_ref, own_ref, other_ref, cos_ref, sin_ref, dq_ref, keep_ref, send_ref, do_buf):
    core, odd = pos_ref[1], pos_ref[2]
    chunk = own_ref.shape[0] // NX
    width = heads * head
    for side, part_ref in ((core, own_ref), (1 - core, other_ref)):
        for idx in range(NX):
            do_buf[half_rows(side, idx, chunk), :] = part_ref[chunk_rows(idx, chunk), :]
    cos_tab, sin_tab = cos_ref[...], sin_ref[...]
    k_rot = rotate(seq_ref[0, :, width : width + head].astype(F32), cos_tab, sin_tab).astype(BF16)
    values = seq_ref[0, :, width + head :]
    d_keys = jnp.zeros(k_rot.shape, F32)
    d_values = jnp.zeros(k_rot.shape, F32)
    for idx in range(heads):
        lanes = slice(idx * head, (idx + 1) * head)
        q_rot = rotate(seq_ref[0, :, lanes].astype(F32), cos_tab, sin_tab).astype(BF16)
        d_out = do_buf[:, lanes]
        probs = head_probs(q_rot, k_rot, head**-0.5)
        d_values += dot_tn(probs.astype(BF16), d_out)
        d_probs = dot_nt(d_out, values).astype(BF16).astype(F32)
        d_scores = probs * (d_probs - jnp.sum(d_probs * probs, axis=-1, keepdims=True))
        d_scores = (d_scores * head**-0.5).astype(BF16)
        d_q_rot = dot_nn(d_scores, k_rot).astype(BF16)
        dq_ref[0, :, lanes] = rotate_back(d_q_rot.astype(F32), cos_tab, sin_tab).astype(BF16)
        d_keys += dot_tn(d_scores, q_rot)

    @pl.when(odd == 0)
    def _():
        keep_ref[0] = d_keys
        send_ref[0] = d_values

    @pl.when(odd == 1)
    def _():
        keep_ref[0] = d_values
        send_ref[0] = d_keys


def attn_post_kernel(heads, head, pos_ref, dq_ref, keep_ref, got_ref, cos_ref, sin_ref, own_ref, other_ref, third_buf):
    core, odd = pos_ref[1], pos_ref[2]
    chunk = own_ref.shape[0] // NX
    width = heads * head
    total = (keep_ref[0] + got_ref[0]).astype(BF16)

    @pl.when(odd == 0)
    def _():
        third_buf[...] = rotate_back(total.astype(F32), cos_ref[...], sin_ref[...]).astype(BF16)

    @pl.when(odd == 1)
    def _():
        third_buf[...] = total

    for side, out_ref in ((core, own_ref), (1 - core, other_ref)):
        for idx in range(NX):
            rows = half_rows(side, idx, chunk)
            out_ref[chunk_rows(idx, chunk), :width] = dq_ref[0, rows, :]
            out_ref[chunk_rows(idx, chunk), width:] = third_buf[rows, :]


def per_sequence(kernel, pos, args, specs, out_specs, out_shape, scratch, flops):
    return pl.pallas_call(
        kernel,
        grid_spec=pltpu.PrefetchScalarGridSpec(num_scalar_prefetch=1, grid=(2,), in_specs=specs, out_specs=out_specs, scratch_shapes=scratch),
        out_shape=out_shape,
        compiler_params=params(),
        cost_estimate=cost(flops, 4e6),
    )(pos, *args)


def own_spec(rows, width):
    return pl.BlockSpec((rows, width), lambda i, pos: (2 * pos[1] + i, 0))


def pair_spec(rows, width):
    return pl.BlockSpec((rows, width), lambda i, pos: (i, 0))


def seq_spec(seq, width):
    return pl.BlockSpec((1, seq, width), lambda i, pos: (i, 0, 0))


def table_spec(table):
    return pl.BlockSpec(table.shape, lambda i, pos: (0, 0))


def attn_fwd(pos, qkv_tok, other, own_third, other_third, cos_tab, sin_tab):
    seq, head = cos_tab.shape
    width = qkv_tok.shape[1] - head
    rows = seq // 2
    half = jax.ShapeDtypeStruct((seq, width), BF16)
    return per_sequence(
        functools.partial(attn_fwd_kernel, width // head, head),
        pos,
        (qkv_tok, other, own_third, other_third, cos_tab, sin_tab),
        [own_spec(rows, width + head), pair_spec(rows, width + head), pair_spec(rows, head), pair_spec(rows, head), table_spec(cos_tab), table_spec(sin_tab)],
        [seq_spec(seq, width + 2 * head), pair_spec(rows, width), pair_spec(rows, width)],
        [jax.ShapeDtypeStruct((2, seq, width + 2 * head), BF16), half, half],
        [pltpu.VMEM((seq, width), BF16)],
        16e9,
    )


def attn_bwd(pos, qkv_seq, d_attn, other, cos_tab, sin_tab):
    seq, head = cos_tab.shape
    width = d_attn.shape[1]
    rows = seq // 2
    part = jax.ShapeDtypeStruct((2, seq, head), F32)
    return per_sequence(
        functools.partial(attn_bwd_kernel, width // head, head),
        pos,
        (qkv_seq, d_attn, other, cos_tab, sin_tab),
        [seq_spec(seq, width + 2 * head), own_spec(rows, width), pair_spec(rows, width), table_spec(cos_tab), table_spec(sin_tab)],
        [seq_spec(seq, width), seq_spec(seq, head), seq_spec(seq, head)],
        [jax.ShapeDtypeStruct((2, seq, width), BF16), part, part],
        [pltpu.VMEM((seq, width), BF16)],
        16e9,
    )


def attn_post(pos, d_queries, keep, got, cos_tab, sin_tab):
    seq, head = cos_tab.shape
    width = d_queries.shape[2]
    rows = seq // 2
    half = jax.ShapeDtypeStruct((seq, width + head), BF16)
    return per_sequence(
        functools.partial(attn_post_kernel, width // head, head),
        pos,
        (d_queries, keep, got, cos_tab, sin_tab),
        [seq_spec(seq, width), seq_spec(seq, head), seq_spec(seq, head), table_spec(cos_tab), table_spec(sin_tab)],
        [pair_spec(rows, width + head), pair_spec(rows, width + head)],
        [half, half],
        [pltpu.VMEM((seq, head), BF16)],
        2e9,
    )


def act_fwd_kernel(half, ab_ref, u_ref, ut_ref):
    gate_val = ab_ref[:, :half].astype(F32)
    up_val = ab_ref[:, half:].astype(F32)
    act_val = gate_val * jax.nn.sigmoid(gate_val) * up_val
    u_ref[...] = act_val.astype(BF16)
    ut_ref[...] = act_val.T.astype(BF16)


def act_fwd(gate_up):
    tokens, width = gate_up.shape
    half = width // 2
    rows = tokens // 4
    return pl.pallas_call(
        functools.partial(act_fwd_kernel, half),
        grid=(4,),
        in_specs=[pl.BlockSpec((rows, width), lambda i: (i, 0))],
        out_specs=[pl.BlockSpec((rows, half), lambda i: (i, 0)), pl.BlockSpec((half, rows), lambda i: (0, i))],
        out_shape=[jax.ShapeDtypeStruct((tokens, half), BF16), jax.ShapeDtypeStruct((half, tokens), BF16)],
        compiler_params=params(),
        cost_estimate=cost(4e9, 8e6),
        name="act_fwd",
    )(gate_up)


def act_bwd_kernel(half, ab_ref, du_ref, dab_ref, dabt_ref):
    gate_val = ab_ref[:, :half].astype(F32)
    up_val = ab_ref[:, half:].astype(F32)
    d_act = du_ref[...].astype(F32)
    sig = jax.nn.sigmoid(gate_val)
    d_silu = d_act * up_val
    d_gate = d_silu * sig + d_silu * gate_val * (sig * (1.0 - sig))
    d_up = d_act * (gate_val * sig)
    dab_ref[:, :half] = d_gate.astype(BF16)
    dab_ref[:, half:] = d_up.astype(BF16)
    dabt_ref[:half, :] = d_gate.T.astype(BF16)
    dabt_ref[half:, :] = d_up.T.astype(BF16)


def act_bwd(gate_up, d_mixed):
    tokens, width = gate_up.shape
    half = width // 2
    rows = tokens // 4
    return pl.pallas_call(
        functools.partial(act_bwd_kernel, half),
        grid=(4,),
        in_specs=[pl.BlockSpec((rows, width), lambda i: (i, 0)), pl.BlockSpec((rows, half), lambda i: (i, 0))],
        out_specs=[pl.BlockSpec((rows, width), lambda i: (i, 0)), pl.BlockSpec((width, rows), lambda i: (0, i))],
        out_shape=[jax.ShapeDtypeStruct((tokens, width), BF16), jax.ShapeDtypeStruct((width, tokens), BF16)],
        compiler_params=params(),
        cost_estimate=cost(8e9, 14e6),
        name="act_bwd",
    )(gate_up, d_mixed)


def piece_block(pos_ref, step, other):
    core = pos_ref[1]
    return lax.rem(pos_ref[0] + step, NZ) * NC + (1 - core if other else core)


def half_start(pos_ref, part, half):
    return pl.multiple_of((1 - pos_ref[2] if part else pos_ref[2]) * half, half)


def nn_kernel(keys, first, count_out, pos_ref, acts_ref, *refs):
    count = len(keys)
    halves = refs[: 2 * count]
    outs = refs[2 * count : 2 * count + count_out]
    acts_buf, w_buf, total, acts_sem, w_sem = refs[2 * count + count_out :]
    block = acts_buf.shape[1] // count
    half = block // 2
    copies = []
    for idx in range(count):
        cols = pl.ds(pl.multiple_of(piece_block(pos_ref, *keys[idx]) * block, block), block)
        copies.append([pltpu.make_async_copy(acts_ref.at[:, cols], acts_buf.at[:, pl.ds(idx * block, block)], acts_sem.at[idx])])
        for part in range(2):
            rows = pl.ds(idx * block + half_start(pos_ref, part, half), half)
            copies[-1].append(pltpu.make_async_copy(halves[2 * idx + part], w_buf.at[rows], w_sem.at[2 * idx + part]))
    for group in copies:
        for copy in group:
            copy.start()
    for lo, hi in ((0, first), (first, count)):
        for group in copies[lo:hi]:
            for copy in group:
                copy.wait()
        depth = pl.ds(lo * block, (hi - lo) * block)
        start = 0
        for out_ref in outs:
            width = out_ref.shape[1]

            def step(out_lo, size, start=start, out_ref=out_ref, depth=depth, hi=hi):
                cols = pl.ds(pl.multiple_of(start + out_lo, 128), size)
                part = dot_nn(acts_buf[:, depth], w_buf[depth, cols])
                if hi == count:
                    out_ref[:, pl.ds(pl.multiple_of(out_lo, 128), size)] = (total[:, cols] + part).astype(BF16)
                else:
                    total[:, cols] = part

            whole = width // TILE
            if whole:
                pl.loop(0, whole)(lambda n: step(n * TILE, TILE))
            if width % TILE:
                step(whole * TILE, width % TILE)
            start += width


def nn_pieces(pos, acts, parts, widths):
    keys = [(step, other) for step in (0, 1, 3, 2) for other in range(2)]
    halves = [parts[step][other][part] for step, other in keys for part in range(2)]
    tokens, depth = acts.shape
    width = sum(widths)
    count = len(keys)
    anywhere = pl.BlockSpec(memory_space=pl.ANY)
    return pl.pallas_call(
        functools.partial(nn_kernel, keys, 2, len(widths)),
        grid_spec=pltpu.PrefetchScalarGridSpec(
            num_scalar_prefetch=1,
            grid=(1,),
            in_specs=[anywhere] * (1 + 2 * count),
            out_specs=[pl.BlockSpec((tokens, size), lambda i, pos: (0, 0)) for size in widths],
            scratch_shapes=[
                pltpu.VMEM((tokens, depth), BF16),
                pltpu.VMEM((depth, width), BF16),
                pltpu.VMEM((tokens, width), F32),
                pltpu.SemaphoreType.DMA((count,)),
                pltpu.SemaphoreType.DMA((2 * count,)),
            ],
        ),
        out_shape=[jax.ShapeDtypeStruct((tokens, size), BF16) for size in widths],
        compiler_params=params(),
        cost_estimate=cost(2 * tokens * depth * width, 2 * depth * (tokens + width)),
    )(pos, acts, *halves)


def nt_kernel(keys, count_left, pos_ref, *refs):
    count = len(keys)
    lefts = refs[:count_left]
    halves = refs[count_left : count_left + 2 * count]
    out_ref, left_buf, w_buf, out_buf, left_sem, w_sem, out_sem = refs[count_left + 2 * count :]
    block = out_buf.shape[2]
    half = block // 2
    slots = w_buf.shape[0]
    left_copies = []
    start = 0
    for idx, left in enumerate(lefts):
        left_copies.append(pltpu.make_async_copy(left, left_buf.at[:, pl.ds(start, left.shape[1])], left_sem.at[idx]))
        left_copies[-1].start()
        start += left.shape[1]

    def copies(idx):
        for part in range(2):
            rows = pl.ds(half_start(pos_ref, part, half), half)
            yield pltpu.make_async_copy(halves[2 * idx + part], w_buf.at[idx % slots, rows], w_sem.at[idx % slots, part])

    def out_copy(idx):
        cols = pl.ds(pl.multiple_of(piece_block(pos_ref, *keys[idx]) * block, block), block)
        return pltpu.make_async_copy(out_buf.at[idx % 2], out_ref.at[:, cols], out_sem.at[idx % 2])

    for idx in range(slots - 1):
        for copy in copies(idx):
            copy.start()
    for idx in range(count):
        if idx + slots - 1 < count:
            for copy in copies(idx + slots - 1):
                copy.start()
        for copy in copies(idx):
            copy.wait()
        if idx == 0:
            for copy in left_copies:
                copy.wait()
        if idx >= 2:
            out_copy(idx - 2).wait()
        out_buf[idx % 2] = dot_nt(left_buf[...], w_buf[idx % slots])
        out_copy(idx).start()
    for idx in range(count - 2, count):
        out_copy(idx).wait()


def nt_pieces(pos, lefts, parts):
    keys = [(step, other) for step in range(NZ) for other in range(2)]
    halves = [parts[step][other][part] for step, other in keys for part in range(2)]
    tokens = lefts[0].shape[0]
    block = 2 * halves[0].shape[0]
    depth = block * len(keys)
    width = halves[0].shape[1]
    slots = 3
    anywhere = pl.BlockSpec(memory_space=pl.ANY)
    return pl.pallas_call(
        functools.partial(nt_kernel, keys, len(lefts)),
        grid_spec=pltpu.PrefetchScalarGridSpec(
            num_scalar_prefetch=1,
            grid=(1,),
            in_specs=[anywhere] * (len(lefts) + len(halves)),
            out_specs=anywhere,
            scratch_shapes=[
                pltpu.VMEM((tokens, width), BF16),
                pltpu.VMEM((slots, block, width), BF16),
                pltpu.VMEM((2, tokens, block), F32),
                pltpu.SemaphoreType.DMA((len(lefts),)),
                pltpu.SemaphoreType.DMA((slots, 2)),
                pltpu.SemaphoreType.DMA((2,)),
            ],
        ),
        out_shape=jax.ShapeDtypeStruct((tokens, depth), F32),
        compiler_params=params(),
        cost_estimate=cost(2 * tokens * depth * width, 2 * depth * width + 4 * tokens * depth),
    )(pos, *lefts, *halves)


def picked_cols(pos_ref, idx, block):
    return pl.ds(pl.multiple_of((NC * idx + 1 - pos_ref[1]) * block, block), block)


def dma_kernel(kernel, pos, args, out_shape, scratch):
    anywhere = pl.BlockSpec(memory_space=pl.ANY)
    return pl.pallas_call(
        kernel,
        grid_spec=pltpu.PrefetchScalarGridSpec(
            num_scalar_prefetch=1, grid=(1,), in_specs=[anywhere] * len(args), out_specs=[anywhere] * len(out_shape), scratch_shapes=scratch
        ),
        out_shape=out_shape,
        compiler_params=params(),
        cost_estimate=cost(3e9, 16e6),
    )(pos, *args)


def pick_cols(pos, acts):
    tokens, depth = acts.shape
    block = depth // (NC * NZ)

    def kernel(pos_ref, in_ref, out_ref, buf, in_sem, out_sem):
        reads = [pltpu.make_async_copy(in_ref.at[:, picked_cols(pos_ref, idx, block)], buf.at[idx], in_sem.at[idx]) for idx in range(NZ)]
        writes = [pltpu.make_async_copy(buf.at[idx], out_ref.at[:, pl.ds(idx * block, block)], out_sem.at[idx]) for idx in range(NZ)]
        for read in reads:
            read.start()
        for read, write in zip(reads, writes):
            read.wait()
            write.start()
        for write in writes:
            write.wait()

    sems = pltpu.SemaphoreType.DMA((NZ,))
    return dma_kernel(kernel, pos, [acts], [jax.ShapeDtypeStruct((tokens, depth // 2), BF16)], [pltpu.VMEM((NZ, tokens, block), BF16), sems, sems])[0]


def settle_y(pos, own, left, right, far):
    chunk, depth = own.shape
    half = chunk // 2
    sources = [(0, 0, own), (3, 0, left), (1, 0, right), (2, 0, far[0]), (2, half, far[1])]

    def kernel(pos_ref, *refs):
        ins, (out0, out1, buf, in_sem, out_sem) = refs[: len(sources)], refs[len(sources) :]
        reads = []
        for idx, (step, start, array) in enumerate(sources):
            row = pl.multiple_of(lax.rem(pos_ref[3] + step, NY) * chunk, chunk) + start
            reads.append(pltpu.make_async_copy(ins[idx], buf.at[pl.ds(row, array.shape[0])], in_sem.at[idx]))
            reads[-1].start()
        for read in reads:
            read.wait()
        writes = [pltpu.make_async_copy(buf.at[pl.ds(idx * 2 * chunk, 2 * chunk)], out, out_sem.at[idx]) for idx, out in enumerate((out0, out1))]
        for write in writes:
            write.start()
        for write in writes:
            write.wait()

    out = jax.ShapeDtypeStruct((2 * chunk, depth), BF16)
    scratch = [pltpu.VMEM((NY * chunk, depth), BF16), pltpu.SemaphoreType.DMA((len(sources),)), pltpu.SemaphoreType.DMA((2,))]
    return dma_kernel(kernel, pos, [array for _, _, array in sources], [out, out], scratch)


def settle_x(pos, parts):
    sources = [(step, half, parts[step][half]) for step in range(NX) for half in range(2)]
    chunk = sources[0][2].shape[0] // 2
    depth = sources[0][2].shape[1]
    block = depth // (NC * NZ)
    blocks = 2 * len(sources)

    def kernel(pos_ref, *refs):
        ins, (all_ref, out_ref, buf, in_sem, all_sem, out_sem) = refs[: len(sources)], refs[len(sources) :]
        reads = []
        rows = []
        for idx, (step, half, _) in enumerate(sources):
            x_pos = lax.rem(pos_ref[4] + step, NX)
            for part in range(2):
                rows.append(pl.ds(pl.multiple_of(((2 * half + part) * NX + x_pos) * chunk, chunk), chunk))
                reads.append(pltpu.make_async_copy(ins[idx].at[pl.ds(part * chunk, chunk)], buf.at[rows[-1]], in_sem.at[2 * idx + part]))
                reads[-1].start()
        writes = []
        for idx in range(blocks):
            reads[idx].wait()
            writes.append(pltpu.make_async_copy(buf.at[rows[idx]], all_ref.at[rows[idx]], all_sem.at[idx]))
            for col in range(NZ):
                cols = picked_cols(pos_ref, col, block)
                writes.append(pltpu.make_async_copy(buf.at[rows[idx], cols], out_ref.at[rows[idx], pl.ds(col * block, block)], out_sem.at[idx, col]))
            for write in writes[-1 - NZ :]:
                write.start()
        for write in writes:
            write.wait()

    tokens = blocks * chunk
    out_shape = [jax.ShapeDtypeStruct((tokens, depth), BF16), jax.ShapeDtypeStruct((tokens, depth // 2), BF16)]
    scratch = [pltpu.VMEM((tokens, depth), BF16), pltpu.SemaphoreType.DMA((blocks,)), pltpu.SemaphoreType.DMA((blocks,)), pltpu.SemaphoreType.DMA((blocks, NZ))]
    return dma_kernel(kernel, pos, [array for _, _, array in sources], out_shape, scratch)


def grad_kernel(heights, pos_ref, *refs):
    pairs = len(heights)
    ins = refs[: 6 * pairs]
    outs = refs[6 * pairs : 6 * pairs + 2 * NZ]
    buf, sem = refs[6 * pairs + 2 * NZ :]
    step = pl.program_id(0)
    slot = lax.rem(step, 2)

    def out_copy(idx, part):
        return pltpu.make_async_copy(buf.at[idx % 2, part], outs[2 * idx + part], sem.at[idx % 2, part])

    for idx in range(2, NZ):

        @pl.when(step == idx)
        def _(idx=idx):
            for part in range(2):
                out_copy(idx - 2, part).wait()

    start = 0
    for idx, height in enumerate(heights):
        own, recv, acts0, acts1, recv0, recv1 = ins[6 * idx : 6 * idx + 6]
        for part, acts, acts_recv in ((0, acts0, recv0), (1, acts1, recv1)):
            buf[slot, part, start : start + height, :] = dot_nn(own[...], acts[...]) + dot_nn(recv[...], acts_recv[...])
        start += height
    for idx in range(NZ):

        @pl.when(step == idx)
        def _(idx=idx):
            for part in range(2):
                out_copy(idx, part).start()

    @pl.when(step == NZ - 1)
    def _():
        for idx in (NZ - 2, NZ - 1):
            for part in range(2):
                out_copy(idx, part).wait()


def grad_pieces(pos, pairs):
    tokens, depth = pairs[0][2].shape
    cols = depth // (NZ * NY)
    in_specs = []
    args = []

    def z_of(n, pos):
        return lax.rem(pos[0] + jnp.where(n == 0, 2, jnp.where(n == 1, 1, jnp.where(n == 2, 3, 0))), NZ)

    def bit(pos, part):
        return 1 - pos[2] if part else pos[2]

    for own, recv, acts, acts_recv, height, block in pairs:
        in_specs += [pl.BlockSpec((height, tokens), lambda n, pos, block=block: (block, 0))] * 2
        in_specs += [pl.BlockSpec((tokens, cols), lambda n, pos, part=part: (0, z_of(n, pos) * NY + 2 * pos[1] + bit(pos, part))) for part in range(2)]
        in_specs += [pl.BlockSpec((tokens, cols), lambda n, pos, part=part: (0, z_of(n, pos) * 2 + bit(pos, part))) for part in range(2)]
        args += [own, recv, acts, acts, acts_recv, acts_recv]
    heights = [pair[4] for pair in pairs]
    rows = sum(heights)
    return pl.pallas_call(
        functools.partial(grad_kernel, heights),
        grid_spec=pltpu.PrefetchScalarGridSpec(
            num_scalar_prefetch=1,
            grid=(NZ,),
            in_specs=in_specs,
            out_specs=[pl.BlockSpec(memory_space=pl.ANY)] * (2 * NZ),
            scratch_shapes=[pltpu.VMEM((2, 2, rows, cols), F32), pltpu.SemaphoreType.DMA((2, 2))],
        ),
        out_shape=[jax.ShapeDtypeStruct((rows, cols), F32)] * (2 * NZ),
        compiler_params=params(),
        cost_estimate=cost(4 * rows * tokens * cols * 2 * NZ, 4 * tokens * cols * 2 * NZ),
        name="grad",
    )(pos, *args)


def place(pos, first, second, height, block, transpose):
    cols = first.shape[1]
    spec = pl.BlockSpec((height, cols), lambda n, pos: (block, 0))

    def kernel(pos_ref, first_ref, second_ref, out_ref):
        for idx, ref in enumerate((first_ref, second_ref)):

            @pl.when(pl.program_id(0) == idx)
            def _(ref=ref):
                out_ref[...] = ref[...].T if transpose else ref[...]

    def order(n, pos):
        return jnp.where(n == 0, pos[2], 1 - pos[2])

    return pl.pallas_call(
        kernel,
        grid_spec=pltpu.PrefetchScalarGridSpec(
            num_scalar_prefetch=1,
            grid=(2,),
            in_specs=[spec, spec],
            out_specs=pl.BlockSpec((cols, height), lambda n, pos: (0, order(n, pos))) if transpose else pl.BlockSpec((height, cols), lambda n, pos: (order(n, pos), 0)),
        ),
        out_shape=jax.ShapeDtypeStruct((cols, 2 * height) if transpose else (2 * height, cols), F32),
        compiler_params=params(),
        cost_estimate=cost(2e9, 16 * height * cols),
    )(pos, first, second)


def after(val, *earlier):
    return lax.optimization_barrier((val, *earlier))[0]


def ring(step, size):
    return [(src, (src + step) % size) for src in range(size)]


def hop_z(val, step):
    return lax.ppermute(val, "z", ring(step, NZ))


def hop_y(val, step):
    return lax.ppermute(val, "y", ring(step, NY))


def hop_x(val, step):
    return lax.ppermute(val, "x", ring(step, NX))


def swap_c(val):
    return lax.ppermute(val, "c", [(0, 1), (1, 0)])


def swap_y(val):
    return lax.ppermute(val, "y", [(src, src ^ 1) for src in range(NY)])


def turn(val, flip):
    def place_of(y_pos, c_pos):
        return y_pos * NC + c_pos

    pairs = [(place_of(2 * a + b, c), place_of(2 * c + (b ^ flip), a)) for a in range(2) for b in range(2) for c in range(NC)]
    return lax.ppermute(val, ("y", "c"), pairs)


def swap_yc(val):
    pairs = [(y_pos * NC + c_pos, (y_pos ^ 1) * NC + 1 - c_pos) for y_pos in range(NY) for c_pos in range(NC)]
    return lax.ppermute(val, ("y", "c"), pairs)


def dot_nn(left, right):
    return lax.dot_general(left, right, (((1,), (0,)), ((), ())), preferred_element_type=F32)


def dot_nt(left, right):
    return lax.dot_general(left, right, (((1,), (1,)), ((), ())), preferred_element_type=F32)


def dot_tn(left, right):
    return lax.dot_general(left, right, (((0,), (0,)), ((), ())), preferred_element_type=F32)


def solution(mesh):
    wide_mesh = Mesh(mesh.devices.reshape(NZ, NY, NX, NC), ("z", "y", "x", "c"))
    rows = ("z", "y")
    cols = ("x", "c")
    act_spec = P(rows, cols, None)
    col_spec = P(rows, cols)
    row_spec = P(cols, rows)

    def layer(x_in, dy_in, norm_gain, w_qkv, w_out, w_gate, w_up, w_down, rope_cos, rope_sin):
        z_pos = lax.axis_index("z")
        y_pos = lax.axis_index("y")
        c_pos = lax.axis_index("c")
        even_y = y_pos % 2 == 0
        first_c = c_pos == 0
        pos = jnp.stack([z_pos, c_pos, y_pos % 2, y_pos, lax.axis_index("x")]).astype(jnp.int32)
        head = 2 * rope_cos.shape[1]
        seq = rope_cos.shape[0]
        ff_blk = w_gate.shape[1] // 2
        o_blk = w_out.shape[0] // 2
        qkv_blk = o_blk + head

        def gather_rows(blocks):
            return [turn(jnp.where(even_y, blocks[flip], blocks[1 - flip]), flip) for flip in range(2)]

        def gather_weight(piece):
            left = [hop_z(half, 1) for half in piece]
            right = [hop_z(half, -1) for half in piece]
            far = [hop_z(left[0], 1), hop_z(right[1], -1)]
            parts = []
            for mine in (piece, right, far, left):
                parts.append((mine, [swap_c(half) for half in mine]))
            return parts

        def grad_start(pairs, *earlier):
            far0, far1, up0, up1, down0, down1, own0, own1 = grad_pieces(after(pos, *earlier), pairs)
            far = (hop_z(far0, 1), hop_z(far1, -1))
            direct = (hop_z(up1, 1), hop_z(down0, -1))
            return (up0, down1), far, direct, (own0, own1)

        def grad_pass(state, *earlier):
            (up0, down1), far, direct, own = state
            passed = (hop_z(up0 + after(far[0], *earlier), 1), hop_z(down1 + far[1], -1))
            return direct, passed, own

        def grad_back(state, *earlier):
            direct, passed, own = state
            first = own[0] + after(passed[0], *earlier) + direct[1]
            second = own[1] + direct[0] + passed[1]
            return turn(first, 0), turn(second, 1)

        def my_rows(val, mine):
            return lax.dynamic_slice_in_dim(val, (c_pos if mine else 1 - c_pos) * seq, seq, axis=0)

        def both_rows(own, other):
            got = swap_c(other)
            return jnp.concatenate([jnp.where(first_c, own, got), jnp.where(first_c, got, own)], axis=0)

        cos_tab = jnp.concatenate([rope_cos, rope_cos], axis=1)
        sin_tab = jnp.concatenate([-rope_sin, rope_sin], axis=1)

        def qkv_cols(bit):
            first = 2 * head * bit
            third = HEAD_GROUP * head + head * bit
            return [w_qkv[:, first : first + 2 * head], w_qkv[:, third : third + head]]

        def block(weight, bit):
            size = weight.shape[1] // 2
            return weight[:, bit * size : (bit + 1) * size]

        down_t = w_down.T
        out_t = w_out.T
        wf_piece = gather_rows([jnp.concatenate([block(w_gate, j), block(w_up, j), *qkv_cols(j)], axis=1) for j in range(2)])
        ws_piece = gather_rows([jnp.concatenate([block(down_t, j), block(out_t, j)], axis=1) for j in range(2)])

        x_rows = x_in[0].astype(F32)
        normed, norm_pull = jax.vjp(lambda row_vals: norm_fwd(row_vals, norm_gain), x_rows)
        h_all = lax.all_gather(after(normed.astype(BF16), *wf_piece), ("y", "x"), axis=0, tiled=True)
        dy_own = dy_in[0]
        dy_half = dy_own.shape[0] // 2
        dy_left = hop_y(dy_own, 1)
        dy_right = hop_y(dy_own, -1)
        dy_far = [hop_y(dy_left[:dy_half], 1), hop_y(dy_right[dy_half:], -1)]
        dy_piece = settle_y(pos, dy_own, dy_left, dy_right, dy_far)
        dx_left = [hop_x(half, 1) for half in dy_piece]
        dx_right = [hop_x(half, -1) for half in dy_piece]
        dx_far = [hop_x(dx_left[0], 1), hop_x(dx_right[1], -1)]
        wf_parts = gather_weight(wf_piece)
        ws_parts = gather_weight(ws_piece)

        gate_up, qkv_tok = nn_pieces(pos, h_all, wf_parts, (2 * ff_blk, qkv_blk))
        third = qkv_tok[:, o_blk:]
        qkv_other = swap_c(my_rows(qkv_tok, False))
        third_own = swap_y(my_rows(third, True))
        third_other = swap_yc(my_rows(third, False))
        act_val, act_t = act_fwd(after(gate_up, qkv_tok))
        act_recv = swap_c(act_t)
        dy_all, dy_picked = settle_x(after(pos, act_t), (dy_piece, dx_right, dx_far, dx_left))
        dy_recv = swap_c(dy_picked)
        qkv_seq, attn_own, attn_other = attn_fwd(after(pos, dy_picked), qkv_tok, qkv_other, third_own, third_other, cos_tab, sin_tab)
        attn_tok = both_rows(attn_own, attn_other)
        g_act = grad_start([(act_t, act_recv, dy_all, dy_recv, ff_blk, 0)], attn_own)
        h_picked = pick_cols(after(pos, g_act[3][0]), h_all)
        h_recv = swap_c(h_picked)
        y_part = nt_pieces(after(pos, h_picked), [act_val, attn_tok], ws_parts)
        mix_sum = lax.psum_scatter(y_part, ("y", "x"), scatter_dimension=0, tiled=True)
        y_out = (x_rows + mix_sum).astype(BF16)[None]

        d_act, d_attn = nn_pieces(after(pos, y_part), dy_all, ws_parts, (ff_blk, o_blk))
        d_attn_other = swap_c(my_rows(d_attn, False))
        g_act = grad_pass(g_act, d_attn)
        d_gate_up, d_gate_up_t = act_bwd(gate_up, d_act)
        d_gate_up_recv = swap_c(d_gate_up_t)
        d_queries, keep, send = attn_bwd(after(pos, d_gate_up_t), qkv_seq, d_attn, d_attn_other, cos_tab, sin_tab)
        got = swap_y(send)
        g_gate = grad_start([(d_gate_up_t, d_gate_up_recv, h_all, h_recv, ff_blk, 0)], d_queries)
        g_up = grad_start([(d_gate_up_t, d_gate_up_recv, h_all, h_recv, ff_blk, 1)], g_gate[3][0])
        d_own, d_other = attn_post(after(pos, g_up[3][0]), d_queries, keep, got, cos_tab, sin_tab)
        d_qkv = both_rows(d_own, d_other)
        g_gate = grad_pass(g_gate, d_own)
        dh_part = nt_pieces(pos, [d_gate_up, d_qkv], wf_parts)
        d_h = lax.psum_scatter(dh_part, ("y", "x"), scatter_dimension=0, tiled=True)
        d_h = d_h.astype(BF16)
        dx_out = (dy_in[0].astype(F32) + norm_pull(d_h.astype(F32))[0]).astype(BF16)[None]

        attn_t = attn_tok.T
        d_qkv_t = d_qkv.T
        attn_recv = swap_c(attn_t)
        d_qkv_recv = swap_c(d_qkv_t)
        g_up = grad_pass(g_up, dh_part)
        g_attn = grad_start([(attn_t, attn_recv, dy_all, dy_recv, o_blk, 0), (d_qkv_t, d_qkv_recv, h_all, h_recv, qkv_blk, 0)], dh_part)
        b_act = grad_back(g_act, g_attn[3][0])
        g_attn = grad_pass(g_attn, b_act[0])
        b_gate = grad_back(g_gate)
        b_up = grad_back(g_up)
        b_attn = grad_back(g_attn)
        dw_down = place(pos, *b_act, ff_blk, 0, False)
        dw_gate = place(pos, *b_gate, ff_blk, 0, True)
        dw_up = place(pos, *b_up, ff_blk, 0, True)
        dw_out = place(pos, *b_attn, o_blk, 0, False)
        dw_q = place(pos, *b_attn, 2 * head, 1, True)
        dw_kv = place(pos, *b_attn, head, 2 * o_blk // head, True)
        dw_qkv = jnp.concatenate([dw_q, dw_kv], axis=1)
        return y_out, dx_out, dw_qkv, dw_out, dw_gate, dw_up, dw_down


    return jax.shard_map(
        layer,
        mesh=wide_mesh,
        in_specs=(act_spec, act_spec, P(), col_spec, row_spec, col_spec, col_spec, row_spec, P(), P()),
        out_specs=(act_spec, act_spec, col_spec, row_spec, col_spec, col_spec, row_spec),
        check_vma=False,
    )
```

```python
import functools

import jax
import jax.numpy as jnp
from jax import lax
from jax.experimental import pallas as pl
from jax.experimental.pallas import tpu as pltpu
from jax.sharding import Mesh, PartitionSpec as P


NORM_EPS = 1e-5
NZ = 4
NY = 4
NX = 4
NC = 2
HEAD_GROUP = 4
F32 = jnp.float32
BF16 = jnp.bfloat16
VMEM_LIMIT = 60 * 1024 * 1024
TILE = 256


def norm_fwd(row_vals, norm_gain):
    return row_vals * lax.rsqrt(jnp.mean(row_vals * row_vals, axis=-1, keepdims=True) + NORM_EPS) * norm_gain


def rotate(wide, cos_tab, sin_tab):
    return wide * cos_tab + pltpu.roll(wide, wide.shape[-1] // 2, wide.ndim - 1) * sin_tab


def rotate_back(wide, cos_tab, sin_tab):
    return wide * cos_tab - pltpu.roll(wide, wide.shape[-1] // 2, wide.ndim - 1) * sin_tab


def cost(flops, bytes_accessed):
    return pl.CostEstimate(flops=int(flops) // 20, bytes_accessed=int(bytes_accessed), transcendentals=0)


def params(**extra):
    return pltpu.CompilerParams(vmem_limit_bytes=VMEM_LIMIT, **extra)


def head_probs(q_rot, k_rot, scale):
    scores = dot_nt(q_rot, k_rot) * scale
    row_ids = lax.broadcasted_iota(jnp.int32, scores.shape, 0)
    col_ids = lax.broadcasted_iota(jnp.int32, scores.shape, 1)
    scores = jnp.where(row_ids >= col_ids, scores, -1e30)
    weights = jnp.exp(scores - jnp.max(scores, axis=-1, keepdims=True))
    return weights / jnp.sum(weights, axis=-1, keepdims=True)


def half_rows(core, idx, chunk):
    return pl.ds(pl.multiple_of((NC * idx + core) * chunk, chunk), chunk)


def chunk_rows(idx, chunk):
    return slice(idx * chunk, (idx + 1) * chunk)


def attn_fwd_kernel(heads, head, pos_ref, own_ref, other_ref, own_third_ref, other_third_ref, cos_ref, sin_ref, seq_ref, o_ref, o_other_ref, o_buf):
    core, odd = pos_ref[1], pos_ref[2]
    chunk = own_ref.shape[0] // NX
    width = heads * head
    mine = pl.ds(pl.multiple_of(width + odd * head, head), head)
    theirs = pl.ds(pl.multiple_of(width + (1 - odd) * head, head), head)
    for side, part_ref, third_ref in ((core, own_ref, own_third_ref), (1 - core, other_ref, other_third_ref)):
        for idx in range(NX):
            rows = half_rows(side, idx, chunk)
            seq_ref[0, rows, pl.ds(0, width)] = part_ref[chunk_rows(idx, chunk), :width]
            seq_ref[0, rows, mine] = part_ref[chunk_rows(idx, chunk), width:]
            seq_ref[0, rows, theirs] = third_ref[chunk_rows(idx, chunk), :]
    cos_tab, sin_tab = cos_ref[...], sin_ref[...]
    k_rot = rotate(seq_ref[0, :, width : width + head].astype(F32), cos_tab, sin_tab).astype(BF16)
    values = seq_ref[0, :, width + head :]
    for idx in range(heads):
        lanes = slice(idx * head, (idx + 1) * head)
        q_rot = rotate(seq_ref[0, :, lanes].astype(F32), cos_tab, sin_tab).astype(BF16)
        probs = head_probs(q_rot, k_rot, head**-0.5)
        o_buf[:, lanes] = dot_nn(probs.astype(BF16), values).astype(BF16)
    for side, out_ref in ((core, o_ref), (1 - core, o_other_ref)):
        for idx in range(NX):
            out_ref[chunk_rows(idx, chunk), :] = o_buf[half_rows(side, idx, chunk), :]


def attn_bwd_kernel(heads, head, pos_ref, seq_ref, own_ref, other_ref, cos_ref, sin_ref, dq_ref, keep_ref, send_ref, do_buf):
    core, odd = pos_ref[1], pos_ref[2]
    chunk = own_ref.shape[0] // NX
    width = heads * head
    for side, part_ref in ((core, own_ref), (1 - core, other_ref)):
        for idx in range(NX):
            do_buf[half_rows(side, idx, chunk), :] = part_ref[chunk_rows(idx, chunk), :]
    cos_tab, sin_tab = cos_ref[...], sin_ref[...]
    k_rot = rotate(seq_ref[0, :, width : width + head].astype(F32), cos_tab, sin_tab).astype(BF16)
    values = seq_ref[0, :, width + head :]
    d_keys = jnp.zeros(k_rot.shape, F32)
    d_values = jnp.zeros(k_rot.shape, F32)
    for idx in range(heads):
        lanes = slice(idx * head, (idx + 1) * head)
        q_rot = rotate(seq_ref[0, :, lanes].astype(F32), cos_tab, sin_tab).astype(BF16)
        d_out = do_buf[:, lanes]
        probs = head_probs(q_rot, k_rot, head**-0.5)
        d_values += dot_tn(probs.astype(BF16), d_out)
        d_probs = dot_nt(d_out, values).astype(BF16).astype(F32)
        d_scores = probs * (d_probs - jnp.sum(d_probs * probs, axis=-1, keepdims=True))
        d_scores = (d_scores * head**-0.5).astype(BF16)
        d_q_rot = dot_nn(d_scores, k_rot).astype(BF16)
        dq_ref[0, :, lanes] = rotate_back(d_q_rot.astype(F32), cos_tab, sin_tab).astype(BF16)
        d_keys += dot_tn(d_scores, q_rot)

    @pl.when(odd == 0)
    def _():
        keep_ref[0] = d_keys
        send_ref[0] = d_values

    @pl.when(odd == 1)
    def _():
        keep_ref[0] = d_values
        send_ref[0] = d_keys


def attn_post_kernel(heads, head, pos_ref, dq_ref, keep_ref, got_ref, cos_ref, sin_ref, own_ref, other_ref, third_buf):
    core, odd = pos_ref[1], pos_ref[2]
    chunk = own_ref.shape[0] // NX
    width = heads * head
    total = (keep_ref[0] + got_ref[0]).astype(BF16)

    @pl.when(odd == 0)
    def _():
        third_buf[...] = rotate_back(total.astype(F32), cos_ref[...], sin_ref[...]).astype(BF16)

    @pl.when(odd == 1)
    def _():
        third_buf[...] = total

    for side, out_ref in ((core, own_ref), (1 - core, other_ref)):
        for idx in range(NX):
            rows = half_rows(side, idx, chunk)
            out_ref[chunk_rows(idx, chunk), :width] = dq_ref[0, rows, :]
            out_ref[chunk_rows(idx, chunk), width:] = third_buf[rows, :]


def per_sequence(kernel, pos, args, specs, out_specs, out_shape, scratch, flops):
    return pl.pallas_call(
        kernel,
        grid_spec=pltpu.PrefetchScalarGridSpec(num_scalar_prefetch=1, grid=(2,), in_specs=specs, out_specs=out_specs, scratch_shapes=scratch),
        out_shape=out_shape,
        compiler_params=params(),
        cost_estimate=cost(flops, 4e6),
    )(pos, *args)


def own_spec(rows, width):
    return pl.BlockSpec((rows, width), lambda i, pos: (2 * pos[1] + i, 0))


def pair_spec(rows, width):
    return pl.BlockSpec((rows, width), lambda i, pos: (i, 0))


def seq_spec(seq, width):
    return pl.BlockSpec((1, seq, width), lambda i, pos: (i, 0, 0))


def table_spec(table):
    return pl.BlockSpec(table.shape, lambda i, pos: (0, 0))


def attn_fwd(pos, qkv_tok, other, own_third, other_third, cos_tab, sin_tab):
    seq, head = cos_tab.shape
    width = qkv_tok.shape[1] - head
    rows = seq // 2
    half = jax.ShapeDtypeStruct((seq, width), BF16)
    return per_sequence(
        functools.partial(attn_fwd_kernel, width // head, head),
        pos,
        (qkv_tok, other, own_third, other_third, cos_tab, sin_tab),
        [own_spec(rows, width + head), pair_spec(rows, width + head), pair_spec(rows, head), pair_spec(rows, head), table_spec(cos_tab), table_spec(sin_tab)],
        [seq_spec(seq, width + 2 * head), pair_spec(rows, width), pair_spec(rows, width)],
        [jax.ShapeDtypeStruct((2, seq, width + 2 * head), BF16), half, half],
        [pltpu.VMEM((seq, width), BF16)],
        16e9,
    )


def attn_bwd(pos, qkv_seq, d_attn, other, cos_tab, sin_tab):
    seq, head = cos_tab.shape
    width = d_attn.shape[1]
    rows = seq // 2
    part = jax.ShapeDtypeStruct((2, seq, head), F32)
    return per_sequence(
        functools.partial(attn_bwd_kernel, width // head, head),
        pos,
        (qkv_seq, d_attn, other, cos_tab, sin_tab),
        [seq_spec(seq, width + 2 * head), own_spec(rows, width), pair_spec(rows, width), table_spec(cos_tab), table_spec(sin_tab)],
        [seq_spec(seq, width), seq_spec(seq, head), seq_spec(seq, head)],
        [jax.ShapeDtypeStruct((2, seq, width), BF16), part, part],
        [pltpu.VMEM((seq, width), BF16)],
        16e9,
    )


def attn_post(pos, d_queries, keep, got, cos_tab, sin_tab):
    seq, head = cos_tab.shape
    width = d_queries.shape[2]
    rows = seq // 2
    half = jax.ShapeDtypeStruct((seq, width + head), BF16)
    return per_sequence(
        functools.partial(attn_post_kernel, width // head, head),
        pos,
        (d_queries, keep, got, cos_tab, sin_tab),
        [seq_spec(seq, width), seq_spec(seq, head), seq_spec(seq, head), table_spec(cos_tab), table_spec(sin_tab)],
        [pair_spec(rows, width + head), pair_spec(rows, width + head)],
        [half, half],
        [pltpu.VMEM((seq, head), BF16)],
        2e9,
    )


def act_fwd_kernel(half, ab_ref, u_ref, ut_ref):
    gate_val = ab_ref[:, :half].astype(F32)
    up_val = ab_ref[:, half:].astype(F32)
    act_val = gate_val * jax.nn.sigmoid(gate_val) * up_val
    u_ref[...] = act_val.astype(BF16)
    ut_ref[...] = act_val.T.astype(BF16)


def act_fwd(gate_up):
    tokens, width = gate_up.shape
    half = width // 2
    rows = tokens // 4
    return pl.pallas_call(
        functools.partial(act_fwd_kernel, half),
        grid=(4,),
        in_specs=[pl.BlockSpec((rows, width), lambda i: (i, 0))],
        out_specs=[pl.BlockSpec((rows, half), lambda i: (i, 0)), pl.BlockSpec((half, rows), lambda i: (0, i))],
        out_shape=[jax.ShapeDtypeStruct((tokens, half), BF16), jax.ShapeDtypeStruct((half, tokens), BF16)],
        compiler_params=params(),
        cost_estimate=cost(4e9, 8e6),
        name="act_fwd",
    )(gate_up)


def act_bwd_kernel(half, ab_ref, du_ref, dab_ref, dabt_ref):
    gate_val = ab_ref[:, :half].astype(F32)
    up_val = ab_ref[:, half:].astype(F32)
    d_act = du_ref[...].astype(F32)
    sig = jax.nn.sigmoid(gate_val)
    d_silu = d_act * up_val
    d_gate = d_silu * sig + d_silu * gate_val * (sig * (1.0 - sig))
    d_up = d_act * (gate_val * sig)
    dab_ref[:, :half] = d_gate.astype(BF16)
    dab_ref[:, half:] = d_up.astype(BF16)
    dabt_ref[:half, :] = d_gate.T.astype(BF16)
    dabt_ref[half:, :] = d_up.T.astype(BF16)


def act_bwd(gate_up, d_mixed):
    tokens, width = gate_up.shape
    half = width // 2
    rows = tokens // 4
    return pl.pallas_call(
        functools.partial(act_bwd_kernel, half),
        grid=(4,),
        in_specs=[pl.BlockSpec((rows, width), lambda i: (i, 0)), pl.BlockSpec((rows, half), lambda i: (i, 0))],
        out_specs=[pl.BlockSpec((rows, width), lambda i: (i, 0)), pl.BlockSpec((width, rows), lambda i: (0, i))],
        out_shape=[jax.ShapeDtypeStruct((tokens, width), BF16), jax.ShapeDtypeStruct((width, tokens), BF16)],
        compiler_params=params(),
        cost_estimate=cost(8e9, 14e6),
        name="act_bwd",
    )(gate_up, d_mixed)


def piece_block(pos_ref, step, other):
    core = pos_ref[1]
    return lax.rem(pos_ref[0] + step, NZ) * NC + (1 - core if other else core)


def half_start(pos_ref, part, half):
    return pl.multiple_of((1 - pos_ref[2] if part else pos_ref[2]) * half, half)


def nn_kernel(keys, first, count_out, which, pos_ref, acts_ref, *refs):
    count = len(keys)
    halves = refs[: 2 * count]
    outs = refs[2 * count : 2 * count + count_out]
    acts_buf, w_buf, total, acts_sem, w_sem = refs[2 * count + count_out :]
    block = acts_buf.shape[1] // count
    half = block // 2
    copies = []
    for idx in range(count):
        cols = pl.ds(pl.multiple_of(piece_block(pos_ref, *keys[idx]) * block, block), block)
        copies.append([pltpu.make_async_copy(acts_ref.at[which, :, cols], acts_buf.at[:, pl.ds(idx * block, block)], acts_sem.at[idx])])
        for part in range(2):
            rows = pl.ds(idx * block + half_start(pos_ref, part, half), half)
            copies[-1].append(pltpu.make_async_copy(halves[2 * idx + part], w_buf.at[rows], w_sem.at[2 * idx + part]))
    for group in copies:
        for copy in group:
            copy.start()
    for lo, hi in ((0, first), (first, count)):
        for group in copies[lo:hi]:
            for copy in group:
                copy.wait()
        depth = pl.ds(lo * block, (hi - lo) * block)
        start = 0
        for out_ref in outs:
            width = out_ref.shape[1]

            def step(out_lo, size, start=start, out_ref=out_ref, depth=depth, hi=hi):
                cols = pl.ds(pl.multiple_of(start + out_lo, 128), size)
                part = dot_nn(acts_buf[:, depth], w_buf[depth, cols])
                if hi == count:
                    out_ref[:, pl.ds(pl.multiple_of(out_lo, 128), size)] = (total[:, cols] + part).astype(BF16)
                else:
                    total[:, cols] = part

            whole = width // TILE
            if whole:
                pl.loop(0, whole)(lambda n: step(n * TILE, TILE))
            if width % TILE:
                step(whole * TILE, width % TILE)
            start += width


def nn_pieces(pos, acts, which, parts, widths):
    keys = [(step, other) for step in (0, 1, 3, 2) for other in range(2)]
    halves = [parts[step][other][part] for step, other in keys for part in range(2)]
    _, tokens, depth = acts.shape
    width = sum(widths)
    count = len(keys)
    anywhere = pl.BlockSpec(memory_space=pl.ANY)
    return pl.pallas_call(
        functools.partial(nn_kernel, keys, 2, len(widths), which),
        grid_spec=pltpu.PrefetchScalarGridSpec(
            num_scalar_prefetch=1,
            grid=(1,),
            in_specs=[anywhere] * (1 + 2 * count),
            out_specs=[pl.BlockSpec((tokens, size), lambda i, pos: (0, 0)) for size in widths],
            scratch_shapes=[
                pltpu.VMEM((tokens, depth), BF16),
                pltpu.VMEM((depth, width), BF16),
                pltpu.VMEM((tokens, width), F32),
                pltpu.SemaphoreType.DMA((count,)),
                pltpu.SemaphoreType.DMA((2 * count,)),
            ],
        ),
        out_shape=[jax.ShapeDtypeStruct((tokens, size), BF16) for size in widths],
        compiler_params=params(),
        cost_estimate=cost(2 * tokens * depth * width, 2 * depth * (tokens + width)),
    )(pos, acts, *halves)


def nt_kernel(keys, sides, pos_ref, *refs):
    count_left = len(sides)
    count = len(keys)
    lefts = refs[:count_left]
    halves = refs[count_left : count_left + 2 * count]
    out_ref, left_buf, w_buf, out_buf, left_sem, w_sem, out_sem = refs[count_left + 2 * count :]
    block = out_buf.shape[2]
    half = block // 2
    slots = w_buf.shape[0]
    left_copies = []
    start = 0
    for idx, (left, side) in enumerate(zip(lefts, sides)):
        rows, width = left.shape
        first = 0 if side is None else pl.multiple_of((1 - pos_ref[1] if side else pos_ref[1]) * rows, rows)
        left_copies.append(pltpu.make_async_copy(left, left_buf.at[pl.ds(first, rows), pl.ds(start, width)], left_sem.at[idx]))
        left_copies[-1].start()
        start += 0 if side == 0 else width

    def copies(idx):
        for part in range(2):
            rows = pl.ds(half_start(pos_ref, part, half), half)
            yield pltpu.make_async_copy(halves[2 * idx + part], w_buf.at[idx % slots, rows], w_sem.at[idx % slots, part])

    def out_copy(idx):
        cols = pl.ds(pl.multiple_of(piece_block(pos_ref, *keys[idx]) * block, block), block)
        return pltpu.make_async_copy(out_buf.at[idx % 2], out_ref.at[:, cols], out_sem.at[idx % 2])

    for idx in range(slots - 1):
        for copy in copies(idx):
            copy.start()
    for idx in range(count):
        if idx + slots - 1 < count:
            for copy in copies(idx + slots - 1):
                copy.start()
        for copy in copies(idx):
            copy.wait()
        if idx == 0:
            for copy in left_copies:
                copy.wait()
        if idx >= 2:
            out_copy(idx - 2).wait()
        out_buf[idx % 2] = dot_nt(left_buf[...], w_buf[idx % slots])
        out_copy(idx).start()
    for idx in range(count - 2, count):
        out_copy(idx).wait()


def nt_pieces(pos, lefts, parts):
    sides = (None, 0, 1)
    keys = [(step, other) for step in range(NZ) for other in range(2)]
    halves = [parts[step][other][part] for step, other in keys for part in range(2)]
    tokens = lefts[0].shape[0]
    block = 2 * halves[0].shape[0]
    depth = block * len(keys)
    width = halves[0].shape[1]
    slots = 3
    anywhere = pl.BlockSpec(memory_space=pl.ANY)
    return pl.pallas_call(
        functools.partial(nt_kernel, keys, sides),
        grid_spec=pltpu.PrefetchScalarGridSpec(
            num_scalar_prefetch=1,
            grid=(1,),
            in_specs=[anywhere] * (len(lefts) + len(halves)),
            out_specs=anywhere,
            scratch_shapes=[
                pltpu.VMEM((tokens, width), BF16),
                pltpu.VMEM((slots, block, width), BF16),
                pltpu.VMEM((2, tokens, block), F32),
                pltpu.SemaphoreType.DMA((len(lefts),)),
                pltpu.SemaphoreType.DMA((slots, 2)),
                pltpu.SemaphoreType.DMA((2,)),
            ],
        ),
        out_shape=jax.ShapeDtypeStruct((tokens, depth), F32),
        compiler_params=params(),
        cost_estimate=cost(2 * tokens * depth * width, 2 * depth * width + 4 * tokens * depth),
    )(pos, *lefts, *halves)


def picked_cols(pos_ref, idx, block):
    return pl.ds(pl.multiple_of((NC * idx + 1 - pos_ref[1]) * block, block), block)


def dma_kernel(kernel, pos, args, out_shape, scratch):
    anywhere = pl.BlockSpec(memory_space=pl.ANY)
    return pl.pallas_call(
        kernel,
        grid_spec=pltpu.PrefetchScalarGridSpec(
            num_scalar_prefetch=1, grid=(1,), in_specs=[anywhere] * len(args), out_specs=[anywhere] * len(out_shape), scratch_shapes=scratch
        ),
        out_shape=out_shape,
        compiler_params=params(),
        cost_estimate=cost(3e9, 16e6),
    )(pos, *args)


def pick_cols(pos, acts):
    count, tokens, depth = acts.shape
    block = depth // (NC * NZ)
    places = [(which, idx) for which in range(count) for idx in range(NZ)]

    def kernel(pos_ref, in_ref, out_ref, buf, in_sem, out_sem):
        copies = []
        for slot, (which, idx) in enumerate(places):
            read = pltpu.make_async_copy(in_ref.at[which, :, picked_cols(pos_ref, idx, block)], buf.at[slot], in_sem.at[slot])
            write = pltpu.make_async_copy(buf.at[slot], out_ref.at[which, :, pl.ds(idx * block, block)], out_sem.at[slot])
            copies.append((read, write))
            read.start()
        for read, write in copies:
            read.wait()
            write.start()
        for _, write in copies:
            write.wait()

    sems = pltpu.SemaphoreType.DMA((len(places),))
    out = jax.ShapeDtypeStruct((count, tokens, depth // 2), BF16)
    return dma_kernel(kernel, pos, [acts], [out], [pltpu.VMEM((len(places), tokens, block), BF16), sems, sems])[0]


def grad_kernel(heights, pos_ref, *refs):
    pairs = len(heights)
    ins = refs[: 6 * pairs]
    outs = refs[6 * pairs : 6 * pairs + 2 * NZ]
    buf, sem = refs[6 * pairs + 2 * NZ :]
    step = pl.program_id(0)
    slot = lax.rem(step, 2)

    def out_copy(idx, part):
        return pltpu.make_async_copy(buf.at[idx % 2, part], outs[2 * idx + part], sem.at[idx % 2, part])

    for idx in range(2, NZ):

        @pl.when(step == idx)
        def _(idx=idx):
            for part in range(2):
                out_copy(idx - 2, part).wait()

    start = 0
    for idx, height in enumerate(heights):
        own, recv, acts0, acts1, recv0, recv1 = ins[6 * idx : 6 * idx + 6]
        for part, acts, acts_recv in ((0, acts0, recv0), (1, acts1, recv1)):
            buf[slot, part, start : start + height, :] = dot_nn(own[...], acts[...]) + dot_nn(recv[...], acts_recv[...])
        start += height
    for idx in range(NZ):

        @pl.when(step == idx)
        def _(idx=idx):
            for part in range(2):
                out_copy(idx, part).start()

    @pl.when(step == NZ - 1)
    def _():
        for idx in (NZ - 2, NZ - 1):
            for part in range(2):
                out_copy(idx, part).wait()


def grad_pieces(pos, pairs):
    _, tokens, depth = pairs[0][2].shape
    cols = depth // (NZ * NY)
    in_specs = []
    args = []

    def z_of(n, pos):
        return lax.rem(pos[0] + jnp.where(n == 0, 2, jnp.where(n == 1, 1, jnp.where(n == 2, 3, 0))), NZ)

    def bit(pos, part):
        return 1 - pos[2] if part else pos[2]

    for own, recv, acts, acts_recv, height, block, which in pairs:
        in_specs += [pl.BlockSpec((height, tokens), lambda n, pos, block=block: (block, 0))] * 2
        for part in range(2):
            in_specs.append(pl.BlockSpec((None, tokens, cols), lambda n, pos, part=part, which=which: (which, 0, z_of(n, pos) * NY + 2 * pos[1] + bit(pos, part))))
        for part in range(2):
            in_specs.append(pl.BlockSpec((None, tokens, cols), lambda n, pos, part=part, which=which: (which, 0, z_of(n, pos) * 2 + bit(pos, part))))
        args += [own, recv, acts, acts, acts_recv, acts_recv]
    heights = [pair[4] for pair in pairs]
    rows = sum(heights)
    return pl.pallas_call(
        functools.partial(grad_kernel, heights),
        grid_spec=pltpu.PrefetchScalarGridSpec(
            num_scalar_prefetch=1,
            grid=(NZ,),
            in_specs=in_specs,
            out_specs=[pl.BlockSpec(memory_space=pl.ANY)] * (2 * NZ),
            scratch_shapes=[pltpu.VMEM((2, 2, rows, cols), F32), pltpu.SemaphoreType.DMA((2, 2))],
        ),
        out_shape=[jax.ShapeDtypeStruct((rows, cols), F32)] * (2 * NZ),
        compiler_params=params(),
        cost_estimate=cost(4 * rows * tokens * cols * 2 * NZ, 4 * tokens * cols * 2 * NZ),
        name="grad",
    )(pos, *args)


def place(pos, first, second, height, block, transpose):
    cols = first.shape[1]
    spec = pl.BlockSpec((height, cols), lambda n, pos: (block, 0))

    def kernel(pos_ref, first_ref, second_ref, out_ref):
        for idx, ref in enumerate((first_ref, second_ref)):

            @pl.when(pl.program_id(0) == idx)
            def _(ref=ref):
                out_ref[...] = ref[...].T if transpose else ref[...]

    def order(n, pos):
        return jnp.where(n == 0, pos[2], 1 - pos[2])

    return pl.pallas_call(
        kernel,
        grid_spec=pltpu.PrefetchScalarGridSpec(
            num_scalar_prefetch=1,
            grid=(2,),
            in_specs=[spec, spec],
            out_specs=pl.BlockSpec((cols, height), lambda n, pos: (0, order(n, pos))) if transpose else pl.BlockSpec((height, cols), lambda n, pos: (order(n, pos), 0)),
        ),
        out_shape=jax.ShapeDtypeStruct((cols, 2 * height) if transpose else (2 * height, cols), F32),
        compiler_params=params(),
        cost_estimate=cost(2e9, 16 * height * cols),
    )(pos, first, second)


def after(val, *earlier):
    return lax.optimization_barrier((val, *earlier))[0]


def ring(step, size):
    return [(src, (src + step) % size) for src in range(size)]


def hop_z(val, step):
    return lax.ppermute(val, "z", ring(step, NZ))


def swap_c(val):
    return lax.ppermute(val, "c", [(0, 1), (1, 0)])


def swap_y(val):
    return lax.ppermute(val, "y", [(src, src ^ 1) for src in range(NY)])


def turn(val, flip):
    def place_of(y_pos, c_pos):
        return y_pos * NC + c_pos

    pairs = [(place_of(2 * a + b, c), place_of(2 * c + (b ^ flip), a)) for a in range(2) for b in range(2) for c in range(NC)]
    return lax.ppermute(val, ("y", "c"), pairs)


def swap_yc(val):
    pairs = [(y_pos * NC + c_pos, (y_pos ^ 1) * NC + 1 - c_pos) for y_pos in range(NY) for c_pos in range(NC)]
    return lax.ppermute(val, ("y", "c"), pairs)


def dot_nn(left, right):
    return lax.dot_general(left, right, (((1,), (0,)), ((), ())), preferred_element_type=F32)


def dot_nt(left, right):
    return lax.dot_general(left, right, (((1,), (1,)), ((), ())), preferred_element_type=F32)


def dot_tn(left, right):
    return lax.dot_general(left, right, (((0,), (0,)), ((), ())), preferred_element_type=F32)


def solution(mesh):
    wide_mesh = Mesh(mesh.devices.reshape(NZ, NY, NX, NC), ("z", "y", "x", "c"))
    rows = ("z", "y")
    cols = ("x", "c")
    act_spec = P(rows, cols, None)
    col_spec = P(rows, cols)
    row_spec = P(cols, rows)

    def layer(x_in, dy_in, norm_gain, w_qkv, w_out, w_gate, w_up, w_down, rope_cos, rope_sin):
        z_pos = lax.axis_index("z")
        y_pos = lax.axis_index("y")
        c_pos = lax.axis_index("c")
        even_y = y_pos % 2 == 0
        first_c = c_pos == 0
        pos = jnp.stack([z_pos, c_pos, y_pos % 2]).astype(jnp.int32)
        head = 2 * rope_cos.shape[1]
        seq = rope_cos.shape[0]
        ff_blk = w_gate.shape[1] // 2
        o_blk = w_out.shape[0] // 2
        qkv_blk = o_blk + head

        def gather_rows(blocks):
            return [turn(jnp.where(even_y, blocks[flip], blocks[1 - flip]), flip) for flip in range(2)]

        def gather_weight(piece):
            left = [hop_z(half, 1) for half in piece]
            right = [hop_z(half, -1) for half in piece]
            far = [hop_z(left[0], 1), hop_z(right[1], -1)]
            parts = []
            for mine in (piece, right, far, left):
                parts.append((mine, [swap_c(half) for half in mine]))
            return parts

        def grad_start(pairs, *earlier):
            far0, far1, up0, up1, down0, down1, own0, own1 = grad_pieces(after(pos, *earlier), pairs)
            far = (hop_z(far0, 1), hop_z(far1, -1))
            direct = (hop_z(up1, 1), hop_z(down0, -1))
            return (up0, down1), far, direct, (own0, own1)

        def grad_pass(state, *earlier):
            (up0, down1), far, direct, own = state
            sums = (up0 + after(far[0], *earlier), down1 + far[1])
            passed = (hop_z(sums[0], 1), hop_z(sums[1], -1))
            return direct, passed, own, sums

        def grad_back(state, *earlier):
            direct, passed, own = state[:3]
            first = own[0] + after(passed[0], *earlier) + direct[1]
            second = own[1] + direct[0] + passed[1]
            return turn(first, 0), turn(second, 1)

        def my_rows(val, mine):
            return lax.dynamic_slice_in_dim(val, (c_pos if mine else 1 - c_pos) * seq, seq, axis=0)

        def both_rows(own, got):
            return jnp.concatenate([jnp.where(first_c, own, got), jnp.where(first_c, got, own)], axis=0)

        cos_tab = jnp.concatenate([rope_cos, rope_cos], axis=1)
        sin_tab = jnp.concatenate([-rope_sin, rope_sin], axis=1)

        def qkv_cols(bit):
            first = 2 * head * bit
            third = HEAD_GROUP * head + head * bit
            return [w_qkv[:, first : first + 2 * head], w_qkv[:, third : third + head]]

        def block(weight, bit):
            size = weight.shape[1] // 2
            return weight[:, bit * size : (bit + 1) * size]

        down_t = w_down.T
        out_t = w_out.T
        wf_piece = gather_rows([jnp.concatenate([block(w_gate, j), block(w_up, j), *qkv_cols(j)], axis=1) for j in range(2)])
        ws_piece = gather_rows([jnp.concatenate([block(down_t, j), block(out_t, j)], axis=1) for j in range(2)])

        x_rows = x_in[0].astype(F32)
        normed, norm_pull = jax.vjp(lambda row_vals: norm_fwd(row_vals, norm_gain), x_rows)
        both = jnp.stack([normed.astype(BF16), dy_in[0]])
        both_all = lax.all_gather(after(both, *wf_piece), ("y", "x"), axis=1, tiled=True)
        wf_parts = gather_weight(wf_piece)
        ws_parts = gather_weight(ws_piece)

        gate_up, qkv_tok = nn_pieces(pos, both_all, 0, wf_parts, (2 * ff_blk, qkv_blk))
        third = qkv_tok[:, o_blk:]
        qkv_other = swap_c(my_rows(qkv_tok, False))
        third_own = swap_y(my_rows(third, True))
        third_other = swap_yc(my_rows(third, False))
        act_val, act_t = act_fwd(after(gate_up, qkv_tok))
        act_recv = swap_c(act_t)
        qkv_seq, attn_own, attn_other = attn_fwd(after(pos, act_t), qkv_tok, qkv_other, third_own, third_other, cos_tab, sin_tab)
        attn_got = swap_c(attn_other)
        picked = pick_cols(after(pos, attn_own), both_all)
        both_recv = swap_c(picked)
        y_part = nt_pieces(after(pos, picked), [act_val, attn_own, attn_got], ws_parts)
        mix_sum = lax.psum_scatter(y_part, ("y", "x"), scatter_dimension=0, tiled=True)
        y_out = (x_rows + mix_sum).astype(BF16)[None]

        g_act = grad_start([(act_t, act_recv, both_all, both_recv, ff_blk, 0, 1)], y_part)
        d_act, d_attn = nn_pieces(after(pos, g_act[3][0]), both_all, 1, ws_parts, (ff_blk, o_blk))
        d_attn_other = swap_c(my_rows(d_attn, False))
        d_gate_up, d_gate_up_t = act_bwd(gate_up, d_act)
        d_gate_up_recv = swap_c(d_gate_up_t)
        d_queries, keep, send = attn_bwd(after(pos, d_gate_up_t), qkv_seq, d_attn, d_attn_other, cos_tab, sin_tab)
        got = swap_y(send)
        g_act = grad_pass(g_act, d_queries)
        g_gate = grad_start([(d_gate_up_t, d_gate_up_recv, both_all, both_recv, ff_blk, 0, 0)], *g_act[3])
        d_own, d_other = attn_post(after(pos, g_gate[3][0]), d_queries, keep, got, cos_tab, sin_tab)
        d_got = swap_c(d_other)
        dh_part = nt_pieces(pos, [d_gate_up, d_own, d_got], wf_parts)
        d_h = lax.psum_scatter(dh_part, ("y", "x"), scatter_dimension=0, tiled=True)
        d_h = d_h.astype(BF16)
        dx_out = (dy_in[0].astype(F32) + norm_pull(d_h.astype(F32))[0]).astype(BF16)[None]
        g_up = grad_start([(d_gate_up_t, d_gate_up_recv, both_all, both_recv, ff_blk, 1, 0)], dh_part)
        g_gate = grad_pass(g_gate, g_up[3][0])

        attn_t = both_rows(attn_own, attn_got).T
        d_qkv_t = both_rows(d_own, d_got).T
        attn_recv = swap_c(attn_t)
        d_qkv_recv = swap_c(d_qkv_t)
        g_attn = grad_start([(attn_t, attn_recv, both_all, both_recv, o_blk, 0, 1), (d_qkv_t, d_qkv_recv, both_all, both_recv, qkv_blk, 0, 0)], *g_gate[3])
        g_up = grad_pass(g_up, g_attn[3][0])
        b_act = grad_back(g_act, g_attn[3][0])
        g_attn = grad_pass(g_attn)
        b_gate = grad_back(g_gate)
        b_up = grad_back(g_up)
        b_attn = grad_back(g_attn)
        dw_down = place(pos, *b_act, ff_blk, 0, False)
        dw_gate = place(pos, *b_gate, ff_blk, 0, True)
        dw_up = place(pos, *b_up, ff_blk, 0, True)
        dw_out = place(pos, *b_attn, o_blk, 0, False)
        dw_q = place(pos, *b_attn, 2 * head, 1, True)
        dw_kv = place(pos, *b_attn, head, 2 * o_blk // head, True)
        dw_qkv = jnp.concatenate([dw_q, dw_kv], axis=1)
        return y_out, dx_out, dw_qkv, dw_out, dw_gate, dw_up, dw_down


    return jax.shard_map(
        layer,
        mesh=wide_mesh,
        in_specs=(act_spec, act_spec, P(), col_spec, row_spec, col_spec, col_spec, row_spec, P(), P()),
        out_specs=(act_spec, act_spec, col_spec, row_spec, col_spec, col_spec, row_spec),
        check_vma=False,
    )
```

```python
import functools

import jax
import jax.numpy as jnp
from jax import lax
from jax.experimental import pallas as pl
from jax.experimental.pallas import tpu as pltpu
from jax.sharding import Mesh, PartitionSpec as P


NORM_EPS = 1e-5
NZ = 4
NY = 4
NX = 4
NC = 2
HEAD_GROUP = 4
F32 = jnp.float32
BF16 = jnp.bfloat16
VMEM_LIMIT = 60 * 1024 * 1024
TILE = 512


def norm_fwd(row_vals, norm_gain):
    return row_vals * lax.rsqrt(jnp.mean(row_vals * row_vals, axis=-1, keepdims=True) + NORM_EPS) * norm_gain


def rotate(wide, cos_tab, sin_tab):
    return wide * cos_tab + pltpu.roll(wide, wide.shape[-1] // 2, wide.ndim - 1) * sin_tab


def rotate_back(wide, cos_tab, sin_tab):
    return wide * cos_tab - pltpu.roll(wide, wide.shape[-1] // 2, wide.ndim - 1) * sin_tab


def cost(flops, bytes_accessed):
    return pl.CostEstimate(flops=int(flops) // 20, bytes_accessed=int(bytes_accessed), transcendentals=0)


def params(**extra):
    return pltpu.CompilerParams(vmem_limit_bytes=VMEM_LIMIT, **extra)


def head_probs(q_rot, k_rot, scale):
    scores = dot_nt(q_rot, k_rot) * scale
    row_ids = lax.broadcasted_iota(jnp.int32, scores.shape, 0)
    col_ids = lax.broadcasted_iota(jnp.int32, scores.shape, 1)
    scores = jnp.where(row_ids >= col_ids, scores, -1e30)
    weights = jnp.exp(scores - jnp.max(scores, axis=-1, keepdims=True))
    return weights / jnp.sum(weights, axis=-1, keepdims=True)


def half_rows(core, idx, chunk):
    return pl.ds(pl.multiple_of((NC * idx + core) * chunk, chunk), chunk)


def chunk_rows(idx, chunk):
    return slice(idx * chunk, (idx + 1) * chunk)


def attn_fwd_kernel(heads, head, pos_ref, own_ref, other_ref, own_third_ref, other_third_ref, cos_ref, sin_ref, seq_ref, o_ref, o_other_ref, o_buf):
    core, odd = pos_ref[1], pos_ref[2]
    chunk = own_ref.shape[0] // NX
    width = heads * head
    mine = pl.ds(pl.multiple_of(width + odd * head, head), head)
    theirs = pl.ds(pl.multiple_of(width + (1 - odd) * head, head), head)
    for side, part_ref, third_ref in ((core, own_ref, own_third_ref), (1 - core, other_ref, other_third_ref)):
        for idx in range(NX):
            rows = half_rows(side, idx, chunk)
            seq_ref[0, rows, pl.ds(0, width)] = part_ref[chunk_rows(idx, chunk), :width]
            seq_ref[0, rows, mine] = part_ref[chunk_rows(idx, chunk), width:]
            seq_ref[0, rows, theirs] = third_ref[chunk_rows(idx, chunk), :]
    cos_tab, sin_tab = cos_ref[...], sin_ref[...]
    k_rot = rotate(seq_ref[0, :, width : width + head].astype(F32), cos_tab, sin_tab).astype(BF16)
    values = seq_ref[0, :, width + head :]
    for idx in range(heads):
        lanes = slice(idx * head, (idx + 1) * head)
        q_rot = rotate(seq_ref[0, :, lanes].astype(F32), cos_tab, sin_tab).astype(BF16)
        probs = head_probs(q_rot, k_rot, head**-0.5)
        o_buf[:, lanes] = dot_nn(probs.astype(BF16), values).astype(BF16)
    for side, out_ref in ((core, o_ref), (1 - core, o_other_ref)):
        for idx in range(NX):
            out_ref[chunk_rows(idx, chunk), :] = o_buf[half_rows(side, idx, chunk), :]


def attn_bwd_kernel(heads, head, pos_ref, seq_ref, own_ref, other_ref, cos_ref, sin_ref, dq_ref, keep_ref, send_ref, do_buf):
    core, odd = pos_ref[1], pos_ref[2]
    chunk = own_ref.shape[0] // NX
    width = heads * head
    for side, part_ref in ((core, own_ref), (1 - core, other_ref)):
        for idx in range(NX):
            do_buf[half_rows(side, idx, chunk), :] = part_ref[chunk_rows(idx, chunk), :]
    cos_tab, sin_tab = cos_ref[...], sin_ref[...]
    k_rot = rotate(seq_ref[0, :, width : width + head].astype(F32), cos_tab, sin_tab).astype(BF16)
    values = seq_ref[0, :, width + head :]
    d_keys = jnp.zeros(k_rot.shape, F32)
    d_values = jnp.zeros(k_rot.shape, F32)
    for idx in range(heads):
        lanes = slice(idx * head, (idx + 1) * head)
        q_rot = rotate(seq_ref[0, :, lanes].astype(F32), cos_tab, sin_tab).astype(BF16)
        d_out = do_buf[:, lanes]
        probs = head_probs(q_rot, k_rot, head**-0.5)
        d_values += dot_tn(probs.astype(BF16), d_out)
        d_probs = dot_nt(d_out, values).astype(BF16).astype(F32)
        d_scores = probs * (d_probs - jnp.sum(d_probs * probs, axis=-1, keepdims=True))
        d_scores = (d_scores * head**-0.5).astype(BF16)
        d_q_rot = dot_nn(d_scores, k_rot).astype(BF16)
        dq_ref[0, :, lanes] = rotate_back(d_q_rot.astype(F32), cos_tab, sin_tab).astype(BF16)
        d_keys += dot_tn(d_scores, q_rot)

    @pl.when(odd == 0)
    def _():
        keep_ref[0] = d_keys
        send_ref[0] = d_values

    @pl.when(odd == 1)
    def _():
        keep_ref[0] = d_values
        send_ref[0] = d_keys


def attn_post_kernel(heads, head, pos_ref, dq_ref, keep_ref, got_ref, cos_ref, sin_ref, own_ref, other_ref, third_buf):
    core, odd = pos_ref[1], pos_ref[2]
    chunk = own_ref.shape[0] // NX
    width = heads * head
    total = (keep_ref[0] + got_ref[0]).astype(BF16)

    @pl.when(odd == 0)
    def _():
        third_buf[...] = rotate_back(total.astype(F32), cos_ref[...], sin_ref[...]).astype(BF16)

    @pl.when(odd == 1)
    def _():
        third_buf[...] = total

    for side, out_ref in ((core, own_ref), (1 - core, other_ref)):
        for idx in range(NX):
            rows = half_rows(side, idx, chunk)
            out_ref[chunk_rows(idx, chunk), :width] = dq_ref[0, rows, :]
            out_ref[chunk_rows(idx, chunk), width:] = third_buf[rows, :]


def per_sequence(kernel, pos, args, specs, out_specs, out_shape, scratch, flops):
    return pl.pallas_call(
        kernel,
        grid_spec=pltpu.PrefetchScalarGridSpec(num_scalar_prefetch=1, grid=(2,), in_specs=specs, out_specs=out_specs, scratch_shapes=scratch),
        out_shape=out_shape,
        compiler_params=params(),
        cost_estimate=cost(flops, 4e6),
    )(pos, *args)


def own_spec(rows, width):
    return pl.BlockSpec((rows, width), lambda i, pos: (2 * pos[1] + i, 0))


def pair_spec(rows, width):
    return pl.BlockSpec((rows, width), lambda i, pos: (i, 0))


def seq_spec(seq, width):
    return pl.BlockSpec((1, seq, width), lambda i, pos: (i, 0, 0))


def table_spec(table):
    return pl.BlockSpec(table.shape, lambda i, pos: (0, 0))


def attn_fwd(pos, qkv_tok, other, own_third, other_third, cos_tab, sin_tab):
    seq, head = cos_tab.shape
    width = qkv_tok.shape[1] - head
    rows = seq // 2
    half = jax.ShapeDtypeStruct((seq, width), BF16)
    return per_sequence(
        functools.partial(attn_fwd_kernel, width // head, head),
        pos,
        (qkv_tok, other, own_third, other_third, cos_tab, sin_tab),
        [own_spec(rows, width + head), pair_spec(rows, width + head), pair_spec(rows, head), pair_spec(rows, head), table_spec(cos_tab), table_spec(sin_tab)],
        [seq_spec(seq, width + 2 * head), pair_spec(rows, width), pair_spec(rows, width)],
        [jax.ShapeDtypeStruct((2, seq, width + 2 * head), BF16), half, half],
        [pltpu.VMEM((seq, width), BF16)],
        16e9,
    )


def attn_bwd(pos, qkv_seq, d_attn, other, cos_tab, sin_tab):
    seq, head = cos_tab.shape
    width = d_attn.shape[1]
    rows = seq // 2
    part = jax.ShapeDtypeStruct((2, seq, head), F32)
    return per_sequence(
        functools.partial(attn_bwd_kernel, width // head, head),
        pos,
        (qkv_seq, d_attn, other, cos_tab, sin_tab),
        [seq_spec(seq, width + 2 * head), own_spec(rows, width), pair_spec(rows, width), table_spec(cos_tab), table_spec(sin_tab)],
        [seq_spec(seq, width), seq_spec(seq, head), seq_spec(seq, head)],
        [jax.ShapeDtypeStruct((2, seq, width), BF16), part, part],
        [pltpu.VMEM((seq, width), BF16)],
        16e9,
    )


def attn_post(pos, d_queries, keep, got, cos_tab, sin_tab):
    seq, head = cos_tab.shape
    width = d_queries.shape[2]
    rows = seq // 2
    half = jax.ShapeDtypeStruct((seq, width + head), BF16)
    return per_sequence(
        functools.partial(attn_post_kernel, width // head, head),
        pos,
        (d_queries, keep, got, cos_tab, sin_tab),
        [seq_spec(seq, width), seq_spec(seq, head), seq_spec(seq, head), table_spec(cos_tab), table_spec(sin_tab)],
        [pair_spec(rows, width + head), pair_spec(rows, width + head)],
        [half, half],
        [pltpu.VMEM((seq, head), BF16)],
        2e9,
    )


def act_fwd_kernel(half, ab_ref, u_ref, ut_ref):
    gate_val = ab_ref[:, :half].astype(F32)
    up_val = ab_ref[:, half:].astype(F32)
    act_val = gate_val * jax.nn.sigmoid(gate_val) * up_val
    u_ref[...] = act_val.astype(BF16)
    ut_ref[...] = act_val.T.astype(BF16)


def act_fwd(gate_up):
    tokens, width = gate_up.shape
    half = width // 2
    rows = tokens // 4
    return pl.pallas_call(
        functools.partial(act_fwd_kernel, half),
        grid=(4,),
        in_specs=[pl.BlockSpec((rows, width), lambda i: (i, 0))],
        out_specs=[pl.BlockSpec((rows, half), lambda i: (i, 0)), pl.BlockSpec((half, rows), lambda i: (0, i))],
        out_shape=[jax.ShapeDtypeStruct((tokens, half), BF16), jax.ShapeDtypeStruct((half, tokens), BF16)],
        compiler_params=params(),
        cost_estimate=cost(4e9, 8e6),
        name="act_fwd",
    )(gate_up)


def act_bwd_kernel(half, ab_ref, du_ref, dab_ref, dabt_ref):
    gate_val = ab_ref[:, :half].astype(F32)
    up_val = ab_ref[:, half:].astype(F32)
    d_act = du_ref[...].astype(F32)
    sig = jax.nn.sigmoid(gate_val)
    d_silu = d_act * up_val
    d_gate = d_silu * sig + d_silu * gate_val * (sig * (1.0 - sig))
    d_up = d_act * (gate_val * sig)
    dab_ref[:, :half] = d_gate.astype(BF16)
    dab_ref[:, half:] = d_up.astype(BF16)
    dabt_ref[:half, :] = d_gate.T.astype(BF16)
    dabt_ref[half:, :] = d_up.T.astype(BF16)


def act_bwd(gate_up, d_mixed):
    tokens, width = gate_up.shape
    half = width // 2
    rows = tokens // 4
    return pl.pallas_call(
        functools.partial(act_bwd_kernel, half),
        grid=(4,),
        in_specs=[pl.BlockSpec((rows, width), lambda i: (i, 0)), pl.BlockSpec((rows, half), lambda i: (i, 0))],
        out_specs=[pl.BlockSpec((rows, width), lambda i: (i, 0)), pl.BlockSpec((width, rows), lambda i: (0, i))],
        out_shape=[jax.ShapeDtypeStruct((tokens, width), BF16), jax.ShapeDtypeStruct((width, tokens), BF16)],
        compiler_params=params(),
        cost_estimate=cost(8e9, 14e6),
        name="act_bwd",
    )(gate_up, d_mixed)


def piece_block(pos_ref, step, other):
    core = pos_ref[1]
    return lax.rem(pos_ref[0] + step, NZ) * NC + (1 - core if other else core)


def half_start(pos_ref, part, half):
    return pl.multiple_of((1 - pos_ref[2] if part else pos_ref[2]) * half, half)


def nn_kernel(keys, first, count_out, pos_ref, acts_ref, *refs):
    count = len(keys)
    halves = refs[: 2 * count]
    outs = refs[2 * count : 2 * count + count_out]
    acts_buf, w_buf, total, acts_sem, w_sem = refs[2 * count + count_out :]
    block = acts_buf.shape[1] // count
    half = block // 2
    copies = []
    for idx in range(count):
        cols = pl.ds(pl.multiple_of(piece_block(pos_ref, *keys[idx]) * block, block), block)
        copies.append([pltpu.make_async_copy(acts_ref.at[:, cols], acts_buf.at[:, pl.ds(idx * block, block)], acts_sem.at[idx])])
        for part in range(2):
            rows = pl.ds(idx * block + half_start(pos_ref, part, half), half)
            copies[-1].append(pltpu.make_async_copy(halves[2 * idx + part], w_buf.at[rows], w_sem.at[2 * idx + part]))
    for group in copies:
        for copy in group:
            copy.start()
    for lo, hi in ((0, first), (first, count)):
        for group in copies[lo:hi]:
            for copy in group:
                copy.wait()
        depth = pl.ds(lo * block, (hi - lo) * block)
        start = 0
        for out_ref in outs:
            width = out_ref.shape[1]

            def step(out_lo, size, start=start, out_ref=out_ref, depth=depth, hi=hi):
                cols = pl.ds(pl.multiple_of(start + out_lo, 128), size)
                part = dot_nn(acts_buf[:, depth], w_buf[depth, cols])
                if hi == count:
                    out_ref[:, pl.ds(pl.multiple_of(out_lo, 128), size)] = (total[:, cols] + part).astype(BF16)
                else:
                    total[:, cols] = part

            whole = width // TILE
            if whole:
                pl.loop(0, whole)(lambda n: step(n * TILE, TILE))
            if width % TILE:
                step(whole * TILE, width % TILE)
            start += width


def nn_pieces(pos, acts, parts, widths):
    keys = [(step, other) for step in (0, 1, 3, 2) for other in range(2)]
    halves = [parts[step][other][part] for step, other in keys for part in range(2)]
    tokens, depth = acts.shape
    width = sum(widths)
    count = len(keys)
    anywhere = pl.BlockSpec(memory_space=pl.ANY)
    return pl.pallas_call(
        functools.partial(nn_kernel, keys, 2, len(widths)),
        grid_spec=pltpu.PrefetchScalarGridSpec(
            num_scalar_prefetch=1,
            grid=(1,),
            in_specs=[anywhere] * (1 + 2 * count),
            out_specs=[pl.BlockSpec((tokens, size), lambda i, pos: (0, 0)) for size in widths],
            scratch_shapes=[
                pltpu.VMEM((tokens, depth), BF16),
                pltpu.VMEM((depth, width), BF16),
                pltpu.VMEM((tokens, width), F32),
                pltpu.SemaphoreType.DMA((count,)),
                pltpu.SemaphoreType.DMA((2 * count,)),
            ],
        ),
        out_shape=[jax.ShapeDtypeStruct((tokens, size), BF16) for size in widths],
        compiler_params=params(),
        cost_estimate=cost(2 * tokens * depth * width, 2 * depth * (tokens + width)),
    )(pos, acts, *halves)


def nt_kernel(keys, sides, pos_ref, *refs):
    count_left = len(sides)
    count = len(keys)
    lefts = refs[:count_left]
    halves = refs[count_left : count_left + 2 * count]
    out_ref, left_buf, w_buf, out_buf, left_sem, w_sem, out_sem = refs[count_left + 2 * count :]
    block = out_buf.shape[2]
    half = block // 2
    slots = w_buf.shape[0]
    left_copies = []
    start = 0
    for idx, (left, side) in enumerate(zip(lefts, sides)):
        rows, width = left.shape
        first = 0 if side is None else pl.multiple_of((1 - pos_ref[1] if side else pos_ref[1]) * rows, rows)
        left_copies.append(pltpu.make_async_copy(left, left_buf.at[pl.ds(first, rows), pl.ds(start, width)], left_sem.at[idx]))
        left_copies[-1].start()
        start += 0 if side == 0 else width

    def copies(idx):
        for part in range(2):
            rows = pl.ds(half_start(pos_ref, part, half), half)
            yield pltpu.make_async_copy(halves[2 * idx + part], w_buf.at[idx % slots, rows], w_sem.at[idx % slots, part])

    def out_copy(idx):
        cols = pl.ds(pl.multiple_of(piece_block(pos_ref, *keys[idx]) * block, block), block)
        return pltpu.make_async_copy(out_buf.at[idx % 2], out_ref.at[:, cols], out_sem.at[idx % 2])

    for idx in range(slots - 1):
        for copy in copies(idx):
            copy.start()
    for idx in range(count):
        if idx + slots - 1 < count:
            for copy in copies(idx + slots - 1):
                copy.start()
        for copy in copies(idx):
            copy.wait()
        if idx == 0:
            for copy in left_copies:
                copy.wait()
        if idx >= 2:
            out_copy(idx - 2).wait()
        out_buf[idx % 2] = dot_nt(left_buf[...], w_buf[idx % slots])
        out_copy(idx).start()
    for idx in range(count - 2, count):
        out_copy(idx).wait()


def nt_pieces(pos, lefts, parts):
    sides = (None, 0, 1)
    keys = [(step, other) for step in range(NZ) for other in range(2)]
    halves = [parts[step][other][part] for step, other in keys for part in range(2)]
    tokens = lefts[0].shape[0]
    block = 2 * halves[0].shape[0]
    depth = block * len(keys)
    width = halves[0].shape[1]
    slots = 3
    anywhere = pl.BlockSpec(memory_space=pl.ANY)
    return pl.pallas_call(
        functools.partial(nt_kernel, keys, sides),
        grid_spec=pltpu.PrefetchScalarGridSpec(
            num_scalar_prefetch=1,
            grid=(1,),
            in_specs=[anywhere] * (len(lefts) + len(halves)),
            out_specs=anywhere,
            scratch_shapes=[
                pltpu.VMEM((tokens, width), BF16),
                pltpu.VMEM((slots, block, width), BF16),
                pltpu.VMEM((2, tokens, block), F32),
                pltpu.SemaphoreType.DMA((len(lefts),)),
                pltpu.SemaphoreType.DMA((slots, 2)),
                pltpu.SemaphoreType.DMA((2,)),
            ],
        ),
        out_shape=jax.ShapeDtypeStruct((tokens, depth), F32),
        compiler_params=params(),
        cost_estimate=cost(2 * tokens * depth * width, 2 * depth * width + 4 * tokens * depth),
    )(pos, *lefts, *halves)


def picked_cols(pos_ref, idx, block):
    return pl.ds(pl.multiple_of((NC * idx + 1 - pos_ref[1]) * block, block), block)


def dma_kernel(kernel, pos, args, out_shape, scratch):
    anywhere = pl.BlockSpec(memory_space=pl.ANY)
    return pl.pallas_call(
        kernel,
        grid_spec=pltpu.PrefetchScalarGridSpec(
            num_scalar_prefetch=1, grid=(1,), in_specs=[anywhere] * len(args), out_specs=[anywhere] * len(out_shape), scratch_shapes=scratch
        ),
        out_shape=out_shape,
        compiler_params=params(),
        cost_estimate=cost(3e9, 16e6),
    )(pos, *args)


def pick_cols(pos, acts):
    tokens, depth = acts.shape
    block = depth // (NC * NZ)

    def kernel(pos_ref, in_ref, out_ref, buf, in_sem, out_sem):
        reads = [pltpu.make_async_copy(in_ref.at[:, picked_cols(pos_ref, idx, block)], buf.at[idx], in_sem.at[idx]) for idx in range(NZ)]
        writes = [pltpu.make_async_copy(buf.at[idx], out_ref.at[:, pl.ds(idx * block, block)], out_sem.at[idx]) for idx in range(NZ)]
        for read in reads:
            read.start()
        for read, write in zip(reads, writes):
            read.wait()
            write.start()
        for write in writes:
            write.wait()

    sems = pltpu.SemaphoreType.DMA((NZ,))
    return dma_kernel(kernel, pos, [acts], [jax.ShapeDtypeStruct((tokens, depth // 2), BF16)], [pltpu.VMEM((NZ, tokens, block), BF16), sems, sems])[0]


def grad_kernel(heights, pos_ref, *refs):
    pairs = len(heights)
    ins = refs[: 6 * pairs]
    outs = refs[6 * pairs : 6 * pairs + 2 * NZ]
    buf, sem = refs[6 * pairs + 2 * NZ :]
    step = pl.program_id(0)
    slot = lax.rem(step, 2)

    def out_copy(idx, part):
        return pltpu.make_async_copy(buf.at[idx % 2, part], outs[2 * idx + part], sem.at[idx % 2, part])

    for idx in range(2, NZ):

        @pl.when(step == idx)
        def _(idx=idx):
            for part in range(2):
                out_copy(idx - 2, part).wait()

    start = 0
    for idx, height in enumerate(heights):
        own, recv, acts0, acts1, recv0, recv1 = ins[6 * idx : 6 * idx + 6]
        for part, acts, acts_recv in ((0, acts0, recv0), (1, acts1, recv1)):
            buf[slot, part, start : start + height, :] = dot_nn(own[...], acts[...]) + dot_nn(recv[...], acts_recv[...])
        start += height
    for idx in range(NZ):

        @pl.when(step == idx)
        def _(idx=idx):
            for part in range(2):
                out_copy(idx, part).start()

    @pl.when(step == NZ - 1)
    def _():
        for idx in (NZ - 2, NZ - 1):
            for part in range(2):
                out_copy(idx, part).wait()


def grad_pieces(pos, pairs):
    tokens, depth = pairs[0][2].shape
    cols = depth // (NZ * NY)
    in_specs = []
    args = []

    def z_of(n, pos):
        return lax.rem(pos[0] + jnp.where(n == 0, 2, jnp.where(n == 1, 1, jnp.where(n == 2, 3, 0))), NZ)

    def bit(pos, part):
        return 1 - pos[2] if part else pos[2]

    for own, recv, acts, acts_recv, height, block in pairs:
        in_specs += [pl.BlockSpec((height, tokens), lambda n, pos, block=block: (block, 0))] * 2
        in_specs += [pl.BlockSpec((tokens, cols), lambda n, pos, part=part: (0, z_of(n, pos) * NY + 2 * pos[1] + bit(pos, part))) for part in range(2)]
        in_specs += [pl.BlockSpec((tokens, cols), lambda n, pos, part=part: (0, z_of(n, pos) * 2 + bit(pos, part))) for part in range(2)]
        args += [own, recv, acts, acts, acts_recv, acts_recv]
    heights = [pair[4] for pair in pairs]
    rows = sum(heights)
    return pl.pallas_call(
        functools.partial(grad_kernel, heights),
        grid_spec=pltpu.PrefetchScalarGridSpec(
            num_scalar_prefetch=1,
            grid=(NZ,),
            in_specs=in_specs,
            out_specs=[pl.BlockSpec(memory_space=pl.ANY)] * (2 * NZ),
            scratch_shapes=[pltpu.VMEM((2, 2, rows, cols), F32), pltpu.SemaphoreType.DMA((2, 2))],
        ),
        out_shape=[jax.ShapeDtypeStruct((rows, cols), F32)] * (2 * NZ),
        compiler_params=params(),
        cost_estimate=cost(4 * rows * tokens * cols * 2 * NZ, 4 * tokens * cols * 2 * NZ),
        name="grad",
    )(pos, *args)


def place(pos, first, second, height, block, transpose):
    cols = first.shape[1]
    spec = pl.BlockSpec((height, cols), lambda n, pos: (block, 0))

    def kernel(pos_ref, first_ref, second_ref, out_ref):
        for idx, ref in enumerate((first_ref, second_ref)):

            @pl.when(pl.program_id(0) == idx)
            def _(ref=ref):
                out_ref[...] = ref[...].T if transpose else ref[...]

    def order(n, pos):
        return jnp.where(n == 0, pos[2], 1 - pos[2])

    return pl.pallas_call(
        kernel,
        grid_spec=pltpu.PrefetchScalarGridSpec(
            num_scalar_prefetch=1,
            grid=(2,),
            in_specs=[spec, spec],
            out_specs=pl.BlockSpec((cols, height), lambda n, pos: (0, order(n, pos))) if transpose else pl.BlockSpec((height, cols), lambda n, pos: (order(n, pos), 0)),
        ),
        out_shape=jax.ShapeDtypeStruct((cols, 2 * height) if transpose else (2 * height, cols), F32),
        compiler_params=params(),
        cost_estimate=cost(2e9, 16 * height * cols),
    )(pos, first, second)


def place_attn(pos, first, second, o_blk, head):
    rows, cols = first.shape
    qk = 2 * head

    def kernel(pos_ref, first_ref, second_ref, out_ref, qkv_ref):
        for idx, ref in enumerate((first_ref, second_ref)):
            bit = 1 - pos_ref[2] if idx else pos_ref[2]
            out_ref[pl.ds(pl.multiple_of(bit * o_blk, o_blk), o_blk), :] = ref[:o_blk, :]
            qkv_ref[:, pl.ds(pl.multiple_of(bit * qk, qk), qk)] = ref[o_blk : o_blk + qk, :].T
            qkv_ref[:, pl.ds(pl.multiple_of(2 * qk + bit * head, head), head)] = ref[o_blk + qk :, :].T

    def whole(*shape):
        return pl.BlockSpec(shape, lambda n, pos: (0, 0))

    shapes = ((2 * o_blk, cols), (cols, 2 * (qk + head)))
    return pl.pallas_call(
        kernel,
        grid_spec=pltpu.PrefetchScalarGridSpec(num_scalar_prefetch=1, grid=(1,), in_specs=[whole(rows, cols)] * 2, out_specs=[whole(*shape) for shape in shapes]),
        out_shape=[jax.ShapeDtypeStruct(shape, F32) for shape in shapes],
        compiler_params=params(),
        cost_estimate=cost(2e9, 16 * rows * cols),
        name="p_attn",
    )(pos, first, second)


def after(val, *earlier):
    return lax.optimization_barrier((val, *earlier))[0]


def ring(step, size):
    return [(src, (src + step) % size) for src in range(size)]


def hop_z(val, step):
    return lax.ppermute(val, "z", ring(step, NZ))


def swap_c(val):
    return lax.ppermute(val, "c", [(0, 1), (1, 0)])


def swap_y(val):
    return lax.ppermute(val, "y", [(src, src ^ 1) for src in range(NY)])


def turn(val, flip):
    def place_of(y_pos, c_pos):
        return y_pos * NC + c_pos

    pairs = [(place_of(2 * a + b, c), place_of(2 * c + (b ^ flip), a)) for a in range(2) for b in range(2) for c in range(NC)]
    return lax.ppermute(val, ("y", "c"), pairs)


def swap_yc(val):
    pairs = [(y_pos * NC + c_pos, (y_pos ^ 1) * NC + 1 - c_pos) for y_pos in range(NY) for c_pos in range(NC)]
    return lax.ppermute(val, ("y", "c"), pairs)


def dot_nn(left, right):
    return lax.dot_general(left, right, (((1,), (0,)), ((), ())), preferred_element_type=F32)


def dot_nt(left, right):
    return lax.dot_general(left, right, (((1,), (1,)), ((), ())), preferred_element_type=F32)


def dot_tn(left, right):
    return lax.dot_general(left, right, (((0,), (0,)), ((), ())), preferred_element_type=F32)


def solution(mesh):
    wide_mesh = Mesh(mesh.devices.reshape(NZ, NY, NX, NC), ("z", "y", "x", "c"))
    rows = ("z", "y")
    cols = ("x", "c")
    act_spec = P(rows, cols, None)
    col_spec = P(rows, cols)
    row_spec = P(cols, rows)

    def layer(x_in, dy_in, norm_gain, w_qkv, w_out, w_gate, w_up, w_down, rope_cos, rope_sin):
        z_pos = lax.axis_index("z")
        y_pos = lax.axis_index("y")
        c_pos = lax.axis_index("c")
        even_y = y_pos % 2 == 0
        first_c = c_pos == 0
        pos = jnp.stack([z_pos, c_pos, y_pos % 2]).astype(jnp.int32)
        head = 2 * rope_cos.shape[1]
        seq = rope_cos.shape[0]
        ff_blk = w_gate.shape[1] // 2
        o_blk = w_out.shape[0] // 2
        qkv_blk = o_blk + head

        def gather_rows(blocks):
            return [turn(jnp.where(even_y, blocks[flip], blocks[1 - flip]), flip) for flip in range(2)]

        def gather_weight(piece):
            left, right = [], []
            for part in (1, 0):
                left.insert(0, hop_z(piece[part], 1))
                right.insert(0, hop_z(piece[part], -1))
            far = [hop_z(left[0], 1), hop_z(right[1], -1)]
            parts = []
            for mine in (piece, right, far, left):
                parts.append((mine, [swap_c(half) for half in mine]))
            return parts

        def grad_start(pairs, *earlier):
            far0, far1, up0, up1, down0, down1, own0, own1 = grad_pieces(after(pos, *earlier), pairs)
            far = (hop_z(far0, 1), hop_z(far1, -1))
            direct = (hop_z(up1, 1), hop_z(down0, -1))
            return (up0, down1), far, direct, (own0, own1)

        def grad_pass(state, *earlier):
            (up0, down1), far, direct, own = state
            sums = (up0 + after(far[0], *earlier), down1 + far[1])
            passed = (hop_z(sums[0], 1), hop_z(sums[1], -1))
            return direct, passed, own, sums

        def grad_back(state, *earlier):
            direct, passed, own = state[:3]
            first = own[0] + after(passed[0], *earlier) + direct[1]
            second = own[1] + direct[0] + passed[1]
            return turn(first, 0), turn(second, 1)

        def my_rows(val, mine):
            return lax.dynamic_slice_in_dim(val, (c_pos if mine else 1 - c_pos) * seq, seq, axis=0)

        def both_rows(own, got):
            return jnp.concatenate([jnp.where(first_c, own, got), jnp.where(first_c, got, own)], axis=0)

        cos_tab = jnp.concatenate([rope_cos, rope_cos], axis=1)
        sin_tab = jnp.concatenate([-rope_sin, rope_sin], axis=1)

        def qkv_cols(bit):
            first = 2 * head * bit
            third = HEAD_GROUP * head + head * bit
            return [w_qkv[:, first : first + 2 * head], w_qkv[:, third : third + head]]

        def block(weight, bit):
            size = weight.shape[1] // 2
            return weight[:, bit * size : (bit + 1) * size]

        down_t = w_down.T
        out_t = w_out.T
        wf_piece = gather_rows([jnp.concatenate([block(w_gate, j), block(w_up, j), *qkv_cols(j)], axis=1) for j in range(2)])
        ws_piece = gather_rows([jnp.concatenate([block(down_t, j), block(out_t, j)], axis=1) for j in range(2)])

        x_rows = x_in[0].astype(F32)
        normed, norm_pull = jax.vjp(lambda row_vals: norm_fwd(row_vals, norm_gain), x_rows)
        h_all = lax.all_gather(after(normed.astype(BF16), wf_piece[0], wf_piece[1]), ("y", "x"), axis=0, tiled=True)
        dy_all = lax.all_gather(after(dy_in[0], *wf_piece), ("y", "x"), axis=0, tiled=True)
        wf_parts = gather_weight(wf_piece)
        ws_parts = gather_weight(ws_piece)

        gate_up, qkv_tok = nn_pieces(pos, h_all, wf_parts, (2 * ff_blk, qkv_blk))
        third = qkv_tok[:, o_blk:]
        qkv_other = swap_c(my_rows(qkv_tok, False))
        third_own = swap_y(my_rows(third, True))
        third_other = swap_yc(my_rows(third, False))
        act_val, act_t = act_fwd(after(gate_up, qkv_tok))
        act_recv = swap_c(act_t)
        qkv_seq, attn_own, attn_other = attn_fwd(after(pos, act_t), qkv_tok, qkv_other, third_own, third_other, cos_tab, sin_tab)
        attn_got = swap_c(attn_other)
        y_part = nt_pieces(after(pos, attn_own), [act_val, attn_own, attn_got], ws_parts)
        mix_sum = lax.psum_scatter(y_part, ("y", "x"), scatter_dimension=0, tiled=True)
        y_out = (x_rows + mix_sum).astype(BF16)[None]

        dy_picked = pick_cols(after(pos, y_part), dy_all)
        dy_recv = swap_c(dy_picked)
        g_act = grad_start([(act_t, act_recv, dy_all, dy_recv, ff_blk, 0)], y_part)
        h_picked = pick_cols(after(pos, g_act[3][0]), h_all)
        h_recv = swap_c(h_picked)
        d_act, d_attn = nn_pieces(after(pos, h_picked), dy_all, ws_parts, (ff_blk, o_blk))
        d_attn_other = swap_c(my_rows(d_attn, False))
        d_gate_up, d_gate_up_t = act_bwd(gate_up, d_act)
        d_gate_up_recv = swap_c(d_gate_up_t)
        d_queries, keep, send = attn_bwd(after(pos, d_gate_up_t), qkv_seq, d_attn, d_attn_other, cos_tab, sin_tab)
        got = swap_y(send)
        g_act = grad_pass(g_act, d_queries)
        g_gate = grad_start([(d_gate_up_t, d_gate_up_recv, h_all, h_recv, ff_blk, 0)], *g_act[3])
        g_up = grad_start([(d_gate_up_t, d_gate_up_recv, h_all, h_recv, ff_blk, 1)], g_gate[3][0])
        d_own, d_other = attn_post(after(pos, g_up[3][0]), d_queries, keep, got, cos_tab, sin_tab)
        d_got = swap_c(d_other)
        dh_part = nt_pieces(pos, [d_gate_up, d_own, d_got], wf_parts)
        d_h = lax.psum_scatter(dh_part, ("y", "x"), scatter_dimension=0, tiled=True)
        d_h = d_h.astype(BF16)
        dx_out = (dy_in[0].astype(F32) + norm_pull(d_h.astype(F32))[0]).astype(BF16)[None]
        g_gate = grad_pass(g_gate, dh_part)

        attn_t = both_rows(attn_own, attn_got).T
        d_qkv_t = both_rows(d_own, d_got).T
        attn_recv = swap_c(attn_t)
        d_qkv_recv = swap_c(d_qkv_t)
        g_attn = grad_start([(attn_t, attn_recv, dy_all, dy_recv, o_blk, 0), (d_qkv_t, d_qkv_recv, h_all, h_recv, qkv_blk, 0)], *g_gate[3])
        g_up = grad_pass(g_up, g_attn[3][0])
        b_act = grad_back(g_act, g_attn[3][0])
        g_attn = grad_pass(g_attn)
        b_gate = grad_back(g_gate)
        b_up = grad_back(g_up)
        b_attn = grad_back(g_attn)
        dw_down = place(pos, *b_act, ff_blk, 0, False)
        dw_gate = place(pos, *b_gate, ff_blk, 0, True)
        dw_up = place(pos, *b_up, ff_blk, 0, True)
        dw_out, dw_qkv = place_attn(after(pos, dx_out, dw_up), *b_attn, o_blk, head)
        return y_out, dx_out, dw_qkv, dw_out, dw_gate, dw_up, dw_down


    return jax.shard_map(
        layer,
        mesh=wide_mesh,
        in_specs=(act_spec, act_spec, P(), col_spec, row_spec, col_spec, col_spec, row_spec, P(), P()),
        out_specs=(act_spec, act_spec, col_spec, row_spec, col_spec, col_spec, row_spec),
        check_vma=False,
    )
```

```python
import functools

import jax
import jax.numpy as jnp
from jax import lax
from jax.experimental import pallas as pl
from jax.experimental.pallas import tpu as pltpu
from jax.sharding import Mesh, PartitionSpec as P


NORM_EPS = 1e-5
NZ = 4
NY = 4
NX = 4
NC = 2
HEAD_GROUP = 4
F32 = jnp.float32
BF16 = jnp.bfloat16
VMEM_LIMIT = 60 * 1024 * 1024


def norm_fwd(row_vals, norm_gain):
    return row_vals * lax.rsqrt(jnp.mean(row_vals * row_vals, axis=-1, keepdims=True) + NORM_EPS) * norm_gain


def rotate(wide, cos_tab, sin_tab):
    return wide * cos_tab + pltpu.roll(wide, wide.shape[-1] // 2, wide.ndim - 1) * sin_tab


def rotate_back(wide, cos_tab, sin_tab):
    return wide * cos_tab - pltpu.roll(wide, wide.shape[-1] // 2, wide.ndim - 1) * sin_tab


def cost(flops, bytes_accessed):
    return pl.CostEstimate(flops=int(flops) // 20, bytes_accessed=int(bytes_accessed), transcendentals=0)


def params(**extra):
    return pltpu.CompilerParams(vmem_limit_bytes=VMEM_LIMIT, **extra)


def head_probs(q_rot, k_rot, scale):
    scores = dot_nt(q_rot, k_rot) * scale
    row_ids = lax.broadcasted_iota(jnp.int32, scores.shape, 0)
    col_ids = lax.broadcasted_iota(jnp.int32, scores.shape, 1)
    scores = jnp.where(row_ids >= col_ids, scores, -1e30)
    weights = jnp.exp(scores - jnp.max(scores, axis=-1, keepdims=True))
    return weights / jnp.sum(weights, axis=-1, keepdims=True)


def half_rows(core, idx, chunk):
    return pl.ds(pl.multiple_of((NC * idx + core) * chunk, chunk), chunk)


def chunk_rows(idx, chunk):
    return slice(idx * chunk, (idx + 1) * chunk)


def attn_fwd_kernel(heads, head, pos_ref, own_ref, other_ref, own_third_ref, other_third_ref, cos_ref, sin_ref, seq_ref, o_ref, o_other_ref, o_buf):
    core, odd = pos_ref[1], pos_ref[2]
    chunk = own_ref.shape[0] // NX
    width = heads * head
    mine = pl.ds(pl.multiple_of(width + odd * head, head), head)
    theirs = pl.ds(pl.multiple_of(width + (1 - odd) * head, head), head)
    for side, part_ref, third_ref in ((core, own_ref, own_third_ref), (1 - core, other_ref, other_third_ref)):
        for idx in range(NX):
            rows = half_rows(side, idx, chunk)
            seq_ref[0, rows, pl.ds(0, width)] = part_ref[chunk_rows(idx, chunk), :width]
            seq_ref[0, rows, mine] = part_ref[chunk_rows(idx, chunk), width:]
            seq_ref[0, rows, theirs] = third_ref[chunk_rows(idx, chunk), :]
    cos_tab, sin_tab = cos_ref[...], sin_ref[...]
    k_rot = rotate(seq_ref[0, :, width : width + head].astype(F32), cos_tab, sin_tab).astype(BF16)
    values = seq_ref[0, :, width + head :]
    for idx in range(heads):
        lanes = slice(idx * head, (idx + 1) * head)
        q_rot = rotate(seq_ref[0, :, lanes].astype(F32), cos_tab, sin_tab).astype(BF16)
        probs = head_probs(q_rot, k_rot, head**-0.5)
        o_buf[:, lanes] = dot_nn(probs.astype(BF16), values).astype(BF16)
    for side, out_ref in ((core, o_ref), (1 - core, o_other_ref)):
        for idx in range(NX):
            out_ref[chunk_rows(idx, chunk), :] = o_buf[half_rows(side, idx, chunk), :]


def attn_bwd_kernel(heads, head, pos_ref, seq_ref, own_ref, other_ref, cos_ref, sin_ref, dq_ref, keep_ref, send_ref, do_buf):
    core, odd = pos_ref[1], pos_ref[2]
    chunk = own_ref.shape[0] // NX
    width = heads * head
    for side, part_ref in ((core, own_ref), (1 - core, other_ref)):
        for idx in range(NX):
            do_buf[half_rows(side, idx, chunk), :] = part_ref[chunk_rows(idx, chunk), :]
    cos_tab, sin_tab = cos_ref[...], sin_ref[...]
    k_rot = rotate(seq_ref[0, :, width : width + head].astype(F32), cos_tab, sin_tab).astype(BF16)
    values = seq_ref[0, :, width + head :]
    d_keys = jnp.zeros(k_rot.shape, F32)
    d_values = jnp.zeros(k_rot.shape, F32)
    for idx in range(heads):
        lanes = slice(idx * head, (idx + 1) * head)
        q_rot = rotate(seq_ref[0, :, lanes].astype(F32), cos_tab, sin_tab).astype(BF16)
        d_out = do_buf[:, lanes]
        probs = head_probs(q_rot, k_rot, head**-0.5)
        d_values += dot_tn(probs.astype(BF16), d_out)
        d_probs = dot_nt(d_out, values).astype(BF16).astype(F32)
        d_scores = probs * (d_probs - jnp.sum(d_probs * probs, axis=-1, keepdims=True))
        d_scores = (d_scores * head**-0.5).astype(BF16)
        d_q_rot = dot_nn(d_scores, k_rot).astype(BF16)
        dq_ref[0, :, lanes] = rotate_back(d_q_rot.astype(F32), cos_tab, sin_tab).astype(BF16)
        d_keys += dot_tn(d_scores, q_rot)

    @pl.when(odd == 0)
    def _():
        keep_ref[0] = d_keys
        send_ref[0] = d_values

    @pl.when(odd == 1)
    def _():
        keep_ref[0] = d_values
        send_ref[0] = d_keys


def attn_post_kernel(heads, head, pos_ref, dq_ref, keep_ref, got_ref, cos_ref, sin_ref, own_ref, other_ref, third_buf):
    core, odd = pos_ref[1], pos_ref[2]
    chunk = own_ref.shape[0] // NX
    width = heads * head
    total = (keep_ref[0] + got_ref[0]).astype(BF16)

    @pl.when(odd == 0)
    def _():
        third_buf[...] = rotate_back(total.astype(F32), cos_ref[...], sin_ref[...]).astype(BF16)

    @pl.when(odd == 1)
    def _():
        third_buf[...] = total

    for side, out_ref in ((core, own_ref), (1 - core, other_ref)):
        for idx in range(NX):
            rows = half_rows(side, idx, chunk)
            out_ref[chunk_rows(idx, chunk), :width] = dq_ref[0, rows, :]
            out_ref[chunk_rows(idx, chunk), width:] = third_buf[rows, :]


def per_sequence(kernel, pos, args, specs, out_specs, out_shape, scratch, flops):
    return pl.pallas_call(
        kernel,
        grid_spec=pltpu.PrefetchScalarGridSpec(num_scalar_prefetch=1, grid=(2,), in_specs=specs, out_specs=out_specs, scratch_shapes=scratch),
        out_shape=out_shape,
        compiler_params=params(),
        cost_estimate=cost(flops, 4e6),
    )(pos, *args)


def own_spec(rows, width):
    return pl.BlockSpec((rows, width), lambda i, pos: (2 * pos[1] + i, 0))


def pair_spec(rows, width):
    return pl.BlockSpec((rows, width), lambda i, pos: (i, 0))


def seq_spec(seq, width):
    return pl.BlockSpec((1, seq, width), lambda i, pos: (i, 0, 0))


def table_spec(table):
    return pl.BlockSpec(table.shape, lambda i, pos: (0, 0))


def attn_fwd(pos, qkv_tok, other, own_third, other_third, cos_tab, sin_tab):
    seq, head = cos_tab.shape
    width = qkv_tok.shape[1] - head
    rows = seq // 2
    half = jax.ShapeDtypeStruct((seq, width), BF16)
    return per_sequence(
        functools.partial(attn_fwd_kernel, width // head, head),
        pos,
        (qkv_tok, other, own_third, other_third, cos_tab, sin_tab),
        [own_spec(rows, width + head), pair_spec(rows, width + head), pair_spec(rows, head), pair_spec(rows, head), table_spec(cos_tab), table_spec(sin_tab)],
        [seq_spec(seq, width + 2 * head), pair_spec(rows, width), pair_spec(rows, width)],
        [jax.ShapeDtypeStruct((2, seq, width + 2 * head), BF16), half, half],
        [pltpu.VMEM((seq, width), BF16)],
        16e9,
    )


def attn_bwd(pos, qkv_seq, d_attn, other, cos_tab, sin_tab):
    seq, head = cos_tab.shape
    width = d_attn.shape[1]
    rows = seq // 2
    part = jax.ShapeDtypeStruct((2, seq, head), F32)
    return per_sequence(
        functools.partial(attn_bwd_kernel, width // head, head),
        pos,
        (qkv_seq, d_attn, other, cos_tab, sin_tab),
        [seq_spec(seq, width + 2 * head), own_spec(rows, width), pair_spec(rows, width), table_spec(cos_tab), table_spec(sin_tab)],
        [seq_spec(seq, width), seq_spec(seq, head), seq_spec(seq, head)],
        [jax.ShapeDtypeStruct((2, seq, width), BF16), part, part],
        [pltpu.VMEM((seq, width), BF16)],
        16e9,
    )


def attn_post(pos, d_queries, keep, got, cos_tab, sin_tab):
    seq, head = cos_tab.shape
    width = d_queries.shape[2]
    rows = seq // 2
    half = jax.ShapeDtypeStruct((seq, width + head), BF16)
    return per_sequence(
        functools.partial(attn_post_kernel, width // head, head),
        pos,
        (d_queries, keep, got, cos_tab, sin_tab),
        [seq_spec(seq, width), seq_spec(seq, head), seq_spec(seq, head), table_spec(cos_tab), table_spec(sin_tab)],
        [pair_spec(rows, width + head), pair_spec(rows, width + head)],
        [half, half],
        [pltpu.VMEM((seq, head), BF16)],
        2e9,
    )


def act_fwd_kernel(half, ab_ref, u_ref, ut_ref):
    gate_val = ab_ref[:, :half].astype(F32)
    up_val = ab_ref[:, half:].astype(F32)
    act_val = gate_val * jax.nn.sigmoid(gate_val) * up_val
    u_ref[...] = act_val.astype(BF16)
    ut_ref[...] = act_val.T.astype(BF16)


def act_fwd(gate_up):
    tokens, width = gate_up.shape
    half = width // 2
    rows = tokens // 4
    return pl.pallas_call(
        functools.partial(act_fwd_kernel, half),
        grid=(4,),
        in_specs=[pl.BlockSpec((rows, width), lambda i: (i, 0))],
        out_specs=[pl.BlockSpec((rows, half), lambda i: (i, 0)), pl.BlockSpec((half, rows), lambda i: (0, i))],
        out_shape=[jax.ShapeDtypeStruct((tokens, half), BF16), jax.ShapeDtypeStruct((half, tokens), BF16)],
        compiler_params=params(),
        cost_estimate=cost(4e9, 8e6),
        name="act_fwd",
    )(gate_up)


def act_bwd_kernel(half, ab_ref, du_ref, dab_ref, dabt_ref):
    gate_val = ab_ref[:, :half].astype(F32)
    up_val = ab_ref[:, half:].astype(F32)
    d_act = du_ref[...].astype(F32)
    sig = jax.nn.sigmoid(gate_val)
    d_silu = d_act * up_val
    d_gate = d_silu * sig + d_silu * gate_val * (sig * (1.0 - sig))
    d_up = d_act * (gate_val * sig)
    dab_ref[:, :half] = d_gate.astype(BF16)
    dab_ref[:, half:] = d_up.astype(BF16)
    dabt_ref[:half, :] = d_gate.T.astype(BF16)
    dabt_ref[half:, :] = d_up.T.astype(BF16)


def act_bwd(gate_up, d_mixed):
    tokens, width = gate_up.shape
    half = width // 2
    rows = tokens // 4
    return pl.pallas_call(
        functools.partial(act_bwd_kernel, half),
        grid=(4,),
        in_specs=[pl.BlockSpec((rows, width), lambda i: (i, 0)), pl.BlockSpec((rows, half), lambda i: (i, 0))],
        out_specs=[pl.BlockSpec((rows, width), lambda i: (i, 0)), pl.BlockSpec((width, rows), lambda i: (0, i))],
        out_shape=[jax.ShapeDtypeStruct((tokens, width), BF16), jax.ShapeDtypeStruct((width, tokens), BF16)],
        compiler_params=params(),
        cost_estimate=cost(8e9, 14e6),
        name="act_bwd",
    )(gate_up, d_mixed)


def piece_block(pos_ref, step, other):
    core = pos_ref[1]
    return lax.rem(pos_ref[0] + step, NZ) * NC + (1 - core if other else core)


def half_start(pos_ref, part, half):
    return pl.multiple_of((1 - pos_ref[2] if part else pos_ref[2]) * half, half)


def nn_kernel(keys, first, count_out, tile, pos_ref, acts_ref, *refs):
    count = len(keys)
    halves = refs[: 2 * count]
    outs = refs[2 * count : 2 * count + count_out]
    acts_buf, w_buf, total, acts_sem, w_sem = refs[2 * count + count_out :]
    block = acts_buf.shape[1] // count
    half = block // 2
    copies = []
    for idx in range(count):
        cols = pl.ds(pl.multiple_of(piece_block(pos_ref, *keys[idx]) * block, block), block)
        copies.append([pltpu.make_async_copy(acts_ref.at[:, cols], acts_buf.at[:, pl.ds(idx * block, block)], acts_sem.at[idx])])
        for part in range(2):
            rows = pl.ds(idx * block + half_start(pos_ref, part, half), half)
            copies[-1].append(pltpu.make_async_copy(halves[2 * idx + part], w_buf.at[rows], w_sem.at[2 * idx + part]))
    for group in copies:
        for copy in group:
            copy.start()
    for lo, hi in ((0, first), (first, count)):
        for group in copies[lo:hi]:
            for copy in group:
                copy.wait()
        depth = pl.ds(lo * block, (hi - lo) * block)
        start = 0
        for out_ref in outs:
            width = out_ref.shape[1]

            def step(out_lo, size, start=start, out_ref=out_ref, depth=depth, hi=hi):
                cols = pl.ds(pl.multiple_of(start + out_lo, 128), size)
                part = dot_nn(acts_buf[:, depth], w_buf[depth, cols])
                if hi == count:
                    out_ref[:, pl.ds(pl.multiple_of(out_lo, 128), size)] = (total[:, cols] + part).astype(BF16)
                else:
                    total[:, cols] = part

            whole = width // tile
            if whole:
                pl.loop(0, whole)(lambda n: step(n * tile, tile))
            if width % tile:
                step(whole * tile, width % tile)
            start += width


def nn_pieces(pos, acts, parts, widths, tile):
    keys = [(step, other) for step in (0, 1, 3, 2) for other in range(2)]
    halves = [parts[step][other][part] for step, other in keys for part in range(2)]
    tokens, depth = acts.shape
    width = sum(widths)
    count = len(keys)
    anywhere = pl.BlockSpec(memory_space=pl.ANY)
    return pl.pallas_call(
        functools.partial(nn_kernel, keys, 2, len(widths), tile),
        grid_spec=pltpu.PrefetchScalarGridSpec(
            num_scalar_prefetch=1,
            grid=(1,),
            in_specs=[anywhere] * (1 + 2 * count),
            out_specs=[pl.BlockSpec((tokens, size), lambda i, pos: (0, 0)) for size in widths],
            scratch_shapes=[
                pltpu.VMEM((tokens, depth), BF16),
                pltpu.VMEM((depth, width), BF16),
                pltpu.VMEM((tokens, width), F32),
                pltpu.SemaphoreType.DMA((count,)),
                pltpu.SemaphoreType.DMA((2 * count,)),
            ],
        ),
        out_shape=[jax.ShapeDtypeStruct((tokens, size), BF16) for size in widths],
        compiler_params=params(),
        cost_estimate=cost(2 * tokens * depth * width, 2 * depth * (tokens + width)),
    )(pos, acts, *halves)


def nt_kernel(keys, sides, pos_ref, *refs):
    count_left = len(sides)
    count = len(keys)
    lefts = refs[:count_left]
    halves = refs[count_left : count_left + 2 * count]
    out_ref, left_buf, w_buf, out_buf, left_sem, w_sem, out_sem = refs[count_left + 2 * count :]
    block = out_buf.shape[2]
    half = block // 2
    slots = w_buf.shape[0]
    left_copies = []
    start = 0
    for idx, (left, side) in enumerate(zip(lefts, sides)):
        rows, width = left.shape
        first = 0 if side is None else pl.multiple_of((1 - pos_ref[1] if side else pos_ref[1]) * rows, rows)
        left_copies.append(pltpu.make_async_copy(left, left_buf.at[pl.ds(first, rows), pl.ds(start, width)], left_sem.at[idx]))
        left_copies[-1].start()
        start += 0 if side == 0 else width

    def copies(idx):
        for part in range(2):
            rows = pl.ds(half_start(pos_ref, part, half), half)
            yield pltpu.make_async_copy(halves[2 * idx + part], w_buf.at[idx % slots, rows], w_sem.at[idx % slots, part])

    def out_copy(idx):
        cols = pl.ds(pl.multiple_of(piece_block(pos_ref, *keys[idx]) * block, block), block)
        return pltpu.make_async_copy(out_buf.at[idx % 2], out_ref.at[:, cols], out_sem.at[idx % 2])

    for idx in range(slots - 1):
        for copy in copies(idx):
            copy.start()
    for idx in range(count):
        if idx + slots - 1 < count:
            for copy in copies(idx + slots - 1):
                copy.start()
        for copy in copies(idx):
            copy.wait()
        if idx == 0:
            for copy in left_copies:
                copy.wait()
        if idx >= 2:
            out_copy(idx - 2).wait()
        out_buf[idx % 2] = dot_nt(left_buf[...], w_buf[idx % slots])
        out_copy(idx).start()
    for idx in range(count - 2, count):
        out_copy(idx).wait()


def nt_pieces(pos, lefts, parts):
    sides = (None, 0, 1)
    keys = [(step, other) for step in range(NZ) for other in range(2)]
    halves = [parts[step][other][part] for step, other in keys for part in range(2)]
    tokens = lefts[0].shape[0]
    block = 2 * halves[0].shape[0]
    depth = block * len(keys)
    width = halves[0].shape[1]
    slots = 3
    anywhere = pl.BlockSpec(memory_space=pl.ANY)
    return pl.pallas_call(
        functools.partial(nt_kernel, keys, sides),
        grid_spec=pltpu.PrefetchScalarGridSpec(
            num_scalar_prefetch=1,
            grid=(1,),
            in_specs=[anywhere] * (len(lefts) + len(halves)),
            out_specs=anywhere,
            scratch_shapes=[
                pltpu.VMEM((tokens, width), BF16),
                pltpu.VMEM((slots, block, width), BF16),
                pltpu.VMEM((2, tokens, block), F32),
                pltpu.SemaphoreType.DMA((len(lefts),)),
                pltpu.SemaphoreType.DMA((slots, 2)),
                pltpu.SemaphoreType.DMA((2,)),
            ],
        ),
        out_shape=jax.ShapeDtypeStruct((tokens, depth), F32),
        compiler_params=params(),
        cost_estimate=cost(2 * tokens * depth * width, 2 * depth * width + 4 * tokens * depth),
    )(pos, *lefts, *halves)


def picked_cols(pos_ref, idx, block):
    return pl.ds(pl.multiple_of((NC * idx + 1 - pos_ref[1]) * block, block), block)


def dma_kernel(kernel, pos, args, out_shape, scratch):
    anywhere = pl.BlockSpec(memory_space=pl.ANY)
    return pl.pallas_call(
        kernel,
        grid_spec=pltpu.PrefetchScalarGridSpec(
            num_scalar_prefetch=1, grid=(1,), in_specs=[anywhere] * len(args), out_specs=[anywhere] * len(out_shape), scratch_shapes=scratch
        ),
        out_shape=out_shape,
        compiler_params=params(),
        cost_estimate=cost(3e9, 16e6),
    )(pos, *args)


def pick_cols(pos, acts):
    tokens, depth = acts.shape
    block = depth // (NC * NZ)

    def kernel(pos_ref, in_ref, out_ref, buf, in_sem, out_sem):
        reads = [pltpu.make_async_copy(in_ref.at[:, picked_cols(pos_ref, idx, block)], buf.at[idx], in_sem.at[idx]) for idx in range(NZ)]
        writes = [pltpu.make_async_copy(buf.at[idx], out_ref.at[:, pl.ds(idx * block, block)], out_sem.at[idx]) for idx in range(NZ)]
        for read in reads:
            read.start()
        for read, write in zip(reads, writes):
            read.wait()
            write.start()
        for write in writes:
            write.wait()

    sems = pltpu.SemaphoreType.DMA((NZ,))
    return dma_kernel(kernel, pos, [acts], [jax.ShapeDtypeStruct((tokens, depth // 2), BF16)], [pltpu.VMEM((NZ, tokens, block), BF16), sems, sems])[0]


def grad_kernel(heights, pos_ref, *refs):
    pairs = len(heights)
    ins = refs[: 6 * pairs]
    outs = refs[6 * pairs : 6 * pairs + 2 * NZ]
    buf, sem = refs[6 * pairs + 2 * NZ :]
    step = pl.program_id(0)
    slot = lax.rem(step, 2)

    def out_copy(idx, part):
        return pltpu.make_async_copy(buf.at[idx % 2, part], outs[2 * idx + part], sem.at[idx % 2, part])

    for idx in range(2, NZ):

        @pl.when(step == idx)
        def _(idx=idx):
            for part in range(2):
                out_copy(idx - 2, part).wait()

    start = 0
    for idx, height in enumerate(heights):
        own, recv, acts0, acts1, recv0, recv1 = ins[6 * idx : 6 * idx + 6]
        for part, acts, acts_recv in ((0, acts0, recv0), (1, acts1, recv1)):
            buf[slot, part, start : start + height, :] = dot_nn(own[...], acts[...]) + dot_nn(recv[...], acts_recv[...])
        start += height
    for idx in range(NZ):

        @pl.when(step == idx)
        def _(idx=idx):
            for part in range(2):
                out_copy(idx, part).start()

    @pl.when(step == NZ - 1)
    def _():
        for idx in (NZ - 2, NZ - 1):
            for part in range(2):
                out_copy(idx, part).wait()


def grad_pieces(pos, pairs):
    tokens, depth = pairs[0][2].shape
    cols = depth // (NZ * NY)
    in_specs = []
    args = []

    def z_of(n, pos):
        return lax.rem(pos[0] + jnp.where(n == 0, 2, jnp.where(n == 1, 1, jnp.where(n == 2, 3, 0))), NZ)

    def bit(pos, part):
        return 1 - pos[2] if part else pos[2]

    for own, recv, acts, acts_recv, height, block in pairs:
        in_specs += [pl.BlockSpec((height, tokens), lambda n, pos, block=block: (block, 0))] * 2
        in_specs += [pl.BlockSpec((tokens, cols), lambda n, pos, part=part: (0, z_of(n, pos) * NY + 2 * pos[1] + bit(pos, part))) for part in range(2)]
        in_specs += [pl.BlockSpec((tokens, cols), lambda n, pos, part=part: (0, z_of(n, pos) * 2 + bit(pos, part))) for part in range(2)]
        args += [own, recv, acts, acts, acts_recv, acts_recv]
    heights = [pair[4] for pair in pairs]
    rows = sum(heights)
    return pl.pallas_call(
        functools.partial(grad_kernel, heights),
        grid_spec=pltpu.PrefetchScalarGridSpec(
            num_scalar_prefetch=1,
            grid=(NZ,),
            in_specs=in_specs,
            out_specs=[pl.BlockSpec(memory_space=pl.ANY)] * (2 * NZ),
            scratch_shapes=[pltpu.VMEM((2, 2, rows, cols), F32), pltpu.SemaphoreType.DMA((2, 2))],
        ),
        out_shape=[jax.ShapeDtypeStruct((rows, cols), F32)] * (2 * NZ),
        compiler_params=params(),
        cost_estimate=cost(4 * rows * tokens * cols * 2 * NZ, 4 * tokens * cols * 2 * NZ),
        name="grad",
    )(pos, *args)


def place(pos, first, second, height, block, transpose):
    cols = first.shape[1]
    spec = pl.BlockSpec((height, cols), lambda n, pos: (block, 0))

    def kernel(pos_ref, first_ref, second_ref, out_ref):
        for idx, ref in enumerate((first_ref, second_ref)):

            @pl.when(pl.program_id(0) == idx)
            def _(ref=ref):
                out_ref[...] = ref[...].T if transpose else ref[...]

    def order(n, pos):
        return jnp.where(n == 0, pos[2], 1 - pos[2])

    return pl.pallas_call(
        kernel,
        grid_spec=pltpu.PrefetchScalarGridSpec(
            num_scalar_prefetch=1,
            grid=(2,),
            in_specs=[spec, spec],
            out_specs=pl.BlockSpec((cols, height), lambda n, pos: (0, order(n, pos))) if transpose else pl.BlockSpec((height, cols), lambda n, pos: (order(n, pos), 0)),
        ),
        out_shape=jax.ShapeDtypeStruct((cols, 2 * height) if transpose else (2 * height, cols), F32),
        compiler_params=params(),
        cost_estimate=cost(2e9, 16 * height * cols),
    )(pos, first, second)


def place_attn(pos, first, second, o_blk, head):
    rows, cols = first.shape
    qk = 2 * head

    def kernel(pos_ref, first_ref, second_ref, out_ref, qkv_ref):
        for idx, ref in enumerate((first_ref, second_ref)):
            bit = 1 - pos_ref[2] if idx else pos_ref[2]
            out_ref[pl.ds(pl.multiple_of(bit * o_blk, o_blk), o_blk), :] = ref[:o_blk, :]
            qkv_ref[:, pl.ds(pl.multiple_of(bit * qk, qk), qk)] = ref[o_blk : o_blk + qk, :].T
            qkv_ref[:, pl.ds(pl.multiple_of(2 * qk + bit * head, head), head)] = ref[o_blk + qk :, :].T

    def whole(*shape):
        return pl.BlockSpec(shape, lambda n, pos: (0, 0))

    shapes = ((2 * o_blk, cols), (cols, 2 * (qk + head)))
    return pl.pallas_call(
        kernel,
        grid_spec=pltpu.PrefetchScalarGridSpec(num_scalar_prefetch=1, grid=(1,), in_specs=[whole(rows, cols)] * 2, out_specs=[whole(*shape) for shape in shapes]),
        out_shape=[jax.ShapeDtypeStruct(shape, F32) for shape in shapes],
        compiler_params=params(),
        cost_estimate=cost(2e9, 16 * rows * cols),
        name="p_attn",
    )(pos, first, second)


def after(val, *earlier):
    return lax.optimization_barrier((val, *earlier))[0]


def ring(step, size):
    return [(src, (src + step) % size) for src in range(size)]


def hop_z(val, step):
    return lax.ppermute(val, "z", ring(step, NZ))


def swap_c(val):
    return lax.ppermute(val, "c", [(0, 1), (1, 0)])


def swap_y(val):
    return lax.ppermute(val, "y", [(src, src ^ 1) for src in range(NY)])


def turn(val, flip):
    def place_of(y_pos, c_pos):
        return y_pos * NC + c_pos

    pairs = [(place_of(2 * a + b, c), place_of(2 * c + (b ^ flip), a)) for a in range(2) for b in range(2) for c in range(NC)]
    return lax.ppermute(val, ("y", "c"), pairs)


def swap_yc(val):
    pairs = [(y_pos * NC + c_pos, (y_pos ^ 1) * NC + 1 - c_pos) for y_pos in range(NY) for c_pos in range(NC)]
    return lax.ppermute(val, ("y", "c"), pairs)


def dot_nn(left, right):
    return lax.dot_general(left, right, (((1,), (0,)), ((), ())), preferred_element_type=F32)


def dot_nt(left, right):
    return lax.dot_general(left, right, (((1,), (1,)), ((), ())), preferred_element_type=F32)


def dot_tn(left, right):
    return lax.dot_general(left, right, (((0,), (0,)), ((), ())), preferred_element_type=F32)


def solution(mesh):
    wide_mesh = Mesh(mesh.devices.reshape(NZ, NY, NX, NC), ("z", "y", "x", "c"))
    rows = ("z", "y")
    cols = ("x", "c")
    act_spec = P(rows, cols, None)
    col_spec = P(rows, cols)
    row_spec = P(cols, rows)

    def layer(x_in, dy_in, norm_gain, w_qkv, w_out, w_gate, w_up, w_down, rope_cos, rope_sin):
        z_pos = lax.axis_index("z")
        y_pos = lax.axis_index("y")
        c_pos = lax.axis_index("c")
        even_y = y_pos % 2 == 0
        first_c = c_pos == 0
        pos = jnp.stack([z_pos, c_pos, y_pos % 2]).astype(jnp.int32)
        head = 2 * rope_cos.shape[1]
        seq = rope_cos.shape[0]
        ff_blk = w_gate.shape[1] // 2
        o_blk = w_out.shape[0] // 2
        qkv_blk = o_blk + head

        def gather_rows(blocks):
            return [turn(jnp.where(even_y, blocks[flip], blocks[1 - flip]), flip) for flip in range(2)]

        def gather_weight(piece):
            left, right = [], []
            for part in (1, 0):
                left.insert(0, hop_z(piece[part], 1))
                right.insert(0, hop_z(piece[part], -1))
            far = [hop_z(left[0], 1), hop_z(right[1], -1)]
            parts = []
            for mine in (piece, right, far, left):
                parts.append((mine, [swap_c(half) for half in mine]))
            return parts

        def grad_start(pairs, *earlier):
            far0, far1, up0, up1, down0, down1, own0, own1 = grad_pieces(after(pos, *earlier), pairs)
            far = (hop_z(far0, 1), hop_z(far1, -1))
            direct = (hop_z(up1, 1), hop_z(down0, -1))
            return (up0, down1), far, direct, (own0, own1)

        def grad_pass(state, *earlier):
            (up0, down1), far, direct, own = state
            sums = (up0 + after(far[0], *earlier), down1 + far[1])
            passed = (hop_z(sums[0], 1), hop_z(sums[1], -1))
            return direct, passed, own, sums

        def grad_back(state, *earlier):
            direct, passed, own = state[:3]
            first = own[0] + after(passed[0], *earlier) + direct[1]
            second = own[1] + direct[0] + passed[1]
            return turn(first, 0), turn(second, 1)

        def my_rows(val, mine):
            return lax.dynamic_slice_in_dim(val, (c_pos if mine else 1 - c_pos) * seq, seq, axis=0)

        def both_rows(own, got):
            return jnp.concatenate([jnp.where(first_c, own, got), jnp.where(first_c, got, own)], axis=0)

        cos_tab = jnp.concatenate([rope_cos, rope_cos], axis=1)
        sin_tab = jnp.concatenate([-rope_sin, rope_sin], axis=1)

        def qkv_cols(bit):
            first = 2 * head * bit
            third = HEAD_GROUP * head + head * bit
            return [w_qkv[:, first : first + 2 * head], w_qkv[:, third : third + head]]

        def block(weight, bit):
            size = weight.shape[1] // 2
            return weight[:, bit * size : (bit + 1) * size]

        down_t = w_down.T
        out_t = w_out.T
        wf_piece = gather_rows([jnp.concatenate([block(w_gate, j), block(w_up, j), *qkv_cols(j)], axis=1) for j in range(2)])
        ws_piece = gather_rows([jnp.concatenate([block(down_t, j), block(out_t, j)], axis=1) for j in range(2)])

        x_rows = x_in[0].astype(F32)
        normed, norm_pull = jax.vjp(lambda row_vals: norm_fwd(row_vals, norm_gain), x_rows)
        h_all = lax.all_gather(after(normed.astype(BF16), wf_piece[0], wf_piece[1]), ("y", "x"), axis=0, tiled=True)
        dy_all = lax.all_gather(after(dy_in[0], *wf_piece), ("y", "x"), axis=0, tiled=True)
        wf_parts = gather_weight(wf_piece)
        ws_parts = gather_weight(ws_piece)

        gate_up, qkv_tok = nn_pieces(pos, h_all, wf_parts, (2 * ff_blk, qkv_blk), 512)
        third = qkv_tok[:, o_blk:]
        qkv_other = swap_c(my_rows(qkv_tok, False))
        third_own = swap_y(my_rows(third, True))
        third_other = swap_yc(my_rows(third, False))
        act_val, act_t = act_fwd(after(gate_up, qkv_tok))
        act_recv = swap_c(act_t)
        qkv_seq, attn_own, attn_other = attn_fwd(after(pos, act_t), qkv_tok, qkv_other, third_own, third_other, cos_tab, sin_tab)
        attn_got = swap_c(attn_other)
        y_part = nt_pieces(after(pos, attn_own), [act_val, attn_own, attn_got], ws_parts)
        mix_sum = lax.psum_scatter(y_part, ("y", "x"), scatter_dimension=0, tiled=True)
        y_out = (x_rows + mix_sum).astype(BF16)[None]

        dy_picked = pick_cols(after(pos, y_part), dy_all)
        dy_recv = swap_c(dy_picked)
        h_picked = pick_cols(after(pos, dy_picked), h_all)
        h_recv = swap_c(h_picked)
        g_act = grad_start([(act_t, act_recv, dy_all, dy_recv, ff_blk, 0)], h_picked)
        d_act, d_attn = nn_pieces(after(pos, g_act[3][0]), dy_all, ws_parts, (ff_blk, o_blk), 256)
        d_attn_other = swap_c(my_rows(d_attn, False))
        d_gate_up, d_gate_up_t = act_bwd(gate_up, d_act)
        d_gate_up_recv = swap_c(d_gate_up_t)
        d_queries, keep, send = attn_bwd(after(pos, d_gate_up_t), qkv_seq, d_attn, d_attn_other, cos_tab, sin_tab)
        got = swap_y(send)
        g_act = grad_pass(g_act, d_queries)
        g_gate = grad_start([(d_gate_up_t, d_gate_up_recv, h_all, h_recv, ff_blk, 0)], *g_act[3])
        d_own, d_other = attn_post(after(pos, g_gate[3][0]), d_queries, keep, got, cos_tab, sin_tab)
        d_got = swap_c(d_other)
        dh_part = nt_pieces(pos, [d_gate_up, d_own, d_got], wf_parts)
        d_h = lax.psum_scatter(dh_part, ("y", "x"), scatter_dimension=0, tiled=True)
        d_h = d_h.astype(BF16)
        dx_out = (dy_in[0].astype(F32) + norm_pull(d_h.astype(F32))[0]).astype(BF16)[None]
        g_up = grad_start([(d_gate_up_t, d_gate_up_recv, h_all, h_recv, ff_blk, 1)], dh_part)
        g_gate = grad_pass(g_gate, dh_part)

        attn_t = both_rows(attn_own, attn_got).T
        d_qkv_t = both_rows(d_own, d_got).T
        attn_recv = swap_c(attn_t)
        d_qkv_recv = swap_c(d_qkv_t)
        g_attn = grad_start([(attn_t, attn_recv, dy_all, dy_recv, o_blk, 0), (d_qkv_t, d_qkv_recv, h_all, h_recv, qkv_blk, 0)], *g_gate[3])
        g_up = grad_pass(g_up, g_attn[3][0])
        b_act = grad_back(g_act, g_attn[3][0])
        g_attn = grad_pass(g_attn)
        b_gate = grad_back(g_gate)
        b_up = grad_back(g_up)
        b_attn = grad_back(g_attn)
        dw_down = place(pos, *b_act, ff_blk, 0, False)
        dw_gate = place(pos, *b_gate, ff_blk, 0, True)
        dw_up = place(pos, *b_up, ff_blk, 0, True)
        dw_out, dw_qkv = place_attn(after(pos, dx_out, dw_up), *b_attn, o_blk, head)
        return y_out, dx_out, dw_qkv, dw_out, dw_gate, dw_up, dw_down


    return jax.shard_map(
        layer,
        mesh=wide_mesh,
        in_specs=(act_spec, act_spec, P(), col_spec, row_spec, col_spec, col_spec, row_spec, P(), P()),
        out_specs=(act_spec, act_spec, col_spec, row_spec, col_spec, col_spec, row_spec),
        check_vma=False,
    )
```

```python
import functools

import jax
import jax.numpy as jnp
from jax import lax
from jax.experimental import pallas as pl
from jax.experimental.pallas import tpu as pltpu
from jax.sharding import Mesh, PartitionSpec as P


NORM_EPS = 1e-5
NZ = 4
NY = 4
NX = 4
NC = 2
HEAD_GROUP = 4
F32 = jnp.float32
BF16 = jnp.bfloat16
VMEM_LIMIT = 67043328


def norm_fwd(row_vals, norm_gain):
    return row_vals * lax.rsqrt(jnp.mean(row_vals * row_vals, axis=-1, keepdims=True) + NORM_EPS) * norm_gain


def rotate(wide, cos_tab, sin_tab):
    return wide * cos_tab + pltpu.roll(wide, wide.shape[-1] // 2, wide.ndim - 1) * sin_tab


def rotate_back(wide, cos_tab, sin_tab):
    return wide * cos_tab - pltpu.roll(wide, wide.shape[-1] // 2, wide.ndim - 1) * sin_tab


def cost(flops, bytes_accessed):
    return pl.CostEstimate(flops=int(flops) // 20, bytes_accessed=int(bytes_accessed), transcendentals=0)


def params(**extra):
    return pltpu.CompilerParams(vmem_limit_bytes=VMEM_LIMIT, **extra)


def head_probs(q_rot, k_rot, scale):
    scores = dot_nt(q_rot, k_rot) * scale
    row_ids = lax.broadcasted_iota(jnp.int32, scores.shape, 0)
    col_ids = lax.broadcasted_iota(jnp.int32, scores.shape, 1)
    scores = jnp.where(row_ids >= col_ids, scores, -1e30)
    weights = jnp.exp(scores - jnp.max(scores, axis=-1, keepdims=True))
    return weights / jnp.sum(weights, axis=-1, keepdims=True)


def half_rows(core, idx, chunk):
    return pl.ds(pl.multiple_of((NC * idx + core) * chunk, chunk), chunk)


def chunk_rows(idx, chunk):
    return slice(idx * chunk, (idx + 1) * chunk)


def attn_fwd_kernel(heads, head, pos_ref, own_ref, other_ref, own_third_ref, other_third_ref, cos_ref, sin_ref, seq_ref, o_ref, o_other_ref, o_buf):
    core, odd = pos_ref[1], pos_ref[2]
    chunk = own_ref.shape[0] // NX
    width = heads * head
    mine = pl.ds(pl.multiple_of(width + odd * head, head), head)
    theirs = pl.ds(pl.multiple_of(width + (1 - odd) * head, head), head)
    for side, part_ref, third_ref in ((core, own_ref, own_third_ref), (1 - core, other_ref, other_third_ref)):
        for idx in range(NX):
            rows = half_rows(side, idx, chunk)
            seq_ref[0, rows, pl.ds(0, width)] = part_ref[chunk_rows(idx, chunk), :width]
            seq_ref[0, rows, mine] = part_ref[chunk_rows(idx, chunk), width:]
            seq_ref[0, rows, theirs] = third_ref[chunk_rows(idx, chunk), :]
    cos_tab, sin_tab = cos_ref[...], sin_ref[...]
    k_rot = rotate(seq_ref[0, :, width : width + head].astype(F32), cos_tab, sin_tab).astype(BF16)
    values = seq_ref[0, :, width + head :]
    for idx in range(heads):
        lanes = slice(idx * head, (idx + 1) * head)
        q_rot = rotate(seq_ref[0, :, lanes].astype(F32), cos_tab, sin_tab).astype(BF16)
        probs = head_probs(q_rot, k_rot, head**-0.5)
        o_buf[:, lanes] = dot_nn(probs.astype(BF16), values).astype(BF16)
    for side, out_ref in ((core, o_ref), (1 - core, o_other_ref)):
        for idx in range(NX):
            out_ref[chunk_rows(idx, chunk), :] = o_buf[half_rows(side, idx, chunk), :]


def attn_bwd_kernel(heads, head, pos_ref, seq_ref, own_ref, other_ref, cos_ref, sin_ref, dq_ref, keep_ref, send_ref, do_buf):
    core, odd = pos_ref[1], pos_ref[2]
    chunk = own_ref.shape[0] // NX
    width = heads * head
    for side, part_ref in ((core, own_ref), (1 - core, other_ref)):
        for idx in range(NX):
            do_buf[half_rows(side, idx, chunk), :] = part_ref[chunk_rows(idx, chunk), :]
    cos_tab, sin_tab = cos_ref[...], sin_ref[...]
    k_rot = rotate(seq_ref[0, :, width : width + head].astype(F32), cos_tab, sin_tab).astype(BF16)
    values = seq_ref[0, :, width + head :]
    d_keys = jnp.zeros(k_rot.shape, F32)
    d_values = jnp.zeros(k_rot.shape, F32)
    for idx in range(heads):
        lanes = slice(idx * head, (idx + 1) * head)
        q_rot = rotate(seq_ref[0, :, lanes].astype(F32), cos_tab, sin_tab).astype(BF16)
        d_out = do_buf[:, lanes]
        probs = head_probs(q_rot, k_rot, head**-0.5)
        d_values += dot_tn(probs.astype(BF16), d_out)
        d_probs = dot_nt(d_out, values).astype(BF16).astype(F32)
        d_scores = probs * (d_probs - jnp.sum(d_probs * probs, axis=-1, keepdims=True))
        d_scores = (d_scores * head**-0.5).astype(BF16)
        d_q_rot = dot_nn(d_scores, k_rot).astype(BF16)
        dq_ref[0, :, lanes] = rotate_back(d_q_rot.astype(F32), cos_tab, sin_tab).astype(BF16)
        d_keys += dot_tn(d_scores, q_rot)

    @pl.when(odd == 0)
    def _():
        keep_ref[0] = d_keys
        send_ref[0] = d_values

    @pl.when(odd == 1)
    def _():
        keep_ref[0] = d_values
        send_ref[0] = d_keys


def attn_post_kernel(heads, head, pos_ref, dq_ref, keep_ref, got_ref, cos_ref, sin_ref, own_ref, other_ref, third_buf):
    core, odd = pos_ref[1], pos_ref[2]
    chunk = own_ref.shape[0] // NX
    width = heads * head
    total = (keep_ref[0] + got_ref[0]).astype(BF16)

    @pl.when(odd == 0)
    def _():
        third_buf[...] = rotate_back(total.astype(F32), cos_ref[...], sin_ref[...]).astype(BF16)

    @pl.when(odd == 1)
    def _():
        third_buf[...] = total

    for side, out_ref in ((core, own_ref), (1 - core, other_ref)):
        for idx in range(NX):
            rows = half_rows(side, idx, chunk)
            out_ref[chunk_rows(idx, chunk), :width] = dq_ref[0, rows, :]
            out_ref[chunk_rows(idx, chunk), width:] = third_buf[rows, :]


def per_sequence(kernel, pos, args, specs, out_specs, out_shape, scratch, flops):
    return pl.pallas_call(
        kernel,
        grid_spec=pltpu.PrefetchScalarGridSpec(num_scalar_prefetch=1, grid=(2,), in_specs=specs, out_specs=out_specs, scratch_shapes=scratch),
        out_shape=out_shape,
        compiler_params=params(),
        cost_estimate=cost(flops, 4e6),
    )(pos, *args)


def own_spec(rows, width):
    return pl.BlockSpec((rows, width), lambda i, pos: (2 * pos[1] + i, 0))


def pair_spec(rows, width):
    return pl.BlockSpec((rows, width), lambda i, pos: (i, 0))


def seq_spec(seq, width):
    return pl.BlockSpec((1, seq, width), lambda i, pos: (i, 0, 0))


def table_spec(table):
    return pl.BlockSpec(table.shape, lambda i, pos: (0, 0))


def attn_fwd(pos, qkv_tok, other, own_third, other_third, cos_tab, sin_tab):
    seq, head = cos_tab.shape
    width = qkv_tok.shape[1] - head
    rows = seq // 2
    half = jax.ShapeDtypeStruct((seq, width), BF16)
    return per_sequence(
        functools.partial(attn_fwd_kernel, width // head, head),
        pos,
        (qkv_tok, other, own_third, other_third, cos_tab, sin_tab),
        [own_spec(rows, width + head), pair_spec(rows, width + head), pair_spec(rows, head), pair_spec(rows, head), table_spec(cos_tab), table_spec(sin_tab)],
        [seq_spec(seq, width + 2 * head), pair_spec(rows, width), pair_spec(rows, width)],
        [jax.ShapeDtypeStruct((2, seq, width + 2 * head), BF16), half, half],
        [pltpu.VMEM((seq, width), BF16)],
        16e9,
    )


def attn_bwd(pos, qkv_seq, d_attn, other, cos_tab, sin_tab):
    seq, head = cos_tab.shape
    width = d_attn.shape[1]
    rows = seq // 2
    part = jax.ShapeDtypeStruct((2, seq, head), F32)
    return per_sequence(
        functools.partial(attn_bwd_kernel, width // head, head),
        pos,
        (qkv_seq, d_attn, other, cos_tab, sin_tab),
        [seq_spec(seq, width + 2 * head), own_spec(rows, width), pair_spec(rows, width), table_spec(cos_tab), table_spec(sin_tab)],
        [seq_spec(seq, width), seq_spec(seq, head), seq_spec(seq, head)],
        [jax.ShapeDtypeStruct((2, seq, width), BF16), part, part],
        [pltpu.VMEM((seq, width), BF16)],
        16e9,
    )


def attn_post(pos, d_queries, keep, got, cos_tab, sin_tab):
    seq, head = cos_tab.shape
    width = d_queries.shape[2]
    rows = seq // 2
    half = jax.ShapeDtypeStruct((seq, width + head), BF16)
    return per_sequence(
        functools.partial(attn_post_kernel, width // head, head),
        pos,
        (d_queries, keep, got, cos_tab, sin_tab),
        [seq_spec(seq, width), seq_spec(seq, head), seq_spec(seq, head), table_spec(cos_tab), table_spec(sin_tab)],
        [pair_spec(rows, width + head), pair_spec(rows, width + head)],
        [half, half],
        [pltpu.VMEM((seq, head), BF16)],
        2e9,
    )


def act_fwd_kernel(half, ab_ref, u_ref, ut_ref):
    gate_val = ab_ref[:, :half].astype(F32)
    up_val = ab_ref[:, half:].astype(F32)
    act_val = gate_val * jax.nn.sigmoid(gate_val) * up_val
    u_ref[...] = act_val.astype(BF16)
    ut_ref[...] = act_val.T.astype(BF16)


def act_fwd(gate_up):
    tokens, width = gate_up.shape
    half = width // 2
    rows = tokens // 4
    return pl.pallas_call(
        functools.partial(act_fwd_kernel, half),
        grid=(4,),
        in_specs=[pl.BlockSpec((rows, width), lambda i: (i, 0))],
        out_specs=[pl.BlockSpec((rows, half), lambda i: (i, 0)), pl.BlockSpec((half, rows), lambda i: (0, i))],
        out_shape=[jax.ShapeDtypeStruct((tokens, half), BF16), jax.ShapeDtypeStruct((half, tokens), BF16)],
        compiler_params=params(),
        cost_estimate=cost(4e9, 8e6),
        name="act_fwd",
    )(gate_up)


def act_bwd_kernel(half, ab_ref, du_ref, dab_ref, dabt_ref):
    gate_val = ab_ref[:, :half].astype(F32)
    up_val = ab_ref[:, half:].astype(F32)
    d_act = du_ref[...].astype(F32)
    sig = jax.nn.sigmoid(gate_val)
    d_silu = d_act * up_val
    d_gate = d_silu * sig + d_silu * gate_val * (sig * (1.0 - sig))
    d_up = d_act * (gate_val * sig)
    dab_ref[:, :half] = d_gate.astype(BF16)
    dab_ref[:, half:] = d_up.astype(BF16)
    dabt_ref[:half, :] = d_gate.T.astype(BF16)
    dabt_ref[half:, :] = d_up.T.astype(BF16)


def act_bwd(gate_up, d_mixed):
    tokens, width = gate_up.shape
    half = width // 2
    rows = tokens // 4
    return pl.pallas_call(
        functools.partial(act_bwd_kernel, half),
        grid=(4,),
        in_specs=[pl.BlockSpec((rows, width), lambda i: (i, 0)), pl.BlockSpec((rows, half), lambda i: (i, 0))],
        out_specs=[pl.BlockSpec((rows, width), lambda i: (i, 0)), pl.BlockSpec((width, rows), lambda i: (0, i))],
        out_shape=[jax.ShapeDtypeStruct((tokens, width), BF16), jax.ShapeDtypeStruct((width, tokens), BF16)],
        compiler_params=params(),
        cost_estimate=cost(8e9, 14e6),
        name="act_bwd",
    )(gate_up, d_mixed)


def piece_block(pos_ref, step, other):
    core = pos_ref[1]
    return lax.rem(pos_ref[0] + step, NZ) * NC + (1 - core if other else core)


def half_start(pos_ref, part, half):
    return pl.multiple_of((1 - pos_ref[2] if part else pos_ref[2]) * half, half)


def nn_kernel(keys, first, count_out, tile, pos_ref, acts_ref, *refs):
    count = len(keys)
    halves = refs[: 2 * count]
    outs = refs[2 * count : 2 * count + count_out]
    acts_buf, w_buf, total, acts_sem, w_sem = refs[2 * count + count_out :]
    block = acts_buf.shape[1] // count
    half = block // 2
    copies = []
    for idx in range(count):
        cols = pl.ds(pl.multiple_of(piece_block(pos_ref, *keys[idx]) * block, block), block)
        copies.append([pltpu.make_async_copy(acts_ref.at[:, cols], acts_buf.at[:, pl.ds(idx * block, block)], acts_sem.at[idx])])
        for part in range(2):
            rows = pl.ds(idx * block + half_start(pos_ref, part, half), half)
            copies[-1].append(pltpu.make_async_copy(halves[2 * idx + part], w_buf.at[rows], w_sem.at[2 * idx + part]))
    for group in copies:
        for copy in group:
            copy.start()
    for lo, hi in ((0, first), (first, count)):
        for group in copies[lo:hi]:
            for copy in group:
                copy.wait()
        depth = pl.ds(lo * block, (hi - lo) * block)
        start = 0
        for out_ref in outs:
            width = out_ref.shape[1]

            def step(out_lo, size, start=start, out_ref=out_ref, depth=depth, hi=hi):
                cols = pl.ds(pl.multiple_of(start + out_lo, 128), size)
                part = dot_nn(acts_buf[:, depth], w_buf[depth, cols])
                if hi == count:
                    out_ref[:, pl.ds(pl.multiple_of(out_lo, 128), size)] = (total[:, cols] + part).astype(BF16)
                else:
                    total[:, cols] = part

            whole = width // tile
            if whole:
                pl.loop(0, whole)(lambda n: step(n * tile, tile))
            if width % tile:
                step(whole * tile, width % tile)
            start += width


def nn_pieces(pos, acts, parts, widths, tile):
    keys = [(step, other) for step in (0, 1, 3, 2) for other in range(2)]
    halves = [parts[step][other][part] for step, other in keys for part in range(2)]
    tokens, depth = acts.shape
    width = sum(widths)
    count = len(keys)
    anywhere = pl.BlockSpec(memory_space=pl.ANY)
    return pl.pallas_call(
        functools.partial(nn_kernel, keys, 2, len(widths), tile),
        grid_spec=pltpu.PrefetchScalarGridSpec(
            num_scalar_prefetch=1,
            grid=(1,),
            in_specs=[anywhere] * (1 + 2 * count),
            out_specs=[pl.BlockSpec((tokens, size), lambda i, pos: (0, 0)) for size in widths],
            scratch_shapes=[
                pltpu.VMEM((tokens, depth), BF16),
                pltpu.VMEM((depth, width), BF16),
                pltpu.VMEM((tokens, width), F32),
                pltpu.SemaphoreType.DMA((count,)),
                pltpu.SemaphoreType.DMA((2 * count,)),
            ],
        ),
        out_shape=[jax.ShapeDtypeStruct((tokens, size), BF16) for size in widths],
        compiler_params=params(),
        cost_estimate=cost(2 * tokens * depth * width, 2 * depth * (tokens + width)),
    )(pos, acts, *halves)


def nt_kernel(keys, sides, pos_ref, *refs):
    count_left = len(sides)
    count = len(keys)
    lefts = refs[:count_left]
    halves = refs[count_left : count_left + 2 * count]
    out_ref, left_buf, w_buf, out_buf, left_sem, w_sem, out_sem = refs[count_left + 2 * count :]
    block = out_buf.shape[2]
    half = block // 2
    slots = w_buf.shape[0]
    left_copies = []
    start = 0
    for idx, (left, side) in enumerate(zip(lefts, sides)):
        rows, width = left.shape
        first = 0 if side is None else pl.multiple_of((1 - pos_ref[1] if side else pos_ref[1]) * rows, rows)
        left_copies.append(pltpu.make_async_copy(left, left_buf.at[pl.ds(first, rows), pl.ds(start, width)], left_sem.at[idx]))
        left_copies[-1].start()
        start += 0 if side == 0 else width

    def copies(idx, slot):
        for part in range(2):
            rows = pl.ds(half_start(pos_ref, part, half), half)
            yield pltpu.make_async_copy(halves[2 * idx + part], w_buf.at[slot, rows], w_sem.at[slot, part])

    def out_copy(idx):
        core = pos_ref[1]
        other = lax.rem(idx, 2)
        block_id = lax.rem(pos_ref[0] + idx // 2, NZ) * NC + core + other - 2 * core * other
        slot = lax.rem(idx, 2)
        return pltpu.make_async_copy(out_buf.at[slot], out_ref.at[:, pl.ds(pl.multiple_of(block_id * block, block), block)], out_sem.at[slot])

    for idx in range(slots - 1):
        for copy in copies(idx, idx):
            copy.start()
    for copy in left_copies:
        copy.wait()

    @pl.loop(0, count)
    def _(step):
        slot = lax.rem(step, slots)
        for idx in range(slots - 1, count):

            @pl.when(step + slots - 1 == idx)
            def _(idx=idx):
                for copy in copies(idx, idx % slots):
                    copy.start()

        for copy in copies(0, slot):
            copy.wait()

        @pl.when(step >= 2)
        def _():
            out_copy(step - 2).wait()

        out_buf[lax.rem(step, 2)] = dot_nt(left_buf[...], w_buf[slot])
        out_copy(step).start()

    for idx in range(count - 2, count):
        out_copy(idx).wait()


def nt_pieces(pos, lefts, parts):
    sides = (None, 0, 1)
    keys = [(step, other) for step in range(NZ) for other in range(2)]
    halves = [parts[step][other][part] for step, other in keys for part in range(2)]
    tokens = lefts[0].shape[0]
    block = 2 * halves[0].shape[0]
    depth = block * len(keys)
    width = halves[0].shape[1]
    slots = 3
    anywhere = pl.BlockSpec(memory_space=pl.ANY)
    return pl.pallas_call(
        functools.partial(nt_kernel, keys, sides),
        grid_spec=pltpu.PrefetchScalarGridSpec(
            num_scalar_prefetch=1,
            grid=(1,),
            in_specs=[anywhere] * (len(lefts) + len(halves)),
            out_specs=anywhere,
            scratch_shapes=[
                pltpu.VMEM((tokens, width), BF16),
                pltpu.VMEM((slots, block, width), BF16),
                pltpu.VMEM((2, tokens, block), F32),
                pltpu.SemaphoreType.DMA((len(lefts),)),
                pltpu.SemaphoreType.DMA((slots, 2)),
                pltpu.SemaphoreType.DMA((2,)),
            ],
        ),
        out_shape=jax.ShapeDtypeStruct((tokens, depth), F32),
        compiler_params=params(),
        cost_estimate=cost(2 * tokens * depth * width, 2 * depth * width + 4 * tokens * depth),
    )(pos, *lefts, *halves)


def picked_cols(pos_ref, idx, block):
    return pl.ds(pl.multiple_of((NC * idx + 1 - pos_ref[1]) * block, block), block)


def dma_kernel(kernel, pos, args, out_shape, scratch):
    anywhere = pl.BlockSpec(memory_space=pl.ANY)
    return pl.pallas_call(
        kernel,
        grid_spec=pltpu.PrefetchScalarGridSpec(
            num_scalar_prefetch=1, grid=(1,), in_specs=[anywhere] * len(args), out_specs=[anywhere] * len(out_shape), scratch_shapes=scratch
        ),
        out_shape=out_shape,
        compiler_params=params(),
        cost_estimate=cost(3e9, 16e6),
    )(pos, *args)


def pick_cols(pos, acts):
    tokens, depth = acts.shape
    block = depth // (NC * NZ)

    def kernel(pos_ref, in_ref, out_ref, buf, in_sem, out_sem):
        reads = [pltpu.make_async_copy(in_ref.at[:, picked_cols(pos_ref, idx, block)], buf.at[idx], in_sem.at[idx]) for idx in range(NZ)]
        writes = [pltpu.make_async_copy(buf.at[idx], out_ref.at[:, pl.ds(idx * block, block)], out_sem.at[idx]) for idx in range(NZ)]
        for read in reads:
            read.start()
        for read, write in zip(reads, writes):
            read.wait()
            write.start()
        for write in writes:
            write.wait()

    sems = pltpu.SemaphoreType.DMA((NZ,))
    return dma_kernel(kernel, pos, [acts], [jax.ShapeDtypeStruct((tokens, depth // 2), BF16)], [pltpu.VMEM((NZ, tokens, block), BF16), sems, sems])[0]


def grad_kernel(heights, pos_ref, *refs):
    pairs = len(heights)
    ins = refs[: 4 * pairs]
    outs = refs[4 * pairs : 4 * pairs + 2 * NZ]
    buf, sem = refs[4 * pairs + 2 * NZ :]
    half = buf.shape[2] // 2
    step = pl.program_id(0)
    slot = lax.rem(step, 2)

    def out_copy(idx, part):
        cols = pl.ds(half_start(pos_ref, part, half), half)
        return pltpu.make_async_copy(buf.at[idx % 2, :, cols], outs[2 * idx + part], sem.at[idx % 2, part])

    for idx in range(2, NZ):

        @pl.when(step == idx)
        def _(idx=idx):
            for part in range(2):
                out_copy(idx - 2, part).wait()

    start = 0
    for idx, height in enumerate(heights):
        own, recv, acts, acts_recv = ins[4 * idx : 4 * idx + 4]
        buf[slot, start : start + height, :] = dot_nn(own[...], acts[...]) + dot_nn(recv[...], acts_recv[...])
        start += height
    for idx in range(NZ):

        @pl.when(step == idx)
        def _(idx=idx):
            for part in range(2):
                out_copy(idx, part).start()

    @pl.when(step == NZ - 1)
    def _():
        for idx in (NZ - 2, NZ - 1):
            for part in range(2):
                out_copy(idx, part).wait()


def grad_pieces(pos, pairs):
    tokens, depth = pairs[0][2].shape
    cols = depth // (NZ * NC)
    in_specs = []
    args = []

    def z_of(n, pos):
        return lax.rem(pos[0] + jnp.where(n == 0, 2, jnp.where(n == 1, 1, jnp.where(n == 2, 3, 0))), NZ)

    for own, recv, acts, acts_recv, height, block in pairs:
        in_specs += [pl.BlockSpec((height, tokens), lambda n, pos, block=block: (block, 0))] * 2
        in_specs.append(pl.BlockSpec((tokens, cols), lambda n, pos: (0, z_of(n, pos) * NC + pos[1])))
        in_specs.append(pl.BlockSpec((tokens, cols), lambda n, pos: (0, z_of(n, pos))))
        args += [own, recv, acts, acts_recv]
    heights = [pair[4] for pair in pairs]
    rows = sum(heights)
    return pl.pallas_call(
        functools.partial(grad_kernel, heights),
        grid_spec=pltpu.PrefetchScalarGridSpec(
            num_scalar_prefetch=1,
            grid=(NZ,),
            in_specs=in_specs,
            out_specs=[pl.BlockSpec(memory_space=pl.ANY)] * (2 * NZ),
            scratch_shapes=[pltpu.VMEM((2, rows, cols), F32), pltpu.SemaphoreType.DMA((2, 2))],
        ),
        out_shape=[jax.ShapeDtypeStruct((rows, cols // 2), F32)] * (2 * NZ),
        compiler_params=params(),
        cost_estimate=cost(4 * rows * tokens * cols * NZ, 4 * tokens * cols * NZ),
        name="grad",
    )(pos, *args)


def place(pos, first, second, height, block, transpose):
    cols = first.shape[1]
    spec = pl.BlockSpec((height, cols), lambda n, pos: (block, 0))

    def kernel(pos_ref, first_ref, second_ref, out_ref):
        for idx, ref in enumerate((first_ref, second_ref)):

            @pl.when(pl.program_id(0) == idx)
            def _(ref=ref):
                out_ref[...] = ref[...].T if transpose else ref[...]

    def order(n, pos):
        return jnp.where(n == 0, pos[2], 1 - pos[2])

    return pl.pallas_call(
        kernel,
        grid_spec=pltpu.PrefetchScalarGridSpec(
            num_scalar_prefetch=1,
            grid=(2,),
            in_specs=[spec, spec],
            out_specs=pl.BlockSpec((cols, height), lambda n, pos: (0, order(n, pos))) if transpose else pl.BlockSpec((height, cols), lambda n, pos: (order(n, pos), 0)),
        ),
        out_shape=jax.ShapeDtypeStruct((cols, 2 * height) if transpose else (2 * height, cols), F32),
        compiler_params=params(),
        cost_estimate=cost(2e9, 16 * height * cols),
    )(pos, first, second)


def place_attn(pos, first, second, o_blk, head):
    rows, cols = first.shape
    qk = 2 * head

    def kernel(pos_ref, first_ref, second_ref, out_ref, qkv_ref):
        for idx, ref in enumerate((first_ref, second_ref)):
            bit = 1 - pos_ref[2] if idx else pos_ref[2]
            out_ref[pl.ds(pl.multiple_of(bit * o_blk, o_blk), o_blk), :] = ref[:o_blk, :]
            qkv_ref[:, pl.ds(pl.multiple_of(bit * qk, qk), qk)] = ref[o_blk : o_blk + qk, :].T
            qkv_ref[:, pl.ds(pl.multiple_of(2 * qk + bit * head, head), head)] = ref[o_blk + qk :, :].T

    def whole(*shape):
        return pl.BlockSpec(shape, lambda n, pos: (0, 0))

    shapes = ((2 * o_blk, cols), (cols, 2 * (qk + head)))
    return pl.pallas_call(
        kernel,
        grid_spec=pltpu.PrefetchScalarGridSpec(num_scalar_prefetch=1, grid=(1,), in_specs=[whole(rows, cols)] * 2, out_specs=[whole(*shape) for shape in shapes]),
        out_shape=[jax.ShapeDtypeStruct(shape, F32) for shape in shapes],
        compiler_params=params(),
        cost_estimate=cost(2e9, 16 * rows * cols),
        name="p_attn",
    )(pos, first, second)


def after(val, *earlier):
    return lax.optimization_barrier((val, *earlier))[0]


def ring(step, size):
    return [(src, (src + step) % size) for src in range(size)]


def hop_z(val, step):
    return lax.ppermute(val, "z", ring(step, NZ))


def swap_c(val):
    return lax.ppermute(val, "c", [(0, 1), (1, 0)])


def swap_y(val):
    return lax.ppermute(val, "y", [(src, src ^ 1) for src in range(NY)])


def turn(val, flip):
    def place_of(y_pos, c_pos):
        return y_pos * NC + c_pos

    pairs = [(place_of(2 * a + b, c), place_of(2 * c + (b ^ flip), a)) for a in range(2) for b in range(2) for c in range(NC)]
    return lax.ppermute(val, ("y", "c"), pairs)


def swap_yc(val):
    pairs = [(y_pos * NC + c_pos, (y_pos ^ 1) * NC + 1 - c_pos) for y_pos in range(NY) for c_pos in range(NC)]
    return lax.ppermute(val, ("y", "c"), pairs)


def dot_nn(left, right):
    return lax.dot_general(left, right, (((1,), (0,)), ((), ())), preferred_element_type=F32)


def dot_nt(left, right):
    return lax.dot_general(left, right, (((1,), (1,)), ((), ())), preferred_element_type=F32)


def dot_tn(left, right):
    return lax.dot_general(left, right, (((0,), (0,)), ((), ())), preferred_element_type=F32)


def solution(mesh):
    wide_mesh = Mesh(mesh.devices.reshape(NZ, NY, NX, NC), ("z", "y", "x", "c"))
    rows = ("z", "y")
    cols = ("x", "c")
    act_spec = P(rows, cols, None)
    col_spec = P(rows, cols)
    row_spec = P(cols, rows)

    def layer(x_in, dy_in, norm_gain, w_qkv, w_out, w_gate, w_up, w_down, rope_cos, rope_sin):
        z_pos = lax.axis_index("z")
        y_pos = lax.axis_index("y")
        c_pos = lax.axis_index("c")
        even_y = y_pos % 2 == 0
        first_c = c_pos == 0
        pos = jnp.stack([z_pos, c_pos, y_pos % 2]).astype(jnp.int32)
        head = 2 * rope_cos.shape[1]
        seq = rope_cos.shape[0]
        ff_blk = w_gate.shape[1] // 2
        o_blk = w_out.shape[0] // 2
        qkv_blk = o_blk + head

        def gather_rows(blocks):
            return [turn(jnp.where(even_y, blocks[flip], blocks[1 - flip]), flip) for flip in range(2)]

        def gather_weight(piece):
            left, right = [], []
            for part in (1, 0):
                left.insert(0, hop_z(piece[part], 1))
                right.insert(0, hop_z(piece[part], -1))
            far = [hop_z(left[0], 1), hop_z(right[1], -1)]
            parts = []
            for mine in (piece, right, far, left):
                parts.append((mine, [swap_c(half) for half in mine]))
            return parts

        def grad_start(pairs, *earlier):
            far0, far1, up0, up1, down0, down1, own0, own1 = grad_pieces(after(pos, *earlier), pairs)
            far = (hop_z(far0, 1), hop_z(far1, -1))
            direct = (hop_z(up1, 1), hop_z(down0, -1))
            return (up0, down1), far, direct, (own0, own1)

        def grad_pass(state, *earlier):
            (up0, down1), far, direct, own = state
            sums = (up0 + after(far[0], *earlier), down1 + far[1])
            passed = (hop_z(sums[0], 1), hop_z(sums[1], -1))
            return direct, passed, own, sums

        def grad_back(state, *earlier):
            direct, passed, own = state[:3]
            first = own[0] + after(passed[0], *earlier) + direct[1]
            second = own[1] + direct[0] + passed[1]
            return turn(first, 0), turn(second, 1)

        def my_rows(val, mine):
            return lax.dynamic_slice_in_dim(val, (c_pos if mine else 1 - c_pos) * seq, seq, axis=0)

        def both_rows(own, got):
            return jnp.concatenate([jnp.where(first_c, own, got), jnp.where(first_c, got, own)], axis=0)

        cos_tab = jnp.concatenate([rope_cos, rope_cos], axis=1)
        sin_tab = jnp.concatenate([-rope_sin, rope_sin], axis=1)

        def qkv_cols(bit):
            first = 2 * head * bit
            third = HEAD_GROUP * head + head * bit
            return [w_qkv[:, first : first + 2 * head], w_qkv[:, third : third + head]]

        def block(weight, bit):
            size = weight.shape[1] // 2
            return weight[:, bit * size : (bit + 1) * size]

        down_t = w_down.T
        out_t = w_out.T
        wf_piece = gather_rows([jnp.concatenate([block(w_gate, j), block(w_up, j), *qkv_cols(j)], axis=1) for j in range(2)])
        ws_piece = gather_rows([jnp.concatenate([block(down_t, j), block(out_t, j)], axis=1) for j in range(2)])

        x_rows = after(x_in[0], cos_tab, sin_tab).astype(F32)
        normed, norm_pull = jax.vjp(lambda row_vals: norm_fwd(row_vals, norm_gain), x_rows)
        h_all = lax.all_gather(after(normed.astype(BF16), wf_piece[0], wf_piece[1]), ("y", "x"), axis=0, tiled=True)
        dy_all = lax.all_gather(after(dy_in[0], *wf_piece), ("y", "x"), axis=0, tiled=True)
        wf_parts = gather_weight(wf_piece)
        ws_parts = gather_weight(ws_piece)

        gate_up, qkv_tok = nn_pieces(pos, h_all, wf_parts, (2 * ff_blk, qkv_blk), 512)
        third = qkv_tok[:, o_blk:]
        qkv_other = swap_c(my_rows(qkv_tok, False))
        third_own = swap_y(my_rows(third, True))
        third_other = swap_yc(my_rows(third, False))
        act_val, act_t = act_fwd(after(gate_up, qkv_tok))
        act_recv = swap_c(act_t)
        qkv_seq, attn_own, attn_other = attn_fwd(after(pos, act_t), qkv_tok, qkv_other, third_own, third_other, cos_tab, sin_tab)
        attn_got = swap_c(attn_other)
        y_part = nt_pieces(after(pos, attn_own), [act_val, attn_own, attn_got], ws_parts)
        mix_sum = lax.psum_scatter(y_part, ("y", "x"), scatter_dimension=0, tiled=True)
        y_out = (x_rows + mix_sum).astype(BF16)[None]

        dy_picked = pick_cols(after(pos, y_part), dy_all)
        dy_recv = swap_c(dy_picked)
        h_picked = pick_cols(after(pos, dy_picked), h_all)
        h_recv = swap_c(h_picked)
        g_act = grad_start([(act_t, act_recv, dy_all, dy_recv, ff_blk, 0)], h_picked)
        d_act, d_attn = nn_pieces(after(pos, g_act[3][0]), dy_all, ws_parts, (ff_blk, o_blk), 256)
        d_attn_other = swap_c(my_rows(d_attn, False))
        d_gate_up, d_gate_up_t = act_bwd(gate_up, d_act)
        d_gate_up_recv = swap_c(d_gate_up_t)
        d_queries, keep, send = attn_bwd(after(pos, d_gate_up_t), qkv_seq, d_attn, d_attn_other, cos_tab, sin_tab)
        got = swap_y(send)
        g_act = grad_pass(g_act, d_queries)
        g_gate = grad_start([(d_gate_up_t, d_gate_up_recv, h_all, h_recv, ff_blk, 0)], *g_act[3])
        b_act = grad_back(g_act, g_gate[3][0])
        d_own, d_other = attn_post(after(pos, g_gate[3][0]), d_queries, keep, got, cos_tab, sin_tab)
        d_got = swap_c(d_other)
        dh_part = nt_pieces(pos, [d_gate_up, d_own, d_got], wf_parts)
        d_h = lax.psum_scatter(dh_part, ("y", "x"), scatter_dimension=0, tiled=True)
        d_h = d_h.astype(BF16)
        dx_out = (dy_in[0].astype(F32) + norm_pull(d_h.astype(F32))[0]).astype(BF16)[None]
        g_up = grad_start([(d_gate_up_t, d_gate_up_recv, h_all, h_recv, ff_blk, 1)], dh_part)
        g_gate = grad_pass(g_gate, dh_part)

        attn_t = both_rows(attn_own, attn_got).T
        d_qkv_t = both_rows(d_own, d_got).T
        attn_recv = swap_c(attn_t)
        d_qkv_recv = swap_c(d_qkv_t)
        g_attn = grad_start([(attn_t, attn_recv, dy_all, dy_recv, o_blk, 0), (d_qkv_t, d_qkv_recv, h_all, h_recv, qkv_blk, 0)], *g_gate[3])
        g_up = grad_pass(g_up, g_attn[3][0])
        g_attn = grad_pass(g_attn)
        b_gate = grad_back(g_gate)
        b_up = grad_back(g_up)
        b_attn = grad_back(g_attn)
        dw_down = place(pos, *b_act, ff_blk, 0, False)
        dw_gate = place(pos, *b_gate, ff_blk, 0, True)
        dw_up = place(pos, *b_up, ff_blk, 0, True)
        dw_out, dw_qkv = place_attn(after(pos, dx_out, dw_up), *b_attn, o_blk, head)
        return y_out, dx_out, dw_qkv, dw_out, dw_gate, dw_up, dw_down


    return jax.shard_map(
        layer,
        mesh=wide_mesh,
        in_specs=(act_spec, act_spec, P(), col_spec, row_spec, col_spec, col_spec, row_spec, P(), P()),
        out_specs=(act_spec, act_spec, col_spec, row_spec, col_spec, col_spec, row_spec),
        check_vma=False,
    )
```

```python
import functools

import jax
import jax.numpy as jnp
from jax import lax
from jax.experimental import pallas as pl
from jax.experimental.pallas import tpu as pltpu
from jax.sharding import Mesh, PartitionSpec as P


NORM_EPS = 1e-5
NZ = 4
NY = 4
NX = 4
NC = 2
HEAD_GROUP = 4
F32 = jnp.float32
BF16 = jnp.bfloat16
VMEM_LIMIT = 67043328


def norm_fwd(row_vals, norm_gain):
    return row_vals * lax.rsqrt(jnp.mean(row_vals * row_vals, axis=-1, keepdims=True) + NORM_EPS) * norm_gain


def rotate(wide, cos_tab, sin_tab):
    return wide * cos_tab + pltpu.roll(wide, wide.shape[-1] // 2, wide.ndim - 1) * sin_tab


def rotate_back(wide, cos_tab, sin_tab):
    return wide * cos_tab - pltpu.roll(wide, wide.shape[-1] // 2, wide.ndim - 1) * sin_tab


def cost(flops, bytes_accessed):
    return pl.CostEstimate(flops=int(flops) // 20, bytes_accessed=int(bytes_accessed), transcendentals=0)


def params(**extra):
    return pltpu.CompilerParams(vmem_limit_bytes=VMEM_LIMIT, **extra)


def head_probs(q_rot, k_rot, scale):
    scores = dot_nt(q_rot, k_rot) * scale
    row_ids = lax.broadcasted_iota(jnp.int32, scores.shape, 0)
    col_ids = lax.broadcasted_iota(jnp.int32, scores.shape, 1)
    scores = jnp.where(row_ids >= col_ids, scores, -1e30)
    weights = jnp.exp(scores - jnp.max(scores, axis=-1, keepdims=True))
    return weights / jnp.sum(weights, axis=-1, keepdims=True)


def half_rows(core, idx, chunk):
    return pl.ds(pl.multiple_of((NC * idx + core) * chunk, chunk), chunk)


def chunk_rows(idx, chunk):
    return slice(idx * chunk, (idx + 1) * chunk)


def attn_fwd_kernel(heads, head, pos_ref, own_ref, other_ref, own_third_ref, other_third_ref, cos_ref, sin_ref, seq_ref, o_ref, o_other_ref, o_buf):
    core, odd = pos_ref[1], pos_ref[2]
    chunk = own_ref.shape[0] // NX
    width = heads * head
    mine = pl.ds(pl.multiple_of(width + odd * head, head), head)
    theirs = pl.ds(pl.multiple_of(width + (1 - odd) * head, head), head)
    for side, part_ref, third_ref in ((core, own_ref, own_third_ref), (1 - core, other_ref, other_third_ref)):
        for idx in range(NX):
            rows = half_rows(side, idx, chunk)
            seq_ref[0, rows, pl.ds(0, width)] = part_ref[chunk_rows(idx, chunk), :width]
            seq_ref[0, rows, mine] = part_ref[chunk_rows(idx, chunk), width:]
            seq_ref[0, rows, theirs] = third_ref[chunk_rows(idx, chunk), :]
    cos_tab, sin_tab = cos_ref[...], sin_ref[...]
    k_rot = rotate(seq_ref[0, :, width : width + head].astype(F32), cos_tab, sin_tab).astype(BF16)
    values = seq_ref[0, :, width + head :]
    for idx in range(heads):
        lanes = slice(idx * head, (idx + 1) * head)
        q_rot = rotate(seq_ref[0, :, lanes].astype(F32), cos_tab, sin_tab).astype(BF16)
        probs = head_probs(q_rot, k_rot, head**-0.5)
        o_buf[:, lanes] = dot_nn(probs.astype(BF16), values).astype(BF16)
    for side, out_ref in ((core, o_ref), (1 - core, o_other_ref)):
        for idx in range(NX):
            out_ref[chunk_rows(idx, chunk), :] = o_buf[half_rows(side, idx, chunk), :]


def attn_bwd_kernel(heads, head, pos_ref, seq_ref, own_ref, other_ref, cos_ref, sin_ref, dq_ref, keep_ref, send_ref, do_buf):
    core, odd = pos_ref[1], pos_ref[2]
    chunk = own_ref.shape[0] // NX
    width = heads * head
    for side, part_ref in ((core, own_ref), (1 - core, other_ref)):
        for idx in range(NX):
            do_buf[half_rows(side, idx, chunk), :] = part_ref[chunk_rows(idx, chunk), :]
    cos_tab, sin_tab = cos_ref[...], sin_ref[...]
    k_rot = rotate(seq_ref[0, :, width : width + head].astype(F32), cos_tab, sin_tab).astype(BF16)
    values = seq_ref[0, :, width + head :]
    d_keys = jnp.zeros(k_rot.shape, F32)
    d_values = jnp.zeros(k_rot.shape, F32)
    for idx in range(heads):
        lanes = slice(idx * head, (idx + 1) * head)
        q_rot = rotate(seq_ref[0, :, lanes].astype(F32), cos_tab, sin_tab).astype(BF16)
        d_out = do_buf[:, lanes]
        probs = head_probs(q_rot, k_rot, head**-0.5)
        d_values += dot_tn(probs.astype(BF16), d_out)
        d_probs = dot_nt(d_out, values).astype(BF16).astype(F32)
        d_scores = probs * (d_probs - jnp.sum(d_probs * probs, axis=-1, keepdims=True))
        d_scores = (d_scores * head**-0.5).astype(BF16)
        d_q_rot = dot_nn(d_scores, k_rot).astype(BF16)
        dq_ref[0, :, lanes] = rotate_back(d_q_rot.astype(F32), cos_tab, sin_tab).astype(BF16)
        d_keys += dot_tn(d_scores, q_rot)

    @pl.when(odd == 0)
    def _():
        keep_ref[0] = d_keys
        send_ref[0] = d_values

    @pl.when(odd == 1)
    def _():
        keep_ref[0] = d_values
        send_ref[0] = d_keys


def attn_post_kernel(heads, head, pos_ref, dq_ref, keep_ref, got_ref, cos_ref, sin_ref, own_ref, other_ref, third_buf):
    core, odd = pos_ref[1], pos_ref[2]
    chunk = own_ref.shape[0] // NX
    width = heads * head
    total = (keep_ref[0] + got_ref[0]).astype(BF16)

    @pl.when(odd == 0)
    def _():
        third_buf[...] = rotate_back(total.astype(F32), cos_ref[...], sin_ref[...]).astype(BF16)

    @pl.when(odd == 1)
    def _():
        third_buf[...] = total

    for side, out_ref in ((core, own_ref), (1 - core, other_ref)):
        for idx in range(NX):
            rows = half_rows(side, idx, chunk)
            out_ref[chunk_rows(idx, chunk), :width] = dq_ref[0, rows, :]
            out_ref[chunk_rows(idx, chunk), width:] = third_buf[rows, :]


def per_sequence(kernel, pos, args, specs, out_specs, out_shape, scratch, flops):
    return pl.pallas_call(
        kernel,
        grid_spec=pltpu.PrefetchScalarGridSpec(num_scalar_prefetch=1, grid=(2,), in_specs=specs, out_specs=out_specs, scratch_shapes=scratch),
        out_shape=out_shape,
        compiler_params=params(),
        cost_estimate=cost(flops, 4e6),
    )(pos, *args)


def own_spec(rows, width):
    return pl.BlockSpec((rows, width), lambda i, pos: (2 * pos[1] + i, 0))


def pair_spec(rows, width):
    return pl.BlockSpec((rows, width), lambda i, pos: (i, 0))


def seq_spec(seq, width):
    return pl.BlockSpec((1, seq, width), lambda i, pos: (i, 0, 0))


def table_spec(table):
    return pl.BlockSpec(table.shape, lambda i, pos: (0, 0))


def attn_fwd(pos, qkv_tok, other, own_third, other_third, cos_tab, sin_tab):
    seq, head = cos_tab.shape
    width = qkv_tok.shape[1] - head
    rows = seq // 2
    half = jax.ShapeDtypeStruct((seq, width), BF16)
    return per_sequence(
        functools.partial(attn_fwd_kernel, width // head, head),
        pos,
        (qkv_tok, other, own_third, other_third, cos_tab, sin_tab),
        [own_spec(rows, width + head), pair_spec(rows, width + head), pair_spec(rows, head), pair_spec(rows, head), table_spec(cos_tab), table_spec(sin_tab)],
        [seq_spec(seq, width + 2 * head), pair_spec(rows, width), pair_spec(rows, width)],
        [jax.ShapeDtypeStruct((2, seq, width + 2 * head), BF16), half, half],
        [pltpu.VMEM((seq, width), BF16)],
        16e9,
    )


def attn_bwd(pos, qkv_seq, d_attn, other, cos_tab, sin_tab):
    seq, head = cos_tab.shape
    width = d_attn.shape[1]
    rows = seq // 2
    part = jax.ShapeDtypeStruct((2, seq, head), F32)
    return per_sequence(
        functools.partial(attn_bwd_kernel, width // head, head),
        pos,
        (qkv_seq, d_attn, other, cos_tab, sin_tab),
        [seq_spec(seq, width + 2 * head), own_spec(rows, width), pair_spec(rows, width), table_spec(cos_tab), table_spec(sin_tab)],
        [seq_spec(seq, width), seq_spec(seq, head), seq_spec(seq, head)],
        [jax.ShapeDtypeStruct((2, seq, width), BF16), part, part],
        [pltpu.VMEM((seq, width), BF16)],
        16e9,
    )


def attn_post(pos, d_queries, keep, got, cos_tab, sin_tab):
    seq, head = cos_tab.shape
    width = d_queries.shape[2]
    rows = seq // 2
    half = jax.ShapeDtypeStruct((seq, width + head), BF16)
    return per_sequence(
        functools.partial(attn_post_kernel, width // head, head),
        pos,
        (d_queries, keep, got, cos_tab, sin_tab),
        [seq_spec(seq, width), seq_spec(seq, head), seq_spec(seq, head), table_spec(cos_tab), table_spec(sin_tab)],
        [pair_spec(rows, width + head), pair_spec(rows, width + head)],
        [half, half],
        [pltpu.VMEM((seq, head), BF16)],
        2e9,
    )


def act_fwd_kernel(half, ab_ref, u_ref, ut_ref):
    gate_val = ab_ref[:, :half].astype(F32)
    up_val = ab_ref[:, half:].astype(F32)
    act_val = gate_val * jax.nn.sigmoid(gate_val) * up_val
    u_ref[...] = act_val.astype(BF16)
    ut_ref[...] = act_val.T.astype(BF16)


def act_fwd(gate_up):
    tokens, width = gate_up.shape
    half = width // 2
    rows = tokens // 4
    return pl.pallas_call(
        functools.partial(act_fwd_kernel, half),
        grid=(4,),
        in_specs=[pl.BlockSpec((rows, width), lambda i: (i, 0))],
        out_specs=[pl.BlockSpec((rows, half), lambda i: (i, 0)), pl.BlockSpec((half, rows), lambda i: (0, i))],
        out_shape=[jax.ShapeDtypeStruct((tokens, half), BF16), jax.ShapeDtypeStruct((half, tokens), BF16)],
        compiler_params=params(),
        cost_estimate=cost(4e9, 8e6),
        name="act_fwd",
    )(gate_up)


def act_bwd_kernel(half, ab_ref, du_ref, dab_ref, dabt_ref):
    gate_val = ab_ref[:, :half].astype(F32)
    up_val = ab_ref[:, half:].astype(F32)
    d_act = du_ref[...].astype(F32)
    sig = jax.nn.sigmoid(gate_val)
    d_silu = d_act * up_val
    d_gate = d_silu * sig + d_silu * gate_val * (sig * (1.0 - sig))
    d_up = d_act * (gate_val * sig)
    dab_ref[:, :half] = d_gate.astype(BF16)
    dab_ref[:, half:] = d_up.astype(BF16)
    dabt_ref[:half, :] = d_gate.T.astype(BF16)
    dabt_ref[half:, :] = d_up.T.astype(BF16)


def act_bwd(gate_up, d_mixed):
    tokens, width = gate_up.shape
    half = width // 2
    rows = tokens // 4
    return pl.pallas_call(
        functools.partial(act_bwd_kernel, half),
        grid=(4,),
        in_specs=[pl.BlockSpec((rows, width), lambda i: (i, 0)), pl.BlockSpec((rows, half), lambda i: (i, 0))],
        out_specs=[pl.BlockSpec((rows, width), lambda i: (i, 0)), pl.BlockSpec((width, rows), lambda i: (0, i))],
        out_shape=[jax.ShapeDtypeStruct((tokens, width), BF16), jax.ShapeDtypeStruct((width, tokens), BF16)],
        compiler_params=params(),
        cost_estimate=cost(8e9, 14e6),
        name="act_bwd",
    )(gate_up, d_mixed)


def piece_block(pos_ref, step, other):
    core = pos_ref[1]
    return lax.rem(pos_ref[0] + step, NZ) * NC + (1 - core if other else core)


def half_start(pos_ref, part, half):
    return pl.multiple_of((1 - pos_ref[2] if part else pos_ref[2]) * half, half)


def nn_kernel(keys, first, count_out, tile, pos_ref, acts_ref, *refs):
    count = len(keys)
    halves = refs[: 2 * count]
    outs = refs[2 * count : 2 * count + count_out]
    acts_buf, w_buf, total, acts_sem, w_sem = refs[2 * count + count_out :]
    block = acts_buf.shape[1] // count
    half = block // 2
    copies = []
    for idx in range(count):
        cols = pl.ds(pl.multiple_of(piece_block(pos_ref, *keys[idx]) * block, block), block)
        copies.append([pltpu.make_async_copy(acts_ref.at[:, cols], acts_buf.at[:, pl.ds(idx * block, block)], acts_sem.at[idx])])
        for part in range(2):
            rows = pl.ds(idx * block + half_start(pos_ref, part, half), half)
            copies[-1].append(pltpu.make_async_copy(halves[2 * idx + part], w_buf.at[rows], w_sem.at[2 * idx + part]))
    for group in copies:
        for copy in group:
            copy.start()
    for lo, hi in ((0, first), (first, count)):
        for group in copies[lo:hi]:
            for copy in group:
                copy.wait()
        depth = pl.ds(lo * block, (hi - lo) * block)
        start = 0
        for out_ref in outs:
            width = out_ref.shape[1]

            def step(out_lo, size, start=start, out_ref=out_ref, depth=depth, hi=hi):
                cols = pl.ds(pl.multiple_of(start + out_lo, 128), size)
                part = dot_nn(acts_buf[:, depth], w_buf[depth, cols])
                if hi == count:
                    out_ref[:, pl.ds(pl.multiple_of(out_lo, 128), size)] = (total[:, cols] + part).astype(BF16)
                else:
                    total[:, cols] = part

            whole = width // tile
            if whole:
                pl.loop(0, whole)(lambda n: step(n * tile, tile))
            if width % tile:
                step(whole * tile, width % tile)
            start += width


def nn_pieces(pos, acts, parts, widths, tile):
    keys = [(step, other) for step in (0, 1, 3, 2) for other in range(2)]
    halves = [parts[step][other][part] for step, other in keys for part in range(2)]
    tokens, depth = acts.shape
    width = sum(widths)
    count = len(keys)
    anywhere = pl.BlockSpec(memory_space=pl.ANY)
    return pl.pallas_call(
        functools.partial(nn_kernel, keys, 2, len(widths), tile),
        grid_spec=pltpu.PrefetchScalarGridSpec(
            num_scalar_prefetch=1,
            grid=(1,),
            in_specs=[anywhere] * (1 + 2 * count),
            out_specs=[pl.BlockSpec((tokens, size), lambda i, pos: (0, 0)) for size in widths],
            scratch_shapes=[
                pltpu.VMEM((tokens, depth), BF16),
                pltpu.VMEM((depth, width), BF16),
                pltpu.VMEM((tokens, width), F32),
                pltpu.SemaphoreType.DMA((count,)),
                pltpu.SemaphoreType.DMA((2 * count,)),
            ],
        ),
        out_shape=[jax.ShapeDtypeStruct((tokens, size), BF16) for size in widths],
        compiler_params=params(),
        cost_estimate=cost(2 * tokens * depth * width, 2 * depth * (tokens + width)),
    )(pos, acts, *halves)


def nt_kernel(keys, sides, first_row, pos_ref, *refs):
    count_left = len(sides)
    count = len(keys)
    lefts = refs[:count_left]
    halves = refs[count_left : count_left + 2 * count]
    out_ref, left_buf, w_buf, out_buf, left_sem, w_sem, out_sem = refs[count_left + 2 * count :]
    block = out_buf.shape[2]
    half = block // 2
    slots = w_buf.shape[0]
    left_copies = []
    start = 0
    for idx, (left, side) in enumerate(zip(lefts, sides)):
        chunks, _, width = left.shape
        first = 0 if side is None else (1 - pos_ref[1] if side else pos_ref[1]) * chunks
        source = left.at[:, pl.ds(first_row, left_buf.shape[1]), :]
        left_copies.append(pltpu.make_async_copy(source, left_buf.at[pl.ds(first, chunks), :, pl.ds(start, width)], left_sem.at[idx]))
        left_copies[-1].start()
        start += 0 if side == 0 else width

    def copies(idx, slot):
        for part in range(2):
            rows = pl.ds(half_start(pos_ref, part, half), half)
            yield pltpu.make_async_copy(halves[2 * idx + part], w_buf.at[slot, rows], w_sem.at[slot, part])

    def out_copy(idx):
        core = pos_ref[1]
        other = lax.rem(idx, 2)
        block_id = lax.rem(pos_ref[0] + idx // 2, NZ) * NC + core + other - 2 * core * other
        slot = lax.rem(idx, 2)
        return pltpu.make_async_copy(out_buf.at[slot], out_ref.at[:, pl.ds(pl.multiple_of(block_id * block, block), block)], out_sem.at[slot])

    for idx in range(slots - 1):
        for copy in copies(idx, idx):
            copy.start()
    for copy in left_copies:
        copy.wait()

    @pl.loop(0, count)
    def _(step):
        slot = lax.rem(step, slots)
        for idx in range(slots - 1, count):

            @pl.when(step + slots - 1 == idx)
            def _(idx=idx):
                for copy in copies(idx, idx % slots):
                    copy.start()

        for copy in copies(0, slot):
            copy.wait()

        @pl.when(step >= 2)
        def _():
            out_copy(step - 2).wait()

        out_buf[lax.rem(step, 2)] = dot_nt(left_buf[...].reshape(out_buf.shape[1], left_buf.shape[2]), w_buf[slot])
        out_copy(step).start()

    for idx in range(count - 2, count):
        out_copy(idx).wait()


def nt_pieces(pos, lefts, parts, chunk, first_row, rows):
    sides = (None, 0, 1)
    keys = [(step, other) for step in range(NZ) for other in range(2)]
    halves = [parts[step][other][part] for step, other in keys for part in range(2)]
    lefts = [left.reshape(-1, chunk, left.shape[1]) for left in lefts]
    chunks = lefts[0].shape[0]
    tokens = chunks * rows
    block = 2 * halves[0].shape[0]
    depth = block * len(keys)
    width = halves[0].shape[1]
    slots = 3
    anywhere = pl.BlockSpec(memory_space=pl.ANY)
    return pl.pallas_call(
        functools.partial(nt_kernel, keys, sides, first_row),
        grid_spec=pltpu.PrefetchScalarGridSpec(
            num_scalar_prefetch=1,
            grid=(1,),
            in_specs=[anywhere] * (len(lefts) + len(halves)),
            out_specs=anywhere,
            scratch_shapes=[
                pltpu.VMEM((chunks, rows, width), BF16),
                pltpu.VMEM((slots, block, width), BF16),
                pltpu.VMEM((2, tokens, block), F32),
                pltpu.SemaphoreType.DMA((len(lefts),)),
                pltpu.SemaphoreType.DMA((slots, 2)),
                pltpu.SemaphoreType.DMA((2,)),
            ],
        ),
        out_shape=jax.ShapeDtypeStruct((tokens, depth), F32),
        compiler_params=params(),
        cost_estimate=cost(2 * tokens * depth * width, 2 * depth * width + 4 * tokens * depth),
    )(pos, *lefts, *halves)


def picked_cols(pos_ref, idx, block):
    return pl.ds(pl.multiple_of((NC * idx + 1 - pos_ref[1]) * block, block), block)


def dma_kernel(kernel, pos, args, out_shape, scratch):
    anywhere = pl.BlockSpec(memory_space=pl.ANY)
    return pl.pallas_call(
        kernel,
        grid_spec=pltpu.PrefetchScalarGridSpec(
            num_scalar_prefetch=1, grid=(1,), in_specs=[anywhere] * len(args), out_specs=[anywhere] * len(out_shape), scratch_shapes=scratch
        ),
        out_shape=out_shape,
        compiler_params=params(),
        cost_estimate=cost(3e9, 16e6),
    )(pos, *args)


def pick_cols(pos, acts):
    tokens, depth = acts.shape
    block = depth // (NC * NZ)

    def kernel(pos_ref, in_ref, out_ref, buf, in_sem, out_sem):
        reads = [pltpu.make_async_copy(in_ref.at[:, picked_cols(pos_ref, idx, block)], buf.at[idx], in_sem.at[idx]) for idx in range(NZ)]
        writes = [pltpu.make_async_copy(buf.at[idx], out_ref.at[:, pl.ds(idx * block, block)], out_sem.at[idx]) for idx in range(NZ)]
        for read in reads:
            read.start()
        for read, write in zip(reads, writes):
            read.wait()
            write.start()
        for write in writes:
            write.wait()

    sems = pltpu.SemaphoreType.DMA((NZ,))
    return dma_kernel(kernel, pos, [acts], [jax.ShapeDtypeStruct((tokens, depth // 2), BF16)], [pltpu.VMEM((NZ, tokens, block), BF16), sems, sems])[0]


def grad_kernel(heights, pos_ref, *refs):
    pairs = len(heights)
    ins = refs[: 4 * pairs]
    outs = refs[4 * pairs : 4 * pairs + 2 * NZ]
    buf, sem = refs[4 * pairs + 2 * NZ :]
    half = buf.shape[2] // 2
    step = pl.program_id(0)
    slot = lax.rem(step, 2)

    def out_copy(idx, part):
        cols = pl.ds(half_start(pos_ref, part, half), half)
        return pltpu.make_async_copy(buf.at[idx % 2, :, cols], outs[2 * idx + part], sem.at[idx % 2, part])

    for idx in range(2, NZ):

        @pl.when(step == idx)
        def _(idx=idx):
            for part in range(2):
                out_copy(idx - 2, part).wait()

    start = 0
    for idx, height in enumerate(heights):
        own, recv, acts, acts_recv = ins[4 * idx : 4 * idx + 4]
        buf[slot, start : start + height, :] = dot_nn(own[...], acts[...]) + dot_nn(recv[...], acts_recv[...])
        start += height
    for idx in range(NZ):

        @pl.when(step == idx)
        def _(idx=idx):
            for part in range(2):
                out_copy(idx, part).start()

    @pl.when(step == NZ - 1)
    def _():
        for idx in (NZ - 2, NZ - 1):
            for part in range(2):
                out_copy(idx, part).wait()


def grad_pieces(pos, pairs):
    tokens, depth = pairs[0][2].shape
    cols = depth // (NZ * NC)
    in_specs = []
    args = []

    def z_of(n, pos):
        return lax.rem(pos[0] + jnp.where(n == 0, 2, jnp.where(n == 1, 1, jnp.where(n == 2, 3, 0))), NZ)

    for own, recv, acts, acts_recv, height, block in pairs:
        in_specs += [pl.BlockSpec((height, tokens), lambda n, pos, block=block: (block, 0))] * 2
        in_specs.append(pl.BlockSpec((tokens, cols), lambda n, pos: (0, z_of(n, pos) * NC + pos[1])))
        in_specs.append(pl.BlockSpec((tokens, cols), lambda n, pos: (0, z_of(n, pos))))
        args += [own, recv, acts, acts_recv]
    heights = [pair[4] for pair in pairs]
    rows = sum(heights)
    return pl.pallas_call(
        functools.partial(grad_kernel, heights),
        grid_spec=pltpu.PrefetchScalarGridSpec(
            num_scalar_prefetch=1,
            grid=(NZ,),
            in_specs=in_specs,
            out_specs=[pl.BlockSpec(memory_space=pl.ANY)] * (2 * NZ),
            scratch_shapes=[pltpu.VMEM((2, rows, cols), F32), pltpu.SemaphoreType.DMA((2, 2))],
        ),
        out_shape=[jax.ShapeDtypeStruct((rows, cols // 2), F32)] * (2 * NZ),
        compiler_params=params(),
        cost_estimate=cost(4 * rows * tokens * cols * NZ, 4 * tokens * cols * NZ),
        name="grad",
    )(pos, *args)


def place(pos, first, second, height, block, transpose):
    cols = first.shape[1]
    spec = pl.BlockSpec((height, cols), lambda n, pos: (block, 0))

    def kernel(pos_ref, first_ref, second_ref, out_ref):
        for idx, ref in enumerate((first_ref, second_ref)):

            @pl.when(pl.program_id(0) == idx)
            def _(ref=ref):
                out_ref[...] = ref[...].T if transpose else ref[...]

    def order(n, pos):
        return jnp.where(n == 0, pos[2], 1 - pos[2])

    return pl.pallas_call(
        kernel,
        grid_spec=pltpu.PrefetchScalarGridSpec(
            num_scalar_prefetch=1,
            grid=(2,),
            in_specs=[spec, spec],
            out_specs=pl.BlockSpec((cols, height), lambda n, pos: (0, order(n, pos))) if transpose else pl.BlockSpec((height, cols), lambda n, pos: (order(n, pos), 0)),
        ),
        out_shape=jax.ShapeDtypeStruct((cols, 2 * height) if transpose else (2 * height, cols), F32),
        compiler_params=params(),
        cost_estimate=cost(2e9, 16 * height * cols),
    )(pos, first, second)


def place_attn(pos, first, second, o_blk, head):
    rows, cols = first.shape
    qk = 2 * head

    def kernel(pos_ref, first_ref, second_ref, out_ref, qkv_ref):
        for idx, ref in enumerate((first_ref, second_ref)):
            bit = 1 - pos_ref[2] if idx else pos_ref[2]
            out_ref[pl.ds(pl.multiple_of(bit * o_blk, o_blk), o_blk), :] = ref[:o_blk, :]
            qkv_ref[:, pl.ds(pl.multiple_of(bit * qk, qk), qk)] = ref[o_blk : o_blk + qk, :].T
            qkv_ref[:, pl.ds(pl.multiple_of(2 * qk + bit * head, head), head)] = ref[o_blk + qk :, :].T

    def whole(*shape):
        return pl.BlockSpec(shape, lambda n, pos: (0, 0))

    shapes = ((2 * o_blk, cols), (cols, 2 * (qk + head)))
    return pl.pallas_call(
        kernel,
        grid_spec=pltpu.PrefetchScalarGridSpec(num_scalar_prefetch=1, grid=(1,), in_specs=[whole(rows, cols)] * 2, out_specs=[whole(*shape) for shape in shapes]),
        out_shape=[jax.ShapeDtypeStruct(shape, F32) for shape in shapes],
        compiler_params=params(),
        cost_estimate=cost(2e9, 16 * rows * cols),
        name="p_attn",
    )(pos, first, second)


def after(val, *earlier):
    return lax.optimization_barrier((val, *earlier))[0]


def ring(step, size):
    return [(src, (src + step) % size) for src in range(size)]


def hop_z(val, step):
    return lax.ppermute(val, "z", ring(step, NZ))


def swap_c(val):
    return lax.ppermute(val, "c", [(0, 1), (1, 0)])


def swap_y(val):
    return lax.ppermute(val, "y", [(src, src ^ 1) for src in range(NY)])


def turn(val, flip):
    def place_of(y_pos, c_pos):
        return y_pos * NC + c_pos

    pairs = [(place_of(2 * a + b, c), place_of(2 * c + (b ^ flip), a)) for a in range(2) for b in range(2) for c in range(NC)]
    return lax.ppermute(val, ("y", "c"), pairs)


def swap_yc(val):
    pairs = [(y_pos * NC + c_pos, (y_pos ^ 1) * NC + 1 - c_pos) for y_pos in range(NY) for c_pos in range(NC)]
    return lax.ppermute(val, ("y", "c"), pairs)


def dot_nn(left, right):
    return lax.dot_general(left, right, (((1,), (0,)), ((), ())), preferred_element_type=F32)


def dot_nt(left, right):
    return lax.dot_general(left, right, (((1,), (1,)), ((), ())), preferred_element_type=F32)


def dot_tn(left, right):
    return lax.dot_general(left, right, (((0,), (0,)), ((), ())), preferred_element_type=F32)


def solution(mesh):
    wide_mesh = Mesh(mesh.devices.reshape(NZ, NY, NX, NC), ("z", "y", "x", "c"))
    rows = ("z", "y")
    cols = ("x", "c")
    act_spec = P(rows, cols, None)
    col_spec = P(rows, cols)
    row_spec = P(cols, rows)

    def layer(x_in, dy_in, norm_gain, w_qkv, w_out, w_gate, w_up, w_down, rope_cos, rope_sin):
        z_pos = lax.axis_index("z")
        y_pos = lax.axis_index("y")
        c_pos = lax.axis_index("c")
        even_y = y_pos % 2 == 0
        first_c = c_pos == 0
        pos = jnp.stack([z_pos, c_pos, y_pos % 2]).astype(jnp.int32)
        chunk = x_in.shape[1]
        head = 2 * rope_cos.shape[1]
        seq = rope_cos.shape[0]
        ff_blk = w_gate.shape[1] // 2
        o_blk = w_out.shape[0] // 2
        qkv_blk = o_blk + head

        def gather_rows(blocks):
            return [turn(jnp.where(even_y, blocks[flip], blocks[1 - flip]), flip) for flip in range(2)]

        def gather_weight(piece):
            left, right = [], []
            for part in (1, 0):
                left.insert(0, hop_z(piece[part], 1))
                right.insert(0, hop_z(piece[part], -1))
            far = [hop_z(left[0], 1), hop_z(right[1], -1)]
            parts = []
            for mine in (piece, right, far, left):
                parts.append((mine, [swap_c(half) for half in mine]))
            return parts

        def grad_start(pairs, *earlier):
            far0, far1, up0, up1, down0, down1, own0, own1 = grad_pieces(after(pos, *earlier), pairs)
            far = (hop_z(far0, 1), hop_z(far1, -1))
            direct = (hop_z(up1, 1), hop_z(down0, -1))
            return (up0, down1), far, direct, (own0, own1)

        def grad_pass(state, *earlier):
            (up0, down1), far, direct, own = state
            sums = (up0 + after(far[0], *earlier), down1 + far[1])
            passed = (hop_z(sums[0], 1), hop_z(sums[1], -1))
            return direct, passed, own, sums

        def grad_back(state, *earlier):
            direct, passed, own = state[:3]
            first = own[0] + after(passed[0], *earlier) + direct[1]
            second = own[1] + direct[0] + passed[1]
            return turn(first, 0), turn(second, 1)

        def my_rows(val, mine):
            return lax.dynamic_slice_in_dim(val, (c_pos if mine else 1 - c_pos) * seq, seq, axis=0)

        def both_rows(own, got):
            return jnp.concatenate([jnp.where(first_c, own, got), jnp.where(first_c, got, own)], axis=0)

        cos_tab = jnp.concatenate([rope_cos, rope_cos], axis=1)
        sin_tab = jnp.concatenate([-rope_sin, rope_sin], axis=1)

        def qkv_cols(bit):
            first = 2 * head * bit
            third = HEAD_GROUP * head + head * bit
            return [w_qkv[:, first : first + 2 * head], w_qkv[:, third : third + head]]

        def block(weight, bit):
            size = weight.shape[1] // 2
            return weight[:, bit * size : (bit + 1) * size]

        down_t = w_down.T
        out_t = w_out.T
        wf_piece = gather_rows([jnp.concatenate([block(w_gate, j), block(w_up, j), *qkv_cols(j)], axis=1) for j in range(2)])
        ws_piece = gather_rows([jnp.concatenate([block(down_t, j), block(out_t, j)], axis=1) for j in range(2)])

        x_rows = after(x_in[0], cos_tab, sin_tab).astype(F32)
        normed, norm_pull = jax.vjp(lambda row_vals: norm_fwd(row_vals, norm_gain), x_rows)
        h_all = lax.all_gather(after(normed.astype(BF16), wf_piece[0], wf_piece[1]), ("y", "x"), axis=0, tiled=True)
        dy_all = lax.all_gather(after(dy_in[0], *wf_piece), ("y", "x"), axis=0, tiled=True)
        wf_parts = gather_weight(wf_piece)
        ws_parts = gather_weight(ws_piece)

        gate_up, qkv_tok = nn_pieces(pos, h_all, wf_parts, (2 * ff_blk, qkv_blk), 512)
        third = qkv_tok[:, o_blk:]
        qkv_other = swap_c(my_rows(qkv_tok, False))
        third_own = swap_y(my_rows(third, True))
        third_other = swap_yc(my_rows(third, False))
        act_val, act_t = act_fwd(after(gate_up, qkv_tok))
        act_recv = swap_c(act_t)
        h_picked = pick_cols(after(pos, act_t), h_all)
        h_recv = swap_c(h_picked)
        qkv_seq, attn_own, attn_other = attn_fwd(after(pos, h_picked), qkv_tok, qkv_other, third_own, third_other, cos_tab, sin_tab)
        attn_got = swap_c(attn_other)
        y_part = nt_pieces(after(pos, attn_own), [act_val, attn_own, attn_got], ws_parts, chunk, 0, chunk)
        mix_sum = lax.psum_scatter(y_part, ("y", "x"), scatter_dimension=0, tiled=True)
        y_out = (x_rows + mix_sum).astype(BF16)[None]

        dy_picked = pick_cols(after(pos, y_part), dy_all)
        dy_recv = swap_c(dy_picked)
        g_act = grad_start([(act_t, act_recv, dy_all, dy_recv, ff_blk, 0)], dy_picked)
        d_act, d_attn = nn_pieces(after(pos, g_act[3][0]), dy_all, ws_parts, (ff_blk, o_blk), 256)
        d_attn_other = swap_c(my_rows(d_attn, False))
        d_gate_up, d_gate_up_t = act_bwd(gate_up, d_act)
        d_gate_up_recv = swap_c(d_gate_up_t)
        d_queries, keep, send = attn_bwd(after(pos, d_gate_up_t), qkv_seq, d_attn, d_attn_other, cos_tab, sin_tab)
        got = swap_y(send)
        g_act = grad_pass(g_act, d_queries)
        g_gate = grad_start([(d_gate_up_t, d_gate_up_recv, h_all, h_recv, ff_blk, 0)], *g_act[3])
        d_own, d_other = attn_post(after(pos, g_gate[3][0]), d_queries, keep, got, cos_tab, sin_tab)
        d_got = swap_c(d_other)
        half = chunk // 2
        dh_low = nt_pieces(pos, [d_gate_up, d_own, d_got], wf_parts, chunk, 0, half)
        d_h_low = lax.psum_scatter(dh_low, ("y", "x"), scatter_dimension=0, tiled=True)
        g_gate = grad_pass(g_gate, dh_low)
        g_up = grad_start([(d_gate_up_t, d_gate_up_recv, h_all, h_recv, ff_blk, 1)], *g_gate[3])
        dh_high = nt_pieces(after(pos, g_up[3][0]), [d_gate_up, d_own, d_got], wf_parts, chunk, half, half)
        d_h_high = lax.psum_scatter(dh_high, ("y", "x"), scatter_dimension=0, tiled=True)
        b_act = grad_back(g_act, dh_high)
        d_h = jnp.concatenate([d_h_low, d_h_high], axis=0).astype(BF16)
        dx_out = (dy_in[0].astype(F32) + norm_pull(d_h.astype(F32))[0]).astype(BF16)[None]

        attn_t = both_rows(attn_own, attn_got).T
        d_qkv_t = both_rows(d_own, d_got).T
        attn_recv = swap_c(attn_t)
        d_qkv_recv = swap_c(d_qkv_t)
        g_attn = grad_start([(attn_t, attn_recv, dy_all, dy_recv, o_blk, 0), (d_qkv_t, d_qkv_recv, h_all, h_recv, qkv_blk, 0)], dh_high)
        g_up = grad_pass(g_up, g_attn[3][0])
        g_attn = grad_pass(g_attn)
        b_gate = grad_back(g_gate)
        b_up = grad_back(g_up)
        b_attn = grad_back(g_attn)
        dw_down = place(pos, *b_act, ff_blk, 0, False)
        dw_gate = place(pos, *b_gate, ff_blk, 0, True)
        dw_up = place(pos, *b_up, ff_blk, 0, True)
        dw_out, dw_qkv = place_attn(after(pos, dx_out, dw_up), *b_attn, o_blk, head)
        return y_out, dx_out, dw_qkv, dw_out, dw_gate, dw_up, dw_down


    return jax.shard_map(
        layer,
        mesh=wide_mesh,
        in_specs=(act_spec, act_spec, P(), col_spec, row_spec, col_spec, col_spec, row_spec, P(), P()),
        out_specs=(act_spec, act_spec, col_spec, row_spec, col_spec, col_spec, row_spec),
        check_vma=False,
    )
```

```python
import functools

import jax
import jax.numpy as jnp
from jax import lax
from jax.experimental import pallas as pl
from jax.experimental.pallas import tpu as pltpu
from jax.sharding import Mesh, PartitionSpec as P


NORM_EPS = 1e-5
NZ = 4
NY = 4
NX = 4
NC = 2
HEAD_GROUP = 4
F32 = jnp.float32
BF16 = jnp.bfloat16
VMEM_LIMIT = 67043328


def norm_fwd(row_vals, norm_gain):
    return row_vals * lax.rsqrt(jnp.mean(row_vals * row_vals, axis=-1, keepdims=True) + NORM_EPS) * norm_gain


def rotate(wide, cos_tab, sin_tab):
    return wide * cos_tab + pltpu.roll(wide, wide.shape[-1] // 2, wide.ndim - 1) * sin_tab


def rotate_back(wide, cos_tab, sin_tab):
    return wide * cos_tab - pltpu.roll(wide, wide.shape[-1] // 2, wide.ndim - 1) * sin_tab


def cost(flops, bytes_accessed):
    return pl.CostEstimate(flops=int(flops) // 20, bytes_accessed=int(bytes_accessed), transcendentals=0)


def params(**extra):
    return pltpu.CompilerParams(vmem_limit_bytes=VMEM_LIMIT, **extra)


def head_probs(q_rot, k_rot, scale):
    scores = dot_nt(q_rot, k_rot) * scale
    row_ids = lax.broadcasted_iota(jnp.int32, scores.shape, 0)
    col_ids = lax.broadcasted_iota(jnp.int32, scores.shape, 1)
    scores = jnp.where(row_ids >= col_ids, scores, -1e30)
    weights = jnp.exp(scores - jnp.max(scores, axis=-1, keepdims=True))
    return weights / jnp.sum(weights, axis=-1, keepdims=True)


def half_rows(core, idx, chunk):
    return pl.ds(pl.multiple_of((NC * idx + core) * chunk, chunk), chunk)


def chunk_rows(idx, chunk):
    return slice(idx * chunk, (idx + 1) * chunk)


def attn_fwd_kernel(heads, head, pos_ref, own_ref, other_ref, own_third_ref, other_third_ref, cos_ref, sin_ref, seq_ref, o_ref, o_other_ref, o_buf):
    core, odd = pos_ref[1], pos_ref[2]
    chunk = own_ref.shape[0] // NX
    width = heads * head
    mine = pl.ds(pl.multiple_of(width + odd * head, head), head)
    theirs = pl.ds(pl.multiple_of(width + (1 - odd) * head, head), head)
    for side, part_ref, third_ref in ((core, own_ref, own_third_ref), (1 - core, other_ref, other_third_ref)):
        for idx in range(NX):
            rows = half_rows(side, idx, chunk)
            seq_ref[0, rows, pl.ds(0, width)] = part_ref[chunk_rows(idx, chunk), :width]
            seq_ref[0, rows, mine] = part_ref[chunk_rows(idx, chunk), width:]
            seq_ref[0, rows, theirs] = third_ref[chunk_rows(idx, chunk), :]
    cos_tab, sin_tab = cos_ref[...], sin_ref[...]
    k_rot = rotate(seq_ref[0, :, width : width + head].astype(F32), cos_tab, sin_tab).astype(BF16)
    values = seq_ref[0, :, width + head :]
    for idx in range(heads):
        lanes = slice(idx * head, (idx + 1) * head)
        q_rot = rotate(seq_ref[0, :, lanes].astype(F32), cos_tab, sin_tab).astype(BF16)
        probs = head_probs(q_rot, k_rot, head**-0.5)
        o_buf[:, lanes] = dot_nn(probs.astype(BF16), values).astype(BF16)
    for side, out_ref in ((core, o_ref), (1 - core, o_other_ref)):
        for idx in range(NX):
            out_ref[chunk_rows(idx, chunk), :] = o_buf[half_rows(side, idx, chunk), :]


def attn_bwd_kernel(heads, head, pos_ref, seq_ref, own_ref, other_ref, cos_ref, sin_ref, dq_ref, keep_ref, send_ref, do_buf):
    core, odd = pos_ref[1], pos_ref[2]
    chunk = own_ref.shape[0] // NX
    width = heads * head
    for side, part_ref in ((core, own_ref), (1 - core, other_ref)):
        for idx in range(NX):
            do_buf[half_rows(side, idx, chunk), :] = part_ref[chunk_rows(idx, chunk), :]
    cos_tab, sin_tab = cos_ref[...], sin_ref[...]
    k_rot = rotate(seq_ref[0, :, width : width + head].astype(F32), cos_tab, sin_tab).astype(BF16)
    values = seq_ref[0, :, width + head :]
    d_keys = jnp.zeros(k_rot.shape, F32)
    d_values = jnp.zeros(k_rot.shape, F32)
    for idx in range(heads):
        lanes = slice(idx * head, (idx + 1) * head)
        q_rot = rotate(seq_ref[0, :, lanes].astype(F32), cos_tab, sin_tab).astype(BF16)
        d_out = do_buf[:, lanes]
        probs = head_probs(q_rot, k_rot, head**-0.5)
        d_values += dot_tn(probs.astype(BF16), d_out)
        d_probs = dot_nt(d_out, values).astype(BF16).astype(F32)
        d_scores = probs * (d_probs - jnp.sum(d_probs * probs, axis=-1, keepdims=True))
        d_scores = (d_scores * head**-0.5).astype(BF16)
        d_q_rot = dot_nn(d_scores, k_rot).astype(BF16)
        dq_ref[0, :, lanes] = rotate_back(d_q_rot.astype(F32), cos_tab, sin_tab).astype(BF16)
        d_keys += dot_tn(d_scores, q_rot)

    @pl.when(odd == 0)
    def _():
        keep_ref[0] = d_keys
        send_ref[0] = d_values

    @pl.when(odd == 1)
    def _():
        keep_ref[0] = d_values
        send_ref[0] = d_keys


def attn_post_kernel(heads, head, pos_ref, dq_ref, keep_ref, got_ref, cos_ref, sin_ref, own_ref, other_ref, third_buf):
    core, odd = pos_ref[1], pos_ref[2]
    chunk = own_ref.shape[0] // NX
    width = heads * head
    total = (keep_ref[0] + got_ref[0]).astype(BF16)

    @pl.when(odd == 0)
    def _():
        third_buf[...] = rotate_back(total.astype(F32), cos_ref[...], sin_ref[...]).astype(BF16)

    @pl.when(odd == 1)
    def _():
        third_buf[...] = total

    for side, out_ref in ((core, own_ref), (1 - core, other_ref)):
        for idx in range(NX):
            rows = half_rows(side, idx, chunk)
            out_ref[chunk_rows(idx, chunk), :width] = dq_ref[0, rows, :]
            out_ref[chunk_rows(idx, chunk), width:] = third_buf[rows, :]


def per_sequence(kernel, pos, args, specs, out_specs, out_shape, scratch, flops):
    return pl.pallas_call(
        kernel,
        grid_spec=pltpu.PrefetchScalarGridSpec(num_scalar_prefetch=1, grid=(2,), in_specs=specs, out_specs=out_specs, scratch_shapes=scratch),
        out_shape=out_shape,
        compiler_params=params(),
        cost_estimate=cost(flops, 4e6),
    )(pos, *args)


def own_spec(rows, width):
    return pl.BlockSpec((rows, width), lambda i, pos: (2 * pos[1] + i, 0))


def pair_spec(rows, width):
    return pl.BlockSpec((rows, width), lambda i, pos: (i, 0))


def seq_spec(seq, width):
    return pl.BlockSpec((1, seq, width), lambda i, pos: (i, 0, 0))


def table_spec(table):
    return pl.BlockSpec(table.shape, lambda i, pos: (0, 0))


def attn_fwd(pos, qkv_tok, other, own_third, other_third, cos_tab, sin_tab):
    seq, head = cos_tab.shape
    width = qkv_tok.shape[1] - head
    rows = seq // 2
    half = jax.ShapeDtypeStruct((seq, width), BF16)
    return per_sequence(
        functools.partial(attn_fwd_kernel, width // head, head),
        pos,
        (qkv_tok, other, own_third, other_third, cos_tab, sin_tab),
        [own_spec(rows, width + head), pair_spec(rows, width + head), pair_spec(rows, head), pair_spec(rows, head), table_spec(cos_tab), table_spec(sin_tab)],
        [seq_spec(seq, width + 2 * head), pair_spec(rows, width), pair_spec(rows, width)],
        [jax.ShapeDtypeStruct((2, seq, width + 2 * head), BF16), half, half],
        [pltpu.VMEM((seq, width), BF16)],
        16e9,
    )


def attn_bwd(pos, qkv_seq, d_attn, other, cos_tab, sin_tab):
    seq, head = cos_tab.shape
    width = d_attn.shape[1]
    rows = seq // 2
    part = jax.ShapeDtypeStruct((2, seq, head), F32)
    return per_sequence(
        functools.partial(attn_bwd_kernel, width // head, head),
        pos,
        (qkv_seq, d_attn, other, cos_tab, sin_tab),
        [seq_spec(seq, width + 2 * head), own_spec(rows, width), pair_spec(rows, width), table_spec(cos_tab), table_spec(sin_tab)],
        [seq_spec(seq, width), seq_spec(seq, head), seq_spec(seq, head)],
        [jax.ShapeDtypeStruct((2, seq, width), BF16), part, part],
        [pltpu.VMEM((seq, width), BF16)],
        16e9,
    )


def attn_post(pos, d_queries, keep, got, cos_tab, sin_tab):
    seq, head = cos_tab.shape
    width = d_queries.shape[2]
    rows = seq // 2
    half = jax.ShapeDtypeStruct((seq, width + head), BF16)
    return per_sequence(
        functools.partial(attn_post_kernel, width // head, head),
        pos,
        (d_queries, keep, got, cos_tab, sin_tab),
        [seq_spec(seq, width), seq_spec(seq, head), seq_spec(seq, head), table_spec(cos_tab), table_spec(sin_tab)],
        [pair_spec(rows, width + head), pair_spec(rows, width + head)],
        [half, half],
        [pltpu.VMEM((seq, head), BF16)],
        2e9,
    )


def act_fwd_kernel(half, ab_ref, u_ref, ut_ref):
    gate_val = ab_ref[:, :half].astype(F32)
    up_val = ab_ref[:, half:].astype(F32)
    act_val = gate_val * jax.nn.sigmoid(gate_val) * up_val
    u_ref[...] = act_val.astype(BF16)
    ut_ref[...] = act_val.T.astype(BF16)


def act_fwd(gate_up):
    tokens, width = gate_up.shape
    half = width // 2
    rows = tokens // 4
    return pl.pallas_call(
        functools.partial(act_fwd_kernel, half),
        grid=(4,),
        in_specs=[pl.BlockSpec((rows, width), lambda i: (i, 0))],
        out_specs=[pl.BlockSpec((rows, half), lambda i: (i, 0)), pl.BlockSpec((half, rows), lambda i: (0, i))],
        out_shape=[jax.ShapeDtypeStruct((tokens, half), BF16), jax.ShapeDtypeStruct((half, tokens), BF16)],
        compiler_params=params(),
        cost_estimate=cost(4e9, 8e6),
        name="act_fwd",
    )(gate_up)


def act_bwd_kernel(half, ab_ref, du_ref, dab_ref, dabt_ref):
    gate_val = ab_ref[:, :half].astype(F32)
    up_val = ab_ref[:, half:].astype(F32)
    d_act = du_ref[...].astype(F32)
    sig = jax.nn.sigmoid(gate_val)
    d_silu = d_act * up_val
    d_gate = d_silu * sig + d_silu * gate_val * (sig * (1.0 - sig))
    d_up = d_act * (gate_val * sig)
    dab_ref[:, :half] = d_gate.astype(BF16)
    dab_ref[:, half:] = d_up.astype(BF16)
    dabt_ref[:half, :] = d_gate.T.astype(BF16)
    dabt_ref[half:, :] = d_up.T.astype(BF16)


def act_bwd(gate_up, d_mixed):
    tokens, width = gate_up.shape
    half = width // 2
    rows = tokens // 4
    return pl.pallas_call(
        functools.partial(act_bwd_kernel, half),
        grid=(4,),
        in_specs=[pl.BlockSpec((rows, width), lambda i: (i, 0)), pl.BlockSpec((rows, half), lambda i: (i, 0))],
        out_specs=[pl.BlockSpec((rows, width), lambda i: (i, 0)), pl.BlockSpec((width, rows), lambda i: (0, i))],
        out_shape=[jax.ShapeDtypeStruct((tokens, width), BF16), jax.ShapeDtypeStruct((width, tokens), BF16)],
        compiler_params=params(),
        cost_estimate=cost(8e9, 14e6),
        name="act_bwd",
    )(gate_up, d_mixed)


def piece_block(pos_ref, step, other):
    core = pos_ref[1]
    return lax.rem(pos_ref[0] + step, NZ) * NC + (1 - core if other else core)


def half_start(pos_ref, part, half):
    return pl.multiple_of((1 - pos_ref[2] if part else pos_ref[2]) * half, half)


def nn_kernel(keys, first, count_out, tile, pos_ref, acts_ref, *refs):
    count = len(keys)
    halves = refs[: 2 * count]
    outs = refs[2 * count : 2 * count + count_out]
    acts_buf, w_buf, total, acts_sem, w_sem = refs[2 * count + count_out :]
    block = acts_buf.shape[1] // count
    half = block // 2
    copies = []
    for idx in range(count):
        cols = pl.ds(pl.multiple_of(piece_block(pos_ref, *keys[idx]) * block, block), block)
        copies.append([pltpu.make_async_copy(acts_ref.at[:, cols], acts_buf.at[:, pl.ds(idx * block, block)], acts_sem.at[idx])])
        for part in range(2):
            rows = pl.ds(idx * block + half_start(pos_ref, part, half), half)
            copies[-1].append(pltpu.make_async_copy(halves[2 * idx + part], w_buf.at[rows], w_sem.at[2 * idx + part]))
    for group in copies:
        for copy in group:
            copy.start()
    for lo, hi in ((0, first), (first, count)):
        for group in copies[lo:hi]:
            for copy in group:
                copy.wait()
        depth = pl.ds(lo * block, (hi - lo) * block)
        start = 0
        for out_ref in outs:
            width = out_ref.shape[1]

            def step(out_lo, size, start=start, out_ref=out_ref, depth=depth, hi=hi):
                cols = pl.ds(pl.multiple_of(start + out_lo, 128), size)
                part = dot_nn(acts_buf[:, depth], w_buf[depth, cols])
                if hi == count:
                    out_ref[:, pl.ds(pl.multiple_of(out_lo, 128), size)] = (total[:, cols] + part).astype(BF16)
                else:
                    total[:, cols] = part

            whole = width // tile
            if whole:
                pl.loop(0, whole)(lambda n: step(n * tile, tile))
            if width % tile:
                step(whole * tile, width % tile)
            start += width


def nn_pieces(pos, acts, parts, widths, tile):
    keys = [(step, other) for step in (0, 1, 3, 2) for other in range(2)]
    halves = [parts[step][other][part] for step, other in keys for part in range(2)]
    tokens, depth = acts.shape
    width = sum(widths)
    count = len(keys)
    anywhere = pl.BlockSpec(memory_space=pl.ANY)
    return pl.pallas_call(
        functools.partial(nn_kernel, keys, 2, len(widths), tile),
        grid_spec=pltpu.PrefetchScalarGridSpec(
            num_scalar_prefetch=1,
            grid=(1,),
            in_specs=[anywhere] * (1 + 2 * count),
            out_specs=[pl.BlockSpec((tokens, size), lambda i, pos: (0, 0)) for size in widths],
            scratch_shapes=[
                pltpu.VMEM((tokens, depth), BF16),
                pltpu.VMEM((depth, width), BF16),
                pltpu.VMEM((tokens, width), F32),
                pltpu.SemaphoreType.DMA((count,)),
                pltpu.SemaphoreType.DMA((2 * count,)),
            ],
        ),
        out_shape=[jax.ShapeDtypeStruct((tokens, size), BF16) for size in widths],
        compiler_params=params(),
        cost_estimate=cost(2 * tokens * depth * width, 2 * depth * (tokens + width)),
    )(pos, acts, *halves)


def nt_kernel(keys, sides, first_row, pos_ref, *refs):
    count_left = len(sides)
    count = len(keys)
    lefts = refs[:count_left]
    halves = refs[count_left : count_left + 2 * count]
    out_ref, left_buf, w_buf, out_buf, left_sem, w_sem, out_sem = refs[count_left + 2 * count :]
    block = out_buf.shape[2]
    half = block // 2
    slots = w_buf.shape[0]
    left_copies = []
    start = 0
    for idx, (left, side) in enumerate(zip(lefts, sides)):
        chunks, _, width = left.shape
        first = 0 if side is None else (1 - pos_ref[1] if side else pos_ref[1]) * chunks
        source = left.at[:, pl.ds(first_row, left_buf.shape[1]), :]
        left_copies.append(pltpu.make_async_copy(source, left_buf.at[pl.ds(first, chunks), :, pl.ds(start, width)], left_sem.at[idx]))
        left_copies[-1].start()
        start += 0 if side == 0 else width

    def copies(idx, slot):
        for part in range(2):
            rows = pl.ds(half_start(pos_ref, part, half), half)
            yield pltpu.make_async_copy(halves[2 * idx + part], w_buf.at[slot, rows], w_sem.at[slot, part])

    def out_copy(idx):
        core = pos_ref[1]
        other = lax.rem(idx, 2)
        block_id = lax.rem(pos_ref[0] + idx // 2, NZ) * NC + core + other - 2 * core * other
        slot = lax.rem(idx, 2)
        return pltpu.make_async_copy(out_buf.at[slot], out_ref.at[:, pl.ds(pl.multiple_of(block_id * block, block), block)], out_sem.at[slot])

    for idx in range(slots - 1):
        for copy in copies(idx, idx):
            copy.start()
    for copy in left_copies:
        copy.wait()

    @pl.loop(0, count)
    def _(step):
        slot = lax.rem(step, slots)
        for idx in range(slots - 1, count):

            @pl.when(step + slots - 1 == idx)
            def _(idx=idx):
                for copy in copies(idx, idx % slots):
                    copy.start()

        for copy in copies(0, slot):
            copy.wait()

        @pl.when(step >= 2)
        def _():
            out_copy(step - 2).wait()

        out_buf[lax.rem(step, 2)] = dot_nt(left_buf[...].reshape(out_buf.shape[1], left_buf.shape[2]), w_buf[slot])
        out_copy(step).start()

    for idx in range(count - 2, count):
        out_copy(idx).wait()


def nt_pieces(pos, lefts, parts, chunk, first_row, rows):
    sides = (None, 0, 1)
    keys = [(step, other) for step in range(NZ) for other in range(2)]
    halves = [parts[step][other][part] for step, other in keys for part in range(2)]
    lefts = [left.reshape(-1, chunk, left.shape[1]) for left in lefts]
    chunks = lefts[0].shape[0]
    tokens = chunks * rows
    block = 2 * halves[0].shape[0]
    depth = block * len(keys)
    width = halves[0].shape[1]
    slots = 3
    anywhere = pl.BlockSpec(memory_space=pl.ANY)
    return pl.pallas_call(
        functools.partial(nt_kernel, keys, sides, first_row),
        grid_spec=pltpu.PrefetchScalarGridSpec(
            num_scalar_prefetch=1,
            grid=(1,),
            in_specs=[anywhere] * (len(lefts) + len(halves)),
            out_specs=anywhere,
            scratch_shapes=[
                pltpu.VMEM((chunks, rows, width), BF16),
                pltpu.VMEM((slots, block, width), BF16),
                pltpu.VMEM((2, tokens, block), F32),
                pltpu.SemaphoreType.DMA((len(lefts),)),
                pltpu.SemaphoreType.DMA((slots, 2)),
                pltpu.SemaphoreType.DMA((2,)),
            ],
        ),
        out_shape=jax.ShapeDtypeStruct((tokens, depth), F32),
        compiler_params=params(),
        cost_estimate=cost(2 * tokens * depth * width, 2 * depth * width + 4 * tokens * depth),
    )(pos, *lefts, *halves)


def picked_cols(pos_ref, idx, block):
    return pl.ds(pl.multiple_of((NC * idx + 1 - pos_ref[1]) * block, block), block)


def dma_kernel(kernel, pos, args, out_shape, scratch):
    anywhere = pl.BlockSpec(memory_space=pl.ANY)
    return pl.pallas_call(
        kernel,
        grid_spec=pltpu.PrefetchScalarGridSpec(
            num_scalar_prefetch=1, grid=(1,), in_specs=[anywhere] * len(args), out_specs=[anywhere] * len(out_shape), scratch_shapes=scratch
        ),
        out_shape=out_shape,
        compiler_params=params(),
        cost_estimate=cost(3e9, 16e6),
    )(pos, *args)


def pick_cols(pos, acts):
    tokens, depth = acts.shape
    block = depth // (NC * NZ)

    def kernel(pos_ref, in_ref, out_ref, buf, in_sem, out_sem):
        reads = [pltpu.make_async_copy(in_ref.at[:, picked_cols(pos_ref, idx, block)], buf.at[idx], in_sem.at[idx]) for idx in range(NZ)]
        writes = [pltpu.make_async_copy(buf.at[idx], out_ref.at[:, pl.ds(idx * block, block)], out_sem.at[idx]) for idx in range(NZ)]
        for read in reads:
            read.start()
        for read, write in zip(reads, writes):
            read.wait()
            write.start()
        for write in writes:
            write.wait()

    sems = pltpu.SemaphoreType.DMA((NZ,))
    return dma_kernel(kernel, pos, [acts], [jax.ShapeDtypeStruct((tokens, depth // 2), BF16)], [pltpu.VMEM((NZ, tokens, block), BF16), sems, sems])[0]


def grad_kernel(heights, pos_ref, *refs):
    pairs = len(heights)
    ins = refs[: 4 * pairs]
    outs = refs[4 * pairs : 4 * pairs + 2 * NZ]
    buf, sem = refs[4 * pairs + 2 * NZ :]
    half = buf.shape[2] // 2
    step = pl.program_id(0)
    slot = lax.rem(step, 2)

    def out_copy(idx, part):
        cols = pl.ds(half_start(pos_ref, part, half), half)
        return pltpu.make_async_copy(buf.at[idx % 2, :, cols], outs[2 * idx + part], sem.at[idx % 2, part])

    for idx in range(2, NZ):

        @pl.when(step == idx)
        def _(idx=idx):
            for part in range(2):
                out_copy(idx - 2, part).wait()

    start = 0
    for idx, height in enumerate(heights):
        own, recv, acts, acts_recv = ins[4 * idx : 4 * idx + 4]
        buf[slot, start : start + height, :] = dot_nn(own[...], acts[...]) + dot_nn(recv[...], acts_recv[...])
        start += height
    for idx in range(NZ):

        @pl.when(step == idx)
        def _(idx=idx):
            for part in range(2):
                out_copy(idx, part).start()

    @pl.when(step == NZ - 1)
    def _():
        for idx in (NZ - 2, NZ - 1):
            for part in range(2):
                out_copy(idx, part).wait()


def grad_pieces(pos, pairs):
    tokens, depth = pairs[0][2].shape
    cols = depth // (NZ * NC)
    in_specs = []
    args = []

    def z_of(n, pos):
        return lax.rem(pos[0] + jnp.where(n == 0, 2, jnp.where(n == 1, 1, jnp.where(n == 2, 3, 0))), NZ)

    for own, recv, acts, acts_recv, height, block in pairs:
        in_specs += [pl.BlockSpec((height, tokens), lambda n, pos, block=block: (block, 0))] * 2
        in_specs.append(pl.BlockSpec((tokens, cols), lambda n, pos: (0, z_of(n, pos) * NC + pos[1])))
        in_specs.append(pl.BlockSpec((tokens, cols), lambda n, pos: (0, z_of(n, pos))))
        args += [own, recv, acts, acts_recv]
    heights = [pair[4] for pair in pairs]
    rows = sum(heights)
    return pl.pallas_call(
        functools.partial(grad_kernel, heights),
        grid_spec=pltpu.PrefetchScalarGridSpec(
            num_scalar_prefetch=1,
            grid=(NZ,),
            in_specs=in_specs,
            out_specs=[pl.BlockSpec(memory_space=pl.ANY)] * (2 * NZ),
            scratch_shapes=[pltpu.VMEM((2, rows, cols), F32), pltpu.SemaphoreType.DMA((2, 2))],
        ),
        out_shape=[jax.ShapeDtypeStruct((rows, cols // 2), F32)] * (2 * NZ),
        compiler_params=params(),
        cost_estimate=cost(4 * rows * tokens * cols * NZ, 4 * tokens * cols * NZ),
        name="grad",
    )(pos, *args)


def sources(pos_ref, own_ref, first_ref, second_ref):
    return ((pos_ref[3] == 1, 0, own_ref), (pos_ref[3] == 0, 0, first_ref), (True, 1, second_ref))


def place(pos, own, first, second, height, block, transpose):
    cols = first.shape[1]
    spec = pl.BlockSpec((height, cols), lambda n, pos: (block, 0))

    def kernel(pos_ref, own_ref, first_ref, second_ref, out_ref):
        for chosen, idx, ref in sources(pos_ref, own_ref, first_ref, second_ref):

            @pl.when(jnp.logical_and(pl.program_id(0) == idx, chosen))
            def _(ref=ref):
                out_ref[...] = ref[...].T if transpose else ref[...]

    def order(n, pos):
        return jnp.where(n == 0, pos[2], 1 - pos[2])

    return pl.pallas_call(
        kernel,
        grid_spec=pltpu.PrefetchScalarGridSpec(
            num_scalar_prefetch=1,
            grid=(2,),
            in_specs=[spec] * 3,
            out_specs=pl.BlockSpec((cols, height), lambda n, pos: (0, order(n, pos))) if transpose else pl.BlockSpec((height, cols), lambda n, pos: (order(n, pos), 0)),
        ),
        out_shape=jax.ShapeDtypeStruct((cols, 2 * height) if transpose else (2 * height, cols), F32),
        compiler_params=params(),
        cost_estimate=cost(2e9, 16 * height * cols),
    )(pos, own, first, second)


def place_attn(pos, own, first, second, o_blk, head):
    rows, cols = first.shape
    qk = 2 * head

    def kernel(pos_ref, own_ref, first_ref, second_ref, out_ref, qkv_ref):
        for chosen, idx, ref in sources(pos_ref, own_ref, first_ref, second_ref):

            @pl.when(chosen)
            def _(idx=idx, ref=ref):
                bit = 1 - pos_ref[2] if idx else pos_ref[2]
                out_ref[pl.ds(pl.multiple_of(bit * o_blk, o_blk), o_blk), :] = ref[:o_blk, :]
                qkv_ref[:, pl.ds(pl.multiple_of(bit * qk, qk), qk)] = ref[o_blk : o_blk + qk, :].T
                qkv_ref[:, pl.ds(pl.multiple_of(2 * qk + bit * head, head), head)] = ref[o_blk + qk :, :].T

    def whole(*shape):
        return pl.BlockSpec(shape, lambda n, pos: (0, 0))

    shapes = ((2 * o_blk, cols), (cols, 2 * (qk + head)))
    return pl.pallas_call(
        kernel,
        grid_spec=pltpu.PrefetchScalarGridSpec(num_scalar_prefetch=1, grid=(1,), in_specs=[whole(rows, cols)] * 3, out_specs=[whole(*shape) for shape in shapes]),
        out_shape=[jax.ShapeDtypeStruct(shape, F32) for shape in shapes],
        compiler_params=params(),
        cost_estimate=cost(2e9, 16 * rows * cols),
        name="p_attn",
    )(pos, own, first, second)


def after(val, *earlier):
    return lax.optimization_barrier((val, *earlier))[0]


def ring(step, size):
    return [(src, (src + step) % size) for src in range(size)]


def hop_z(val, step):
    return lax.ppermute(val, "z", ring(step, NZ))


def swap_c(val):
    return lax.ppermute(val, "c", [(0, 1), (1, 0)])


def swap_y(val):
    return lax.ppermute(val, "y", [(src, src ^ 1) for src in range(NY)])


def turn(val, flip, home):
    def place_of(y_pos, c_pos):
        return y_pos * NC + c_pos

    pairs = [(place_of(2 * a + b, c), place_of(2 * c + (b ^ flip), a)) for a in range(2) for b in range(2) for c in range(NC) if home or flip or a != c]
    return lax.ppermute(val, ("y", "c"), pairs)


def swap_yc(val):
    pairs = [(y_pos * NC + c_pos, (y_pos ^ 1) * NC + 1 - c_pos) for y_pos in range(NY) for c_pos in range(NC)]
    return lax.ppermute(val, ("y", "c"), pairs)


def dot_nn(left, right):
    return lax.dot_general(left, right, (((1,), (0,)), ((), ())), preferred_element_type=F32)


def dot_nt(left, right):
    return lax.dot_general(left, right, (((1,), (1,)), ((), ())), preferred_element_type=F32)


def dot_tn(left, right):
    return lax.dot_general(left, right, (((0,), (0,)), ((), ())), preferred_element_type=F32)


def solution(mesh):
    wide_mesh = Mesh(mesh.devices.reshape(NZ, NY, NX, NC), ("z", "y", "x", "c"))
    rows = ("z", "y")
    cols = ("x", "c")
    act_spec = P(rows, cols, None)
    col_spec = P(rows, cols)
    row_spec = P(cols, rows)

    def layer(x_in, dy_in, norm_gain, w_qkv, w_out, w_gate, w_up, w_down, rope_cos, rope_sin):
        z_pos = lax.axis_index("z")
        y_pos = lax.axis_index("y")
        c_pos = lax.axis_index("c")
        even_y = y_pos % 2 == 0
        first_c = c_pos == 0
        pos = jnp.stack([z_pos, c_pos, y_pos % 2, y_pos // 2 == c_pos]).astype(jnp.int32)
        chunk = x_in.shape[1]
        head = 2 * rope_cos.shape[1]
        seq = rope_cos.shape[0]
        ff_blk = w_gate.shape[1] // 2
        o_blk = w_out.shape[0] // 2
        qkv_blk = o_blk + head

        def gather_rows(blocks):
            return [turn(jnp.where(even_y, blocks[flip], blocks[1 - flip]), flip, True) for flip in range(2)]

        def gather_weight(piece):
            left, right = [], []
            for part in (1, 0):
                left.insert(0, hop_z(piece[part], 1))
                right.insert(0, hop_z(piece[part], -1))
            far = [hop_z(left[0], 1), hop_z(right[1], -1)]
            parts = []
            for mine in (piece, right, far, left):
                parts.append((mine, [swap_c(half) for half in mine]))
            return parts

        def grad_start(pairs, *earlier):
            far0, far1, up0, up1, down0, down1, own0, own1 = grad_pieces(after(pos, *earlier), pairs)
            far = (hop_z(far0, 1), hop_z(far1, -1))
            direct = (hop_z(up1, 1), hop_z(down0, -1))
            return (up0, down1), far, direct, (own0, own1)

        def grad_pass(state, *earlier):
            (up0, down1), far, direct, own = state
            sums = (up0 + after(far[0], *earlier), down1 + far[1])
            passed = (hop_z(sums[0], 1), hop_z(sums[1], -1))
            return direct, passed, own, sums

        def grad_back(state, *earlier):
            direct, passed, own = state[:3]
            first = own[0] + after(passed[0], *earlier) + direct[1]
            second = own[1] + direct[0] + passed[1]
            return first, turn(first, 0, False), turn(second, 1, False)

        def my_rows(val, mine):
            return lax.dynamic_slice_in_dim(val, (c_pos if mine else 1 - c_pos) * seq, seq, axis=0)

        def both_rows(own, got):
            return jnp.concatenate([jnp.where(first_c, own, got), jnp.where(first_c, got, own)], axis=0)

        cos_tab = jnp.concatenate([rope_cos, rope_cos], axis=1)
        sin_tab = jnp.concatenate([-rope_sin, rope_sin], axis=1)

        def qkv_cols(bit):
            first = 2 * head * bit
            third = HEAD_GROUP * head + head * bit
            return [w_qkv[:, first : first + 2 * head], w_qkv[:, third : third + head]]

        def block(weight, bit):
            size = weight.shape[1] // 2
            return weight[:, bit * size : (bit + 1) * size]

        down_t = w_down.T
        out_t = w_out.T
        wf_piece = gather_rows([jnp.concatenate([block(w_gate, j), block(w_up, j), *qkv_cols(j)], axis=1) for j in range(2)])
        ws_piece = gather_rows([jnp.concatenate([block(down_t, j), block(out_t, j)], axis=1) for j in range(2)])

        x_rows = after(x_in[0], cos_tab, sin_tab).astype(F32)
        normed, norm_pull = jax.vjp(lambda row_vals: norm_fwd(row_vals, norm_gain), x_rows)
        h_all = lax.all_gather(after(normed.astype(BF16), wf_piece[0], wf_piece[1]), ("y", "x"), axis=0, tiled=True)
        dy_all = lax.all_gather(after(dy_in[0], *wf_piece), ("y", "x"), axis=0, tiled=True)
        wf_parts = gather_weight(wf_piece)
        ws_parts = gather_weight(ws_piece)

        gate_up, qkv_tok = nn_pieces(pos, h_all, wf_parts, (2 * ff_blk, qkv_blk), 512)
        third = qkv_tok[:, o_blk:]
        qkv_other = swap_c(my_rows(qkv_tok, False))
        third_own = swap_y(my_rows(third, True))
        third_other = swap_yc(my_rows(third, False))
        act_val, act_t = act_fwd(after(gate_up, qkv_tok))
        act_recv = swap_c(act_t)
        h_picked = pick_cols(after(pos, act_t), h_all)
        h_recv = swap_c(h_picked)
        qkv_seq, attn_own, attn_other = attn_fwd(after(pos, h_picked), qkv_tok, qkv_other, third_own, third_other, cos_tab, sin_tab)
        attn_got = swap_c(attn_other)
        y_part = nt_pieces(after(pos, attn_own), [act_val, attn_own, attn_got], ws_parts, chunk, 0, chunk)
        mix_sum = lax.psum_scatter(y_part, ("y", "x"), scatter_dimension=0, tiled=True)
        y_out = (x_rows + mix_sum).astype(BF16)[None]

        dy_picked = pick_cols(after(pos, y_part), dy_all)
        dy_recv = swap_c(dy_picked)
        g_act = grad_start([(act_t, act_recv, dy_all, dy_recv, ff_blk, 0)], dy_picked)
        d_act, d_attn = nn_pieces(after(pos, g_act[3][0]), dy_all, ws_parts, (ff_blk, o_blk), 256)
        d_attn_other = swap_c(my_rows(d_attn, False))
        d_gate_up, d_gate_up_t = act_bwd(gate_up, d_act)
        d_gate_up_recv = swap_c(d_gate_up_t)
        d_queries, keep, send = attn_bwd(after(pos, d_gate_up_t), qkv_seq, d_attn, d_attn_other, cos_tab, sin_tab)
        got = swap_y(send)
        g_act = grad_pass(g_act, d_queries)
        g_gate = grad_start([(d_gate_up_t, d_gate_up_recv, h_all, h_recv, ff_blk, 0)], *g_act[3])
        d_own, d_other = attn_post(after(pos, g_gate[3][0]), d_queries, keep, got, cos_tab, sin_tab)
        d_got = swap_c(d_other)
        dh_part = nt_pieces(pos, [d_gate_up, d_own, d_got], wf_parts, chunk, 0, chunk)
        d_h = lax.psum_scatter(dh_part, ("y", "x"), scatter_dimension=0, tiled=True)
        g_gate = grad_pass(g_gate, dh_part)
        g_up = grad_start([(d_gate_up_t, d_gate_up_recv, h_all, h_recv, ff_blk, 1)], *g_gate[3])
        b_act = grad_back(g_act, g_up[3][0])
        d_h = d_h.astype(BF16)
        dx_out = (dy_in[0].astype(F32) + norm_pull(d_h.astype(F32))[0]).astype(BF16)[None]

        attn_t = both_rows(attn_own, attn_got).T
        d_qkv_t = both_rows(d_own, d_got).T
        attn_recv = swap_c(attn_t)
        d_qkv_recv = swap_c(d_qkv_t)
        g_attn = grad_start([(attn_t, attn_recv, dy_all, dy_recv, o_blk, 0), (d_qkv_t, d_qkv_recv, h_all, h_recv, qkv_blk, 0)], g_up[3][0])
        g_up = grad_pass(g_up, g_attn[3][0])
        g_attn = grad_pass(g_attn)
        b_gate = grad_back(g_gate)
        b_up = grad_back(g_up)
        b_attn = grad_back(g_attn)
        dw_down = place(pos, *b_act, ff_blk, 0, False)
        dw_gate = place(pos, *b_gate, ff_blk, 0, True)
        dw_up = place(pos, *b_up, ff_blk, 0, True)
        dw_out, dw_qkv = place_attn(after(pos, dx_out, dw_up), *b_attn, o_blk, head)
        return y_out, dx_out, dw_qkv, dw_out, dw_gate, dw_up, dw_down


    return jax.shard_map(
        layer,
        mesh=wide_mesh,
        in_specs=(act_spec, act_spec, P(), col_spec, row_spec, col_spec, col_spec, row_spec, P(), P()),
        out_specs=(act_spec, act_spec, col_spec, row_spec, col_spec, col_spec, row_spec),
        check_vma=False,
    )
```

```python
import functools

import jax
import jax.numpy as jnp
from jax import lax
from jax.experimental import pallas as pl
from jax.experimental.pallas import tpu as pltpu
from jax.sharding import Mesh, PartitionSpec as P


NORM_EPS = 1e-5
NZ = 4
NY = 4
NX = 4
NC = 2
HEAD_GROUP = 4
F32 = jnp.float32
BF16 = jnp.bfloat16
VMEM_LIMIT = 67043328


def norm_fwd(row_vals, norm_gain):
    return row_vals * lax.rsqrt(jnp.mean(row_vals * row_vals, axis=-1, keepdims=True) + NORM_EPS) * norm_gain


def rotate(wide, cos_tab, sin_tab):
    return wide * cos_tab + pltpu.roll(wide, wide.shape[-1] // 2, wide.ndim - 1) * sin_tab


def rotate_back(wide, cos_tab, sin_tab):
    return wide * cos_tab - pltpu.roll(wide, wide.shape[-1] // 2, wide.ndim - 1) * sin_tab


def cost(flops, bytes_accessed):
    return pl.CostEstimate(flops=int(flops) // 20, bytes_accessed=int(bytes_accessed), transcendentals=0)


def params(**extra):
    return pltpu.CompilerParams(vmem_limit_bytes=VMEM_LIMIT, **extra)


def head_probs(q_rot, k_rot, scale):
    scores = dot_nt(q_rot, k_rot) * scale
    row_ids = lax.broadcasted_iota(jnp.int32, scores.shape, 0)
    col_ids = lax.broadcasted_iota(jnp.int32, scores.shape, 1)
    scores = jnp.where(row_ids >= col_ids, scores, -1e30)
    weights = jnp.exp(scores - jnp.max(scores, axis=-1, keepdims=True))
    return weights / jnp.sum(weights, axis=-1, keepdims=True)


def half_rows(core, idx, chunk):
    return pl.ds(pl.multiple_of((NC * idx + core) * chunk, chunk), chunk)


def chunk_rows(idx, chunk):
    return slice(idx * chunk, (idx + 1) * chunk)


def attn_fwd_kernel(heads, head, pos_ref, own_ref, other_ref, own_third_ref, other_third_ref, cos_ref, sin_ref, seq_ref, o_ref, o_other_ref, o_buf):
    core, odd = pos_ref[1], pos_ref[2]
    chunk = own_ref.shape[0] // NX
    width = heads * head
    mine = pl.ds(pl.multiple_of(width + odd * head, head), head)
    theirs = pl.ds(pl.multiple_of(width + (1 - odd) * head, head), head)
    for side, part_ref, third_ref in ((core, own_ref, own_third_ref), (1 - core, other_ref, other_third_ref)):
        for idx in range(NX):
            rows = half_rows(side, idx, chunk)
            seq_ref[0, rows, pl.ds(0, width)] = part_ref[chunk_rows(idx, chunk), :width]
            seq_ref[0, rows, mine] = part_ref[chunk_rows(idx, chunk), width:]
            seq_ref[0, rows, theirs] = third_ref[chunk_rows(idx, chunk), :]
    cos_tab, sin_tab = cos_ref[...], sin_ref[...]
    k_rot = rotate(seq_ref[0, :, width : width + head].astype(F32), cos_tab, sin_tab).astype(BF16)
    values = seq_ref[0, :, width + head :]
    for idx in range(heads):
        lanes = slice(idx * head, (idx + 1) * head)
        q_rot = rotate(seq_ref[0, :, lanes].astype(F32), cos_tab, sin_tab).astype(BF16)
        probs = head_probs(q_rot, k_rot, head**-0.5)
        o_buf[:, lanes] = dot_nn(probs.astype(BF16), values).astype(BF16)
    for side, out_ref in ((core, o_ref), (1 - core, o_other_ref)):
        for idx in range(NX):
            out_ref[chunk_rows(idx, chunk), :] = o_buf[half_rows(side, idx, chunk), :]


def attn_bwd_kernel(heads, head, pos_ref, seq_ref, own_ref, other_ref, cos_ref, sin_ref, dq_ref, keep_ref, send_ref, do_buf):
    core, odd = pos_ref[1], pos_ref[2]
    chunk = own_ref.shape[0] // NX
    width = heads * head
    for side, part_ref in ((core, own_ref), (1 - core, other_ref)):
        for idx in range(NX):
            do_buf[half_rows(side, idx, chunk), :] = part_ref[chunk_rows(idx, chunk), :]
    cos_tab, sin_tab = cos_ref[...], sin_ref[...]
    k_rot = rotate(seq_ref[0, :, width : width + head].astype(F32), cos_tab, sin_tab).astype(BF16)
    values = seq_ref[0, :, width + head :]
    d_keys = jnp.zeros(k_rot.shape, F32)
    d_values = jnp.zeros(k_rot.shape, F32)
    for idx in range(heads):
        lanes = slice(idx * head, (idx + 1) * head)
        q_rot = rotate(seq_ref[0, :, lanes].astype(F32), cos_tab, sin_tab).astype(BF16)
        d_out = do_buf[:, lanes]
        probs = head_probs(q_rot, k_rot, head**-0.5)
        d_values += dot_tn(probs.astype(BF16), d_out)
        d_probs = dot_nt(d_out, values).astype(BF16).astype(F32)
        d_scores = probs * (d_probs - jnp.sum(d_probs * probs, axis=-1, keepdims=True))
        d_scores = (d_scores * head**-0.5).astype(BF16)
        d_q_rot = dot_nn(d_scores, k_rot).astype(BF16)
        dq_ref[0, :, lanes] = rotate_back(d_q_rot.astype(F32), cos_tab, sin_tab).astype(BF16)
        d_keys += dot_tn(d_scores, q_rot)

    @pl.when(odd == 0)
    def _():
        keep_ref[0] = d_keys
        send_ref[0] = d_values

    @pl.when(odd == 1)
    def _():
        keep_ref[0] = d_values
        send_ref[0] = d_keys


def attn_post_kernel(heads, head, pos_ref, dq_ref, keep_ref, got_ref, cos_ref, sin_ref, own_ref, other_ref, third_buf):
    core, odd = pos_ref[1], pos_ref[2]
    chunk = own_ref.shape[0] // NX
    width = heads * head
    total = (keep_ref[0] + got_ref[0]).astype(BF16)

    @pl.when(odd == 0)
    def _():
        third_buf[...] = rotate_back(total.astype(F32), cos_ref[...], sin_ref[...]).astype(BF16)

    @pl.when(odd == 1)
    def _():
        third_buf[...] = total

    for side, out_ref in ((core, own_ref), (1 - core, other_ref)):
        for idx in range(NX):
            rows = half_rows(side, idx, chunk)
            out_ref[chunk_rows(idx, chunk), :width] = dq_ref[0, rows, :]
            out_ref[chunk_rows(idx, chunk), width:] = third_buf[rows, :]


def per_sequence(kernel, pos, args, specs, out_specs, out_shape, scratch, flops):
    return pl.pallas_call(
        kernel,
        grid_spec=pltpu.PrefetchScalarGridSpec(num_scalar_prefetch=1, grid=(2,), in_specs=specs, out_specs=out_specs, scratch_shapes=scratch),
        out_shape=out_shape,
        compiler_params=params(),
        cost_estimate=cost(flops, 4e6),
    )(pos, *args)


def own_spec(rows, width):
    return pl.BlockSpec((rows, width), lambda i, pos: (2 * pos[1] + i, 0))


def pair_spec(rows, width):
    return pl.BlockSpec((rows, width), lambda i, pos: (i, 0))


def seq_spec(seq, width):
    return pl.BlockSpec((1, seq, width), lambda i, pos: (i, 0, 0))


def table_spec(table):
    return pl.BlockSpec(table.shape, lambda i, pos: (0, 0))


def attn_fwd(pos, qkv_tok, other, own_third, other_third, cos_tab, sin_tab):
    seq, head = cos_tab.shape
    width = qkv_tok.shape[1] - head
    rows = seq // 2
    half = jax.ShapeDtypeStruct((seq, width), BF16)
    return per_sequence(
        functools.partial(attn_fwd_kernel, width // head, head),
        pos,
        (qkv_tok, other, own_third, other_third, cos_tab, sin_tab),
        [own_spec(rows, width + head), pair_spec(rows, width + head), pair_spec(rows, head), pair_spec(rows, head), table_spec(cos_tab), table_spec(sin_tab)],
        [seq_spec(seq, width + 2 * head), pair_spec(rows, width), pair_spec(rows, width)],
        [jax.ShapeDtypeStruct((2, seq, width + 2 * head), BF16), half, half],
        [pltpu.VMEM((seq, width), BF16)],
        16e9,
    )


def attn_bwd(pos, qkv_seq, d_attn, other, cos_tab, sin_tab):
    seq, head = cos_tab.shape
    width = d_attn.shape[1]
    rows = seq // 2
    part = jax.ShapeDtypeStruct((2, seq, head), F32)
    return per_sequence(
        functools.partial(attn_bwd_kernel, width // head, head),
        pos,
        (qkv_seq, d_attn, other, cos_tab, sin_tab),
        [seq_spec(seq, width + 2 * head), own_spec(rows, width), pair_spec(rows, width), table_spec(cos_tab), table_spec(sin_tab)],
        [seq_spec(seq, width), seq_spec(seq, head), seq_spec(seq, head)],
        [jax.ShapeDtypeStruct((2, seq, width), BF16), part, part],
        [pltpu.VMEM((seq, width), BF16)],
        16e9,
    )


def attn_post(pos, d_queries, keep, got, cos_tab, sin_tab):
    seq, head = cos_tab.shape
    width = d_queries.shape[2]
    rows = seq // 2
    half = jax.ShapeDtypeStruct((seq, width + head), BF16)
    return per_sequence(
        functools.partial(attn_post_kernel, width // head, head),
        pos,
        (d_queries, keep, got, cos_tab, sin_tab),
        [seq_spec(seq, width), seq_spec(seq, head), seq_spec(seq, head), table_spec(cos_tab), table_spec(sin_tab)],
        [pair_spec(rows, width + head), pair_spec(rows, width + head)],
        [half, half],
        [pltpu.VMEM((seq, head), BF16)],
        2e9,
    )


def act_fwd_kernel(half, ab_ref, u_ref, ut_ref):
    gate_val = ab_ref[:, :half].astype(F32)
    up_val = ab_ref[:, half:].astype(F32)
    act_val = gate_val * jax.nn.sigmoid(gate_val) * up_val
    u_ref[...] = act_val.astype(BF16)
    ut_ref[...] = act_val.T.astype(BF16)


def act_fwd(gate_up):
    tokens, width = gate_up.shape
    half = width // 2
    rows = tokens // 4
    return pl.pallas_call(
        functools.partial(act_fwd_kernel, half),
        grid=(4,),
        in_specs=[pl.BlockSpec((rows, width), lambda i: (i, 0))],
        out_specs=[pl.BlockSpec((rows, half), lambda i: (i, 0)), pl.BlockSpec((half, rows), lambda i: (0, i))],
        out_shape=[jax.ShapeDtypeStruct((tokens, half), BF16), jax.ShapeDtypeStruct((half, tokens), BF16)],
        compiler_params=params(),
        cost_estimate=cost(4e9, 8e6),
        name="act_fwd",
    )(gate_up)


def act_bwd_kernel(half, ab_ref, du_ref, dab_ref, dabt_ref):
    gate_val = ab_ref[:, :half].astype(F32)
    up_val = ab_ref[:, half:].astype(F32)
    d_act = du_ref[...].astype(F32)
    sig = jax.nn.sigmoid(gate_val)
    d_silu = d_act * up_val
    d_gate = d_silu * sig + d_silu * gate_val * (sig * (1.0 - sig))
    d_up = d_act * (gate_val * sig)
    dab_ref[:, :half] = d_gate.astype(BF16)
    dab_ref[:, half:] = d_up.astype(BF16)
    dabt_ref[:half, :] = d_gate.T.astype(BF16)
    dabt_ref[half:, :] = d_up.T.astype(BF16)


def act_bwd(gate_up, d_mixed):
    tokens, width = gate_up.shape
    half = width // 2
    rows = tokens // 4
    return pl.pallas_call(
        functools.partial(act_bwd_kernel, half),
        grid=(4,),
        in_specs=[pl.BlockSpec((rows, width), lambda i: (i, 0)), pl.BlockSpec((rows, half), lambda i: (i, 0))],
        out_specs=[pl.BlockSpec((rows, width), lambda i: (i, 0)), pl.BlockSpec((width, rows), lambda i: (0, i))],
        out_shape=[jax.ShapeDtypeStruct((tokens, width), BF16), jax.ShapeDtypeStruct((width, tokens), BF16)],
        compiler_params=params(),
        cost_estimate=cost(8e9, 14e6),
        name="act_bwd",
    )(gate_up, d_mixed)


def piece_block(pos_ref, step, other):
    core = pos_ref[1]
    return lax.rem(pos_ref[0] + step, NZ) * NC + (1 - core if other else core)


def half_start(pos_ref, part, half):
    return pl.multiple_of((1 - pos_ref[2] if part else pos_ref[2]) * half, half)


def nn_kernel(keys, first, count_out, tile, pos_ref, acts_ref, *refs):
    count = len(keys)
    halves = refs[: 2 * count]
    outs = refs[2 * count : 2 * count + count_out]
    acts_buf, w_buf, total, acts_sem, w_sem = refs[2 * count + count_out :]
    block = acts_buf.shape[1] // count
    half = block // 2
    copies = []
    for idx in range(count):
        cols = pl.ds(pl.multiple_of(piece_block(pos_ref, *keys[idx]) * block, block), block)
        copies.append([pltpu.make_async_copy(acts_ref.at[:, cols], acts_buf.at[:, pl.ds(idx * block, block)], acts_sem.at[idx])])
        for part in range(2):
            rows = pl.ds(idx * block + half_start(pos_ref, part, half), half)
            copies[-1].append(pltpu.make_async_copy(halves[2 * idx + part], w_buf.at[rows], w_sem.at[2 * idx + part]))
    for group in copies:
        for copy in group:
            copy.start()
    for lo, hi in ((0, first), (first, count)):
        for group in copies[lo:hi]:
            for copy in group:
                copy.wait()
        depth = pl.ds(lo * block, (hi - lo) * block)
        start = 0
        for out_ref in outs:
            width = out_ref.shape[1]

            def step(out_lo, size, start=start, out_ref=out_ref, depth=depth, hi=hi):
                cols = pl.ds(pl.multiple_of(start + out_lo, 128), size)
                part = dot_nn(acts_buf[:, depth], w_buf[depth, cols])
                if hi == count:
                    out_ref[:, pl.ds(pl.multiple_of(out_lo, 128), size)] = (total[:, cols] + part).astype(BF16)
                else:
                    total[:, cols] = part

            whole = width // tile
            if whole:
                pl.loop(0, whole)(lambda n: step(n * tile, tile))
            if width % tile:
                step(whole * tile, width % tile)
            start += width


def nn_pieces(pos, acts, parts, widths, tile):
    keys = [(step, other) for step in (0, 1, 3, 2) for other in range(2)]
    halves = [parts[step][other][part] for step, other in keys for part in range(2)]
    tokens, depth = acts.shape
    width = sum(widths)
    count = len(keys)
    anywhere = pl.BlockSpec(memory_space=pl.ANY)
    return pl.pallas_call(
        functools.partial(nn_kernel, keys, 2, len(widths), tile),
        grid_spec=pltpu.PrefetchScalarGridSpec(
            num_scalar_prefetch=1,
            grid=(1,),
            in_specs=[anywhere] * (1 + 2 * count),
            out_specs=[pl.BlockSpec((tokens, size), lambda i, pos: (0, 0)) for size in widths],
            scratch_shapes=[
                pltpu.VMEM((tokens, depth), BF16),
                pltpu.VMEM((depth, width), BF16),
                pltpu.VMEM((tokens, width), F32),
                pltpu.SemaphoreType.DMA((count,)),
                pltpu.SemaphoreType.DMA((2 * count,)),
            ],
        ),
        out_shape=[jax.ShapeDtypeStruct((tokens, size), BF16) for size in widths],
        compiler_params=params(),
        cost_estimate=cost(2 * tokens * depth * width, 2 * depth * (tokens + width)),
    )(pos, acts, *halves)


def nt_kernel(keys, sides, first_row, pos_ref, *refs):
    count_left = len(sides)
    count = len(keys)
    lefts = refs[:count_left]
    halves = refs[count_left : count_left + 2 * count]
    out_ref, left_buf, w_buf, out_buf, left_sem, w_sem, out_sem = refs[count_left + 2 * count :]
    block = out_buf.shape[2]
    half = block // 2
    slots = w_buf.shape[0]
    left_copies = []
    start = 0
    for idx, (left, side) in enumerate(zip(lefts, sides)):
        chunks, _, width = left.shape
        first = 0 if side is None else (1 - pos_ref[1] if side else pos_ref[1]) * chunks
        source = left.at[:, pl.ds(first_row, left_buf.shape[1]), :]
        left_copies.append(pltpu.make_async_copy(source, left_buf.at[pl.ds(first, chunks), :, pl.ds(start, width)], left_sem.at[idx]))
        left_copies[-1].start()
        start += 0 if side == 0 else width

    def copies(idx, slot):
        for part in range(2):
            rows = pl.ds(half_start(pos_ref, part, half), half)
            yield pltpu.make_async_copy(halves[2 * idx + part], w_buf.at[slot, rows], w_sem.at[slot, part])

    def out_copy(idx):
        core = pos_ref[1]
        other = lax.rem(idx, 2)
        block_id = lax.rem(pos_ref[0] + idx // 2, NZ) * NC + core + other - 2 * core * other
        slot = lax.rem(idx, 2)
        return pltpu.make_async_copy(out_buf.at[slot], out_ref.at[:, pl.ds(pl.multiple_of(block_id * block, block), block)], out_sem.at[slot])

    for idx in range(slots - 1):
        for copy in copies(idx, idx):
            copy.start()
    for copy in left_copies:
        copy.wait()

    @pl.loop(0, count)
    def _(step):
        slot = lax.rem(step, slots)
        for idx in range(slots - 1, count):

            @pl.when(step + slots - 1 == idx)
            def _(idx=idx):
                for copy in copies(idx, idx % slots):
                    copy.start()

        for copy in copies(0, slot):
            copy.wait()

        @pl.when(step >= 2)
        def _():
            out_copy(step - 2).wait()

        out_buf[lax.rem(step, 2)] = dot_nt(left_buf[...].reshape(out_buf.shape[1], left_buf.shape[2]), w_buf[slot])
        out_copy(step).start()

    for idx in range(count - 2, count):
        out_copy(idx).wait()


def nt_pieces(pos, lefts, parts, chunk, first_row, rows):
    sides = (None, 0, 1)
    keys = [(step, other) for step in range(NZ) for other in range(2)]
    halves = [parts[step][other][part] for step, other in keys for part in range(2)]
    lefts = [left.reshape(-1, chunk, left.shape[1]) for left in lefts]
    chunks = lefts[0].shape[0]
    tokens = chunks * rows
    block = 2 * halves[0].shape[0]
    depth = block * len(keys)
    width = halves[0].shape[1]
    slots = 3
    anywhere = pl.BlockSpec(memory_space=pl.ANY)
    return pl.pallas_call(
        functools.partial(nt_kernel, keys, sides, first_row),
        grid_spec=pltpu.PrefetchScalarGridSpec(
            num_scalar_prefetch=1,
            grid=(1,),
            in_specs=[anywhere] * (len(lefts) + len(halves)),
            out_specs=anywhere,
            scratch_shapes=[
                pltpu.VMEM((chunks, rows, width), BF16),
                pltpu.VMEM((slots, block, width), BF16),
                pltpu.VMEM((2, tokens, block), F32),
                pltpu.SemaphoreType.DMA((len(lefts),)),
                pltpu.SemaphoreType.DMA((slots, 2)),
                pltpu.SemaphoreType.DMA((2,)),
            ],
        ),
        out_shape=jax.ShapeDtypeStruct((tokens, depth), F32),
        compiler_params=params(),
        cost_estimate=cost(2 * tokens * depth * width, 2 * depth * width + 4 * tokens * depth),
    )(pos, *lefts, *halves)


def picked_cols(pos_ref, idx, block):
    return pl.ds(pl.multiple_of((NC * idx + 1 - pos_ref[1]) * block, block), block)


def dma_kernel(kernel, pos, args, out_shape, scratch):
    anywhere = pl.BlockSpec(memory_space=pl.ANY)
    return pl.pallas_call(
        kernel,
        grid_spec=pltpu.PrefetchScalarGridSpec(
            num_scalar_prefetch=1, grid=(1,), in_specs=[anywhere] * len(args), out_specs=[anywhere] * len(out_shape), scratch_shapes=scratch
        ),
        out_shape=out_shape,
        compiler_params=params(),
        cost_estimate=cost(3e9, 16e6),
    )(pos, *args)


def pick_cols(pos, acts):
    tokens, depth = acts.shape
    block = depth // (NC * NZ)

    def kernel(pos_ref, in_ref, out_ref, buf, in_sem, out_sem):
        reads = [pltpu.make_async_copy(in_ref.at[:, picked_cols(pos_ref, idx, block)], buf.at[idx], in_sem.at[idx]) for idx in range(NZ)]
        writes = [pltpu.make_async_copy(buf.at[idx], out_ref.at[:, pl.ds(idx * block, block)], out_sem.at[idx]) for idx in range(NZ)]
        for read in reads:
            read.start()
        for read, write in zip(reads, writes):
            read.wait()
            write.start()
        for write in writes:
            write.wait()

    sems = pltpu.SemaphoreType.DMA((NZ,))
    return dma_kernel(kernel, pos, [acts], [jax.ShapeDtypeStruct((tokens, depth // 2), BF16)], [pltpu.VMEM((NZ, tokens, block), BF16), sems, sems])[0]


def grad_kernel(heights, pos_ref, *refs):
    pairs = len(heights)
    ins = refs[: 4 * pairs]
    outs = refs[4 * pairs : 4 * pairs + 2 * NZ]
    buf, sem = refs[4 * pairs + 2 * NZ :]
    half = buf.shape[2] // 2
    step = pl.program_id(0)
    slot = lax.rem(step, 2)

    def out_copy(idx, part):
        cols = pl.ds(half_start(pos_ref, part, half), half)
        return pltpu.make_async_copy(buf.at[idx % 2, :, cols], outs[2 * idx + part], sem.at[idx % 2, part])

    for idx in range(2, NZ):

        @pl.when(step == idx)
        def _(idx=idx):
            for part in range(2):
                out_copy(idx - 2, part).wait()

    start = 0
    for idx, height in enumerate(heights):
        own, recv, acts, acts_recv = ins[4 * idx : 4 * idx + 4]
        buf[slot, start : start + height, :] = dot_nn(own[...], acts[...]) + dot_nn(recv[...], acts_recv[...])
        start += height
    for idx in range(NZ):

        @pl.when(step == idx)
        def _(idx=idx):
            for part in range(2):
                out_copy(idx, part).start()

    @pl.when(step == NZ - 1)
    def _():
        for idx in (NZ - 2, NZ - 1):
            for part in range(2):
                out_copy(idx, part).wait()


def grad_pieces(pos, pairs):
    tokens, depth = pairs[0][2].shape
    cols = depth // (NZ * NC)
    in_specs = []
    args = []

    def z_of(n, pos):
        return lax.rem(pos[0] + jnp.where(n == 0, 2, jnp.where(n == 1, 1, jnp.where(n == 2, 3, 0))), NZ)

    for own, recv, acts, acts_recv, height, block in pairs:
        in_specs += [pl.BlockSpec((height, tokens), lambda n, pos, block=block: (block, 0))] * 2
        in_specs.append(pl.BlockSpec((tokens, cols), lambda n, pos: (0, z_of(n, pos) * NC + pos[1])))
        in_specs.append(pl.BlockSpec((tokens, cols), lambda n, pos: (0, z_of(n, pos))))
        args += [own, recv, acts, acts_recv]
    heights = [pair[4] for pair in pairs]
    rows = sum(heights)
    return pl.pallas_call(
        functools.partial(grad_kernel, heights),
        grid_spec=pltpu.PrefetchScalarGridSpec(
            num_scalar_prefetch=1,
            grid=(NZ,),
            in_specs=in_specs,
            out_specs=[pl.BlockSpec(memory_space=pl.ANY)] * (2 * NZ),
            scratch_shapes=[pltpu.VMEM((2, rows, cols), F32), pltpu.SemaphoreType.DMA((2, 2))],
        ),
        out_shape=[jax.ShapeDtypeStruct((rows, cols // 2), F32)] * (2 * NZ),
        compiler_params=params(),
        cost_estimate=cost(4 * rows * tokens * cols * NZ, 4 * tokens * cols * NZ),
        name="grad",
    )(pos, *args)


def sources(pos_ref, own_ref, first_ref, second_ref):
    return ((pos_ref[3] == 1, 0, own_ref), (pos_ref[3] == 0, 0, first_ref), (True, 1, second_ref))


def place(pos, own, first, second, height, block, transpose):
    cols = first.shape[1]
    spec = pl.BlockSpec((height, cols), lambda n, pos: (block, 0))

    def kernel(pos_ref, own_ref, first_ref, second_ref, out_ref):
        for chosen, idx, ref in sources(pos_ref, own_ref, first_ref, second_ref):

            @pl.when(jnp.logical_and(pl.program_id(0) == idx, chosen))
            def _(ref=ref):
                out_ref[...] = ref[...].T if transpose else ref[...]

    def order(n, pos):
        return jnp.where(n == 0, pos[2], 1 - pos[2])

    return pl.pallas_call(
        kernel,
        grid_spec=pltpu.PrefetchScalarGridSpec(
            num_scalar_prefetch=1,
            grid=(2,),
            in_specs=[spec] * 3,
            out_specs=pl.BlockSpec((cols, height), lambda n, pos: (0, order(n, pos))) if transpose else pl.BlockSpec((height, cols), lambda n, pos: (order(n, pos), 0)),
        ),
        out_shape=jax.ShapeDtypeStruct((cols, 2 * height) if transpose else (2 * height, cols), F32),
        compiler_params=params(),
        cost_estimate=cost(2e9, 16 * height * cols),
    )(pos, own, first, second)


def place_attn(pos, own, first, second, o_blk, head):
    rows, cols = first.shape
    qk = 2 * head

    def kernel(pos_ref, own_ref, first_ref, second_ref, out_ref, qkv_ref):
        for chosen, idx, ref in sources(pos_ref, own_ref, first_ref, second_ref):

            @pl.when(chosen)
            def _(idx=idx, ref=ref):
                bit = 1 - pos_ref[2] if idx else pos_ref[2]
                out_ref[pl.ds(pl.multiple_of(bit * o_blk, o_blk), o_blk), :] = ref[:o_blk, :]
                qkv_ref[:, pl.ds(pl.multiple_of(bit * qk, qk), qk)] = ref[o_blk : o_blk + qk, :].T
                qkv_ref[:, pl.ds(pl.multiple_of(2 * qk + bit * head, head), head)] = ref[o_blk + qk :, :].T

    def whole(*shape):
        return pl.BlockSpec(shape, lambda n, pos: (0, 0))

    shapes = ((2 * o_blk, cols), (cols, 2 * (qk + head)))
    return pl.pallas_call(
        kernel,
        grid_spec=pltpu.PrefetchScalarGridSpec(num_scalar_prefetch=1, grid=(1,), in_specs=[whole(rows, cols)] * 3, out_specs=[whole(*shape) for shape in shapes]),
        out_shape=[jax.ShapeDtypeStruct(shape, F32) for shape in shapes],
        compiler_params=params(),
        cost_estimate=cost(2e9, 16 * rows * cols),
        name="p_attn",
    )(pos, own, first, second)


def after(val, *earlier):
    return lax.optimization_barrier((val, *earlier))[0]


def ring(step, size):
    return [(src, (src + step) % size) for src in range(size)]


def hop_z(val, step):
    return lax.ppermute(val, "z", ring(step, NZ))


def swap_c(val):
    return lax.ppermute(val, "c", [(0, 1), (1, 0)])


def swap_y(val):
    return lax.ppermute(val, "y", [(src, src ^ 1) for src in range(NY)])


def turn(val, flip, home):
    def place_of(y_pos, c_pos):
        return y_pos * NC + c_pos

    pairs = [(place_of(2 * a + b, c), place_of(2 * c + (b ^ flip), a)) for a in range(2) for b in range(2) for c in range(NC) if home or flip or a != c]
    return lax.ppermute(val, ("y", "c"), pairs)


def swap_yc(val):
    pairs = [(y_pos * NC + c_pos, (y_pos ^ 1) * NC + 1 - c_pos) for y_pos in range(NY) for c_pos in range(NC)]
    return lax.ppermute(val, ("y", "c"), pairs)


def dot_nn(left, right):
    return lax.dot_general(left, right, (((1,), (0,)), ((), ())), preferred_element_type=F32)


def dot_nt(left, right):
    return lax.dot_general(left, right, (((1,), (1,)), ((), ())), preferred_element_type=F32)


def dot_tn(left, right):
    return lax.dot_general(left, right, (((0,), (0,)), ((), ())), preferred_element_type=F32)


def solution(mesh):
    wide_mesh = Mesh(mesh.devices.reshape(NZ, NY, NX, NC), ("z", "y", "x", "c"))
    rows = ("z", "y")
    cols = ("x", "c")
    act_spec = P(rows, cols, None)
    col_spec = P(rows, cols)
    row_spec = P(cols, rows)

    def layer(x_in, dy_in, norm_gain, w_qkv, w_out, w_gate, w_up, w_down, rope_cos, rope_sin):
        z_pos = lax.axis_index("z")
        y_pos = lax.axis_index("y")
        c_pos = lax.axis_index("c")
        even_y = y_pos % 2 == 0
        first_c = c_pos == 0
        pos = jnp.stack([z_pos, c_pos, y_pos % 2, y_pos // 2 == c_pos]).astype(jnp.int32)
        chunk = x_in.shape[1]
        head = 2 * rope_cos.shape[1]
        seq = rope_cos.shape[0]
        ff_blk = w_gate.shape[1] // 2
        o_blk = w_out.shape[0] // 2
        qkv_blk = o_blk + head

        def gather_rows(blocks):
            got = []
            for flip in (1, 0):
                got.insert(0, turn(jnp.where(even_y, blocks[flip], blocks[1 - flip]), flip, True))
            return got

        def gather_weight(piece):
            left, right = [], []
            for part in (1, 0):
                left.insert(0, hop_z(piece[part], 1))
                right.insert(0, hop_z(piece[part], -1))
            far = [hop_z(left[0], 1), hop_z(right[1], -1)]
            parts = []
            for mine in (piece, right, far, left):
                parts.append((mine, [swap_c(half) for half in mine]))
            return parts

        def grad_start(pairs, *earlier):
            far0, far1, up0, up1, down0, down1, own0, own1 = grad_pieces(after(pos, *earlier), pairs)
            far = (hop_z(far0, 1), hop_z(far1, -1))
            direct = (hop_z(up1, 1), hop_z(down0, -1))
            return (up0, down1), far, direct, (own0, own1)

        def grad_pass(state, *earlier):
            (up0, down1), far, direct, own = state
            sums = (up0 + after(far[0], *earlier), down1 + far[1])
            passed = (hop_z(sums[0], 1), hop_z(sums[1], -1))
            return direct, passed, own, sums

        def grad_back(state, *earlier):
            direct, passed, own = state[:3]
            first = own[0] + after(passed[0], *earlier) + direct[1]
            second = own[1] + direct[0] + passed[1]
            return first, turn(first, 0, False), turn(second, 1, False)

        def my_rows(val, mine):
            return lax.dynamic_slice_in_dim(val, (c_pos if mine else 1 - c_pos) * seq, seq, axis=0)

        def both_rows(own, got):
            return jnp.concatenate([jnp.where(first_c, own, got), jnp.where(first_c, got, own)], axis=0)

        cos_tab = jnp.concatenate([rope_cos, rope_cos], axis=1)
        sin_tab = jnp.concatenate([-rope_sin, rope_sin], axis=1)

        def qkv_cols(bit):
            first = 2 * head * bit
            third = HEAD_GROUP * head + head * bit
            return [w_qkv[:, first : first + 2 * head], w_qkv[:, third : third + head]]

        def block(weight, bit):
            size = weight.shape[1] // 2
            return weight[:, bit * size : (bit + 1) * size]

        down_t = w_down.T
        out_t = w_out.T
        wf_piece = gather_rows([jnp.concatenate([block(w_gate, j), block(w_up, j), *qkv_cols(j)], axis=1) for j in range(2)])
        ws_piece = gather_rows([jnp.concatenate([block(down_t, j), block(out_t, j)], axis=1) for j in range(2)])

        x_rows = after(x_in[0], cos_tab, sin_tab).astype(F32)
        normed, norm_pull = jax.vjp(lambda row_vals: norm_fwd(row_vals, norm_gain), x_rows)
        h_all = lax.all_gather(after(normed.astype(BF16), wf_piece[1]), ("y", "x"), axis=0, tiled=True)
        dy_all = lax.all_gather(after(dy_in[0], wf_piece[1]), ("y", "x"), axis=0, tiled=True)
        wf_parts = gather_weight(wf_piece)
        ws_parts = gather_weight(ws_piece)

        gate_up, qkv_tok = nn_pieces(pos, h_all, wf_parts, (2 * ff_blk, qkv_blk), 512)
        third = qkv_tok[:, o_blk:]
        qkv_other = swap_c(my_rows(qkv_tok, False))
        third_own = swap_y(my_rows(third, True))
        third_other = swap_yc(my_rows(third, False))
        act_val, act_t = act_fwd(after(gate_up, qkv_tok))
        act_recv = swap_c(act_t)
        qkv_seq, attn_own, attn_other = attn_fwd(after(pos, act_t), qkv_tok, qkv_other, third_own, third_other, cos_tab, sin_tab)
        attn_got = swap_c(attn_other)
        y_part = nt_pieces(after(pos, attn_own), [act_val, attn_own, attn_got], ws_parts, chunk, 0, chunk)
        mix_sum = lax.psum_scatter(y_part, ("y", "x"), scatter_dimension=0, tiled=True)
        y_out = (x_rows + mix_sum).astype(BF16)[None]

        h_picked = pick_cols(after(pos, y_part), h_all)
        h_recv = swap_c(h_picked)
        dy_picked = pick_cols(after(pos, h_picked), dy_all)
        dy_recv = swap_c(dy_picked)
        g_act = grad_start([(act_t, act_recv, dy_all, dy_recv, ff_blk, 0)], dy_picked)
        d_act, d_attn = nn_pieces(after(pos, g_act[3][0]), dy_all, ws_parts, (ff_blk, o_blk), 256)
        d_attn_other = swap_c(my_rows(d_attn, False))
        d_gate_up, d_gate_up_t = act_bwd(gate_up, d_act)
        d_gate_up_recv = swap_c(d_gate_up_t)
        d_queries, keep, send = attn_bwd(after(pos, d_gate_up_t), qkv_seq, d_attn, d_attn_other, cos_tab, sin_tab)
        got = swap_y(send)
        g_act = grad_pass(g_act, d_queries)
        g_gate = grad_start([(d_gate_up_t, d_gate_up_recv, h_all, h_recv, ff_blk, 0)], *g_act[3])
        b_act = grad_back(g_act, g_gate[3][0])
        d_own, d_other = attn_post(after(pos, g_gate[3][0]), d_queries, keep, got, cos_tab, sin_tab)
        d_got = swap_c(d_other)
        dh_part = nt_pieces(pos, [d_gate_up, d_own, d_got], wf_parts, chunk, 0, chunk)
        d_h = lax.psum_scatter(dh_part, ("y", "x"), scatter_dimension=0, tiled=True)
        g_gate = grad_pass(g_gate, dh_part)
        g_up = grad_start([(d_gate_up_t, d_gate_up_recv, h_all, h_recv, ff_blk, 1)], *g_gate[3])
        d_h = d_h.astype(BF16)
        dx_out = (dy_in[0].astype(F32) + norm_pull(d_h.astype(F32))[0]).astype(BF16)[None]

        attn_t = both_rows(attn_own, attn_got).T
        d_qkv_t = both_rows(d_own, d_got).T
        attn_recv = swap_c(attn_t)
        d_qkv_recv = swap_c(d_qkv_t)
        g_attn = grad_start([(attn_t, attn_recv, dy_all, dy_recv, o_blk, 0), (d_qkv_t, d_qkv_recv, h_all, h_recv, qkv_blk, 0)], g_up[3][0])
        g_up = grad_pass(g_up, g_attn[3][0])
        g_attn = grad_pass(g_attn)
        b_gate = grad_back(g_gate)
        b_up = grad_back(g_up)
        b_attn = grad_back(g_attn)
        dw_down = place(pos, *b_act, ff_blk, 0, False)
        dw_gate = place(pos, *b_gate, ff_blk, 0, True)
        dw_up = place(pos, *b_up, ff_blk, 0, True)
        dw_out, dw_qkv = place_attn(after(pos, dx_out, dw_up), *b_attn, o_blk, head)
        return y_out, dx_out, dw_qkv, dw_out, dw_gate, dw_up, dw_down


    return jax.shard_map(
        layer,
        mesh=wide_mesh,
        in_specs=(act_spec, act_spec, P(), col_spec, row_spec, col_spec, col_spec, row_spec, P(), P()),
        out_specs=(act_spec, act_spec, col_spec, row_spec, col_spec, col_spec, row_spec),
        check_vma=False,
    )
```

```python
import functools

import jax
import jax.numpy as jnp
from jax import lax
from jax.experimental import pallas as pl
from jax.experimental.pallas import tpu as pltpu
from jax.sharding import Mesh, PartitionSpec as P


NORM_EPS = 1e-5
NZ = 4
NY = 4
NX = 4
NC = 2
HEAD_GROUP = 4
F32 = jnp.float32
BF16 = jnp.bfloat16
VMEM_LIMIT = 67043328


def norm_fwd(row_vals, norm_gain):
    return row_vals * lax.rsqrt(jnp.mean(row_vals * row_vals, axis=-1, keepdims=True) + NORM_EPS) * norm_gain


def rotate(wide, cos_tab, sin_tab):
    return wide * cos_tab + pltpu.roll(wide, wide.shape[-1] // 2, wide.ndim - 1) * sin_tab


def rotate_back(wide, cos_tab, sin_tab):
    return wide * cos_tab - pltpu.roll(wide, wide.shape[-1] // 2, wide.ndim - 1) * sin_tab


def cost(flops, bytes_accessed):
    return pl.CostEstimate(flops=int(flops) // 20, bytes_accessed=int(bytes_accessed), transcendentals=0)


def params(**extra):
    return pltpu.CompilerParams(vmem_limit_bytes=VMEM_LIMIT, **extra)


def head_probs(q_rot, k_rot, scale):
    scores = dot_nt(q_rot, k_rot) * scale
    row_ids = lax.broadcasted_iota(jnp.int32, scores.shape, 0)
    col_ids = lax.broadcasted_iota(jnp.int32, scores.shape, 1)
    scores = jnp.where(row_ids >= col_ids, scores, -1e30)
    weights = jnp.exp(scores - jnp.max(scores, axis=-1, keepdims=True))
    return weights / jnp.sum(weights, axis=-1, keepdims=True)


def half_rows(core, idx, chunk):
    return pl.ds(pl.multiple_of((NC * idx + core) * chunk, chunk), chunk)


def chunk_rows(idx, chunk):
    return slice(idx * chunk, (idx + 1) * chunk)


def attn_fwd_kernel(heads, head, pos_ref, own_ref, other_ref, own_third_ref, other_third_ref, cos_ref, sin_ref, seq_ref, o_ref, o_other_ref, o_buf):
    core, odd = pos_ref[1], pos_ref[2]
    chunk = own_ref.shape[0] // NX
    width = heads * head
    mine = pl.ds(pl.multiple_of(width + odd * head, head), head)
    theirs = pl.ds(pl.multiple_of(width + (1 - odd) * head, head), head)
    for side, part_ref, third_ref in ((core, own_ref, own_third_ref), (1 - core, other_ref, other_third_ref)):
        for idx in range(NX):
            rows = half_rows(side, idx, chunk)
            seq_ref[0, rows, pl.ds(0, width)] = part_ref[chunk_rows(idx, chunk), :width]
            seq_ref[0, rows, mine] = part_ref[chunk_rows(idx, chunk), width:]
            seq_ref[0, rows, theirs] = third_ref[chunk_rows(idx, chunk), :]
    cos_tab, sin_tab = cos_ref[...], sin_ref[...]
    k_rot = rotate(seq_ref[0, :, width : width + head].astype(F32), cos_tab, sin_tab).astype(BF16)
    values = seq_ref[0, :, width + head :]
    for idx in range(heads):
        lanes = slice(idx * head, (idx + 1) * head)
        q_rot = rotate(seq_ref[0, :, lanes].astype(F32), cos_tab, sin_tab).astype(BF16)
        probs = head_probs(q_rot, k_rot, head**-0.5)
        o_buf[:, lanes] = dot_nn(probs.astype(BF16), values).astype(BF16)
    for side, out_ref in ((core, o_ref), (1 - core, o_other_ref)):
        for idx in range(NX):
            out_ref[chunk_rows(idx, chunk), :] = o_buf[half_rows(side, idx, chunk), :]


def attn_bwd_kernel(heads, head, pos_ref, seq_ref, own_ref, other_ref, cos_ref, sin_ref, dq_ref, keep_ref, send_ref, do_buf):
    core, odd = pos_ref[1], pos_ref[2]
    chunk = own_ref.shape[0] // NX
    width = heads * head
    for side, part_ref in ((core, own_ref), (1 - core, other_ref)):
        for idx in range(NX):
            do_buf[half_rows(side, idx, chunk), :] = part_ref[chunk_rows(idx, chunk), :]
    cos_tab, sin_tab = cos_ref[...], sin_ref[...]
    k_rot = rotate(seq_ref[0, :, width : width + head].astype(F32), cos_tab, sin_tab).astype(BF16)
    values = seq_ref[0, :, width + head :]
    d_keys = jnp.zeros(k_rot.shape, F32)
    d_values = jnp.zeros(k_rot.shape, F32)
    for idx in range(heads):
        lanes = slice(idx * head, (idx + 1) * head)
        q_rot = rotate(seq_ref[0, :, lanes].astype(F32), cos_tab, sin_tab).astype(BF16)
        d_out = do_buf[:, lanes]
        probs = head_probs(q_rot, k_rot, head**-0.5)
        d_values += dot_tn(probs.astype(BF16), d_out)
        d_probs = dot_nt(d_out, values).astype(BF16).astype(F32)
        d_scores = probs * (d_probs - jnp.sum(d_probs * probs, axis=-1, keepdims=True))
        d_scores = (d_scores * head**-0.5).astype(BF16)
        d_q_rot = dot_nn(d_scores, k_rot).astype(BF16)
        dq_ref[0, :, lanes] = rotate_back(d_q_rot.astype(F32), cos_tab, sin_tab).astype(BF16)
        d_keys += dot_tn(d_scores, q_rot)

    @pl.when(odd == 0)
    def _():
        keep_ref[0] = d_keys
        send_ref[0] = d_values

    @pl.when(odd == 1)
    def _():
        keep_ref[0] = d_values
        send_ref[0] = d_keys


def attn_post_kernel(heads, head, pos_ref, dq_ref, keep_ref, got_ref, cos_ref, sin_ref, own_ref, other_ref, third_buf):
    core, odd = pos_ref[1], pos_ref[2]
    chunk = own_ref.shape[0] // NX
    width = heads * head
    total = (keep_ref[0] + got_ref[0]).astype(BF16)

    @pl.when(odd == 0)
    def _():
        third_buf[...] = rotate_back(total.astype(F32), cos_ref[...], sin_ref[...]).astype(BF16)

    @pl.when(odd == 1)
    def _():
        third_buf[...] = total

    for side, out_ref in ((core, own_ref), (1 - core, other_ref)):
        for idx in range(NX):
            rows = half_rows(side, idx, chunk)
            out_ref[chunk_rows(idx, chunk), :width] = dq_ref[0, rows, :]
            out_ref[chunk_rows(idx, chunk), width:] = third_buf[rows, :]


def per_sequence(kernel, pos, args, specs, out_specs, out_shape, scratch, flops):
    return pl.pallas_call(
        kernel,
        grid_spec=pltpu.PrefetchScalarGridSpec(num_scalar_prefetch=1, grid=(2,), in_specs=specs, out_specs=out_specs, scratch_shapes=scratch),
        out_shape=out_shape,
        compiler_params=params(),
        cost_estimate=cost(flops, 4e6),
    )(pos, *args)


def own_spec(rows, width):
    return pl.BlockSpec((rows, width), lambda i, pos: (2 * pos[1] + i, 0))


def pair_spec(rows, width):
    return pl.BlockSpec((rows, width), lambda i, pos: (i, 0))


def seq_spec(seq, width):
    return pl.BlockSpec((1, seq, width), lambda i, pos: (i, 0, 0))


def table_spec(table):
    return pl.BlockSpec(table.shape, lambda i, pos: (0, 0))


def attn_fwd(pos, qkv_tok, other, own_third, other_third, cos_tab, sin_tab):
    seq, head = cos_tab.shape
    width = qkv_tok.shape[1] - head
    rows = seq // 2
    half = jax.ShapeDtypeStruct((seq, width), BF16)
    return per_sequence(
        functools.partial(attn_fwd_kernel, width // head, head),
        pos,
        (qkv_tok, other, own_third, other_third, cos_tab, sin_tab),
        [own_spec(rows, width + head), pair_spec(rows, width + head), pair_spec(rows, head), pair_spec(rows, head), table_spec(cos_tab), table_spec(sin_tab)],
        [seq_spec(seq, width + 2 * head), pair_spec(rows, width), pair_spec(rows, width)],
        [jax.ShapeDtypeStruct((2, seq, width + 2 * head), BF16), half, half],
        [pltpu.VMEM((seq, width), BF16)],
        16e9,
    )


def attn_bwd(pos, qkv_seq, d_attn, other, cos_tab, sin_tab):
    seq, head = cos_tab.shape
    width = d_attn.shape[1]
    rows = seq // 2
    part = jax.ShapeDtypeStruct((2, seq, head), F32)
    return per_sequence(
        functools.partial(attn_bwd_kernel, width // head, head),
        pos,
        (qkv_seq, d_attn, other, cos_tab, sin_tab),
        [seq_spec(seq, width + 2 * head), own_spec(rows, width), pair_spec(rows, width), table_spec(cos_tab), table_spec(sin_tab)],
        [seq_spec(seq, width), seq_spec(seq, head), seq_spec(seq, head)],
        [jax.ShapeDtypeStruct((2, seq, width), BF16), part, part],
        [pltpu.VMEM((seq, width), BF16)],
        16e9,
    )


def attn_post(pos, d_queries, keep, got, cos_tab, sin_tab):
    seq, head = cos_tab.shape
    width = d_queries.shape[2]
    rows = seq // 2
    half = jax.ShapeDtypeStruct((seq, width + head), BF16)
    return per_sequence(
        functools.partial(attn_post_kernel, width // head, head),
        pos,
        (d_queries, keep, got, cos_tab, sin_tab),
        [seq_spec(seq, width), seq_spec(seq, head), seq_spec(seq, head), table_spec(cos_tab), table_spec(sin_tab)],
        [pair_spec(rows, width + head), pair_spec(rows, width + head)],
        [half, half],
        [pltpu.VMEM((seq, head), BF16)],
        2e9,
    )


def act_fwd_kernel(half, ab_ref, u_ref, ut_ref):
    gate_val = ab_ref[:, :half].astype(F32)
    up_val = ab_ref[:, half:].astype(F32)
    act_val = gate_val * jax.nn.sigmoid(gate_val) * up_val
    u_ref[...] = act_val.astype(BF16)
    ut_ref[...] = act_val.T.astype(BF16)


def act_fwd(gate_up):
    tokens, width = gate_up.shape
    half = width // 2
    rows = tokens // 4
    return pl.pallas_call(
        functools.partial(act_fwd_kernel, half),
        grid=(4,),
        in_specs=[pl.BlockSpec((rows, width), lambda i: (i, 0))],
        out_specs=[pl.BlockSpec((rows, half), lambda i: (i, 0)), pl.BlockSpec((half, rows), lambda i: (0, i))],
        out_shape=[jax.ShapeDtypeStruct((tokens, half), BF16), jax.ShapeDtypeStruct((half, tokens), BF16)],
        compiler_params=params(),
        cost_estimate=cost(4e9, 8e6),
        name="act_fwd",
    )(gate_up)


def act_bwd_kernel(half, ab_ref, du_ref, dab_ref, dabt_ref):
    gate_val = ab_ref[:, :half].astype(F32)
    up_val = ab_ref[:, half:].astype(F32)
    d_act = du_ref[...].astype(F32)
    sig = jax.nn.sigmoid(gate_val)
    d_silu = d_act * up_val
    d_gate = d_silu * sig + d_silu * gate_val * (sig * (1.0 - sig))
    d_up = d_act * (gate_val * sig)
    dab_ref[:, :half] = d_gate.astype(BF16)
    dab_ref[:, half:] = d_up.astype(BF16)
    dabt_ref[:half, :] = d_gate.T.astype(BF16)
    dabt_ref[half:, :] = d_up.T.astype(BF16)


def act_bwd(gate_up, d_mixed):
    tokens, width = gate_up.shape
    half = width // 2
    rows = tokens // 4
    return pl.pallas_call(
        functools.partial(act_bwd_kernel, half),
        grid=(4,),
        in_specs=[pl.BlockSpec((rows, width), lambda i: (i, 0)), pl.BlockSpec((rows, half), lambda i: (i, 0))],
        out_specs=[pl.BlockSpec((rows, width), lambda i: (i, 0)), pl.BlockSpec((width, rows), lambda i: (0, i))],
        out_shape=[jax.ShapeDtypeStruct((tokens, width), BF16), jax.ShapeDtypeStruct((width, tokens), BF16)],
        compiler_params=params(),
        cost_estimate=cost(8e9, 14e6),
        name="act_bwd",
    )(gate_up, d_mixed)


def piece_block(pos_ref, step, other):
    core = pos_ref[1]
    return lax.rem(pos_ref[0] + step, NZ) * NC + (1 - core if other else core)


def half_start(pos_ref, part, half):
    return pl.multiple_of((1 - pos_ref[2] if part else pos_ref[2]) * half, half)


def nn_kernel(keys, first, count_out, tile, pos_ref, acts_ref, *refs):
    count = len(keys)
    halves = refs[: 2 * count]
    outs = refs[2 * count : 2 * count + count_out]
    acts_buf, w_buf, total, acts_sem, w_sem = refs[2 * count + count_out :]
    block = acts_buf.shape[1] // count
    half = block // 2
    copies = []
    for idx in range(count):
        cols = pl.ds(pl.multiple_of(piece_block(pos_ref, *keys[idx]) * block, block), block)
        copies.append([pltpu.make_async_copy(acts_ref.at[:, cols], acts_buf.at[:, pl.ds(idx * block, block)], acts_sem.at[idx])])
        for part in range(2):
            rows = pl.ds(idx * block + half_start(pos_ref, part, half), half)
            copies[-1].append(pltpu.make_async_copy(halves[2 * idx + part], w_buf.at[rows], w_sem.at[2 * idx + part]))
    for group in copies:
        for copy in group:
            copy.start()
    for lo, hi in ((0, first), (first, count)):
        for group in copies[lo:hi]:
            for copy in group:
                copy.wait()
        depth = pl.ds(lo * block, (hi - lo) * block)
        start = 0
        for out_ref in outs:
            width = out_ref.shape[1]

            def step(out_lo, size, start=start, out_ref=out_ref, depth=depth, hi=hi):
                cols = pl.ds(pl.multiple_of(start + out_lo, 128), size)
                part = dot_nn(acts_buf[:, depth], w_buf[depth, cols])
                if hi == count:
                    out_ref[:, pl.ds(pl.multiple_of(out_lo, 128), size)] = (total[:, cols] + part).astype(BF16)
                else:
                    total[:, cols] = part

            whole = width // tile
            if whole:
                pl.loop(0, whole)(lambda n: step(n * tile, tile))
            if width % tile:
                step(whole * tile, width % tile)
            start += width


def nn_pieces(pos, acts, parts, widths, tile):
    keys = [(step, other) for step in (0, 1, 3, 2) for other in range(2)]
    halves = [parts[step][other][part] for step, other in keys for part in range(2)]
    tokens, depth = acts.shape
    width = sum(widths)
    count = len(keys)
    anywhere = pl.BlockSpec(memory_space=pl.ANY)
    return pl.pallas_call(
        functools.partial(nn_kernel, keys, 2, len(widths), tile),
        grid_spec=pltpu.PrefetchScalarGridSpec(
            num_scalar_prefetch=1,
            grid=(1,),
            in_specs=[anywhere] * (1 + 2 * count),
            out_specs=[pl.BlockSpec((tokens, size), lambda i, pos: (0, 0)) for size in widths],
            scratch_shapes=[
                pltpu.VMEM((tokens, depth), BF16),
                pltpu.VMEM((depth, width), BF16),
                pltpu.VMEM((tokens, width), F32),
                pltpu.SemaphoreType.DMA((count,)),
                pltpu.SemaphoreType.DMA((2 * count,)),
            ],
        ),
        out_shape=[jax.ShapeDtypeStruct((tokens, size), BF16) for size in widths],
        compiler_params=params(),
        cost_estimate=cost(2 * tokens * depth * width, 2 * depth * (tokens + width)),
    )(pos, acts, *halves)


def nt_kernel(keys, sides, first_row, pos_ref, *refs):
    count_left = len(sides)
    count = len(keys)
    lefts = refs[:count_left]
    halves = refs[count_left : count_left + 2 * count]
    out_ref, left_buf, w_buf, out_buf, left_sem, w_sem, out_sem = refs[count_left + 2 * count :]
    block = out_buf.shape[2]
    half = block // 2
    slots = w_buf.shape[0]
    left_copies = []
    start = 0
    for idx, (left, side) in enumerate(zip(lefts, sides)):
        chunks, _, width = left.shape
        first = 0 if side is None else (1 - pos_ref[1] if side else pos_ref[1]) * chunks
        source = left.at[:, pl.ds(first_row, left_buf.shape[1]), :]
        left_copies.append(pltpu.make_async_copy(source, left_buf.at[pl.ds(first, chunks), :, pl.ds(start, width)], left_sem.at[idx]))
        left_copies[-1].start()
        start += 0 if side == 0 else width

    def copies(idx, slot):
        for part in range(2):
            rows = pl.ds(half_start(pos_ref, part, half), half)
            yield pltpu.make_async_copy(halves[2 * idx + part], w_buf.at[slot, rows], w_sem.at[slot, part])

    def out_copy(idx):
        core = pos_ref[1]
        other = lax.rem(idx, 2)
        block_id = lax.rem(pos_ref[0] + idx // 2, NZ) * NC + core + other - 2 * core * other
        slot = lax.rem(idx, 2)
        return pltpu.make_async_copy(out_buf.at[slot], out_ref.at[:, pl.ds(pl.multiple_of(block_id * block, block), block)], out_sem.at[slot])

    for idx in range(slots - 1):
        for copy in copies(idx, idx):
            copy.start()
    for copy in left_copies:
        copy.wait()

    @pl.loop(0, count)
    def _(step):
        slot = lax.rem(step, slots)
        for idx in range(slots - 1, count):

            @pl.when(step + slots - 1 == idx)
            def _(idx=idx):
                for copy in copies(idx, idx % slots):
                    copy.start()

        for copy in copies(0, slot):
            copy.wait()

        @pl.when(step >= 2)
        def _():
            out_copy(step - 2).wait()

        out_buf[lax.rem(step, 2)] = dot_nt(left_buf[...].reshape(out_buf.shape[1], left_buf.shape[2]), w_buf[slot])
        out_copy(step).start()

    for idx in range(count - 2, count):
        out_copy(idx).wait()


def nt_pieces(pos, lefts, parts, chunk, first_row, rows):
    sides = (None, 0, 1)
    keys = [(step, other) for step in range(NZ) for other in range(2)]
    halves = [parts[step][other][part] for step, other in keys for part in range(2)]
    lefts = [left.reshape(-1, chunk, left.shape[1]) for left in lefts]
    chunks = lefts[0].shape[0]
    tokens = chunks * rows
    block = 2 * halves[0].shape[0]
    depth = block * len(keys)
    width = halves[0].shape[1]
    slots = 3
    anywhere = pl.BlockSpec(memory_space=pl.ANY)
    return pl.pallas_call(
        functools.partial(nt_kernel, keys, sides, first_row),
        grid_spec=pltpu.PrefetchScalarGridSpec(
            num_scalar_prefetch=1,
            grid=(1,),
            in_specs=[anywhere] * (len(lefts) + len(halves)),
            out_specs=anywhere,
            scratch_shapes=[
                pltpu.VMEM((chunks, rows, width), BF16),
                pltpu.VMEM((slots, block, width), BF16),
                pltpu.VMEM((2, tokens, block), F32),
                pltpu.SemaphoreType.DMA((len(lefts),)),
                pltpu.SemaphoreType.DMA((slots, 2)),
                pltpu.SemaphoreType.DMA((2,)),
            ],
        ),
        out_shape=jax.ShapeDtypeStruct((tokens, depth), F32),
        compiler_params=params(),
        cost_estimate=cost(2 * tokens * depth * width, 2 * depth * width + 4 * tokens * depth),
    )(pos, *lefts, *halves)


def picked_cols(pos_ref, idx, block):
    return pl.ds(pl.multiple_of((NC * idx + 1 - pos_ref[1]) * block, block), block)


def dma_kernel(kernel, pos, args, out_shape, scratch):
    anywhere = pl.BlockSpec(memory_space=pl.ANY)
    return pl.pallas_call(
        kernel,
        grid_spec=pltpu.PrefetchScalarGridSpec(
            num_scalar_prefetch=1, grid=(1,), in_specs=[anywhere] * len(args), out_specs=[anywhere] * len(out_shape), scratch_shapes=scratch
        ),
        out_shape=out_shape,
        compiler_params=params(),
        cost_estimate=cost(3e9, 16e6),
    )(pos, *args)


def pick_cols(pos, acts):
    tokens, depth = acts.shape
    block = depth // (NC * NZ)

    def kernel(pos_ref, in_ref, out_ref, buf, in_sem, out_sem):
        reads = [pltpu.make_async_copy(in_ref.at[:, picked_cols(pos_ref, idx, block)], buf.at[idx], in_sem.at[idx]) for idx in range(NZ)]
        writes = [pltpu.make_async_copy(buf.at[idx], out_ref.at[:, pl.ds(idx * block, block)], out_sem.at[idx]) for idx in range(NZ)]
        for read in reads:
            read.start()
        for read, write in zip(reads, writes):
            read.wait()
            write.start()
        for write in writes:
            write.wait()

    sems = pltpu.SemaphoreType.DMA((NZ,))
    return dma_kernel(kernel, pos, [acts], [jax.ShapeDtypeStruct((tokens, depth // 2), BF16)], [pltpu.VMEM((NZ, tokens, block), BF16), sems, sems])[0]


def grad_kernel(heights, pos_ref, *refs):
    pairs = len(heights)
    ins = refs[: 4 * pairs]
    outs = refs[4 * pairs : 4 * pairs + 2 * NZ]
    buf, sem = refs[4 * pairs + 2 * NZ :]
    half = buf.shape[2] // 2
    step = pl.program_id(0)
    slot = lax.rem(step, 2)

    def out_copy(idx, part):
        cols = pl.ds(half_start(pos_ref, part, half), half)
        return pltpu.make_async_copy(buf.at[idx % 2, :, cols], outs[2 * idx + part], sem.at[idx % 2, part])

    for idx in range(2, NZ):

        @pl.when(step == idx)
        def _(idx=idx):
            for part in range(2):
                out_copy(idx - 2, part).wait()

    start = 0
    for idx, height in enumerate(heights):
        own, recv, acts, acts_recv = ins[4 * idx : 4 * idx + 4]
        buf[slot, start : start + height, :] = dot_nn(own[...], acts[...]) + dot_nn(recv[...], acts_recv[...])
        start += height
    for idx in range(NZ):

        @pl.when(step == idx)
        def _(idx=idx):
            for part in range(2):
                out_copy(idx, part).start()

    @pl.when(step == NZ - 1)
    def _():
        for idx in (NZ - 2, NZ - 1):
            for part in range(2):
                out_copy(idx, part).wait()


def grad_pieces(pos, pairs):
    tokens, depth = pairs[0][2].shape
    cols = depth // (NZ * NC)
    in_specs = []
    args = []

    def z_of(n, pos):
        return lax.rem(pos[0] + jnp.where(n == 0, 2, jnp.where(n == 1, 1, jnp.where(n == 2, 3, 0))), NZ)

    for own, recv, acts, acts_recv, height, block in pairs:
        in_specs += [pl.BlockSpec((height, tokens), lambda n, pos, block=block: (block, 0))] * 2
        in_specs.append(pl.BlockSpec((tokens, cols), lambda n, pos: (0, z_of(n, pos) * NC + pos[1])))
        in_specs.append(pl.BlockSpec((tokens, cols), lambda n, pos: (0, z_of(n, pos))))
        args += [own, recv, acts, acts_recv]
    heights = [pair[4] for pair in pairs]
    rows = sum(heights)
    return pl.pallas_call(
        functools.partial(grad_kernel, heights),
        grid_spec=pltpu.PrefetchScalarGridSpec(
            num_scalar_prefetch=1,
            grid=(NZ,),
            in_specs=in_specs,
            out_specs=[pl.BlockSpec(memory_space=pl.ANY)] * (2 * NZ),
            scratch_shapes=[pltpu.VMEM((2, rows, cols), F32), pltpu.SemaphoreType.DMA((2, 2))],
        ),
        out_shape=[jax.ShapeDtypeStruct((rows, cols // 2), F32)] * (2 * NZ),
        compiler_params=params(),
        cost_estimate=cost(4 * rows * tokens * cols * NZ, 4 * tokens * cols * NZ),
        name="grad",
    )(pos, *args)


def sources(pos_ref, own_ref, first_ref, second_ref):
    return ((pos_ref[3] == 1, 0, own_ref), (pos_ref[3] == 0, 0, first_ref), (True, 1, second_ref))


def place(pos, own, first, second, height, block, transpose):
    cols = first.shape[1]
    spec = pl.BlockSpec((height, cols), lambda n, pos: (block, 0))

    def kernel(pos_ref, own_ref, first_ref, second_ref, out_ref):
        for chosen, idx, ref in sources(pos_ref, own_ref, first_ref, second_ref):

            @pl.when(jnp.logical_and(pl.program_id(0) == idx, chosen))
            def _(ref=ref):
                out_ref[...] = ref[...].T if transpose else ref[...]

    def order(n, pos):
        return jnp.where(n == 0, pos[2], 1 - pos[2])

    return pl.pallas_call(
        kernel,
        grid_spec=pltpu.PrefetchScalarGridSpec(
            num_scalar_prefetch=1,
            grid=(2,),
            in_specs=[spec] * 3,
            out_specs=pl.BlockSpec((cols, height), lambda n, pos: (0, order(n, pos))) if transpose else pl.BlockSpec((height, cols), lambda n, pos: (order(n, pos), 0)),
        ),
        out_shape=jax.ShapeDtypeStruct((cols, 2 * height) if transpose else (2 * height, cols), F32),
        compiler_params=params(),
        cost_estimate=cost(2e9, 16 * height * cols),
    )(pos, own, first, second)


def place_attn(pos, own, first, second, o_blk, head):
    rows, cols = first.shape
    qk = 2 * head

    def kernel(pos_ref, own_ref, first_ref, second_ref, out_ref, qkv_ref):
        for chosen, idx, ref in sources(pos_ref, own_ref, first_ref, second_ref):

            @pl.when(chosen)
            def _(idx=idx, ref=ref):
                bit = 1 - pos_ref[2] if idx else pos_ref[2]
                out_ref[pl.ds(pl.multiple_of(bit * o_blk, o_blk), o_blk), :] = ref[:o_blk, :]
                qkv_ref[:, pl.ds(pl.multiple_of(bit * qk, qk), qk)] = ref[o_blk : o_blk + qk, :].T
                qkv_ref[:, pl.ds(pl.multiple_of(2 * qk + bit * head, head), head)] = ref[o_blk + qk :, :].T

    def whole(*shape):
        return pl.BlockSpec(shape, lambda n, pos: (0, 0))

    shapes = ((2 * o_blk, cols), (cols, 2 * (qk + head)))
    return pl.pallas_call(
        kernel,
        grid_spec=pltpu.PrefetchScalarGridSpec(num_scalar_prefetch=1, grid=(1,), in_specs=[whole(rows, cols)] * 3, out_specs=[whole(*shape) for shape in shapes]),
        out_shape=[jax.ShapeDtypeStruct(shape, F32) for shape in shapes],
        compiler_params=params(),
        cost_estimate=cost(2e9, 16 * rows * cols),
        name="p_attn",
    )(pos, own, first, second)


def after(val, *earlier):
    return lax.optimization_barrier((val, *earlier))[0]


def ring(step, size):
    return [(src, (src + step) % size) for src in range(size)]


def hop_z(val, step):
    return lax.ppermute(val, "z", ring(step, NZ))


def swap_c(val):
    return lax.ppermute(val, "c", [(0, 1), (1, 0)])


def swap_y(val):
    return lax.ppermute(val, "y", [(src, src ^ 1) for src in range(NY)])


def turn(val, flip, home):
    def place_of(y_pos, c_pos):
        return y_pos * NC + c_pos

    pairs = [(place_of(2 * a + b, c), place_of(2 * c + (b ^ flip), a)) for a in range(2) for b in range(2) for c in range(NC) if home or flip or a != c]
    return lax.ppermute(val, ("y", "c"), pairs)


def swap_yc(val):
    pairs = [(y_pos * NC + c_pos, (y_pos ^ 1) * NC + 1 - c_pos) for y_pos in range(NY) for c_pos in range(NC)]
    return lax.ppermute(val, ("y", "c"), pairs)


def dot_nn(left, right):
    return lax.dot_general(left, right, (((1,), (0,)), ((), ())), preferred_element_type=F32)


def dot_nt(left, right):
    return lax.dot_general(left, right, (((1,), (1,)), ((), ())), preferred_element_type=F32)


def dot_tn(left, right):
    return lax.dot_general(left, right, (((0,), (0,)), ((), ())), preferred_element_type=F32)


def solution(mesh):
    wide_mesh = Mesh(mesh.devices.reshape(NZ, NY, NX, NC), ("z", "y", "x", "c"))
    rows = ("z", "y")
    cols = ("x", "c")
    act_spec = P(rows, cols, None)
    col_spec = P(rows, cols)
    row_spec = P(cols, rows)

    def layer(x_in, dy_in, norm_gain, w_qkv, w_out, w_gate, w_up, w_down, rope_cos, rope_sin):
        z_pos = lax.axis_index("z")
        y_pos = lax.axis_index("y")
        c_pos = lax.axis_index("c")
        even_y = y_pos % 2 == 0
        first_c = c_pos == 0
        pos = jnp.stack([z_pos, c_pos, y_pos % 2, y_pos // 2 == c_pos]).astype(jnp.int32)
        chunk = x_in.shape[1]
        head = 2 * rope_cos.shape[1]
        seq = rope_cos.shape[0]
        ff_blk = w_gate.shape[1] // 2
        o_blk = w_out.shape[0] // 2
        qkv_blk = o_blk + head

        def gather_rows(blocks):
            got = []
            for flip in (1, 0):
                got.insert(0, turn(jnp.where(even_y, blocks[flip], blocks[1 - flip]), flip, True))
            return got

        def gather_weight(piece):
            left, right = [], []
            for part in (1, 0):
                left.insert(0, hop_z(piece[part], 1))
                right.insert(0, hop_z(piece[part], -1))
            far = [hop_z(left[0], 1), hop_z(right[1], -1)]
            parts = []
            for mine in (piece, right, far, left):
                parts.append((mine, [swap_c(half) for half in mine]))
            return parts

        def grad_start(pairs, *earlier):
            far0, far1, up0, up1, down0, down1, own0, own1 = grad_pieces(after(pos, *earlier), pairs)
            far = (hop_z(far0, 1), hop_z(far1, -1))
            direct = (hop_z(up1, 1), hop_z(down0, -1))
            return (up0, down1), far, direct, (own0, own1)

        def grad_pass(state, *earlier):
            (up0, down1), far, direct, own = state
            sums = (up0 + after(far[0], *earlier), down1 + far[1])
            passed = (hop_z(sums[0], 1), hop_z(sums[1], -1))
            return direct, passed, own, sums

        def grad_back(state, *earlier):
            direct, passed, own = state[:3]
            first = own[0] + after(passed[0], *earlier) + direct[1]
            second = own[1] + direct[0] + passed[1]
            return first, turn(first, 0, False), turn(second, 1, False)

        def my_rows(val, mine):
            return lax.dynamic_slice_in_dim(val, (c_pos if mine else 1 - c_pos) * seq, seq, axis=0)

        def both_rows(own, got):
            return jnp.concatenate([jnp.where(first_c, own, got), jnp.where(first_c, got, own)], axis=0)

        cos_tab = jnp.concatenate([rope_cos, rope_cos], axis=1)
        sin_tab = jnp.concatenate([-rope_sin, rope_sin], axis=1)

        def qkv_cols(bit):
            first = 2 * head * bit
            third = HEAD_GROUP * head + head * bit
            return [w_qkv[:, first : first + 2 * head], w_qkv[:, third : third + head]]

        def block(weight, bit):
            size = weight.shape[1] // 2
            return weight[:, bit * size : (bit + 1) * size]

        down_t = w_down.T
        out_t = w_out.T
        wf_piece = gather_rows([jnp.concatenate([block(w_gate, j), block(w_up, j), *qkv_cols(j)], axis=1) for j in range(2)])
        ws_piece = gather_rows([jnp.concatenate([block(down_t, j), block(out_t, j)], axis=1) for j in range(2)])

        x_rows = after(x_in[0], cos_tab, sin_tab).astype(F32)
        normed, norm_pull = jax.vjp(lambda row_vals: norm_fwd(row_vals, norm_gain), x_rows)
        h_all = lax.all_gather(after(normed.astype(BF16), wf_piece[1]), ("y", "x"), axis=0, tiled=True)
        dy_all = lax.all_gather(after(dy_in[0], wf_piece[1]), ("y", "x"), axis=0, tiled=True)
        wf_parts = gather_weight(wf_piece)
        ws_parts = gather_weight(ws_piece)

        gate_up, qkv_tok = nn_pieces(pos, h_all, wf_parts, (2 * ff_blk, qkv_blk), 512)
        third = qkv_tok[:, o_blk:]
        qkv_other = swap_c(my_rows(qkv_tok, False))
        third_own = swap_y(my_rows(third, True))
        third_other = swap_yc(my_rows(third, False))
        act_val, act_t = act_fwd(after(gate_up, qkv_tok))
        act_recv = swap_c(act_t)
        h_picked = pick_cols(after(pos, act_t), h_all)
        h_recv = swap_c(h_picked)
        qkv_seq, attn_own, attn_other = attn_fwd(after(pos, h_picked), qkv_tok, qkv_other, third_own, third_other, cos_tab, sin_tab)
        attn_got = swap_c(attn_other)
        y_part = nt_pieces(after(pos, attn_own), [act_val, attn_own, attn_got], ws_parts, chunk, 0, chunk)
        mix_sum = lax.psum_scatter(y_part, ("y", "x"), scatter_dimension=0, tiled=True)
        y_out = (x_rows + mix_sum).astype(BF16)[None]

        dy_picked = pick_cols(after(pos, y_part), dy_all)
        dy_recv = swap_c(dy_picked)
        d_act, d_attn = nn_pieces(after(pos, dy_picked), dy_all, ws_parts, (ff_blk, o_blk), 256)
        d_attn_other = swap_c(my_rows(d_attn, False))
        g_act = grad_start([(act_t, act_recv, dy_all, dy_recv, ff_blk, 0)], d_attn)
        d_gate_up, d_gate_up_t = act_bwd(gate_up, after(d_act, g_act[3][0]))
        d_gate_up_recv = swap_c(d_gate_up_t)
        d_queries, keep, send = attn_bwd(after(pos, d_gate_up_t), qkv_seq, d_attn, d_attn_other, cos_tab, sin_tab)
        got = swap_y(send)
        g_act = grad_pass(g_act, d_queries)
        g_gate = grad_start([(d_gate_up_t, d_gate_up_recv, h_all, h_recv, ff_blk, 0)], *g_act[3])
        d_own, d_other = attn_post(after(pos, g_gate[3][0]), d_queries, keep, got, cos_tab, sin_tab)
        d_got = swap_c(d_other)
        dh_part = nt_pieces(pos, [d_gate_up, d_own, d_got], wf_parts, chunk, 0, chunk)
        d_h = lax.psum_scatter(dh_part, ("y", "x"), scatter_dimension=0, tiled=True)
        g_gate = grad_pass(g_gate, dh_part)
        g_up = grad_start([(d_gate_up_t, d_gate_up_recv, h_all, h_recv, ff_blk, 1)], *g_gate[3])
        b_act = grad_back(g_act, g_up[3][0])
        d_h = d_h.astype(BF16)
        dx_out = (dy_in[0].astype(F32) + norm_pull(d_h.astype(F32))[0]).astype(BF16)[None]

        attn_t = both_rows(attn_own, attn_got).T
        d_qkv_t = both_rows(d_own, d_got).T
        attn_recv = swap_c(attn_t)
        d_qkv_recv = swap_c(d_qkv_t)
        g_attn = grad_start([(attn_t, attn_recv, dy_all, dy_recv, o_blk, 0), (d_qkv_t, d_qkv_recv, h_all, h_recv, qkv_blk, 0)], g_up[3][0])
        g_up = grad_pass(g_up, g_attn[3][0])
        g_attn = grad_pass(g_attn)
        b_gate = grad_back(g_gate)
        b_up = grad_back(g_up)
        b_attn = grad_back(g_attn)
        dw_down = place(pos, *b_act, ff_blk, 0, False)
        dw_gate = place(pos, *b_gate, ff_blk, 0, True)
        dw_up = place(pos, *b_up, ff_blk, 0, True)
        dw_out, dw_qkv = place_attn(after(pos, dx_out, dw_up), *b_attn, o_blk, head)
        return y_out, dx_out, dw_qkv, dw_out, dw_gate, dw_up, dw_down


    return jax.shard_map(
        layer,
        mesh=wide_mesh,
        in_specs=(act_spec, act_spec, P(), col_spec, row_spec, col_spec, col_spec, row_spec, P(), P()),
        out_specs=(act_spec, act_spec, col_spec, row_spec, col_spec, col_spec, row_spec),
        check_vma=False,
    )
```

```python
import functools

import jax
import jax.numpy as jnp
from jax import lax
from jax.experimental import pallas as pl
from jax.experimental.pallas import tpu as pltpu
from jax.sharding import Mesh, PartitionSpec as P


NORM_EPS = 1e-5
NZ = 4
NY = 4
NX = 4
NC = 2
HEAD_GROUP = 4
F32 = jnp.float32
BF16 = jnp.bfloat16
VMEM_LIMIT = 67043328


def norm_fwd(row_vals, norm_gain):
    return row_vals * lax.rsqrt(jnp.mean(row_vals * row_vals, axis=-1, keepdims=True) + NORM_EPS) * norm_gain


def rotate(wide, cos_tab, sin_tab):
    return wide * cos_tab + pltpu.roll(wide, wide.shape[-1] // 2, wide.ndim - 1) * sin_tab


def rotate_back(wide, cos_tab, sin_tab):
    return wide * cos_tab - pltpu.roll(wide, wide.shape[-1] // 2, wide.ndim - 1) * sin_tab


def cost(flops, bytes_accessed):
    return pl.CostEstimate(flops=int(flops) // 20, bytes_accessed=int(bytes_accessed), transcendentals=0)


def params(**extra):
    return pltpu.CompilerParams(vmem_limit_bytes=VMEM_LIMIT, **extra)


def head_probs(q_rot, k_rot, scale):
    scores = dot_nt(q_rot, k_rot) * scale
    row_ids = lax.broadcasted_iota(jnp.int32, scores.shape, 0)
    col_ids = lax.broadcasted_iota(jnp.int32, scores.shape, 1)
    scores = jnp.where(row_ids >= col_ids, scores, -1e30)
    weights = jnp.exp(scores - jnp.max(scores, axis=-1, keepdims=True))
    return weights / jnp.sum(weights, axis=-1, keepdims=True)


def half_rows(core, idx, chunk):
    return pl.ds(pl.multiple_of((NC * idx + core) * chunk, chunk), chunk)


def chunk_rows(idx, chunk):
    return slice(idx * chunk, (idx + 1) * chunk)


def attn_fwd_kernel(heads, head, pos_ref, own_ref, other_ref, own_third_ref, other_third_ref, cos_ref, sin_ref, seq_ref, o_ref, o_other_ref, o_buf):
    core, odd = pos_ref[1], pos_ref[2]
    chunk = own_ref.shape[0] // NX
    width = heads * head
    mine = pl.ds(pl.multiple_of(width + odd * head, head), head)
    theirs = pl.ds(pl.multiple_of(width + (1 - odd) * head, head), head)
    for side, part_ref, third_ref in ((core, own_ref, own_third_ref), (1 - core, other_ref, other_third_ref)):
        for idx in range(NX):
            rows = half_rows(side, idx, chunk)
            seq_ref[0, rows, pl.ds(0, width)] = part_ref[chunk_rows(idx, chunk), :width]
            seq_ref[0, rows, mine] = part_ref[chunk_rows(idx, chunk), width:]
            seq_ref[0, rows, theirs] = third_ref[chunk_rows(idx, chunk), :]
    cos_tab, sin_tab = cos_ref[...], sin_ref[...]
    k_rot = rotate(seq_ref[0, :, width : width + head].astype(F32), cos_tab, sin_tab).astype(BF16)
    values = seq_ref[0, :, width + head :]
    for idx in range(heads):
        lanes = slice(idx * head, (idx + 1) * head)
        q_rot = rotate(seq_ref[0, :, lanes].astype(F32), cos_tab, sin_tab).astype(BF16)
        probs = head_probs(q_rot, k_rot, head**-0.5)
        o_buf[:, lanes] = dot_nn(probs.astype(BF16), values).astype(BF16)
    for side, out_ref in ((core, o_ref), (1 - core, o_other_ref)):
        for idx in range(NX):
            out_ref[chunk_rows(idx, chunk), :] = o_buf[half_rows(side, idx, chunk), :]


def attn_bwd_kernel(heads, head, pos_ref, seq_ref, own_ref, other_ref, cos_ref, sin_ref, dq_ref, keep_ref, send_ref, do_buf):
    core, odd = pos_ref[1], pos_ref[2]
    chunk = own_ref.shape[0] // NX
    width = heads * head
    for side, part_ref in ((core, own_ref), (1 - core, other_ref)):
        for idx in range(NX):
            do_buf[half_rows(side, idx, chunk), :] = part_ref[chunk_rows(idx, chunk), :]
    cos_tab, sin_tab = cos_ref[...], sin_ref[...]
    k_rot = rotate(seq_ref[0, :, width : width + head].astype(F32), cos_tab, sin_tab).astype(BF16)
    values = seq_ref[0, :, width + head :]
    d_keys = jnp.zeros(k_rot.shape, F32)
    d_values = jnp.zeros(k_rot.shape, F32)
    for idx in range(heads):
        lanes = slice(idx * head, (idx + 1) * head)
        q_rot = rotate(seq_ref[0, :, lanes].astype(F32), cos_tab, sin_tab).astype(BF16)
        d_out = do_buf[:, lanes]
        probs = head_probs(q_rot, k_rot, head**-0.5)
        d_values += dot_tn(probs.astype(BF16), d_out)
        d_probs = dot_nt(d_out, values).astype(BF16).astype(F32)
        d_scores = probs * (d_probs - jnp.sum(d_probs * probs, axis=-1, keepdims=True))
        d_scores = (d_scores * head**-0.5).astype(BF16)
        d_q_rot = dot_nn(d_scores, k_rot).astype(BF16)
        dq_ref[0, :, lanes] = rotate_back(d_q_rot.astype(F32), cos_tab, sin_tab).astype(BF16)
        d_keys += dot_tn(d_scores, q_rot)

    @pl.when(odd == 0)
    def _():
        keep_ref[0] = d_keys
        send_ref[0] = d_values

    @pl.when(odd == 1)
    def _():
        keep_ref[0] = d_values
        send_ref[0] = d_keys


def attn_post_kernel(heads, head, pos_ref, dq_ref, keep_ref, got_ref, cos_ref, sin_ref, own_ref, other_ref, third_buf):
    core, odd = pos_ref[1], pos_ref[2]
    chunk = own_ref.shape[0] // NX
    width = heads * head
    total = (keep_ref[0] + got_ref[0]).astype(BF16)

    @pl.when(odd == 0)
    def _():
        third_buf[...] = rotate_back(total.astype(F32), cos_ref[...], sin_ref[...]).astype(BF16)

    @pl.when(odd == 1)
    def _():
        third_buf[...] = total

    for side, out_ref in ((core, own_ref), (1 - core, other_ref)):
        for idx in range(NX):
            rows = half_rows(side, idx, chunk)
            out_ref[chunk_rows(idx, chunk), :width] = dq_ref[0, rows, :]
            out_ref[chunk_rows(idx, chunk), width:] = third_buf[rows, :]


def per_sequence(kernel, pos, args, specs, out_specs, out_shape, scratch, flops):
    return pl.pallas_call(
        kernel,
        grid_spec=pltpu.PrefetchScalarGridSpec(num_scalar_prefetch=1, grid=(2,), in_specs=specs, out_specs=out_specs, scratch_shapes=scratch),
        out_shape=out_shape,
        compiler_params=params(),
        cost_estimate=cost(flops, 4e6),
    )(pos, *args)


def own_spec(rows, width):
    return pl.BlockSpec((rows, width), lambda i, pos: (2 * pos[1] + i, 0))


def pair_spec(rows, width):
    return pl.BlockSpec((rows, width), lambda i, pos: (i, 0))


def seq_spec(seq, width):
    return pl.BlockSpec((1, seq, width), lambda i, pos: (i, 0, 0))


def table_spec(table):
    return pl.BlockSpec(table.shape, lambda i, pos: (0, 0))


def attn_fwd(pos, qkv_tok, other, own_third, other_third, cos_tab, sin_tab):
    seq, head = cos_tab.shape
    width = qkv_tok.shape[1] - head
    rows = seq // 2
    half = jax.ShapeDtypeStruct((seq, width), BF16)
    return per_sequence(
        functools.partial(attn_fwd_kernel, width // head, head),
        pos,
        (qkv_tok, other, own_third, other_third, cos_tab, sin_tab),
        [own_spec(rows, width + head), pair_spec(rows, width + head), pair_spec(rows, head), pair_spec(rows, head), table_spec(cos_tab), table_spec(sin_tab)],
        [seq_spec(seq, width + 2 * head), pair_spec(rows, width), pair_spec(rows, width)],
        [jax.ShapeDtypeStruct((2, seq, width + 2 * head), BF16), half, half],
        [pltpu.VMEM((seq, width), BF16)],
        16e9,
    )


def attn_bwd(pos, qkv_seq, d_attn, other, cos_tab, sin_tab):
    seq, head = cos_tab.shape
    width = d_attn.shape[1]
    rows = seq // 2
    part = jax.ShapeDtypeStruct((2, seq, head), F32)
    return per_sequence(
        functools.partial(attn_bwd_kernel, width // head, head),
        pos,
        (qkv_seq, d_attn, other, cos_tab, sin_tab),
        [seq_spec(seq, width + 2 * head), own_spec(rows, width), pair_spec(rows, width), table_spec(cos_tab), table_spec(sin_tab)],
        [seq_spec(seq, width), seq_spec(seq, head), seq_spec(seq, head)],
        [jax.ShapeDtypeStruct((2, seq, width), BF16), part, part],
        [pltpu.VMEM((seq, width), BF16)],
        16e9,
    )


def attn_post(pos, d_queries, keep, got, cos_tab, sin_tab):
    seq, head = cos_tab.shape
    width = d_queries.shape[2]
    rows = seq // 2
    half = jax.ShapeDtypeStruct((seq, width + head), BF16)
    return per_sequence(
        functools.partial(attn_post_kernel, width // head, head),
        pos,
        (d_queries, keep, got, cos_tab, sin_tab),
        [seq_spec(seq, width), seq_spec(seq, head), seq_spec(seq, head), table_spec(cos_tab), table_spec(sin_tab)],
        [pair_spec(rows, width + head), pair_spec(rows, width + head)],
        [half, half],
        [pltpu.VMEM((seq, head), BF16)],
        2e9,
    )


def act_fwd_kernel(half, ab_ref, u_ref, ut_ref):
    gate_val = ab_ref[:, :half].astype(F32)
    up_val = ab_ref[:, half:].astype(F32)
    act_val = gate_val * jax.nn.sigmoid(gate_val) * up_val
    u_ref[...] = act_val.astype(BF16)
    ut_ref[...] = act_val.T.astype(BF16)


def act_fwd(gate_up):
    tokens, width = gate_up.shape
    half = width // 2
    rows = tokens // 4
    return pl.pallas_call(
        functools.partial(act_fwd_kernel, half),
        grid=(4,),
        in_specs=[pl.BlockSpec((rows, width), lambda i: (i, 0))],
        out_specs=[pl.BlockSpec((rows, half), lambda i: (i, 0)), pl.BlockSpec((half, rows), lambda i: (0, i))],
        out_shape=[jax.ShapeDtypeStruct((tokens, half), BF16), jax.ShapeDtypeStruct((half, tokens), BF16)],
        compiler_params=params(),
        cost_estimate=cost(4e9, 8e6),
        name="act_fwd",
    )(gate_up)


def act_bwd_kernel(half, ab_ref, du_ref, dab_ref, dabt_ref):
    gate_val = ab_ref[:, :half].astype(F32)
    up_val = ab_ref[:, half:].astype(F32)
    d_act = du_ref[...].astype(F32)
    sig = jax.nn.sigmoid(gate_val)
    d_silu = d_act * up_val
    d_gate = d_silu * sig + d_silu * gate_val * (sig * (1.0 - sig))
    d_up = d_act * (gate_val * sig)
    dab_ref[:, :half] = d_gate.astype(BF16)
    dab_ref[:, half:] = d_up.astype(BF16)
    dabt_ref[:half, :] = d_gate.T.astype(BF16)
    dabt_ref[half:, :] = d_up.T.astype(BF16)


def act_bwd(gate_up, d_mixed):
    tokens, width = gate_up.shape
    half = width // 2
    rows = tokens // 4
    return pl.pallas_call(
        functools.partial(act_bwd_kernel, half),
        grid=(4,),
        in_specs=[pl.BlockSpec((rows, width), lambda i: (i, 0)), pl.BlockSpec((rows, half), lambda i: (i, 0))],
        out_specs=[pl.BlockSpec((rows, width), lambda i: (i, 0)), pl.BlockSpec((width, rows), lambda i: (0, i))],
        out_shape=[jax.ShapeDtypeStruct((tokens, width), BF16), jax.ShapeDtypeStruct((width, tokens), BF16)],
        compiler_params=params(),
        cost_estimate=cost(8e9, 14e6),
        name="act_bwd",
    )(gate_up, d_mixed)


def piece_block(pos_ref, step, other):
    core = pos_ref[1]
    return lax.rem(pos_ref[0] + step, NZ) * NC + (1 - core if other else core)


def half_start(pos_ref, part, half):
    return pl.multiple_of((1 - pos_ref[2] if part else pos_ref[2]) * half, half)


def nn_kernel(keys, first, count_out, tile, first_col, pos_ref, acts_ref, *refs):
    count = len(keys)
    halves = refs[: 2 * count]
    outs = refs[2 * count : 2 * count + count_out]
    acts_buf, w_buf, total, acts_sem, w_sem = refs[2 * count + count_out :]
    block = acts_buf.shape[1] // count
    half = block // 2
    copies = []
    for idx in range(count):
        cols = pl.ds(pl.multiple_of(piece_block(pos_ref, *keys[idx]) * block, block), block)
        copies.append([pltpu.make_async_copy(acts_ref.at[:, cols], acts_buf.at[:, pl.ds(idx * block, block)], acts_sem.at[idx])])
        for part in range(2):
            rows = pl.ds(idx * block + half_start(pos_ref, part, half), half)
            source = halves[2 * idx + part].at[:, pl.ds(first_col, w_buf.shape[1])]
            copies[-1].append(pltpu.make_async_copy(source, w_buf.at[rows], w_sem.at[2 * idx + part]))
    for group in copies:
        for copy in group:
            copy.start()
    for lo, hi in ((0, first), (first, count)):
        for group in copies[lo:hi]:
            for copy in group:
                copy.wait()
        depth = pl.ds(lo * block, (hi - lo) * block)
        start = 0
        for out_ref in outs:
            width = out_ref.shape[1]

            def step(out_lo, size, start=start, out_ref=out_ref, depth=depth, hi=hi):
                cols = pl.ds(pl.multiple_of(start + out_lo, 128), size)
                part = dot_nn(acts_buf[:, depth], w_buf[depth, cols])
                if hi == count:
                    out_ref[:, pl.ds(pl.multiple_of(out_lo, 128), size)] = (total[:, cols] + part).astype(BF16)
                else:
                    total[:, cols] = part

            whole = width // tile
            if whole:
                pl.loop(0, whole)(lambda n: step(n * tile, tile))
            if width % tile:
                step(whole * tile, width % tile)
            start += width


def nn_pieces(pos, acts, parts, first_col, widths, tile):
    keys = [(step, other) for step in (0, 1, 3, 2) for other in range(2)]
    halves = [parts[step][other][part] for step, other in keys for part in range(2)]
    tokens, depth = acts.shape
    width = sum(widths)
    count = len(keys)
    anywhere = pl.BlockSpec(memory_space=pl.ANY)
    return pl.pallas_call(
        functools.partial(nn_kernel, keys, 2, len(widths), tile, first_col),
        grid_spec=pltpu.PrefetchScalarGridSpec(
            num_scalar_prefetch=1,
            grid=(1,),
            in_specs=[anywhere] * (1 + 2 * count),
            out_specs=[pl.BlockSpec((tokens, size), lambda i, pos: (0, 0)) for size in widths],
            scratch_shapes=[
                pltpu.VMEM((tokens, depth), BF16),
                pltpu.VMEM((depth, width), BF16),
                pltpu.VMEM((tokens, width), F32),
                pltpu.SemaphoreType.DMA((count,)),
                pltpu.SemaphoreType.DMA((2 * count,)),
            ],
        ),
        out_shape=[jax.ShapeDtypeStruct((tokens, size), BF16) for size in widths],
        compiler_params=params(),
        cost_estimate=cost(2 * tokens * depth * width, 2 * depth * (tokens + width)),
    )(pos, acts, *halves)


def nt_kernel(keys, sides, first_row, pos_ref, *refs):
    count_left = len(sides)
    count = len(keys)
    lefts = refs[:count_left]
    halves = refs[count_left : count_left + 2 * count]
    out_ref, left_buf, w_buf, out_buf, left_sem, w_sem, out_sem = refs[count_left + 2 * count :]
    block = out_buf.shape[2]
    half = block // 2
    slots = w_buf.shape[0]
    left_copies = []
    start = 0
    for idx, (left, side) in enumerate(zip(lefts, sides)):
        chunks, _, width = left.shape
        first = 0 if side is None else (1 - pos_ref[1] if side else pos_ref[1]) * chunks
        source = left.at[:, pl.ds(first_row, left_buf.shape[1]), :]
        left_copies.append(pltpu.make_async_copy(source, left_buf.at[pl.ds(first, chunks), :, pl.ds(start, width)], left_sem.at[idx]))
        left_copies[-1].start()
        start += 0 if side == 0 else width

    def copies(idx, slot):
        for part in range(2):
            rows = pl.ds(half_start(pos_ref, part, half), half)
            yield pltpu.make_async_copy(halves[2 * idx + part], w_buf.at[slot, rows], w_sem.at[slot, part])

    def out_copy(idx):
        core = pos_ref[1]
        other = lax.rem(idx, 2)
        block_id = lax.rem(pos_ref[0] + idx // 2, NZ) * NC + core + other - 2 * core * other
        slot = lax.rem(idx, 2)
        return pltpu.make_async_copy(out_buf.at[slot], out_ref.at[:, pl.ds(pl.multiple_of(block_id * block, block), block)], out_sem.at[slot])

    for idx in range(slots - 1):
        for copy in copies(idx, idx):
            copy.start()
    for copy in left_copies:
        copy.wait()

    @pl.loop(0, count)
    def _(step):
        slot = lax.rem(step, slots)
        for idx in range(slots - 1, count):

            @pl.when(step + slots - 1 == idx)
            def _(idx=idx):
                for copy in copies(idx, idx % slots):
                    copy.start()

        for copy in copies(0, slot):
            copy.wait()

        @pl.when(step >= 2)
        def _():
            out_copy(step - 2).wait()

        out_buf[lax.rem(step, 2)] = dot_nt(left_buf[...].reshape(out_buf.shape[1], left_buf.shape[2]), w_buf[slot])
        out_copy(step).start()

    for idx in range(count - 2, count):
        out_copy(idx).wait()


def nt_pieces(pos, lefts, parts, chunk, first_row, rows):
    sides = (None, 0, 1)
    keys = [(step, other) for step in range(NZ) for other in range(2)]
    halves = [parts[step][other][part] for step, other in keys for part in range(2)]
    lefts = [left.reshape(-1, chunk, left.shape[1]) for left in lefts]
    chunks = lefts[0].shape[0]
    tokens = chunks * rows
    block = 2 * halves[0].shape[0]
    depth = block * len(keys)
    width = halves[0].shape[1]
    slots = 3
    anywhere = pl.BlockSpec(memory_space=pl.ANY)
    return pl.pallas_call(
        functools.partial(nt_kernel, keys, sides, first_row),
        grid_spec=pltpu.PrefetchScalarGridSpec(
            num_scalar_prefetch=1,
            grid=(1,),
            in_specs=[anywhere] * (len(lefts) + len(halves)),
            out_specs=anywhere,
            scratch_shapes=[
                pltpu.VMEM((chunks, rows, width), BF16),
                pltpu.VMEM((slots, block, width), BF16),
                pltpu.VMEM((2, tokens, block), F32),
                pltpu.SemaphoreType.DMA((len(lefts),)),
                pltpu.SemaphoreType.DMA((slots, 2)),
                pltpu.SemaphoreType.DMA((2,)),
            ],
        ),
        out_shape=jax.ShapeDtypeStruct((tokens, depth), F32),
        compiler_params=params(),
        cost_estimate=cost(2 * tokens * depth * width, 2 * depth * width + 4 * tokens * depth),
    )(pos, *lefts, *halves)


def picked_cols(pos_ref, idx, block):
    return pl.ds(pl.multiple_of((NC * idx + 1 - pos_ref[1]) * block, block), block)


def dma_kernel(kernel, pos, args, out_shape, scratch):
    anywhere = pl.BlockSpec(memory_space=pl.ANY)
    return pl.pallas_call(
        kernel,
        grid_spec=pltpu.PrefetchScalarGridSpec(
            num_scalar_prefetch=1, grid=(1,), in_specs=[anywhere] * len(args), out_specs=[anywhere] * len(out_shape), scratch_shapes=scratch
        ),
        out_shape=out_shape,
        compiler_params=params(),
        cost_estimate=cost(3e9, 16e6),
    )(pos, *args)


def pick_cols(pos, acts):
    tokens, depth = acts.shape
    block = depth // (NC * NZ)

    def kernel(pos_ref, in_ref, out_ref, buf, in_sem, out_sem):
        reads = [pltpu.make_async_copy(in_ref.at[:, picked_cols(pos_ref, idx, block)], buf.at[idx], in_sem.at[idx]) for idx in range(NZ)]
        writes = [pltpu.make_async_copy(buf.at[idx], out_ref.at[:, pl.ds(idx * block, block)], out_sem.at[idx]) for idx in range(NZ)]
        for read in reads:
            read.start()
        for read, write in zip(reads, writes):
            read.wait()
            write.start()
        for write in writes:
            write.wait()

    sems = pltpu.SemaphoreType.DMA((NZ,))
    return dma_kernel(kernel, pos, [acts], [jax.ShapeDtypeStruct((tokens, depth // 2), BF16)], [pltpu.VMEM((NZ, tokens, block), BF16), sems, sems])[0]


def grad_kernel(heights, pos_ref, *refs):
    pairs = len(heights)
    ins = refs[: 4 * pairs]
    outs = refs[4 * pairs : 4 * pairs + 2 * NZ]
    buf, sem = refs[4 * pairs + 2 * NZ :]
    half = buf.shape[2] // 2
    step = pl.program_id(0)
    slot = lax.rem(step, 2)

    def out_copy(idx, part):
        cols = pl.ds(half_start(pos_ref, part, half), half)
        return pltpu.make_async_copy(buf.at[idx % 2, :, cols], outs[2 * idx + part], sem.at[idx % 2, part])

    for idx in range(2, NZ):

        @pl.when(step == idx)
        def _(idx=idx):
            for part in range(2):
                out_copy(idx - 2, part).wait()

    start = 0
    for idx, height in enumerate(heights):
        own, recv, acts, acts_recv = ins[4 * idx : 4 * idx + 4]
        buf[slot, start : start + height, :] = dot_nn(own[...], acts[...]) + dot_nn(recv[...], acts_recv[...])
        start += height
    for idx in range(NZ):

        @pl.when(step == idx)
        def _(idx=idx):
            for part in range(2):
                out_copy(idx, part).start()

    @pl.when(step == NZ - 1)
    def _():
        for idx in (NZ - 2, NZ - 1):
            for part in range(2):
                out_copy(idx, part).wait()


def grad_pieces(pos, pairs):
    tokens, depth = pairs[0][2].shape
    cols = depth // (NZ * NC)
    in_specs = []
    args = []

    def z_of(n, pos):
        return lax.rem(pos[0] + jnp.where(n == 0, 2, jnp.where(n == 1, 1, jnp.where(n == 2, 3, 0))), NZ)

    for own, recv, acts, acts_recv, height, block in pairs:
        in_specs += [pl.BlockSpec((height, tokens), lambda n, pos, block=block: (block, 0))] * 2
        in_specs.append(pl.BlockSpec((tokens, cols), lambda n, pos: (0, z_of(n, pos) * NC + pos[1])))
        in_specs.append(pl.BlockSpec((tokens, cols), lambda n, pos: (0, z_of(n, pos))))
        args += [own, recv, acts, acts_recv]
    heights = [pair[4] for pair in pairs]
    rows = sum(heights)
    return pl.pallas_call(
        functools.partial(grad_kernel, heights),
        grid_spec=pltpu.PrefetchScalarGridSpec(
            num_scalar_prefetch=1,
            grid=(NZ,),
            in_specs=in_specs,
            out_specs=[pl.BlockSpec(memory_space=pl.ANY)] * (2 * NZ),
            scratch_shapes=[pltpu.VMEM((2, rows, cols), F32), pltpu.SemaphoreType.DMA((2, 2))],
        ),
        out_shape=[jax.ShapeDtypeStruct((rows, cols // 2), F32)] * (2 * NZ),
        compiler_params=params(),
        cost_estimate=cost(4 * rows * tokens * cols * NZ, 4 * tokens * cols * NZ),
        name="grad",
    )(pos, *args)


def sources(pos_ref, own_ref, first_ref, second_ref):
    return ((pos_ref[3] == 1, 0, own_ref), (pos_ref[3] == 0, 0, first_ref), (True, 1, second_ref))


def place(pos, own, first, second, height, block, transpose):
    cols = first.shape[1]
    spec = pl.BlockSpec((height, cols), lambda n, pos: (block, 0))

    def kernel(pos_ref, own_ref, first_ref, second_ref, out_ref):
        for chosen, idx, ref in sources(pos_ref, own_ref, first_ref, second_ref):

            @pl.when(jnp.logical_and(pl.program_id(0) == idx, chosen))
            def _(ref=ref):
                out_ref[...] = ref[...].T if transpose else ref[...]

    def order(n, pos):
        return jnp.where(n == 0, pos[2], 1 - pos[2])

    return pl.pallas_call(
        kernel,
        grid_spec=pltpu.PrefetchScalarGridSpec(
            num_scalar_prefetch=1,
            grid=(2,),
            in_specs=[spec] * 3,
            out_specs=pl.BlockSpec((cols, height), lambda n, pos: (0, order(n, pos))) if transpose else pl.BlockSpec((height, cols), lambda n, pos: (order(n, pos), 0)),
        ),
        out_shape=jax.ShapeDtypeStruct((cols, 2 * height) if transpose else (2 * height, cols), F32),
        compiler_params=params(),
        cost_estimate=cost(2e9, 16 * height * cols),
    )(pos, own, first, second)


def place_attn(pos, own, first, second, o_blk, head):
    rows, cols = first.shape
    qk = 2 * head

    def kernel(pos_ref, own_ref, first_ref, second_ref, out_ref, qkv_ref):
        for chosen, idx, ref in sources(pos_ref, own_ref, first_ref, second_ref):

            @pl.when(chosen)
            def _(idx=idx, ref=ref):
                bit = 1 - pos_ref[2] if idx else pos_ref[2]
                out_ref[pl.ds(pl.multiple_of(bit * o_blk, o_blk), o_blk), :] = ref[:o_blk, :]
                qkv_ref[:, pl.ds(pl.multiple_of(bit * qk, qk), qk)] = ref[o_blk : o_blk + qk, :].T
                qkv_ref[:, pl.ds(pl.multiple_of(2 * qk + bit * head, head), head)] = ref[o_blk + qk :, :].T

    def whole(*shape):
        return pl.BlockSpec(shape, lambda n, pos: (0, 0))

    shapes = ((2 * o_blk, cols), (cols, 2 * (qk + head)))
    return pl.pallas_call(
        kernel,
        grid_spec=pltpu.PrefetchScalarGridSpec(num_scalar_prefetch=1, grid=(1,), in_specs=[whole(rows, cols)] * 3, out_specs=[whole(*shape) for shape in shapes]),
        out_shape=[jax.ShapeDtypeStruct(shape, F32) for shape in shapes],
        compiler_params=params(),
        cost_estimate=cost(2e9, 16 * rows * cols),
        name="p_attn",
    )(pos, own, first, second)


def after(val, *earlier):
    return lax.optimization_barrier((val, *earlier))[0]


def ring(step, size):
    return [(src, (src + step) % size) for src in range(size)]


def hop_z(val, step):
    return lax.ppermute(val, "z", ring(step, NZ))


def swap_c(val):
    return lax.ppermute(val, "c", [(0, 1), (1, 0)])


def swap_y(val):
    return lax.ppermute(val, "y", [(src, src ^ 1) for src in range(NY)])


def turn(val, flip, home):
    def place_of(y_pos, c_pos):
        return y_pos * NC + c_pos

    pairs = [(place_of(2 * a + b, c), place_of(2 * c + (b ^ flip), a)) for a in range(2) for b in range(2) for c in range(NC) if home or flip or a != c]
    return lax.ppermute(val, ("y", "c"), pairs)


def swap_yc(val):
    pairs = [(y_pos * NC + c_pos, (y_pos ^ 1) * NC + 1 - c_pos) for y_pos in range(NY) for c_pos in range(NC)]
    return lax.ppermute(val, ("y", "c"), pairs)


def dot_nn(left, right):
    return lax.dot_general(left, right, (((1,), (0,)), ((), ())), preferred_element_type=F32)


def dot_nt(left, right):
    return lax.dot_general(left, right, (((1,), (1,)), ((), ())), preferred_element_type=F32)


def dot_tn(left, right):
    return lax.dot_general(left, right, (((0,), (0,)), ((), ())), preferred_element_type=F32)


def solution(mesh):
    wide_mesh = Mesh(mesh.devices.reshape(NZ, NY, NX, NC), ("z", "y", "x", "c"))
    rows = ("z", "y")
    cols = ("x", "c")
    act_spec = P(rows, cols, None)
    col_spec = P(rows, cols)
    row_spec = P(cols, rows)

    def layer(x_in, dy_in, norm_gain, w_qkv, w_out, w_gate, w_up, w_down, rope_cos, rope_sin):
        z_pos = lax.axis_index("z")
        y_pos = lax.axis_index("y")
        c_pos = lax.axis_index("c")
        even_y = y_pos % 2 == 0
        first_c = c_pos == 0
        pos = jnp.stack([z_pos, c_pos, y_pos % 2, y_pos // 2 == c_pos]).astype(jnp.int32)
        chunk = x_in.shape[1]
        head = 2 * rope_cos.shape[1]
        seq = rope_cos.shape[0]
        ff_blk = w_gate.shape[1] // 2
        o_blk = w_out.shape[0] // 2
        qkv_blk = o_blk + head

        def gather_rows(blocks):
            got = []
            for flip in (1, 0):
                got.insert(0, turn(jnp.where(even_y, blocks[flip], blocks[1 - flip]), flip, True))
            return got

        def gather_weight(piece):
            left, right = [], []
            for part in (1, 0):
                left.insert(0, hop_z(piece[part], 1))
                right.insert(0, hop_z(piece[part], -1))
            far = [hop_z(left[0], 1), hop_z(right[1], -1)]
            parts = []
            for mine in (piece, right, far, left):
                parts.append((mine, [swap_c(half) for half in mine]))
            return parts

        def grad_start(pairs, *earlier):
            far0, far1, up0, up1, down0, down1, own0, own1 = grad_pieces(after(pos, *earlier), pairs)
            far = (hop_z(far0, 1), hop_z(far1, -1))
            direct = (hop_z(up1, 1), hop_z(down0, -1))
            return (up0, down1), far, direct, (own0, own1)

        def grad_pass(state, *earlier):
            (up0, down1), far, direct, own = state
            sums = (up0 + after(far[0], *earlier), down1 + far[1])
            passed = (hop_z(sums[0], 1), hop_z(sums[1], -1))
            return direct, passed, own, sums

        def grad_back(state, *earlier):
            direct, passed, own = state[:3]
            first = own[0] + after(passed[0], *earlier) + direct[1]
            second = own[1] + direct[0] + passed[1]
            return first, turn(first, 0, False), turn(second, 1, False)

        def my_rows(val, mine):
            return lax.dynamic_slice_in_dim(val, (c_pos if mine else 1 - c_pos) * seq, seq, axis=0)

        def both_rows(own, got):
            return jnp.concatenate([jnp.where(first_c, own, got), jnp.where(first_c, got, own)], axis=0)

        cos_tab = jnp.concatenate([rope_cos, rope_cos], axis=1)
        sin_tab = jnp.concatenate([-rope_sin, rope_sin], axis=1)

        def qkv_cols(bit):
            first = 2 * head * bit
            third = HEAD_GROUP * head + head * bit
            return [w_qkv[:, first : first + 2 * head], w_qkv[:, third : third + head]]

        def block(weight, bit):
            size = weight.shape[1] // 2
            return weight[:, bit * size : (bit + 1) * size]

        down_t = w_down.T
        out_t = w_out.T
        wf_piece = gather_rows([jnp.concatenate([block(w_gate, j), block(w_up, j), *qkv_cols(j)], axis=1) for j in range(2)])
        ws_piece = gather_rows([jnp.concatenate([block(down_t, j), block(out_t, j)], axis=1) for j in range(2)])

        x_rows = after(x_in[0], cos_tab, sin_tab).astype(F32)
        normed, norm_pull = jax.vjp(lambda row_vals: norm_fwd(row_vals, norm_gain), x_rows)
        h_all = lax.all_gather(after(normed.astype(BF16), wf_piece[1]), ("y", "x"), axis=0, tiled=True)
        dy_all = lax.all_gather(after(dy_in[0], wf_piece[1]), ("y", "x"), axis=0, tiled=True)
        wf_parts = gather_weight(wf_piece)
        ws_parts = gather_weight(ws_piece)

        (qkv_tok,) = nn_pieces(pos, h_all, wf_parts, 2 * ff_blk, (qkv_blk,), 512)
        third = qkv_tok[:, o_blk:]
        qkv_other = swap_c(my_rows(qkv_tok, False))
        third_own = swap_y(my_rows(third, True))
        third_other = swap_yc(my_rows(third, False))
        (gate_up,) = nn_pieces(after(pos, qkv_tok), h_all, wf_parts, 0, (2 * ff_blk,), 512)
        act_val, act_t = act_fwd(gate_up)
        act_recv = swap_c(act_t)
        qkv_seq, attn_own, attn_other = attn_fwd(after(pos, act_t), qkv_tok, qkv_other, third_own, third_other, cos_tab, sin_tab)
        attn_got = swap_c(attn_other)
        y_part = nt_pieces(after(pos, attn_own), [act_val, attn_own, attn_got], ws_parts, chunk, 0, chunk)
        mix_sum = lax.psum_scatter(y_part, ("y", "x"), scatter_dimension=0, tiled=True)
        y_out = (x_rows + mix_sum).astype(BF16)[None]

        h_picked = pick_cols(after(pos, y_part), h_all)
        h_recv = swap_c(h_picked)
        dy_picked = pick_cols(after(pos, h_picked), dy_all)
        dy_recv = swap_c(dy_picked)
        d_act, d_attn = nn_pieces(after(pos, dy_picked), dy_all, ws_parts, 0, (ff_blk, o_blk), 256)
        d_attn_other = swap_c(my_rows(d_attn, False))
        g_act = grad_start([(act_t, act_recv, dy_all, dy_recv, ff_blk, 0)], d_attn)
        d_gate_up, d_gate_up_t = act_bwd(gate_up, after(d_act, g_act[3][0]))
        d_gate_up_recv = swap_c(d_gate_up_t)
        d_queries, keep, send = attn_bwd(after(pos, d_gate_up_t), qkv_seq, d_attn, d_attn_other, cos_tab, sin_tab)
        got = swap_y(send)
        g_act = grad_pass(g_act, d_queries)
        g_gate = grad_start([(d_gate_up_t, d_gate_up_recv, h_all, h_recv, ff_blk, 0)], *g_act[3])
        d_own, d_other = attn_post(after(pos, g_gate[3][0]), d_queries, keep, got, cos_tab, sin_tab)
        d_got = swap_c(d_other)
        dh_part = nt_pieces(pos, [d_gate_up, d_own, d_got], wf_parts, chunk, 0, chunk)
        d_h = lax.psum_scatter(dh_part, ("y", "x"), scatter_dimension=0, tiled=True)
        g_gate = grad_pass(g_gate, dh_part)
        g_up = grad_start([(d_gate_up_t, d_gate_up_recv, h_all, h_recv, ff_blk, 1)], *g_gate[3])
        b_act = grad_back(g_act, g_up[3][0])
        d_h = d_h.astype(BF16)
        dx_out = (dy_in[0].astype(F32) + norm_pull(d_h.astype(F32))[0]).astype(BF16)[None]

        attn_t = both_rows(attn_own, attn_got).T
        d_qkv_t = both_rows(d_own, d_got).T
        attn_recv = swap_c(attn_t)
        d_qkv_recv = swap_c(d_qkv_t)
        g_attn = grad_start([(attn_t, attn_recv, dy_all, dy_recv, o_blk, 0), (d_qkv_t, d_qkv_recv, h_all, h_recv, qkv_blk, 0)], g_up[3][0])
        g_up = grad_pass(g_up, g_attn[3][0])
        g_attn = grad_pass(g_attn)
        b_gate = grad_back(g_gate)
        b_up = grad_back(g_up)
        b_attn = grad_back(g_attn)
        dw_down = place(pos, *b_act, ff_blk, 0, False)
        dw_gate = place(pos, *b_gate, ff_blk, 0, True)
        dw_up = place(pos, *b_up, ff_blk, 0, True)
        dw_out, dw_qkv = place_attn(after(pos, dx_out, dw_up), *b_attn, o_blk, head)
        return y_out, dx_out, dw_qkv, dw_out, dw_gate, dw_up, dw_down


    return jax.shard_map(
        layer,
        mesh=wide_mesh,
        in_specs=(act_spec, act_spec, P(), col_spec, row_spec, col_spec, col_spec, row_spec, P(), P()),
        out_specs=(act_spec, act_spec, col_spec, row_spec, col_spec, col_spec, row_spec),
        check_vma=False,
    )
```

```python
import functools

import jax
import jax.numpy as jnp
from jax import lax
from jax.experimental import pallas as pl
from jax.experimental.pallas import tpu as pltpu
from jax.sharding import Mesh, PartitionSpec as P


NORM_EPS = 1e-5
NZ = 4
NY = 4
NX = 4
NC = 2
HEAD_GROUP = 4
F32 = jnp.float32
BF16 = jnp.bfloat16
VMEM_LIMIT = 67043328


def norm_fwd(row_vals, norm_gain):
    return row_vals * lax.rsqrt(jnp.mean(row_vals * row_vals, axis=-1, keepdims=True) + NORM_EPS) * norm_gain


def rotate(wide, cos_tab, sin_tab):
    return wide * cos_tab + pltpu.roll(wide, wide.shape[-1] // 2, wide.ndim - 1) * sin_tab


def rotate_back(wide, cos_tab, sin_tab):
    return wide * cos_tab - pltpu.roll(wide, wide.shape[-1] // 2, wide.ndim - 1) * sin_tab


def cost(flops, bytes_accessed):
    return pl.CostEstimate(flops=int(flops) // 20, bytes_accessed=int(bytes_accessed), transcendentals=0)


def params(**extra):
    return pltpu.CompilerParams(vmem_limit_bytes=VMEM_LIMIT, **extra)


def head_probs(q_rot, k_rot, scale):
    scores = dot_nt(q_rot, k_rot) * scale
    row_ids = lax.broadcasted_iota(jnp.int32, scores.shape, 0)
    col_ids = lax.broadcasted_iota(jnp.int32, scores.shape, 1)
    scores = jnp.where(row_ids >= col_ids, scores, -1e30)
    weights = jnp.exp(scores - jnp.max(scores, axis=-1, keepdims=True))
    return weights / jnp.sum(weights, axis=-1, keepdims=True)


def half_rows(core, idx, chunk):
    return pl.ds(pl.multiple_of((NC * idx + core) * chunk, chunk), chunk)


def chunk_rows(idx, chunk):
    return slice(idx * chunk, (idx + 1) * chunk)


def attn_fwd_kernel(heads, head, pos_ref, own_ref, other_ref, own_third_ref, other_third_ref, cos_ref, sin_ref, seq_ref, o_ref, o_other_ref, o_buf):
    core, odd = pos_ref[1], pos_ref[2]
    chunk = own_ref.shape[0] // NX
    width = heads * head
    mine = pl.ds(pl.multiple_of(width + odd * head, head), head)
    theirs = pl.ds(pl.multiple_of(width + (1 - odd) * head, head), head)
    for side, part_ref, third_ref in ((core, own_ref, own_third_ref), (1 - core, other_ref, other_third_ref)):
        for idx in range(NX):
            rows = half_rows(side, idx, chunk)
            seq_ref[0, rows, pl.ds(0, width)] = part_ref[chunk_rows(idx, chunk), :width]
            seq_ref[0, rows, mine] = part_ref[chunk_rows(idx, chunk), width:]
            seq_ref[0, rows, theirs] = third_ref[chunk_rows(idx, chunk), :]
    cos_tab, sin_tab = cos_ref[...], sin_ref[...]
    k_rot = rotate(seq_ref[0, :, width : width + head].astype(F32), cos_tab, sin_tab).astype(BF16)
    values = seq_ref[0, :, width + head :]
    for idx in range(heads):
        lanes = slice(idx * head, (idx + 1) * head)
        q_rot = rotate(seq_ref[0, :, lanes].astype(F32), cos_tab, sin_tab).astype(BF16)
        probs = head_probs(q_rot, k_rot, head**-0.5)
        o_buf[:, lanes] = dot_nn(probs.astype(BF16), values).astype(BF16)
    for side, out_ref in ((core, o_ref), (1 - core, o_other_ref)):
        for idx in range(NX):
            out_ref[chunk_rows(idx, chunk), :] = o_buf[half_rows(side, idx, chunk), :]


def attn_bwd_kernel(heads, head, pos_ref, seq_ref, own_ref, other_ref, cos_ref, sin_ref, dq_ref, keep_ref, send_ref, do_buf):
    core, odd = pos_ref[1], pos_ref[2]
    chunk = own_ref.shape[0] // NX
    width = heads * head
    for side, part_ref in ((core, own_ref), (1 - core, other_ref)):
        for idx in range(NX):
            do_buf[half_rows(side, idx, chunk), :] = part_ref[chunk_rows(idx, chunk), :]
    cos_tab, sin_tab = cos_ref[...], sin_ref[...]
    k_rot = rotate(seq_ref[0, :, width : width + head].astype(F32), cos_tab, sin_tab).astype(BF16)
    values = seq_ref[0, :, width + head :]
    d_keys = jnp.zeros(k_rot.shape, F32)
    d_values = jnp.zeros(k_rot.shape, F32)
    for idx in range(heads):
        lanes = slice(idx * head, (idx + 1) * head)
        q_rot = rotate(seq_ref[0, :, lanes].astype(F32), cos_tab, sin_tab).astype(BF16)
        d_out = do_buf[:, lanes]
        probs = head_probs(q_rot, k_rot, head**-0.5)
        d_values += dot_tn(probs.astype(BF16), d_out)
        d_probs = dot_nt(d_out, values).astype(BF16).astype(F32)
        d_scores = probs * (d_probs - jnp.sum(d_probs * probs, axis=-1, keepdims=True))
        d_scores = (d_scores * head**-0.5).astype(BF16)
        d_q_rot = dot_nn(d_scores, k_rot).astype(BF16)
        dq_ref[0, :, lanes] = rotate_back(d_q_rot.astype(F32), cos_tab, sin_tab).astype(BF16)
        d_keys += dot_tn(d_scores, q_rot)

    @pl.when(odd == 0)
    def _():
        keep_ref[0] = d_keys
        send_ref[0] = d_values

    @pl.when(odd == 1)
    def _():
        keep_ref[0] = d_values
        send_ref[0] = d_keys


def attn_post_kernel(heads, head, pos_ref, dq_ref, keep_ref, got_ref, cos_ref, sin_ref, own_ref, other_ref, third_buf):
    core, odd = pos_ref[1], pos_ref[2]
    chunk = own_ref.shape[0] // NX
    width = heads * head
    total = (keep_ref[0] + got_ref[0]).astype(BF16)

    @pl.when(odd == 0)
    def _():
        third_buf[...] = rotate_back(total.astype(F32), cos_ref[...], sin_ref[...]).astype(BF16)

    @pl.when(odd == 1)
    def _():
        third_buf[...] = total

    for side, out_ref in ((core, own_ref), (1 - core, other_ref)):
        for idx in range(NX):
            rows = half_rows(side, idx, chunk)
            out_ref[chunk_rows(idx, chunk), :width] = dq_ref[0, rows, :]
            out_ref[chunk_rows(idx, chunk), width:] = third_buf[rows, :]


def per_sequence(kernel, pos, args, specs, out_specs, out_shape, scratch, flops):
    return pl.pallas_call(
        kernel,
        grid_spec=pltpu.PrefetchScalarGridSpec(num_scalar_prefetch=1, grid=(2,), in_specs=specs, out_specs=out_specs, scratch_shapes=scratch),
        out_shape=out_shape,
        compiler_params=params(),
        cost_estimate=cost(flops, 4e6),
    )(pos, *args)


def own_spec(rows, width):
    return pl.BlockSpec((rows, width), lambda i, pos: (2 * pos[1] + i, 0))


def pair_spec(rows, width):
    return pl.BlockSpec((rows, width), lambda i, pos: (i, 0))


def seq_spec(seq, width):
    return pl.BlockSpec((1, seq, width), lambda i, pos: (i, 0, 0))


def table_spec(table):
    return pl.BlockSpec(table.shape, lambda i, pos: (0, 0))


def attn_fwd(pos, qkv_tok, other, own_third, other_third, cos_tab, sin_tab):
    seq, head = cos_tab.shape
    width = qkv_tok.shape[1] - head
    rows = seq // 2
    half = jax.ShapeDtypeStruct((seq, width), BF16)
    return per_sequence(
        functools.partial(attn_fwd_kernel, width // head, head),
        pos,
        (qkv_tok, other, own_third, other_third, cos_tab, sin_tab),
        [own_spec(rows, width + head), pair_spec(rows, width + head), pair_spec(rows, head), pair_spec(rows, head), table_spec(cos_tab), table_spec(sin_tab)],
        [seq_spec(seq, width + 2 * head), pair_spec(rows, width), pair_spec(rows, width)],
        [jax.ShapeDtypeStruct((2, seq, width + 2 * head), BF16), half, half],
        [pltpu.VMEM((seq, width), BF16)],
        16e9,
    )


def attn_bwd(pos, qkv_seq, d_attn, other, cos_tab, sin_tab):
    seq, head = cos_tab.shape
    width = d_attn.shape[1]
    rows = seq // 2
    part = jax.ShapeDtypeStruct((2, seq, head), F32)
    return per_sequence(
        functools.partial(attn_bwd_kernel, width // head, head),
        pos,
        (qkv_seq, d_attn, other, cos_tab, sin_tab),
        [seq_spec(seq, width + 2 * head), own_spec(rows, width), pair_spec(rows, width), table_spec(cos_tab), table_spec(sin_tab)],
        [seq_spec(seq, width), seq_spec(seq, head), seq_spec(seq, head)],
        [jax.ShapeDtypeStruct((2, seq, width), BF16), part, part],
        [pltpu.VMEM((seq, width), BF16)],
        16e9,
    )


def attn_post(pos, d_queries, keep, got, cos_tab, sin_tab):
    seq, head = cos_tab.shape
    width = d_queries.shape[2]
    rows = seq // 2
    half = jax.ShapeDtypeStruct((seq, width + head), BF16)
    return per_sequence(
        functools.partial(attn_post_kernel, width // head, head),
        pos,
        (d_queries, keep, got, cos_tab, sin_tab),
        [seq_spec(seq, width), seq_spec(seq, head), seq_spec(seq, head), table_spec(cos_tab), table_spec(sin_tab)],
        [pair_spec(rows, width + head), pair_spec(rows, width + head)],
        [half, half],
        [pltpu.VMEM((seq, head), BF16)],
        2e9,
    )


def act_fwd_kernel(half, ab_ref, u_ref, ut_ref):
    gate_val = ab_ref[:, :half].astype(F32)
    up_val = ab_ref[:, half:].astype(F32)
    act_val = gate_val * jax.nn.sigmoid(gate_val) * up_val
    u_ref[...] = act_val.astype(BF16)
    ut_ref[...] = act_val.T.astype(BF16)


def act_fwd(gate_up):
    tokens, width = gate_up.shape
    half = width // 2
    rows = tokens // 4
    return pl.pallas_call(
        functools.partial(act_fwd_kernel, half),
        grid=(4,),
        in_specs=[pl.BlockSpec((rows, width), lambda i: (i, 0))],
        out_specs=[pl.BlockSpec((rows, half), lambda i: (i, 0)), pl.BlockSpec((half, rows), lambda i: (0, i))],
        out_shape=[jax.ShapeDtypeStruct((tokens, half), BF16), jax.ShapeDtypeStruct((half, tokens), BF16)],
        compiler_params=params(),
        cost_estimate=cost(4e9, 8e6),
        name="act_fwd",
    )(gate_up)


def act_bwd_kernel(half, ab_ref, du_ref, dab_ref, dabt_ref):
    gate_val = ab_ref[:, :half].astype(F32)
    up_val = ab_ref[:, half:].astype(F32)
    d_act = du_ref[...].astype(F32)
    sig = jax.nn.sigmoid(gate_val)
    d_silu = d_act * up_val
    d_gate = d_silu * sig + d_silu * gate_val * (sig * (1.0 - sig))
    d_up = d_act * (gate_val * sig)
    dab_ref[:, :half] = d_gate.astype(BF16)
    dab_ref[:, half:] = d_up.astype(BF16)
    dabt_ref[:half, :] = d_gate.T.astype(BF16)
    dabt_ref[half:, :] = d_up.T.astype(BF16)


def act_bwd(gate_up, d_mixed):
    tokens, width = gate_up.shape
    half = width // 2
    rows = tokens // 4
    return pl.pallas_call(
        functools.partial(act_bwd_kernel, half),
        grid=(4,),
        in_specs=[pl.BlockSpec((rows, width), lambda i: (i, 0)), pl.BlockSpec((rows, half), lambda i: (i, 0))],
        out_specs=[pl.BlockSpec((rows, width), lambda i: (i, 0)), pl.BlockSpec((width, rows), lambda i: (0, i))],
        out_shape=[jax.ShapeDtypeStruct((tokens, width), BF16), jax.ShapeDtypeStruct((width, tokens), BF16)],
        compiler_params=params(),
        cost_estimate=cost(8e9, 14e6),
        name="act_bwd",
    )(gate_up, d_mixed)


def piece_block(pos_ref, step, other):
    core = pos_ref[1]
    return lax.rem(pos_ref[0] + step, NZ) * NC + (1 - core if other else core)


def half_start(pos_ref, part, half):
    return pl.multiple_of((1 - pos_ref[2] if part else pos_ref[2]) * half, half)


def nn_kernel(keys, first, count_out, tile, first_col, pos_ref, acts_ref, *refs):
    count = len(keys)
    halves = refs[: 2 * count]
    outs = refs[2 * count : 2 * count + count_out]
    acts_buf, w_buf, total, acts_sem, w_sem = refs[2 * count + count_out :]
    block = acts_buf.shape[1] // count
    half = block // 2
    copies = []
    for idx in range(count):
        cols = pl.ds(pl.multiple_of(piece_block(pos_ref, *keys[idx]) * block, block), block)
        copies.append([pltpu.make_async_copy(acts_ref.at[:, cols], acts_buf.at[:, pl.ds(idx * block, block)], acts_sem.at[idx])])
        for part in range(2):
            rows = pl.ds(idx * block + half_start(pos_ref, part, half), half)
            source = halves[2 * idx + part].at[:, pl.ds(first_col, w_buf.shape[1])]
            copies[-1].append(pltpu.make_async_copy(source, w_buf.at[rows], w_sem.at[2 * idx + part]))
    for group in copies:
        for copy in group:
            copy.start()
    for lo, hi in ((0, first), (first, count)):
        for group in copies[lo:hi]:
            for copy in group:
                copy.wait()
        depth = pl.ds(lo * block, (hi - lo) * block)
        start = 0
        for out_ref in outs:
            width = out_ref.shape[1]

            def step(out_lo, size, start=start, out_ref=out_ref, depth=depth, hi=hi):
                cols = pl.ds(pl.multiple_of(start + out_lo, 128), size)
                part = dot_nn(acts_buf[:, depth], w_buf[depth, cols])
                if hi == count:
                    out_ref[:, pl.ds(pl.multiple_of(out_lo, 128), size)] = (total[:, cols] + part).astype(BF16)
                else:
                    total[:, cols] = part

            whole = width // tile
            if whole:
                pl.loop(0, whole)(lambda n: step(n * tile, tile))
            if width % tile:
                step(whole * tile, width % tile)
            start += width


def nn_pieces(pos, acts, parts, first_col, widths, tile):
    keys = [(step, other) for step in (0, 1, 3, 2) for other in range(2)]
    halves = [parts[step][other][part] for step, other in keys for part in range(2)]
    tokens, depth = acts.shape
    width = sum(widths)
    count = len(keys)
    anywhere = pl.BlockSpec(memory_space=pl.ANY)
    return pl.pallas_call(
        functools.partial(nn_kernel, keys, 2, len(widths), tile, first_col),
        grid_spec=pltpu.PrefetchScalarGridSpec(
            num_scalar_prefetch=1,
            grid=(1,),
            in_specs=[anywhere] * (1 + 2 * count),
            out_specs=[pl.BlockSpec((tokens, size), lambda i, pos: (0, 0)) for size in widths],
            scratch_shapes=[
                pltpu.VMEM((tokens, depth), BF16),
                pltpu.VMEM((depth, width), BF16),
                pltpu.VMEM((tokens, width), F32),
                pltpu.SemaphoreType.DMA((count,)),
                pltpu.SemaphoreType.DMA((2 * count,)),
            ],
        ),
        out_shape=[jax.ShapeDtypeStruct((tokens, size), BF16) for size in widths],
        compiler_params=params(),
        cost_estimate=cost(2 * tokens * depth * width, 2 * depth * (tokens + width)),
    )(pos, acts, *halves)


def nt_kernel(keys, sides, first_row, pos_ref, *refs):
    count_left = len(sides)
    count = len(keys)
    lefts = refs[:count_left]
    halves = refs[count_left : count_left + 2 * count]
    out_ref, left_buf, w_buf, out_buf, left_sem, w_sem, out_sem = refs[count_left + 2 * count :]
    block = out_buf.shape[2]
    half = block // 2
    slots = w_buf.shape[0]
    left_copies = []
    start = 0
    for idx, (left, side) in enumerate(zip(lefts, sides)):
        chunks, _, width = left.shape
        first = 0 if side is None else (1 - pos_ref[1] if side else pos_ref[1]) * chunks
        source = left.at[:, pl.ds(first_row, left_buf.shape[1]), :]
        left_copies.append(pltpu.make_async_copy(source, left_buf.at[pl.ds(first, chunks), :, pl.ds(start, width)], left_sem.at[idx]))
        left_copies[-1].start()
        start += 0 if side == 0 else width

    def copies(idx, slot):
        for part in range(2):
            rows = pl.ds(half_start(pos_ref, part, half), half)
            yield pltpu.make_async_copy(halves[2 * idx + part], w_buf.at[slot, rows], w_sem.at[slot, part])

    def out_copy(idx):
        core = pos_ref[1]
        other = lax.rem(idx, 2)
        block_id = lax.rem(pos_ref[0] + idx // 2, NZ) * NC + core + other - 2 * core * other
        slot = lax.rem(idx, 2)
        return pltpu.make_async_copy(out_buf.at[slot], out_ref.at[:, pl.ds(pl.multiple_of(block_id * block, block), block)], out_sem.at[slot])

    for idx in range(slots - 1):
        for copy in copies(idx, idx):
            copy.start()
    for copy in left_copies:
        copy.wait()

    @pl.loop(0, count)
    def _(step):
        slot = lax.rem(step, slots)
        for idx in range(slots - 1, count):

            @pl.when(step + slots - 1 == idx)
            def _(idx=idx):
                for copy in copies(idx, idx % slots):
                    copy.start()

        for copy in copies(0, slot):
            copy.wait()

        @pl.when(step >= 2)
        def _():
            out_copy(step - 2).wait()

        out_buf[lax.rem(step, 2)] = dot_nt(left_buf[...].reshape(out_buf.shape[1], left_buf.shape[2]), w_buf[slot])
        out_copy(step).start()

    for idx in range(count - 2, count):
        out_copy(idx).wait()


def nt_pieces(pos, lefts, parts, chunk, first_row, rows):
    sides = (None, 0, 1)
    keys = [(step, other) for step in range(NZ) for other in range(2)]
    halves = [parts[step][other][part] for step, other in keys for part in range(2)]
    lefts = [left.reshape(-1, chunk, left.shape[1]) for left in lefts]
    chunks = lefts[0].shape[0]
    tokens = chunks * rows
    block = 2 * halves[0].shape[0]
    depth = block * len(keys)
    width = halves[0].shape[1]
    slots = 3
    anywhere = pl.BlockSpec(memory_space=pl.ANY)
    return pl.pallas_call(
        functools.partial(nt_kernel, keys, sides, first_row),
        grid_spec=pltpu.PrefetchScalarGridSpec(
            num_scalar_prefetch=1,
            grid=(1,),
            in_specs=[anywhere] * (len(lefts) + len(halves)),
            out_specs=anywhere,
            scratch_shapes=[
                pltpu.VMEM((chunks, rows, width), BF16),
                pltpu.VMEM((slots, block, width), BF16),
                pltpu.VMEM((2, tokens, block), F32),
                pltpu.SemaphoreType.DMA((len(lefts),)),
                pltpu.SemaphoreType.DMA((slots, 2)),
                pltpu.SemaphoreType.DMA((2,)),
            ],
        ),
        out_shape=jax.ShapeDtypeStruct((tokens, depth), F32),
        compiler_params=params(),
        cost_estimate=cost(2 * tokens * depth * width, 2 * depth * width + 4 * tokens * depth),
    )(pos, *lefts, *halves)


def picked_cols(pos_ref, idx, block):
    return pl.ds(pl.multiple_of((NC * idx + 1 - pos_ref[1]) * block, block), block)


def dma_kernel(kernel, pos, args, out_shape, scratch):
    anywhere = pl.BlockSpec(memory_space=pl.ANY)
    return pl.pallas_call(
        kernel,
        grid_spec=pltpu.PrefetchScalarGridSpec(
            num_scalar_prefetch=1, grid=(1,), in_specs=[anywhere] * len(args), out_specs=[anywhere] * len(out_shape), scratch_shapes=scratch
        ),
        out_shape=out_shape,
        compiler_params=params(),
        cost_estimate=cost(3e9, 16e6),
    )(pos, *args)


def pick_cols(pos, acts):
    tokens, depth = acts.shape
    block = depth // (NC * NZ)

    def kernel(pos_ref, in_ref, out_ref, buf, in_sem, out_sem):
        reads = [pltpu.make_async_copy(in_ref.at[:, picked_cols(pos_ref, idx, block)], buf.at[idx], in_sem.at[idx]) for idx in range(NZ)]
        writes = [pltpu.make_async_copy(buf.at[idx], out_ref.at[:, pl.ds(idx * block, block)], out_sem.at[idx]) for idx in range(NZ)]
        for read in reads:
            read.start()
        for read, write in zip(reads, writes):
            read.wait()
            write.start()
        for write in writes:
            write.wait()

    sems = pltpu.SemaphoreType.DMA((NZ,))
    return dma_kernel(kernel, pos, [acts], [jax.ShapeDtypeStruct((tokens, depth // 2), BF16)], [pltpu.VMEM((NZ, tokens, block), BF16), sems, sems])[0]


def grad_kernel(heights, pos_ref, *refs):
    pairs = len(heights)
    ins = refs[: 4 * pairs]
    outs = refs[4 * pairs : 4 * pairs + 2 * NZ]
    buf, sem = refs[4 * pairs + 2 * NZ :]
    half = buf.shape[2] // 2
    step = pl.program_id(0)
    slot = lax.rem(step, 2)

    def out_copy(idx, part):
        cols = pl.ds(half_start(pos_ref, part, half), half)
        return pltpu.make_async_copy(buf.at[idx % 2, :, cols], outs[2 * idx + part], sem.at[idx % 2, part])

    for idx in range(2, NZ):

        @pl.when(step == idx)
        def _(idx=idx):
            for part in range(2):
                out_copy(idx - 2, part).wait()

    start = 0
    for idx, height in enumerate(heights):
        own, recv, acts, acts_recv = ins[4 * idx : 4 * idx + 4]
        buf[slot, start : start + height, :] = dot_nn(own[...], acts[...]) + dot_nn(recv[...], acts_recv[...])
        start += height
    for idx in range(NZ):

        @pl.when(step == idx)
        def _(idx=idx):
            for part in range(2):
                out_copy(idx, part).start()

    @pl.when(step == NZ - 1)
    def _():
        for idx in (NZ - 2, NZ - 1):
            for part in range(2):
                out_copy(idx, part).wait()


def grad_pieces(pos, pairs):
    tokens, depth = pairs[0][2].shape
    cols = depth // (NZ * NC)
    in_specs = []
    args = []

    def z_of(n, pos):
        return lax.rem(pos[0] + jnp.where(n == 0, 2, jnp.where(n == 1, 1, jnp.where(n == 2, 3, 0))), NZ)

    for own, recv, acts, acts_recv, height, block in pairs:
        in_specs += [pl.BlockSpec((height, tokens), lambda n, pos, block=block: (block, 0))] * 2
        in_specs.append(pl.BlockSpec((tokens, cols), lambda n, pos: (0, z_of(n, pos) * NC + pos[1])))
        in_specs.append(pl.BlockSpec((tokens, cols), lambda n, pos: (0, z_of(n, pos))))
        args += [own, recv, acts, acts_recv]
    heights = [pair[4] for pair in pairs]
    rows = sum(heights)
    return pl.pallas_call(
        functools.partial(grad_kernel, heights),
        grid_spec=pltpu.PrefetchScalarGridSpec(
            num_scalar_prefetch=1,
            grid=(NZ,),
            in_specs=in_specs,
            out_specs=[pl.BlockSpec(memory_space=pl.ANY)] * (2 * NZ),
            scratch_shapes=[pltpu.VMEM((2, rows, cols), F32), pltpu.SemaphoreType.DMA((2, 2))],
        ),
        out_shape=[jax.ShapeDtypeStruct((rows, cols // 2), F32)] * (2 * NZ),
        compiler_params=params(),
        cost_estimate=cost(4 * rows * tokens * cols * NZ, 4 * tokens * cols * NZ),
        name="grad",
    )(pos, *args)


def sources(pos_ref, own_ref, first_ref, second_ref):
    return ((pos_ref[3] == 1, 0, own_ref), (pos_ref[3] == 0, 0, first_ref), (True, 1, second_ref))


def place(pos, own, first, second, height, block, transpose):
    cols = first.shape[1]
    spec = pl.BlockSpec((height, cols), lambda n, pos: (block, 0))

    def kernel(pos_ref, own_ref, first_ref, second_ref, out_ref):
        for chosen, idx, ref in sources(pos_ref, own_ref, first_ref, second_ref):

            @pl.when(jnp.logical_and(pl.program_id(0) == idx, chosen))
            def _(ref=ref):
                out_ref[...] = ref[...].T if transpose else ref[...]

    def order(n, pos):
        return jnp.where(n == 0, pos[2], 1 - pos[2])

    return pl.pallas_call(
        kernel,
        grid_spec=pltpu.PrefetchScalarGridSpec(
            num_scalar_prefetch=1,
            grid=(2,),
            in_specs=[spec] * 3,
            out_specs=pl.BlockSpec((cols, height), lambda n, pos: (0, order(n, pos))) if transpose else pl.BlockSpec((height, cols), lambda n, pos: (order(n, pos), 0)),
        ),
        out_shape=jax.ShapeDtypeStruct((cols, 2 * height) if transpose else (2 * height, cols), F32),
        compiler_params=params(),
        cost_estimate=cost(2e9, 16 * height * cols),
    )(pos, own, first, second)


def place_attn(pos, own, first, second, o_blk, head):
    rows, cols = first.shape
    qk = 2 * head

    def kernel(pos_ref, own_ref, first_ref, second_ref, out_ref, qkv_ref):
        for chosen, idx, ref in sources(pos_ref, own_ref, first_ref, second_ref):

            @pl.when(chosen)
            def _(idx=idx, ref=ref):
                bit = 1 - pos_ref[2] if idx else pos_ref[2]
                out_ref[pl.ds(pl.multiple_of(bit * o_blk, o_blk), o_blk), :] = ref[:o_blk, :]
                qkv_ref[:, pl.ds(pl.multiple_of(bit * qk, qk), qk)] = ref[o_blk : o_blk + qk, :].T
                qkv_ref[:, pl.ds(pl.multiple_of(2 * qk + bit * head, head), head)] = ref[o_blk + qk :, :].T

    def whole(*shape):
        return pl.BlockSpec(shape, lambda n, pos: (0, 0))

    shapes = ((2 * o_blk, cols), (cols, 2 * (qk + head)))
    return pl.pallas_call(
        kernel,
        grid_spec=pltpu.PrefetchScalarGridSpec(num_scalar_prefetch=1, grid=(1,), in_specs=[whole(rows, cols)] * 3, out_specs=[whole(*shape) for shape in shapes]),
        out_shape=[jax.ShapeDtypeStruct(shape, F32) for shape in shapes],
        compiler_params=params(),
        cost_estimate=cost(2e9, 16 * rows * cols),
        name="p_attn",
    )(pos, own, first, second)


def after(val, *earlier):
    return lax.optimization_barrier((val, *earlier))[0]


def ring(step, size):
    return [(src, (src + step) % size) for src in range(size)]


def hop_z(val, step):
    return lax.ppermute(val, "z", ring(step, NZ))


def swap_c(val):
    return lax.ppermute(val, "c", [(0, 1), (1, 0)])


def swap_y(val):
    return lax.ppermute(val, "y", [(src, src ^ 1) for src in range(NY)])


def turn(val, flip, home):
    def place_of(y_pos, c_pos):
        return y_pos * NC + c_pos

    pairs = [(place_of(2 * a + b, c), place_of(2 * c + (b ^ flip), a)) for a in range(2) for b in range(2) for c in range(NC) if home or flip or a != c]
    return lax.ppermute(val, ("y", "c"), pairs)


def swap_yc(val):
    pairs = [(y_pos * NC + c_pos, (y_pos ^ 1) * NC + 1 - c_pos) for y_pos in range(NY) for c_pos in range(NC)]
    return lax.ppermute(val, ("y", "c"), pairs)


def dot_nn(left, right):
    return lax.dot_general(left, right, (((1,), (0,)), ((), ())), preferred_element_type=F32)


def dot_nt(left, right):
    return lax.dot_general(left, right, (((1,), (1,)), ((), ())), preferred_element_type=F32)


def dot_tn(left, right):
    return lax.dot_general(left, right, (((0,), (0,)), ((), ())), preferred_element_type=F32)


def solution(mesh):
    wide_mesh = Mesh(mesh.devices.reshape(NZ, NY, NX, NC), ("z", "y", "x", "c"))
    rows = ("z", "y")
    cols = ("x", "c")
    act_spec = P(rows, cols, None)
    col_spec = P(rows, cols)
    row_spec = P(cols, rows)

    def layer(x_in, dy_in, norm_gain, w_qkv, w_out, w_gate, w_up, w_down, rope_cos, rope_sin):
        z_pos = lax.axis_index("z")
        y_pos = lax.axis_index("y")
        c_pos = lax.axis_index("c")
        even_y = y_pos % 2 == 0
        first_c = c_pos == 0
        pos = jnp.stack([z_pos, c_pos, y_pos % 2, y_pos // 2 == c_pos]).astype(jnp.int32)
        chunk = x_in.shape[1]
        head = 2 * rope_cos.shape[1]
        seq = rope_cos.shape[0]
        ff_blk = w_gate.shape[1] // 2
        o_blk = w_out.shape[0] // 2
        qkv_blk = o_blk + head

        def gather_rows(blocks):
            got = []
            for flip in (1, 0):
                got.insert(0, turn(jnp.where(even_y, blocks[flip], blocks[1 - flip]), flip, True))
            return got

        def gather_weight(piece):
            left, right = [], []
            for part in (1, 0):
                left.insert(0, hop_z(piece[part], 1))
                right.insert(0, hop_z(piece[part], -1))
            far = [hop_z(left[0], 1), hop_z(right[1], -1)]
            parts = []
            for mine in (piece, right, far, left):
                parts.append((mine, [swap_c(half) for half in mine]))
            return parts

        def grad_start(pairs, *earlier):
            far0, far1, up0, up1, down0, down1, own0, own1 = grad_pieces(after(pos, *earlier), pairs)
            far = (hop_z(far0, 1), hop_z(far1, -1))
            direct = (hop_z(up1, 1), hop_z(down0, -1))
            return (up0, down1), far, direct, (own0, own1)

        def grad_pass(state, *earlier):
            (up0, down1), far, direct, own = state
            sums = (up0 + after(far[0], *earlier), down1 + far[1])
            passed = (hop_z(sums[0], 1), hop_z(sums[1], -1))
            return direct, passed, own, sums

        def grad_back(state, *earlier):
            direct, passed, own = state[:3]
            first = own[0] + after(passed[0], *earlier) + direct[1]
            second = own[1] + direct[0] + passed[1]
            return first, turn(first, 0, False), turn(second, 1, False)

        def my_rows(val, mine):
            return lax.dynamic_slice_in_dim(val, (c_pos if mine else 1 - c_pos) * seq, seq, axis=0)

        def both_rows(own, got):
            return jnp.concatenate([jnp.where(first_c, own, got), jnp.where(first_c, got, own)], axis=0)

        cos_tab = jnp.concatenate([rope_cos, rope_cos], axis=1)
        sin_tab = jnp.concatenate([-rope_sin, rope_sin], axis=1)

        def qkv_cols(bit):
            first = 2 * head * bit
            third = HEAD_GROUP * head + head * bit
            return [w_qkv[:, first : first + 2 * head], w_qkv[:, third : third + head]]

        def block(weight, bit):
            size = weight.shape[1] // 2
            return weight[:, bit * size : (bit + 1) * size]

        down_t = w_down.T
        out_t = w_out.T
        wf_piece = gather_rows([jnp.concatenate([block(w_gate, j), block(w_up, j), *qkv_cols(j)], axis=1) for j in range(2)])
        ws_piece = gather_rows([jnp.concatenate([block(down_t, j), block(out_t, j)], axis=1) for j in range(2)])

        x_rows = after(x_in[0], cos_tab, sin_tab).astype(F32)
        normed, norm_pull = jax.vjp(lambda row_vals: norm_fwd(row_vals, norm_gain), x_rows)
        h_all = lax.all_gather(after(normed.astype(BF16), wf_piece[1]), ("y", "x"), axis=0, tiled=True)
        dy_all = lax.all_gather(after(dy_in[0], wf_piece[1]), ("y", "x"), axis=0, tiled=True)
        wf_parts = gather_weight(wf_piece)
        ws_parts = gather_weight(ws_piece)

        (qkv_tok,) = nn_pieces(pos, h_all, wf_parts, 2 * ff_blk, (qkv_blk,), 512)
        third = qkv_tok[:, o_blk:]
        qkv_other = swap_c(my_rows(qkv_tok, False))
        third_own = swap_y(my_rows(third, True))
        third_other = swap_yc(my_rows(third, False))
        (gate_up,) = nn_pieces(after(pos, qkv_tok), h_all, wf_parts, 0, (2 * ff_blk,), 512)
        act_val, act_t = act_fwd(gate_up)
        act_recv = swap_c(act_t)
        qkv_seq, attn_own, attn_other = attn_fwd(after(pos, act_t), qkv_tok, qkv_other, third_own, third_other, cos_tab, sin_tab)
        attn_got = swap_c(attn_other)
        y_part = nt_pieces(after(pos, attn_own), [act_val, attn_own, attn_got], ws_parts, chunk, 0, chunk)
        mix_sum = lax.psum_scatter(y_part, ("y", "x"), scatter_dimension=0, tiled=True)
        y_out = (x_rows + mix_sum).astype(BF16)[None]

        h_picked = pick_cols(after(pos, y_part), h_all)
        h_recv = swap_c(h_picked)
        dy_picked = pick_cols(after(pos, h_picked), dy_all)
        dy_recv = swap_c(dy_picked)
        d_act, d_attn = nn_pieces(after(pos, dy_picked), dy_all, ws_parts, 0, (ff_blk, o_blk), 256)
        d_attn_other = swap_c(my_rows(d_attn, False))
        g_act = grad_start([(act_t, act_recv, dy_all, dy_recv, ff_blk, 0)], d_attn)
        d_gate_up, d_gate_up_t = act_bwd(gate_up, after(d_act, g_act[3][0]))
        d_gate_up_recv = swap_c(d_gate_up_t)
        d_queries, keep, send = attn_bwd(after(pos, d_gate_up_t), qkv_seq, d_attn, d_attn_other, cos_tab, sin_tab)
        got = swap_y(send)
        g_gate = grad_start([(d_gate_up_t, d_gate_up_recv, h_all, h_recv, ff_blk, 0)], d_queries)
        d_own, d_other = attn_post(after(pos, g_gate[3][0]), d_queries, keep, got, cos_tab, sin_tab)
        d_got = swap_c(d_other)
        dh_part = nt_pieces(pos, [d_gate_up, d_own, d_got], wf_parts, chunk, 0, chunk)
        d_h = lax.psum_scatter(dh_part, ("y", "x"), scatter_dimension=0, tiled=True)
        g_act = grad_pass(g_act, dh_part)
        g_gate = grad_pass(g_gate, *g_act[3])
        g_up = grad_start([(d_gate_up_t, d_gate_up_recv, h_all, h_recv, ff_blk, 1)], *g_gate[3])
        b_act = grad_back(g_act, g_up[3][0])
        d_h = d_h.astype(BF16)
        dx_out = (dy_in[0].astype(F32) + norm_pull(d_h.astype(F32))[0]).astype(BF16)[None]

        attn_t = both_rows(attn_own, attn_got).T
        d_qkv_t = both_rows(d_own, d_got).T
        attn_recv = swap_c(attn_t)
        d_qkv_recv = swap_c(d_qkv_t)
        g_attn = grad_start([(attn_t, attn_recv, dy_all, dy_recv, o_blk, 0), (d_qkv_t, d_qkv_recv, h_all, h_recv, qkv_blk, 0)], g_up[3][0])
        g_up = grad_pass(g_up, g_attn[3][0])
        g_attn = grad_pass(g_attn)
        b_gate = grad_back(g_gate)
        b_up = grad_back(g_up)
        b_attn = grad_back(g_attn)
        dw_down = place(pos, *b_act, ff_blk, 0, False)
        dw_gate = place(pos, *b_gate, ff_blk, 0, True)
        dw_up = place(pos, *b_up, ff_blk, 0, True)
        dw_out, dw_qkv = place_attn(after(pos, dx_out, dw_up), *b_attn, o_blk, head)
        return y_out, dx_out, dw_qkv, dw_out, dw_gate, dw_up, dw_down


    return jax.shard_map(
        layer,
        mesh=wide_mesh,
        in_specs=(act_spec, act_spec, P(), col_spec, row_spec, col_spec, col_spec, row_spec, P(), P()),
        out_specs=(act_spec, act_spec, col_spec, row_spec, col_spec, col_spec, row_spec),
        check_vma=False,
    )
```

```python
import functools

import jax
import jax.numpy as jnp
from jax import lax
from jax.experimental import pallas as pl
from jax.experimental.pallas import tpu as pltpu
from jax.sharding import Mesh, PartitionSpec as P


NORM_EPS = 1e-5
NZ = 4
NY = 4
NX = 4
NC = 2
HEAD_GROUP = 4
F32 = jnp.float32
BF16 = jnp.bfloat16
VMEM_LIMIT = 67043328


def norm_fwd(row_vals, norm_gain):
    return row_vals * lax.rsqrt(jnp.mean(row_vals * row_vals, axis=-1, keepdims=True) + NORM_EPS) * norm_gain


def rotate(wide, cos_tab, sin_tab):
    return wide * cos_tab + pltpu.roll(wide, wide.shape[-1] // 2, wide.ndim - 1) * sin_tab


def rotate_back(wide, cos_tab, sin_tab):
    return wide * cos_tab - pltpu.roll(wide, wide.shape[-1] // 2, wide.ndim - 1) * sin_tab


def cost(flops, bytes_accessed):
    return pl.CostEstimate(flops=int(flops) // 20, bytes_accessed=int(bytes_accessed), transcendentals=0)


def params(**extra):
    return pltpu.CompilerParams(vmem_limit_bytes=VMEM_LIMIT, **extra)


def head_probs(q_rot, k_rot, scale):
    scores = dot_nt(q_rot, k_rot) * scale
    row_ids = lax.broadcasted_iota(jnp.int32, scores.shape, 0)
    col_ids = lax.broadcasted_iota(jnp.int32, scores.shape, 1)
    scores = jnp.where(row_ids >= col_ids, scores, -1e30)
    weights = jnp.exp(scores - jnp.max(scores, axis=-1, keepdims=True))
    return weights / jnp.sum(weights, axis=-1, keepdims=True)


def half_rows(core, idx, chunk):
    return pl.ds(pl.multiple_of((NC * idx + core) * chunk, chunk), chunk)


def chunk_rows(idx, chunk):
    return slice(idx * chunk, (idx + 1) * chunk)


def attn_fwd_kernel(heads, head, pos_ref, own_ref, other_ref, own_third_ref, other_third_ref, cos_ref, sin_ref, seq_ref, o_ref, o_other_ref, o_buf):
    core, odd = pos_ref[1], pos_ref[2]
    chunk = own_ref.shape[0] // NX
    width = heads * head
    mine = pl.ds(pl.multiple_of(width + odd * head, head), head)
    theirs = pl.ds(pl.multiple_of(width + (1 - odd) * head, head), head)
    for side, part_ref, third_ref in ((core, own_ref, own_third_ref), (1 - core, other_ref, other_third_ref)):
        for idx in range(NX):
            rows = half_rows(side, idx, chunk)
            seq_ref[0, rows, pl.ds(0, width)] = part_ref[chunk_rows(idx, chunk), :width]
            seq_ref[0, rows, mine] = part_ref[chunk_rows(idx, chunk), width:]
            seq_ref[0, rows, theirs] = third_ref[chunk_rows(idx, chunk), :]
    cos_tab, sin_tab = cos_ref[...], sin_ref[...]
    k_rot = rotate(seq_ref[0, :, width : width + head].astype(F32), cos_tab, sin_tab).astype(BF16)
    values = seq_ref[0, :, width + head :]
    for idx in range(heads):
        lanes = slice(idx * head, (idx + 1) * head)
        q_rot = rotate(seq_ref[0, :, lanes].astype(F32), cos_tab, sin_tab).astype(BF16)
        probs = head_probs(q_rot, k_rot, head**-0.5)
        o_buf[:, lanes] = dot_nn(probs.astype(BF16), values).astype(BF16)
    for side, out_ref in ((core, o_ref), (1 - core, o_other_ref)):
        for idx in range(NX):
            out_ref[chunk_rows(idx, chunk), :] = o_buf[half_rows(side, idx, chunk), :]


def attn_bwd_kernel(heads, head, pos_ref, seq_ref, own_ref, other_ref, cos_ref, sin_ref, dq_ref, keep_ref, send_ref, do_buf):
    core, odd = pos_ref[1], pos_ref[2]
    chunk = own_ref.shape[0] // NX
    width = heads * head
    for side, part_ref in ((core, own_ref), (1 - core, other_ref)):
        for idx in range(NX):
            do_buf[half_rows(side, idx, chunk), :] = part_ref[chunk_rows(idx, chunk), :]
    cos_tab, sin_tab = cos_ref[...], sin_ref[...]
    k_rot = rotate(seq_ref[0, :, width : width + head].astype(F32), cos_tab, sin_tab).astype(BF16)
    values = seq_ref[0, :, width + head :]
    d_keys = jnp.zeros(k_rot.shape, F32)
    d_values = jnp.zeros(k_rot.shape, F32)
    for idx in range(heads):
        lanes = slice(idx * head, (idx + 1) * head)
        q_rot = rotate(seq_ref[0, :, lanes].astype(F32), cos_tab, sin_tab).astype(BF16)
        d_out = do_buf[:, lanes]
        probs = head_probs(q_rot, k_rot, head**-0.5)
        d_values += dot_tn(probs.astype(BF16), d_out)
        d_probs = dot_nt(d_out, values).astype(BF16).astype(F32)
        d_scores = probs * (d_probs - jnp.sum(d_probs * probs, axis=-1, keepdims=True))
        d_scores = (d_scores * head**-0.5).astype(BF16)
        d_q_rot = dot_nn(d_scores, k_rot).astype(BF16)
        dq_ref[0, :, lanes] = rotate_back(d_q_rot.astype(F32), cos_tab, sin_tab).astype(BF16)
        d_keys += dot_tn(d_scores, q_rot)

    @pl.when(odd == 0)
    def _():
        keep_ref[0] = d_keys
        send_ref[0] = d_values

    @pl.when(odd == 1)
    def _():
        keep_ref[0] = d_values
        send_ref[0] = d_keys


def attn_post_kernel(heads, head, pos_ref, dq_ref, keep_ref, got_ref, cos_ref, sin_ref, own_ref, other_ref, third_buf):
    core, odd = pos_ref[1], pos_ref[2]
    chunk = own_ref.shape[0] // NX
    width = heads * head
    total = (keep_ref[0] + got_ref[0]).astype(BF16)

    @pl.when(odd == 0)
    def _():
        third_buf[...] = rotate_back(total.astype(F32), cos_ref[...], sin_ref[...]).astype(BF16)

    @pl.when(odd == 1)
    def _():
        third_buf[...] = total

    for side, out_ref in ((core, own_ref), (1 - core, other_ref)):
        for idx in range(NX):
            rows = half_rows(side, idx, chunk)
            out_ref[chunk_rows(idx, chunk), :width] = dq_ref[0, rows, :]
            out_ref[chunk_rows(idx, chunk), width:] = third_buf[rows, :]


def per_sequence(kernel, pos, args, specs, out_specs, out_shape, scratch, flops):
    return pl.pallas_call(
        kernel,
        grid_spec=pltpu.PrefetchScalarGridSpec(num_scalar_prefetch=1, grid=(2,), in_specs=specs, out_specs=out_specs, scratch_shapes=scratch),
        out_shape=out_shape,
        compiler_params=params(),
        cost_estimate=cost(flops, 4e6),
    )(pos, *args)


def own_spec(rows, width):
    return pl.BlockSpec((rows, width), lambda i, pos: (2 * pos[1] + i, 0))


def pair_spec(rows, width):
    return pl.BlockSpec((rows, width), lambda i, pos: (i, 0))


def seq_spec(seq, width):
    return pl.BlockSpec((1, seq, width), lambda i, pos: (i, 0, 0))


def table_spec(table):
    return pl.BlockSpec(table.shape, lambda i, pos: (0, 0))


def attn_fwd(pos, qkv_tok, other, own_third, other_third, cos_tab, sin_tab):
    seq, head = cos_tab.shape
    width = qkv_tok.shape[1] - head
    rows = seq // 2
    half = jax.ShapeDtypeStruct((seq, width), BF16)
    return per_sequence(
        functools.partial(attn_fwd_kernel, width // head, head),
        pos,
        (qkv_tok, other, own_third, other_third, cos_tab, sin_tab),
        [own_spec(rows, width + head), pair_spec(rows, width + head), pair_spec(rows, head), pair_spec(rows, head), table_spec(cos_tab), table_spec(sin_tab)],
        [seq_spec(seq, width + 2 * head), pair_spec(rows, width), pair_spec(rows, width)],
        [jax.ShapeDtypeStruct((2, seq, width + 2 * head), BF16), half, half],
        [pltpu.VMEM((seq, width), BF16)],
        16e9,
    )


def attn_bwd(pos, qkv_seq, d_attn, other, cos_tab, sin_tab):
    seq, head = cos_tab.shape
    width = d_attn.shape[1]
    rows = seq // 2
    part = jax.ShapeDtypeStruct((2, seq, head), F32)
    return per_sequence(
        functools.partial(attn_bwd_kernel, width // head, head),
        pos,
        (qkv_seq, d_attn, other, cos_tab, sin_tab),
        [seq_spec(seq, width + 2 * head), own_spec(rows, width), pair_spec(rows, width), table_spec(cos_tab), table_spec(sin_tab)],
        [seq_spec(seq, width), seq_spec(seq, head), seq_spec(seq, head)],
        [jax.ShapeDtypeStruct((2, seq, width), BF16), part, part],
        [pltpu.VMEM((seq, width), BF16)],
        16e9,
    )


def attn_post(pos, d_queries, keep, got, cos_tab, sin_tab):
    seq, head = cos_tab.shape
    width = d_queries.shape[2]
    rows = seq // 2
    half = jax.ShapeDtypeStruct((seq, width + head), BF16)
    return per_sequence(
        functools.partial(attn_post_kernel, width // head, head),
        pos,
        (d_queries, keep, got, cos_tab, sin_tab),
        [seq_spec(seq, width), seq_spec(seq, head), seq_spec(seq, head), table_spec(cos_tab), table_spec(sin_tab)],
        [pair_spec(rows, width + head), pair_spec(rows, width + head)],
        [half, half],
        [pltpu.VMEM((seq, head), BF16)],
        2e9,
    )


def act_fwd_kernel(half, ab_ref, u_ref, ut_ref):
    gate_val = ab_ref[:, :half].astype(F32)
    up_val = ab_ref[:, half:].astype(F32)
    act_val = gate_val * jax.nn.sigmoid(gate_val) * up_val
    u_ref[...] = act_val.astype(BF16)
    ut_ref[...] = act_val.T.astype(BF16)


def act_fwd(gate_up):
    tokens, width = gate_up.shape
    half = width // 2
    rows = tokens // 4
    return pl.pallas_call(
        functools.partial(act_fwd_kernel, half),
        grid=(4,),
        in_specs=[pl.BlockSpec((rows, width), lambda i: (i, 0))],
        out_specs=[pl.BlockSpec((rows, half), lambda i: (i, 0)), pl.BlockSpec((half, rows), lambda i: (0, i))],
        out_shape=[jax.ShapeDtypeStruct((tokens, half), BF16), jax.ShapeDtypeStruct((half, tokens), BF16)],
        compiler_params=params(),
        cost_estimate=cost(4e9, 8e6),
        name="act_fwd",
    )(gate_up)


def act_bwd_kernel(half, ab_ref, du_ref, dab_ref, dabt_ref):
    gate_val = ab_ref[:, :half].astype(F32)
    up_val = ab_ref[:, half:].astype(F32)
    d_act = du_ref[...].astype(F32)
    sig = jax.nn.sigmoid(gate_val)
    d_silu = d_act * up_val
    d_gate = d_silu * sig + d_silu * gate_val * (sig * (1.0 - sig))
    d_up = d_act * (gate_val * sig)
    dab_ref[:, :half] = d_gate.astype(BF16)
    dab_ref[:, half:] = d_up.astype(BF16)
    dabt_ref[:half, :] = d_gate.T.astype(BF16)
    dabt_ref[half:, :] = d_up.T.astype(BF16)


def act_bwd(gate_up, d_mixed):
    tokens, width = gate_up.shape
    half = width // 2
    rows = tokens // 4
    return pl.pallas_call(
        functools.partial(act_bwd_kernel, half),
        grid=(4,),
        in_specs=[pl.BlockSpec((rows, width), lambda i: (i, 0)), pl.BlockSpec((rows, half), lambda i: (i, 0))],
        out_specs=[pl.BlockSpec((rows, width), lambda i: (i, 0)), pl.BlockSpec((width, rows), lambda i: (0, i))],
        out_shape=[jax.ShapeDtypeStruct((tokens, width), BF16), jax.ShapeDtypeStruct((width, tokens), BF16)],
        compiler_params=params(),
        cost_estimate=cost(8e9, 14e6),
        name="act_bwd",
    )(gate_up, d_mixed)


def piece_block(pos_ref, step, other):
    core = pos_ref[1]
    return lax.rem(pos_ref[0] + step, NZ) * NC + (1 - core if other else core)


def half_start(pos_ref, part, half):
    return pl.multiple_of((1 - pos_ref[2] if part else pos_ref[2]) * half, half)


def nn_kernel(keys, first, count_out, tile, first_col, pos_ref, acts_ref, *refs):
    count = len(keys)
    halves = refs[: 2 * count]
    outs = refs[2 * count : 2 * count + count_out]
    acts_buf, w_buf, total, acts_sem, w_sem = refs[2 * count + count_out :]
    block = acts_buf.shape[1] // count
    half = block // 2
    copies = []
    for idx in range(count):
        cols = pl.ds(pl.multiple_of(piece_block(pos_ref, *keys[idx]) * block, block), block)
        copies.append([pltpu.make_async_copy(acts_ref.at[:, cols], acts_buf.at[:, pl.ds(idx * block, block)], acts_sem.at[idx])])
        for part in range(2):
            rows = pl.ds(idx * block + half_start(pos_ref, part, half), half)
            source = halves[2 * idx + part].at[:, pl.ds(first_col, w_buf.shape[1])]
            copies[-1].append(pltpu.make_async_copy(source, w_buf.at[rows], w_sem.at[2 * idx + part]))
    for group in copies:
        for copy in group:
            copy.start()
    for lo, hi in ((0, first), (first, count)):
        for group in copies[lo:hi]:
            for copy in group:
                copy.wait()
        depth = pl.ds(lo * block, (hi - lo) * block)
        start = 0
        for out_ref in outs:
            width = out_ref.shape[1]

            def step(out_lo, size, start=start, out_ref=out_ref, depth=depth, hi=hi):
                cols = pl.ds(pl.multiple_of(start + out_lo, 128), size)
                part = dot_nn(acts_buf[:, depth], w_buf[depth, cols])
                if hi == count:
                    out_ref[:, pl.ds(pl.multiple_of(out_lo, 128), size)] = (total[:, cols] + part).astype(BF16)
                else:
                    total[:, cols] = part

            whole = width // tile
            if whole:
                pl.loop(0, whole)(lambda n: step(n * tile, tile))
            if width % tile:
                step(whole * tile, width % tile)
            start += width


def nn_pieces(pos, acts, parts, first_col, widths, tile):
    keys = [(step, other) for step in (0, 1, 3, 2) for other in range(2)]
    halves = [parts[step][other][part] for step, other in keys for part in range(2)]
    tokens, depth = acts.shape
    width = sum(widths)
    count = len(keys)
    anywhere = pl.BlockSpec(memory_space=pl.ANY)
    return pl.pallas_call(
        functools.partial(nn_kernel, keys, 2, len(widths), tile, first_col),
        grid_spec=pltpu.PrefetchScalarGridSpec(
            num_scalar_prefetch=1,
            grid=(1,),
            in_specs=[anywhere] * (1 + 2 * count),
            out_specs=[pl.BlockSpec((tokens, size), lambda i, pos: (0, 0)) for size in widths],
            scratch_shapes=[
                pltpu.VMEM((tokens, depth), BF16),
                pltpu.VMEM((depth, width), BF16),
                pltpu.VMEM((tokens, width), F32),
                pltpu.SemaphoreType.DMA((count,)),
                pltpu.SemaphoreType.DMA((2 * count,)),
            ],
        ),
        out_shape=[jax.ShapeDtypeStruct((tokens, size), BF16) for size in widths],
        compiler_params=params(),
        cost_estimate=cost(2 * tokens * depth * width, 2 * depth * (tokens + width)),
    )(pos, acts, *halves)


def nt_kernel(keys, sides, first_row, pos_ref, *refs):
    count_left = len(sides)
    count = len(keys)
    lefts = refs[:count_left]
    halves = refs[count_left : count_left + 2 * count]
    out_ref, left_buf, w_buf, out_buf, left_sem, w_sem, out_sem = refs[count_left + 2 * count :]
    block = out_buf.shape[2]
    half = block // 2
    slots = w_buf.shape[0]
    left_copies = []
    start = 0
    for idx, (left, side) in enumerate(zip(lefts, sides)):
        chunks, _, width = left.shape
        first = 0 if side is None else (1 - pos_ref[1] if side else pos_ref[1]) * chunks
        source = left.at[:, pl.ds(first_row, left_buf.shape[1]), :]
        left_copies.append(pltpu.make_async_copy(source, left_buf.at[pl.ds(first, chunks), :, pl.ds(start, width)], left_sem.at[idx]))
        left_copies[-1].start()
        start += 0 if side == 0 else width

    def copies(idx, slot):
        for part in range(2):
            rows = pl.ds(half_start(pos_ref, part, half), half)
            yield pltpu.make_async_copy(halves[2 * idx + part], w_buf.at[slot, rows], w_sem.at[slot, part])

    def out_copy(idx):
        core = pos_ref[1]
        other = lax.rem(idx, 2)
        block_id = lax.rem(pos_ref[0] + idx // 2, NZ) * NC + core + other - 2 * core * other
        slot = lax.rem(idx, 2)
        return pltpu.make_async_copy(out_buf.at[slot], out_ref.at[:, pl.ds(pl.multiple_of(block_id * block, block), block)], out_sem.at[slot])

    for idx in range(slots - 1):
        for copy in copies(idx, idx):
            copy.start()
    for copy in left_copies:
        copy.wait()

    @pl.loop(0, count)
    def _(step):
        slot = lax.rem(step, slots)
        for idx in range(slots - 1, count):

            @pl.when(step + slots - 1 == idx)
            def _(idx=idx):
                for copy in copies(idx, idx % slots):
                    copy.start()

        for copy in copies(0, slot):
            copy.wait()

        @pl.when(step >= 2)
        def _():
            out_copy(step - 2).wait()

        out_buf[lax.rem(step, 2)] = dot_nt(left_buf[...].reshape(out_buf.shape[1], left_buf.shape[2]), w_buf[slot])
        out_copy(step).start()

    for idx in range(count - 2, count):
        out_copy(idx).wait()


def nt_pieces(pos, lefts, parts, chunk, first_row, rows):
    sides = (None, 0, 1)
    keys = [(step, other) for step in range(NZ) for other in range(2)]
    halves = [parts[step][other][part] for step, other in keys for part in range(2)]
    lefts = [left.reshape(-1, chunk, left.shape[1]) for left in lefts]
    chunks = lefts[0].shape[0]
    tokens = chunks * rows
    block = 2 * halves[0].shape[0]
    depth = block * len(keys)
    width = halves[0].shape[1]
    slots = 3
    anywhere = pl.BlockSpec(memory_space=pl.ANY)
    return pl.pallas_call(
        functools.partial(nt_kernel, keys, sides, first_row),
        grid_spec=pltpu.PrefetchScalarGridSpec(
            num_scalar_prefetch=1,
            grid=(1,),
            in_specs=[anywhere] * (len(lefts) + len(halves)),
            out_specs=anywhere,
            scratch_shapes=[
                pltpu.VMEM((chunks, rows, width), BF16),
                pltpu.VMEM((slots, block, width), BF16),
                pltpu.VMEM((2, tokens, block), F32),
                pltpu.SemaphoreType.DMA((len(lefts),)),
                pltpu.SemaphoreType.DMA((slots, 2)),
                pltpu.SemaphoreType.DMA((2,)),
            ],
        ),
        out_shape=jax.ShapeDtypeStruct((tokens, depth), F32),
        compiler_params=params(),
        cost_estimate=cost(2 * tokens * depth * width, 2 * depth * width + 4 * tokens * depth),
    )(pos, *lefts, *halves)


def picked_cols(pos_ref, idx, block):
    return pl.ds(pl.multiple_of((NC * idx + 1 - pos_ref[1]) * block, block), block)


def dma_kernel(kernel, pos, args, out_shape, scratch):
    anywhere = pl.BlockSpec(memory_space=pl.ANY)
    return pl.pallas_call(
        kernel,
        grid_spec=pltpu.PrefetchScalarGridSpec(
            num_scalar_prefetch=1, grid=(1,), in_specs=[anywhere] * len(args), out_specs=[anywhere] * len(out_shape), scratch_shapes=scratch
        ),
        out_shape=out_shape,
        compiler_params=params(),
        cost_estimate=cost(3e9, 16e6),
    )(pos, *args)


def pick_cols(pos, acts):
    tokens, depth = acts.shape
    block = depth // (NC * NZ)

    def kernel(pos_ref, in_ref, out_ref, buf, in_sem, out_sem):
        reads = [pltpu.make_async_copy(in_ref.at[:, picked_cols(pos_ref, idx, block)], buf.at[idx], in_sem.at[idx]) for idx in range(NZ)]
        writes = [pltpu.make_async_copy(buf.at[idx], out_ref.at[:, pl.ds(idx * block, block)], out_sem.at[idx]) for idx in range(NZ)]
        for read in reads:
            read.start()
        for read, write in zip(reads, writes):
            read.wait()
            write.start()
        for write in writes:
            write.wait()

    sems = pltpu.SemaphoreType.DMA((NZ,))
    return dma_kernel(kernel, pos, [acts], [jax.ShapeDtypeStruct((tokens, depth // 2), BF16)], [pltpu.VMEM((NZ, tokens, block), BF16), sems, sems])[0]


def grad_kernel(heights, pos_ref, *refs):
    pairs = len(heights)
    ins = refs[: 4 * pairs]
    outs = refs[4 * pairs : 4 * pairs + 2 * NZ]
    buf, sem = refs[4 * pairs + 2 * NZ :]
    half = buf.shape[2] // 2
    step = pl.program_id(0)
    slot = lax.rem(step, 2)

    def out_copy(idx, part):
        cols = pl.ds(half_start(pos_ref, part, half), half)
        return pltpu.make_async_copy(buf.at[idx % 2, :, cols], outs[2 * idx + part], sem.at[idx % 2, part])

    for idx in range(2, NZ):

        @pl.when(step == idx)
        def _(idx=idx):
            for part in range(2):
                out_copy(idx - 2, part).wait()

    start = 0
    for idx, height in enumerate(heights):
        own, recv, acts, acts_recv = ins[4 * idx : 4 * idx + 4]
        buf[slot, start : start + height, :] = dot_nn(own[...], acts[...]) + dot_nn(recv[...], acts_recv[...])
        start += height
    for idx in range(NZ):

        @pl.when(step == idx)
        def _(idx=idx):
            for part in range(2):
                out_copy(idx, part).start()

    @pl.when(step == NZ - 1)
    def _():
        for idx in (NZ - 2, NZ - 1):
            for part in range(2):
                out_copy(idx, part).wait()


def grad_pieces(pos, pairs):
    tokens, depth = pairs[0][2].shape
    cols = depth // (NZ * NC)
    in_specs = []
    args = []

    def z_of(n, pos):
        return lax.rem(pos[0] + jnp.where(n == 0, 2, jnp.where(n == 1, 1, jnp.where(n == 2, 3, 0))), NZ)

    for own, recv, acts, acts_recv, height, block in pairs:
        in_specs += [pl.BlockSpec((height, tokens), lambda n, pos, block=block: (block, 0))] * 2
        in_specs.append(pl.BlockSpec((tokens, cols), lambda n, pos: (0, z_of(n, pos) * NC + pos[1])))
        in_specs.append(pl.BlockSpec((tokens, cols), lambda n, pos: (0, z_of(n, pos))))
        args += [own, recv, acts, acts_recv]
    heights = [pair[4] for pair in pairs]
    rows = sum(heights)
    return pl.pallas_call(
        functools.partial(grad_kernel, heights),
        grid_spec=pltpu.PrefetchScalarGridSpec(
            num_scalar_prefetch=1,
            grid=(NZ,),
            in_specs=in_specs,
            out_specs=[pl.BlockSpec(memory_space=pl.ANY)] * (2 * NZ),
            scratch_shapes=[pltpu.VMEM((2, rows, cols), F32), pltpu.SemaphoreType.DMA((2, 2))],
        ),
        out_shape=[jax.ShapeDtypeStruct((rows, cols // 2), F32)] * (2 * NZ),
        compiler_params=params(),
        cost_estimate=cost(4 * rows * tokens * cols * NZ, 4 * tokens * cols * NZ),
        name="grad",
    )(pos, *args)


def sources(pos_ref, own_ref, first_ref, second_ref):
    return ((pos_ref[3] == 1, 0, own_ref), (pos_ref[3] == 0, 0, first_ref), (True, 1, second_ref))


def place(pos, own, first, second, height, block, transpose):
    cols = first.shape[1]
    spec = pl.BlockSpec((height, cols), lambda n, pos: (block, 0))

    def kernel(pos_ref, own_ref, first_ref, second_ref, out_ref):
        for chosen, idx, ref in sources(pos_ref, own_ref, first_ref, second_ref):

            @pl.when(jnp.logical_and(pl.program_id(0) == idx, chosen))
            def _(ref=ref):
                out_ref[...] = ref[...].T if transpose else ref[...]

    def order(n, pos):
        return jnp.where(n == 0, pos[2], 1 - pos[2])

    return pl.pallas_call(
        kernel,
        grid_spec=pltpu.PrefetchScalarGridSpec(
            num_scalar_prefetch=1,
            grid=(2,),
            in_specs=[spec] * 3,
            out_specs=pl.BlockSpec((cols, height), lambda n, pos: (0, order(n, pos))) if transpose else pl.BlockSpec((height, cols), lambda n, pos: (order(n, pos), 0)),
        ),
        out_shape=jax.ShapeDtypeStruct((cols, 2 * height) if transpose else (2 * height, cols), F32),
        compiler_params=params(),
        cost_estimate=cost(2e9, 16 * height * cols),
    )(pos, own, first, second)


def place_attn(pos, own, first, second, o_blk, head):
    rows, cols = first.shape
    qk = 2 * head

    def kernel(pos_ref, own_ref, first_ref, second_ref, out_ref, qkv_ref):
        for chosen, idx, ref in sources(pos_ref, own_ref, first_ref, second_ref):

            @pl.when(chosen)
            def _(idx=idx, ref=ref):
                bit = 1 - pos_ref[2] if idx else pos_ref[2]
                out_ref[pl.ds(pl.multiple_of(bit * o_blk, o_blk), o_blk), :] = ref[:o_blk, :]
                qkv_ref[:, pl.ds(pl.multiple_of(bit * qk, qk), qk)] = ref[o_blk : o_blk + qk, :].T
                qkv_ref[:, pl.ds(pl.multiple_of(2 * qk + bit * head, head), head)] = ref[o_blk + qk :, :].T

    def whole(*shape):
        return pl.BlockSpec(shape, lambda n, pos: (0, 0))

    shapes = ((2 * o_blk, cols), (cols, 2 * (qk + head)))
    return pl.pallas_call(
        kernel,
        grid_spec=pltpu.PrefetchScalarGridSpec(num_scalar_prefetch=1, grid=(1,), in_specs=[whole(rows, cols)] * 3, out_specs=[whole(*shape) for shape in shapes]),
        out_shape=[jax.ShapeDtypeStruct(shape, F32) for shape in shapes],
        compiler_params=params(),
        cost_estimate=cost(2e9, 16 * rows * cols),
        name="p_attn",
    )(pos, own, first, second)


def after(val, *earlier):
    return lax.optimization_barrier((val, *earlier))[0]


def ring(step, size):
    return [(src, (src + step) % size) for src in range(size)]


def hop_z(val, step):
    return lax.ppermute(val, "z", ring(step, NZ))


def swap_c(val):
    return lax.ppermute(val, "c", [(0, 1), (1, 0)])


def swap_y(val):
    return lax.ppermute(val, "y", [(src, src ^ 1) for src in range(NY)])


def turn(val, flip, home):
    def place_of(y_pos, c_pos):
        return y_pos * NC + c_pos

    pairs = [(place_of(2 * a + b, c), place_of(2 * c + (b ^ flip), a)) for a in range(2) for b in range(2) for c in range(NC) if home or flip or a != c]
    return lax.ppermute(val, ("y", "c"), pairs)


def swap_yc(val):
    pairs = [(y_pos * NC + c_pos, (y_pos ^ 1) * NC + 1 - c_pos) for y_pos in range(NY) for c_pos in range(NC)]
    return lax.ppermute(val, ("y", "c"), pairs)


def dot_nn(left, right):
    return lax.dot_general(left, right, (((1,), (0,)), ((), ())), preferred_element_type=F32)


def dot_nt(left, right):
    return lax.dot_general(left, right, (((1,), (1,)), ((), ())), preferred_element_type=F32)


def dot_tn(left, right):
    return lax.dot_general(left, right, (((0,), (0,)), ((), ())), preferred_element_type=F32)


def solution(mesh):
    wide_mesh = Mesh(mesh.devices.reshape(NZ, NY, NX, NC), ("z", "y", "x", "c"))
    rows = ("z", "y")
    cols = ("x", "c")
    act_spec = P(rows, cols, None)
    col_spec = P(rows, cols)
    row_spec = P(cols, rows)

    def layer(x_in, dy_in, norm_gain, w_qkv, w_out, w_gate, w_up, w_down, rope_cos, rope_sin):
        z_pos = lax.axis_index("z")
        y_pos = lax.axis_index("y")
        c_pos = lax.axis_index("c")
        even_y = y_pos % 2 == 0
        first_c = c_pos == 0
        pos = jnp.stack([z_pos, c_pos, y_pos % 2, y_pos // 2 == c_pos]).astype(jnp.int32)
        chunk = x_in.shape[1]
        head = 2 * rope_cos.shape[1]
        seq = rope_cos.shape[0]
        ff_blk = w_gate.shape[1] // 2
        o_blk = w_out.shape[0] // 2
        qkv_blk = o_blk + head

        def gather_rows(blocks):
            got = []
            for flip in (1, 0):
                got.insert(0, turn(jnp.where(even_y, blocks[flip], blocks[1 - flip]), flip, True))
            return got

        def gather_weight(piece):
            left, right = [], []
            for part in (1, 0):
                left.insert(0, hop_z(piece[part], 1))
                right.insert(0, hop_z(piece[part], -1))
            far = [hop_z(left[0], 1), hop_z(right[1], -1)]
            parts = []
            for mine in (piece, right, far, left):
                parts.append((mine, [swap_c(half) for half in mine]))
            return parts

        def grad_start(pairs, *earlier):
            far0, far1, up0, up1, down0, down1, own0, own1 = grad_pieces(after(pos, *earlier), pairs)
            far = (hop_z(far0, 1), hop_z(far1, -1))
            direct = (hop_z(up1, 1), hop_z(down0, -1))
            return (up0, down1), far, direct, (own0, own1)

        def grad_pass(state, *earlier):
            (up0, down1), far, direct, own = state
            sums = (up0 + after(far[0], *earlier), down1 + far[1])
            passed = (hop_z(sums[0], 1), hop_z(sums[1], -1))
            return direct, passed, own, sums

        def grad_back(state, *earlier):
            direct, passed, own = state[:3]
            first = own[0] + after(passed[0], *earlier) + direct[1]
            second = own[1] + direct[0] + passed[1]
            return first, turn(first, 0, False), turn(second, 1, False)

        def my_rows(val, mine):
            return lax.dynamic_slice_in_dim(val, (c_pos if mine else 1 - c_pos) * seq, seq, axis=0)

        def both_rows(own, got):
            return jnp.concatenate([jnp.where(first_c, own, got), jnp.where(first_c, got, own)], axis=0)

        cos_tab = jnp.concatenate([rope_cos, rope_cos], axis=1)
        sin_tab = jnp.concatenate([-rope_sin, rope_sin], axis=1)

        def qkv_cols(bit):
            first = 2 * head * bit
            third = HEAD_GROUP * head + head * bit
            return [w_qkv[:, first : first + 2 * head], w_qkv[:, third : third + head]]

        def block(weight, bit):
            size = weight.shape[1] // 2
            return weight[:, bit * size : (bit + 1) * size]

        down_t = w_down.T
        out_t = w_out.T
        wf_piece = gather_rows([jnp.concatenate([block(w_gate, j), block(w_up, j), *qkv_cols(j)], axis=1) for j in range(2)])
        ws_piece = gather_rows([jnp.concatenate([block(down_t, j), block(out_t, j)], axis=1) for j in range(2)])

        x_rows = after(x_in[0], cos_tab, sin_tab).astype(F32)
        normed, norm_pull = jax.vjp(lambda row_vals: norm_fwd(row_vals, norm_gain), x_rows)
        h_all = lax.all_gather(after(normed.astype(BF16), wf_piece[1]), ("y", "x"), axis=0, tiled=True)
        dy_all = lax.all_gather(after(dy_in[0], wf_piece[1]), ("y", "x"), axis=0, tiled=True)
        wf_parts = gather_weight(wf_piece)
        ws_parts = gather_weight(ws_piece)

        (qkv_tok,) = nn_pieces(pos, h_all, wf_parts, 2 * ff_blk, (qkv_blk,), 512)
        third = qkv_tok[:, o_blk:]
        qkv_other = swap_c(my_rows(qkv_tok, False))
        third_own = swap_y(my_rows(third, True))
        third_other = swap_yc(my_rows(third, False))
        (gate_up,) = nn_pieces(after(pos, qkv_tok), h_all, wf_parts, 0, (2 * ff_blk,), 512)
        act_val, act_t = act_fwd(gate_up)
        act_recv = swap_c(act_t)
        qkv_seq, attn_own, attn_other = attn_fwd(after(pos, act_t), qkv_tok, qkv_other, third_own, third_other, cos_tab, sin_tab)
        attn_got = swap_c(attn_other)
        y_part = nt_pieces(after(pos, attn_own), [act_val, attn_own, attn_got], ws_parts, chunk, 0, chunk)
        mix_sum = lax.psum_scatter(y_part, ("y", "x"), scatter_dimension=0, tiled=True)
        y_out = (x_rows + mix_sum).astype(BF16)[None]

        dy_picked = pick_cols(after(pos, y_part), dy_all)
        dy_recv = swap_c(dy_picked)
        h_picked = pick_cols(after(pos, dy_picked), h_all)
        h_recv = swap_c(h_picked)
        g_act = grad_start([(act_t, act_recv, dy_all, dy_recv, ff_blk, 0)], h_picked)
        d_act, d_attn = nn_pieces(after(pos, g_act[3][0]), dy_all, ws_parts, 0, (ff_blk, o_blk), 256)
        d_attn_other = swap_c(my_rows(d_attn, False))
        d_gate_up, d_gate_up_t = act_bwd(gate_up, d_act)
        d_gate_up_recv = swap_c(d_gate_up_t)
        d_queries, keep, send = attn_bwd(after(pos, d_gate_up_t), qkv_seq, d_attn, d_attn_other, cos_tab, sin_tab)
        got = swap_y(send)
        g_act = grad_pass(g_act, d_queries)
        g_gate = grad_start([(d_gate_up_t, d_gate_up_recv, h_all, h_recv, ff_blk, 0)], *g_act[3])
        d_own, d_other = attn_post(after(pos, g_gate[3][0]), d_queries, keep, got, cos_tab, sin_tab)
        d_got = swap_c(d_other)
        dh_part = nt_pieces(pos, [d_gate_up, d_own, d_got], wf_parts, chunk, 0, chunk)
        d_h = lax.psum_scatter(dh_part, ("y", "x"), scatter_dimension=0, tiled=True)
        g_gate = grad_pass(g_gate, dh_part)
        g_up = grad_start([(d_gate_up_t, d_gate_up_recv, h_all, h_recv, ff_blk, 1)], *g_gate[3])
        b_act = grad_back(g_act, g_up[3][0])

        attn_t = both_rows(attn_own, attn_got).T
        d_qkv_t = both_rows(d_own, d_got).T
        attn_recv = swap_c(attn_t)
        d_qkv_recv = swap_c(d_qkv_t)
        g_attn = grad_start([(attn_t, attn_recv, dy_all, dy_recv, o_blk, 0), (d_qkv_t, d_qkv_recv, h_all, h_recv, qkv_blk, 0)], g_up[3][0])
        g_up = grad_pass(g_up, g_attn[3][0])
        g_attn = grad_pass(g_attn)
        b_gate = grad_back(g_gate)
        b_up = grad_back(g_up)
        b_attn = grad_back(g_attn)
        dw_down = place(pos, *b_act, ff_blk, 0, False)
        dw_gate = place(pos, *b_gate, ff_blk, 0, True)
        dw_up = place(pos, *b_up, ff_blk, 0, True)
        dw_out, dw_qkv = place_attn(after(pos, dw_up), *b_attn, o_blk, head)
        d_h = after(d_h, dw_out).astype(BF16)
        dx_out = (dy_in[0].astype(F32) + norm_pull(d_h.astype(F32))[0]).astype(BF16)[None]
        return y_out, dx_out, dw_qkv, dw_out, dw_gate, dw_up, dw_down


    return jax.shard_map(
        layer,
        mesh=wide_mesh,
        in_specs=(act_spec, act_spec, P(), col_spec, row_spec, col_spec, col_spec, row_spec, P(), P()),
        out_specs=(act_spec, act_spec, col_spec, row_spec, col_spec, col_spec, row_spec),
        check_vma=False,
    )
```
